32 devices in a mesh: fsdp: 8 (over z, x), tensor: 4 (over y, core).
Axes of the slice: x: 2, y: 2, z: 4, core: 2. Of those that a mesh axis runs over, the one named last changes fastest.
Arguments:
- tokens: bfloat16 [32, 512, 768], P('fsdp', 'tensor'), may hold values from -6 to 6
- lengths: int32 [32], P('fsdp'), may hold values from 128 to 512, as said below
- cotangent: bfloat16 [32, 512, 768], P('fsdp', 'tensor'), may hold values from -6 to 6
- w_query: bfloat16 [768, 768], P('fsdp', 'tensor'), may hold values from -0.21875 to 0.21875
- w_key: bfloat16 [768, 768], P('fsdp', 'tensor'), may hold values from -0.3125 to 0.3125
- w_value: bfloat16 [768, 768], P('fsdp', 'tensor'), may hold values from -0.21875 to 0.21875
- w_output: bfloat16 [768, 768], P('tensor', 'fsdp'), may hold values from -1 to 1
- w_inner: bfloat16 [768, 3072], P('fsdp', 'tensor'), may hold values from -0.21875 to 0.21875
- w_outer: bfloat16 [3072, 768], P('tensor', 'fsdp'), may hold values from -0.15625 to 0.15625
- b_query: float32 [768], P(('fsdp', 'tensor')), may hold values from -3 to 3
- b_value: float32 [768], P(('fsdp', 'tensor')), may hold values from -1.2 to 1.2
- b_output: float32 [768], P(('fsdp', 'tensor')), may hold values from -1.8 to 1.8
- b_inner: float32 [3072], P(('fsdp', 'tensor')), may hold values from -3 to 3
- b_outer: float32 [768], P(('fsdp', 'tensor')), may hold values from -1.8 to 1.8
- gain_first: float32 [768], P(('fsdp', 'tensor')), may hold values from 0.1 to 1.9
- shift_first: float32 [768], P(('fsdp', 'tensor')), may hold values from -1.8 to 1.8
- gain_second: float32 [768], P(('fsdp', 'tensor')), may hold values from 0.1 to 1.9
- shift_second: float32 [768], P(('fsdp', 'tensor')), may hold values from -1.8 to 1.8
Outputs:
- output: bfloat16 [32, 512, 768], P('fsdp', 'tensor')
- input_grad: float32 [32, 512, 768], P('fsdp', 'tensor')
- grad_w_query: float32 [768, 768], P('fsdp', 'tensor')
- grad_w_key: float32 [768, 768], P('fsdp', 'tensor')
- grad_w_value: float32 [768, 768], P('fsdp', 'tensor')
- grad_w_output: float32 [768, 768], P('tensor', 'fsdp')
- grad_w_inner: float32 [768, 3072], P('fsdp', 'tensor')
- grad_w_outer: float32 [3072, 768], P('tensor', 'fsdp')
- grad_b_query: float32 [768], P(('fsdp', 'tensor'))
- grad_b_value: float32 [768], P(('fsdp', 'tensor'))
- grad_b_output: float32 [768], P(('fsdp', 'tensor'))
- grad_b_inner: float32 [3072], P(('fsdp', 'tensor'))
- grad_b_outer: float32 [768], P(('fsdp', 'tensor'))
- grad_gain_first: float32 [768], P(('fsdp', 'tensor'))
- grad_shift_first: float32 [768], P(('fsdp', 'tensor'))
- grad_gain_second: float32 [768], P(('fsdp', 'tensor'))
- grad_shift_second: float32 [768], P(('fsdp', 'tensor'))
The draws below stay inside these ranges and needn't reach their ends.
Inputs may be any that keep to these rules, and one draw needn't show every extreme that they name: Row s holds a sequence in its first lengths[s] slots; in every draw one row is full and one holds exactly 128 slots.
All inputs are finite; a program needn't handle non-finite values.
Results may differ from the reference program's by a relative error of at most 0.025.
Values may be sent and summed in bfloat16 or wider, within the bound.
A program may use at most 192 MiB of HBM per device.

```python
from functools import partial
import jax
import jax.numpy as jnp
from jax import lax

D = 768
HEADS = 12
HEAD = 64
FF = 3072
SLOTS = 512
MIN_LEN = 128
SEQS = 32


def draw_lengths(key, part):
    first_key = jax.random.fold_in(key, 11)
    second_key = jax.random.fold_in(key, 12)
    drawn = jax.random.randint(first_key, (SEQS,), MIN_LEN, SLOTS + 1)
    order = jax.random.permutation(second_key, SEQS)
    drawn = drawn.at[order[0]].set(SLOTS)
    drawn = drawn.at[order[1]].set(MIN_LEN)
    return drawn.astype(jnp.int32)


def raised(values, stream_key, source, target, parts, factor):
    def block_of(dim):
        return (jnp.arange(values.shape[dim]) // (values.shape[dim] // parts)).reshape((-1,) + (1,) * (values.ndim - 1 - dim))

    first = jax.random.permutation(stream_key, parts)[block_of(target)]
    other_side = (block_of(target) + parts // 2) % parts
    return jnp.where((block_of(source) == first) | (block_of(source) == other_side), factor * values, values)


def level_of(key, dims, pieces, low, top_value):
    level, own = 1.0, jax.random.fold_in(key, 6)
    for position, shards_of in pieces:
        steps = jnp.exp(jax.random.uniform(jax.random.fold_in(own, position), (shards_of,), jnp.float32, low / len(pieces), top_value / len(pieces)))
        level = level * jnp.repeat(steps, dims[position] // shards_of).reshape([-1 if axis == position else 1 for axis in range(len(dims))])
    return level


def noise(own_key, shape, width, most, cuts=(), kind=jnp.bfloat16):
    values = width * jax.random.normal(own_key, shape, jnp.float32)
    if cuts:
        values = values * level_of(own_key, shape, cuts, -0.22, 0.18)
    return jnp.clip(values, -most, most).astype(kind)


def bell_draw_with(stream_key, shape, deviation, reach, cuts, heavy, kind=jnp.bfloat16):
    values = deviation * jax.random.normal(stream_key, shape, jnp.float32)
    if cuts:
        values = values * level_of(stream_key, shape, cuts, -0.22, 0.18)
    return jnp.clip(raised(values, jax.random.fold_in(stream_key, 3), *heavy), -reach, reach).astype(kind)


def setup_inputs(seed: int = 0) -> dict:
    key_of = jax.random.split(jax.random.key(seed), 19)
    tokens = bell_draw_with(key_of[0], (SEQS, SLOTS, D), 1.0, 6.0, ((0, 8), (1, 4)), (0, 2, 8, 2.0))
    lengths = draw_lengths(jax.random.fold_in(key_of[18], 71), 0)
    cotangent = bell_draw_with(key_of[2], (SEQS, SLOTS, D), 1.0, 6.0, ((0, 8), (1, 4)), (0, 2, 8, 2.0))
    w_query = noise(key_of[3], (D, D), D ** -0.5, 0.21875, ((0, 8), (1, 4)))
    w_key = noise(key_of[4], (D, D), (D // 2) ** -0.5, 0.3125, ((0, 8), (1, 4)))
    w_value = noise(key_of[5], (D, D), D ** -0.5, 0.21875, ((0, 8), (1, 4)))
    w_output = noise(key_of[6], (D, D), (D // 24) ** -0.5, 1.0, ((0, 4), (1, 8)))
    w_inner = noise(key_of[7], (D, FF), D ** -0.5, 0.21875, ((0, 8), (1, 4)))
    w_outer = noise(key_of[8], (FF, D), (FF // 2) ** -0.5, 0.15625, ((0, 4), (1, 8)))
    b_query = noise(key_of[9], (D,), 0.5, 3.0, ((0, 32),), jnp.float32)
    b_value = noise(key_of[10], (D,), 0.2, 1.2, ((0, 32),), jnp.float32)
    b_output = noise(key_of[11], (D,), 0.3, 1.8, ((0, 32),), jnp.float32)
    b_inner = noise(key_of[12], (FF,), 0.5, 3.0, ((0, 32),), jnp.float32)
    b_outer = noise(key_of[13], (D,), 0.3, 1.8, ((0, 32),), jnp.float32)
    gain_first = jnp.clip(1.0 + 0.18 * jax.random.normal(key_of[14], (D,), jnp.float32), 0.1, 1.9)
    shift_first = noise(key_of[15], (D,), 0.3, 1.8, ((0, 32),), jnp.float32)
    gain_second = jnp.clip(1.0 + 0.18 * jax.random.normal(key_of[16], (D,), jnp.float32), 0.1, 1.9)
    shift_second = noise(key_of[17], (D,), 0.3, 1.8, ((0, 32),), jnp.float32)
    return dict(tokens=tokens, lengths=lengths, cotangent=cotangent, w_query=w_query, w_key=w_key, w_value=w_value, w_output=w_output, w_inner=w_inner, w_outer=w_outer, b_query=b_query, b_value=b_value, b_output=b_output, b_inner=b_inner, b_outer=b_outer, gain_first=gain_first, shift_first=shift_first, gain_second=gain_second, shift_second=shift_second)


@jax.custom_vjp
def low(v):
    return lax.optimization_barrier(v.astype(jnp.bfloat16)).astype(jnp.float32)

@jax.custom_vjp
def low_back(v):
    return v

def low_keep(v):
    return (low(v), None)

def low_pass(kept, grad):
    return (grad,)

def back_keep(v):
    return (v, None)

def back_low(kept, grad):
    return (low(grad),)
low.defvjp(low_keep, low_pass)
low_back.defvjp(back_keep, back_low)
epsilon = 1e-05
root_half = 0.7071067811865476

def matmul(left, right):
    return jnp.dot(left, right, precision=lax.Precision.HIGHEST, preferred_element_type=jnp.float32)

def layer_norm(rows, gain, shift):
    mean = lax.optimization_barrier(jnp.mean(rows, axis=1, keepdims=True))
    centered = rows - mean
    variance = lax.optimization_barrier(jnp.mean(centered * centered, axis=1, keepdims=True))
    return centered * lax.rsqrt(variance + epsilon) * gain + shift

def attend_block(keys, values, key_valid, query_block):
    raw = jnp.einsum('qhd,khd->hqk', query_block, keys, precision=lax.Precision.HIGHEST) * HEAD ** (-0.5)
    scores = low_back(raw)
    masked = jnp.where(key_valid[None, None, :], scores, -1000000000.0)
    top = lax.optimization_barrier(jnp.max(masked, axis=2, keepdims=True))
    expo = jnp.exp(masked - top)
    probs = expo / lax.optimization_barrier(jnp.sum(expo, axis=2, keepdims=True))
    return jnp.einsum('hqk,khd->qhd', low(probs), values, precision=lax.Precision.HIGHEST)

def forward_row(valid, key_valid, tokens, w_query, w_key, w_value, w_output, w_inner, w_outer, b_query, b_value, b_output, b_inner, b_outer, gain_first, shift_first, gain_second, shift_second):
    query = low(low_back(matmul(tokens, w_query) + b_query))
    key_rows = low(low_back(matmul(tokens, w_key)))
    value_rows = low(low_back(matmul(tokens, w_value) + b_value))
    block_rows = min(512, SLOTS)
    query_blocks = query.reshape(SLOTS // block_rows, block_rows, HEADS, HEAD)
    keys = key_rows.reshape(SLOTS, HEADS, HEAD)
    values = value_rows.reshape(SLOTS, HEADS, HEAD)
    blocks = lax.map(jax.checkpoint(partial(attend_block, keys, values, key_valid)), query_blocks)
    context = low(low_back(blocks.reshape(SLOTS, D)))
    attended = low_back(matmul(context, w_output) + b_output)
    first = layer_norm(tokens + attended, gain_first, shift_first)
    inner = low_back(matmul(low(first), w_inner) + b_inner)
    active = low(0.5 * inner * (1.0 + jax.scipy.special.erf(inner * root_half)))
    mixed = low_back(matmul(active, w_outer) + b_outer)
    second = layer_norm(first + mixed, gain_second, shift_second)
    return second * valid[:, None]

def reference(tokens, lengths, cotangent, w_query, w_key, w_value, w_output, w_inner, w_outer, b_query, b_value, b_output, b_inner, b_outer, gain_first, shift_first, gain_second, shift_second):
    params = (w_query.astype(jnp.float32), w_key.astype(jnp.float32), w_value.astype(jnp.float32), w_output.astype(jnp.float32), w_inner.astype(jnp.float32), w_outer.astype(jnp.float32), b_query, b_value, b_output, b_inner, b_outer, gain_first, shift_first, gain_second, shift_second)
    positions = jnp.arange(SLOTS, dtype=jnp.int32)

    def one_sequence(totals, item):
        rows, length, back = item
        key_valid = positions < length
        valid = key_valid.astype(jnp.float32)
        result, pullback = jax.vjp(partial(forward_row, valid, key_valid), rows.astype(jnp.float32), *params)
        grads = pullback(back.astype(jnp.float32))
        totals = tuple((total + grad for total, grad in zip(totals, grads[1:])))
        return (totals, (result.astype(jnp.bfloat16), grads[0]))
    start = tuple((jnp.zeros_like(param) for param in params))
    totals, outputs = lax.scan(one_sequence, start, (tokens, lengths, cotangent))
    return (outputs[0], outputs[1], totals[0], totals[1], totals[2], totals[3], totals[4], totals[5], totals[6], totals[7], totals[8], totals[9], totals[10], totals[11], totals[12], totals[13], totals[14])
```

```python
from functools import partial

import jax
import jax.numpy as jnp
from jax import lax
from jax.experimental import pallas as pl
from jax.experimental.pallas import tpu as pltpu
from jax.sharding import PartitionSpec as P

HEAD = 64


epsilon = 1e-05
root_half = 0.7071067811865476
inverse_root_two_pi = 0.3989422804014327


def gelu_value(inner):
    return 0.5 * inner * (1.0 + jax.scipy.special.erf(inner * root_half))


def gelu_slope(inner):
    return 0.5 * (
        1.0 + jax.scipy.special.erf(inner * root_half)
    ) + inner * inverse_root_two_pi * jnp.exp(-0.5 * inner * inner)


def normalize(rows):
    mean = jnp.mean(rows, axis=1, keepdims=True)
    centered = rows - mean
    variance = jnp.mean(centered * centered, axis=1, keepdims=True)
    factor = lax.rsqrt(variance + epsilon)
    return (centered * factor, factor)


def normalize_back(grad_normed, normed, factor):
    return factor * (
        grad_normed
        - jnp.mean(grad_normed, axis=1, keepdims=True)
        - normed * jnp.mean(grad_normed * normed, axis=1, keepdims=True)
    )


def column_sum(rows):
    return jnp.sum(rows.astype(jnp.float32), axis=0)


def dot_rows(left, right):
    return lax.dot_general(
        left, right, (((0,), (0,)), ((), ())), preferred_element_type=jnp.float32
    )


def dot_back(left, right):
    return lax.dot_general(
        left, right, (((1,), (1,)), ((), ())), preferred_element_type=jnp.float32
    )


def place(values, offset, total_length):
    return lax.dynamic_update_slice(jnp.zeros((total_length,), jnp.float32), values, (offset,))


def block_scores(keys, key_valid, query_block):
    raw = jnp.einsum(
        "qhd,khd->hqk", query_block, keys, preferred_element_type=jnp.float32
    ) * HEAD ** (-0.5)
    return jnp.where(key_valid[None, None, :], raw, -1000000000.0)


def attend_forward(keys, values, key_valid, query_block):
    masked = block_scores(keys, key_valid, query_block)
    top = jnp.max(masked, axis=2, keepdims=True)
    expo = jnp.exp(masked - top)
    total = jnp.sum(expo, axis=2, keepdims=True)
    probs = (expo / total).astype(jnp.bfloat16)
    context = jnp.einsum("hqk,khd->qhd", probs, values, preferred_element_type=jnp.float32)
    return (context, top, total)


def attend_backward(keys, values, key_valid, carry, item):
    key_grad, value_grad = carry
    query_block, context_grad_block, top, total = item
    masked = block_scores(keys, key_valid, query_block)
    probs = jnp.exp(masked - top) / total
    probs_low = probs.astype(jnp.bfloat16)
    prob_grad = jnp.einsum(
        "qhd,khd->hqk", context_grad_block, values, preferred_element_type=jnp.float32
    )
    delta = jnp.sum(prob_grad * probs, axis=2, keepdims=True)
    score_grad = (probs * (prob_grad - delta)).astype(jnp.bfloat16)
    factor = HEAD ** (-0.5)
    query_grad = (
        jnp.einsum("hqk,khd->qhd", score_grad, keys, preferred_element_type=jnp.float32) * factor
    )
    key_grad = (
        key_grad
        + jnp.einsum("hqk,qhd->khd", score_grad, query_block, preferred_element_type=jnp.float32)
        * factor
    )
    value_grad = value_grad + jnp.einsum(
        "hqk,qhd->khd", probs_low, context_grad_block, preferred_element_type=jnp.float32
    )
    return ((key_grad, value_grad), query_grad)


def gather_weights(w_query, w_key, w_value, w_output, w_inner, w_outer):
    return (
        lax.all_gather(w_query, "fsdp", axis=0, tiled=True),
        lax.all_gather(w_key, "fsdp", axis=0, tiled=True),
        lax.all_gather(w_value, "fsdp", axis=0, tiled=True),
        lax.all_gather(w_output, "fsdp", axis=1, tiled=True),
        lax.all_gather(w_inner, "fsdp", axis=0, tiled=True),
        lax.all_gather(w_outer, "fsdp", axis=1, tiled=True),
    )


def split_joint(joint_sum, output_sum, inner_sum, outer_sum, head_width):
    return (
        joint_sum[:, :head_width],
        joint_sum[:, head_width : 2 * head_width],
        joint_sum[:, 2 * head_width :],
        output_sum,
        inner_sum,
        outer_sum,
    )


def add_tuples(left, right):
    return tuple((first_item + second_item for first_item, second_item in zip(left, right)))


def local_generic(
    tokens,
    lengths,
    cotangent,
    w_query,
    w_key,
    w_value,
    w_output,
    w_inner,
    w_outer,
    b_query,
    b_value,
    b_output,
    b_inner,
    b_outer,
    gain_first,
    shift_first,
    gain_second,
    shift_second,
):
    tensor_size = lax.axis_size("tensor")
    tensor_rank = lax.axis_index("tensor")
    micro_count = tokens.shape[0]
    part_rows = tokens.shape[1]
    width = tokens.shape[2]
    seq_rows = part_rows * tensor_size
    head_width = w_query.shape[1]
    inner_width = w_inner.shape[1]
    local_heads = head_width // HEAD
    block_rows = min(512, seq_rows)
    block_count = seq_rows // block_rows
    vector_full = (
        lax.all_gather(b_query, ("fsdp", "tensor"), axis=0, tiled=True),
        lax.all_gather(b_value, ("fsdp", "tensor"), axis=0, tiled=True),
        lax.all_gather(b_output, ("fsdp", "tensor"), axis=0, tiled=True),
        lax.all_gather(b_inner, ("fsdp", "tensor"), axis=0, tiled=True),
        lax.all_gather(b_outer, ("fsdp", "tensor"), axis=0, tiled=True),
        lax.all_gather(gain_first, ("fsdp", "tensor"), axis=0, tiled=True),
        lax.all_gather(shift_first, ("fsdp", "tensor"), axis=0, tiled=True),
        lax.all_gather(gain_second, ("fsdp", "tensor"), axis=0, tiled=True),
        lax.all_gather(shift_second, ("fsdp", "tensor"), axis=0, tiled=True),
    )
    query_bias = lax.dynamic_slice_in_dim(vector_full[0], tensor_rank * head_width, head_width)
    value_bias = lax.dynamic_slice_in_dim(vector_full[1], tensor_rank * head_width, head_width)
    inner_bias = lax.dynamic_slice_in_dim(vector_full[3], tensor_rank * inner_width, inner_width)
    joint_bias = jnp.concatenate([query_bias, jnp.zeros((head_width,), jnp.float32), value_bias])
    grad_query_bias = jnp.zeros((head_width,), jnp.float32)
    grad_value_bias = jnp.zeros((head_width,), jnp.float32)
    grad_inner_bias = jnp.zeros((inner_width,), jnp.float32)
    grad_output_bias = jnp.zeros((width,), jnp.float32)
    grad_outer_bias = jnp.zeros((width,), jnp.float32)
    grad_gain_one = jnp.zeros((width,), jnp.float32)
    grad_shift_one = jnp.zeros((width,), jnp.float32)
    grad_gain_two = jnp.zeros((width,), jnp.float32)
    grad_shift_two = jnp.zeros((width,), jnp.float32)
    local_totals = None
    shard_totals = None
    outputs = []
    input_grads = []
    slot_index = jnp.arange(seq_rows, dtype=jnp.int32)
    part_index = tensor_rank * part_rows + jnp.arange(part_rows, dtype=jnp.int32)
    for micro_index in range(micro_count):
        forward_weights = gather_weights(w_query, w_key, w_value, w_output, w_inner, w_outer)
        joint_w = jnp.concatenate(
            [forward_weights[0], forward_weights[1], forward_weights[2]], axis=1
        )
        output_w = forward_weights[3]
        inner_w = forward_weights[4]
        outer_w = forward_weights[5]
        length = lengths[micro_index]
        key_valid = slot_index < length
        row_valid = (part_index < length).astype(jnp.float32)[:, None]
        own_rows = tokens[micro_index]
        whole = lax.all_gather(own_rows, "tensor", axis=0, tiled=True)
        joint = (jnp.dot(whole, joint_w, preferred_element_type=jnp.float32) + joint_bias).astype(
            jnp.bfloat16
        )
        query = joint[:, :head_width].reshape(block_count, block_rows, local_heads, HEAD)
        keys = joint[:, head_width : 2 * head_width].reshape(seq_rows, local_heads, HEAD)
        values = joint[:, 2 * head_width :].reshape(seq_rows, local_heads, HEAD)
        context_blocks, tops, totals = lax.map(
            partial(attend_forward, keys, values, key_valid), query
        )
        context_low = context_blocks.reshape(seq_rows, head_width).astype(jnp.bfloat16)
        attended = (
            lax.psum_scatter(
                jnp.dot(context_low, output_w, preferred_element_type=jnp.float32).astype(
                    jnp.bfloat16
                ),
                "tensor",
                scatter_dimension=0,
                tiled=True,
            ).astype(jnp.float32)
            + vector_full[2]
        )
        normed_first, factor_first = normalize(own_rows.astype(jnp.float32) + attended)
        first = normed_first * vector_full[5] + vector_full[6]
        first_whole = lax.all_gather(first.astype(jnp.bfloat16), "tensor", axis=0, tiled=True)
        inner = jnp.dot(first_whole, inner_w, preferred_element_type=jnp.float32) + inner_bias
        active = gelu_value(inner).astype(jnp.bfloat16)
        mixed = (
            lax.psum_scatter(
                jnp.dot(active, outer_w, preferred_element_type=jnp.float32).astype(jnp.bfloat16),
                "tensor",
                scatter_dimension=0,
                tiled=True,
            ).astype(jnp.float32)
            + vector_full[4]
        )
        normed_second, factor_second = normalize(first + mixed)
        outputs.append(
            ((normed_second * vector_full[7] + vector_full[8]) * row_valid).astype(jnp.bfloat16)
        )
        backward_weights = gather_weights(w_query, w_key, w_value, w_output, w_inner, w_outer)
        joint_w = jnp.concatenate(
            [backward_weights[0], backward_weights[1], backward_weights[2]], axis=1
        )
        output_w = backward_weights[3]
        inner_w = backward_weights[4]
        outer_w = backward_weights[5]
        out_grad = cotangent[micro_index].astype(jnp.float32) * row_valid
        grad_gain_two = grad_gain_two + column_sum(out_grad * normed_second)
        grad_shift_two = grad_shift_two + column_sum(out_grad)
        sum_grad = normalize_back(out_grad * vector_full[7], normed_second, factor_second)
        mixed_grad = sum_grad.astype(jnp.bfloat16)
        grad_outer_bias = grad_outer_bias + column_sum(mixed_grad)
        mixed_whole = lax.all_gather(mixed_grad, "tensor", axis=0, tiled=True)
        outer_sum = dot_rows(active, mixed_whole)
        inner_grad = (dot_back(mixed_whole, outer_w) * gelu_slope(inner)).astype(jnp.bfloat16)
        grad_inner_bias = grad_inner_bias + column_sum(inner_grad)
        inner_sum = dot_rows(first_whole, inner_grad)
        first_grad = sum_grad + lax.psum_scatter(
            dot_back(inner_grad, inner_w).astype(jnp.bfloat16),
            "tensor",
            scatter_dimension=0,
            tiled=True,
        ).astype(jnp.float32)
        grad_gain_one = grad_gain_one + column_sum(first_grad * normed_first)
        grad_shift_one = grad_shift_one + column_sum(first_grad)
        residual_grad = normalize_back(first_grad * vector_full[5], normed_first, factor_first)
        attended_grad = residual_grad.astype(jnp.bfloat16)
        grad_output_bias = grad_output_bias + column_sum(attended_grad)
        attended_whole = lax.all_gather(attended_grad, "tensor", axis=0, tiled=True)
        output_sum = dot_rows(context_low, attended_whole)
        context_grad = (
            dot_back(attended_whole, output_w)
            .astype(jnp.bfloat16)
            .reshape(block_count, block_rows, local_heads, HEAD)
        )
        empty = jnp.zeros((seq_rows, local_heads, HEAD), jnp.float32)
        carried, query_grad = lax.scan(
            partial(attend_backward, keys, values, key_valid),
            (empty, empty),
            (query, context_grad, tops, totals),
        )
        joint_grad = jnp.concatenate(
            [
                query_grad.reshape(seq_rows, head_width),
                carried[0].reshape(seq_rows, head_width),
                carried[1].reshape(seq_rows, head_width),
            ],
            axis=1,
        ).astype(jnp.bfloat16)
        grad_query_bias = grad_query_bias + column_sum(joint_grad[:, :head_width])
        grad_value_bias = grad_value_bias + column_sum(joint_grad[:, 2 * head_width :])
        joint_sum = dot_rows(whole, joint_grad)
        input_grads.append(
            residual_grad
            + lax.psum_scatter(
                dot_back(joint_grad, joint_w).astype(jnp.bfloat16),
                "tensor",
                scatter_dimension=0,
                tiled=True,
            ).astype(jnp.float32)
        )
        batch_sums = (joint_sum, output_sum, inner_sum, outer_sum)
        local_totals = batch_sums if local_totals is None else add_tuples(local_totals, batch_sums)
    pieces = split_joint(
        local_totals[0], local_totals[1], local_totals[2], local_totals[3], head_width
    )
    shard_totals = (
        lax.psum_scatter(pieces[0], "fsdp", scatter_dimension=0, tiled=True),
        lax.psum_scatter(pieces[1], "fsdp", scatter_dimension=0, tiled=True),
        lax.psum_scatter(pieces[2], "fsdp", scatter_dimension=0, tiled=True),
        lax.psum_scatter(pieces[3], "fsdp", scatter_dimension=1, tiled=True),
        lax.psum_scatter(pieces[4], "fsdp", scatter_dimension=0, tiled=True),
        lax.psum_scatter(pieces[5], "fsdp", scatter_dimension=1, tiled=True),
    )
    vector_grads = (
        lax.psum_scatter(
            place(grad_query_bias, tensor_rank * head_width, width),
            ("fsdp", "tensor"),
            scatter_dimension=0,
            tiled=True,
        ),
        lax.psum_scatter(
            place(grad_value_bias, tensor_rank * head_width, width),
            ("fsdp", "tensor"),
            scatter_dimension=0,
            tiled=True,
        ),
        lax.psum_scatter(grad_output_bias, ("fsdp", "tensor"), scatter_dimension=0, tiled=True),
        lax.psum_scatter(
            place(grad_inner_bias, tensor_rank * inner_width, inner_width * tensor_size),
            ("fsdp", "tensor"),
            scatter_dimension=0,
            tiled=True,
        ),
        lax.psum_scatter(grad_outer_bias, ("fsdp", "tensor"), scatter_dimension=0, tiled=True),
        lax.psum_scatter(grad_gain_one, ("fsdp", "tensor"), scatter_dimension=0, tiled=True),
        lax.psum_scatter(grad_shift_one, ("fsdp", "tensor"), scatter_dimension=0, tiled=True),
        lax.psum_scatter(grad_gain_two, ("fsdp", "tensor"), scatter_dimension=0, tiled=True),
        lax.psum_scatter(grad_shift_two, ("fsdp", "tensor"), scatter_dimension=0, tiled=True),
    )
    return (
        jnp.stack(outputs),
        jnp.stack(input_grads),
        shard_totals[0],
        shard_totals[1],
        shard_totals[2],
        shard_totals[3],
        shard_totals[4],
        shard_totals[5],
        vector_grads[0],
        vector_grads[1],
        vector_grads[2],
        vector_grads[3],
        vector_grads[4],
        vector_grads[5],
        vector_grads[6],
        vector_grads[7],
        vector_grads[8],
    )


MESH = pl.DeviceIdType.MESH
WIDTH = 768
HIDDEN = 3072
HALF = WIDTH // 2
KINDS = 3
VECTOR_ROWS = (8 * WIDTH + HIDDEN) // 128


def fits(sizes):
    fsdp = sizes["fsdp"]
    return sizes["tensor"] == 4 and fsdp % 2 == 0 and WIDTH % (16 * fsdp) == 0


class Place:
    def __init__(self, fsdp_size):
        self.f = lax.axis_index("fsdp")
        self.t = lax.axis_index("tensor")
        self.nz = fsdp_size // 2
        self.z = self.f // 2
        self.x = self.f % 2
        self.y = self.t // 2
        self.c = self.t % 2
        self.tx = self.t + 2 - 4 * self.y
        self.core = (self.f, self.t + 1 - 2 * self.c)
        self.along_y = (self.f, self.tx)
        self.along_x = (self.f + 1 - 2 * self.x, self.t)

    def z_at(self, step):
        return (self.z + step) % self.nz

    def z_back(self, step):
        return (self.z + self.nz - step) % self.nz

    def along_z(self, step):
        return (self.z_at(step) * 2 + self.x, self.t)

    def in_group(self, step):
        return (self.f, (self.t + step) % 4)


class Net:
    def __init__(self, send_sems, recv_sems):
        self.send_sems = send_sems
        self.recv_sems = recv_sems
        self.count = 0
        self.sent = []

    def send(self, source, target, device):
        copy = pltpu.make_async_remote_copy(
            src_ref=source,
            dst_ref=target,
            send_sem=self.send_sems.at[self.count],
            recv_sem=self.recv_sems.at[self.count],
            device_id=device,
            device_id_type=MESH,
        )
        self.count += 1
        copy.start()
        self.sent.append(copy)
        return copy

    def close(self):
        for copy in self.sent:
            copy.wait_send()


def greet(place):
    barrier = pltpu.get_barrier_semaphore()
    peers = [place.in_group(1), place.in_group(2), place.in_group(3), place.along_x]
    peers += [place.along_z(step) for step in range(1, place.nz)]
    for peer in peers:
        pl.semaphore_signal(barrier, inc=1, device_id=peer, device_id_type=MESH)
    pl.semaphore_wait(barrier, len(peers))


def wait_all(copies):
    for copy in copies:
        copy.wait_recv()


def vector_steps(place):
    steps = [place.core, place.along_y, place.along_x]
    stride = 1
    while stride < place.nz:
        z = place.z
        other = z + stride - 2 * stride * ((z // stride) % 2)
        steps.append((other * 2 + place.x, place.t))
        stride *= 2
    return steps


def gather_kernel(
    fsdp_size, own_ref, tokens_ref, cot_ref, vec_ref,
    w_ref, rows_ref, back_ref, total_ref,
    vec_slots, send_sems, recv_sems, local_sems,
):
    place = Place(fsdp_size)
    nz = place.nz
    part = own_ref.shape[1]
    t, tx = place.t, place.tx
    net = Net(send_sems, recv_sems)
    greet(place)
    a_cols = pl.ds(0, HALF)
    b_cols = pl.ds(HALF, HALF)

    def rows_of(z, x):
        return pl.ds(pl.multiple_of((z * 2 + x) * part, part), part)

    own_rows = rows_of(place.z, place.x)
    token_in = [
        net.send(tokens_ref.at[(t + step) % 4], rows_ref.at[t], place.in_group(step))
        for step in (2, 1, 3)
    ]
    keeps = []

    def keep(source, target):
        copy = pltpu.make_async_copy(source, target, local_sems.at[len(keeps)])
        copy.start()
        keeps.append(copy)

    keep(tokens_ref.at[t], rows_ref.at[t])
    keep(cot_ref.at[t], back_ref.at[t])
    for k in range(KINDS):
        keep(own_ref.at[k], w_ref.at[k, t, own_rows])
    a_in, b_in = [], []
    for k in range(KINDS):
        a_in.append([
            net.send(own_ref.at[k, :, a_cols], w_ref.at[k, t, own_rows, a_cols], place.along_z(step))
            for step in range(1, nz)
        ])
        b_in.append(net.send(own_ref.at[k, :, b_cols], w_ref.at[k, t, own_rows, b_cols], place.along_y))
    total_ref[...] = vec_ref[...]
    for index, peer in enumerate(vector_steps(place)):
        copy = net.send(total_ref, vec_slots.at[index], peer)
        copy.wait()
        net.sent.pop()
        total_ref[...] += vec_slots[index]
    for copy in keeps:
        copy.wait()
    for k in range(KINDS):
        wait_all(a_in[k])
        a_x = [
            net.send(w_ref.at[k, t, rows_of(z, place.x), a_cols], w_ref.at[k, t, rows_of(z, place.x), a_cols], place.along_x)
            for z in range(nz)
        ]
        b_in[k].wait_recv()
        b_z = [
            net.send(w_ref.at[k, which, own_rows, b_cols], w_ref.at[k, which, own_rows, b_cols], place.along_z(step))
            for step in range(1, nz)
            for which in (t, tx)
        ]
        wait_all(a_x)
        a_y = net.send(w_ref.at[k, t, :, a_cols], w_ref.at[k, t, :, a_cols], place.along_y)
        a_c = [net.send(w_ref.at[k, t, :, a_cols], w_ref.at[k, t, :, a_cols], place.core)]
        wait_all(b_z)
        b_x = [
            net.send(w_ref.at[k, which, rows_of(z, place.x), b_cols], w_ref.at[k, which, rows_of(z, place.x), b_cols], place.along_x)
            for z in range(nz)
            for which in (t, tx)
        ]
        a_y.wait_recv()
        a_c.append(net.send(w_ref.at[k, tx, :, a_cols], w_ref.at[k, tx, :, a_cols], place.core))
        wait_all(b_x)
        b_c = [
            net.send(w_ref.at[k, which, :, b_cols], w_ref.at[k, which, :, b_cols], place.core)
            for which in (t, tx)
        ]
        if k == 0:
            cot_in = [
                net.send(cot_ref.at[(t + step) % 4], back_ref.at[t], place.in_group(step))
                for step in (2, 1, 3)
            ]
        wait_all(a_c + b_c)
    wait_all(token_in)
    wait_all(cot_in)
    net.close()


def reduce_kernel(
    fsdp_size, grad_ref, out_ref, back_ref, vec_ref,
    sum_ref, out_slots, back_slots, total_ref,
    half_c, half_y_a, half_x_a, half_z_a, half_x_b, half_z_b, half_y_b, vec_slots,
    send_sems, recv_sems, local_sems,
):
    place = Place(fsdp_size)
    nz = place.nz
    part = sum_ref.shape[1]
    t = place.t
    net = Net(send_sems, recv_sems)
    greet(place)
    a_cols = pl.ds(0, HALF)
    b_cols = pl.ds(HALF, HALF)
    f32 = jnp.float32
    bf16 = jnp.bfloat16

    def rows_of(z, x):
        return pl.ds(pl.multiple_of((z * 2 + x) * part, part), part)

    keeps = []

    def keep(source, target):
        copy = pltpu.make_async_copy(source, target, local_sems.at[len(keeps)])
        copy.start()
        keeps.append(copy)

    x_other = 1 - place.x
    core_in = [
        [
            net.send(grad_ref.at[k, y * 2 + 1 - place.c], half_c.at[k, y], place.core)
            for y in range(2)
        ]
        for k in range(KINDS)
    ]
    total_ref[...] = vec_ref[...]
    for index, peer in enumerate(vector_steps(place)):
        copy = net.send(total_ref, vec_slots.at[index], peer)
        copy.wait()
        net.sent.pop()
        total_ref[...] += vec_slots[index]
    row_in = []
    keep(out_ref.at[t], out_slots.at[t])
    keep(back_ref.at[t], back_slots.at[t])
    for k in range(KINDS):
        for y in range(2):
            core_in[k][y].wait_recv()
            half_c[k, y] = (half_c[k, y].astype(f32) + grad_ref[k, y * 2 + place.c].astype(f32)).astype(bf16)
        a_y = net.send(half_c.at[k, 1 - place.y, :, a_cols], half_y_a.at[k], place.along_y)
        b_x = [
            net.send(half_c.at[k, y, rows_of(z, x_other), b_cols], half_x_b.at[k, y, z], place.along_x)
            for z in range(nz)
            for y in range(2)
        ]
        if k == 0:
            for step in (2, 1, 3):
                row_in.append(net.send(out_ref.at[(t + step) % 4], out_slots.at[t], place.in_group(step)))
                row_in.append(net.send(back_ref.at[(t + step) % 4], back_slots.at[t], place.in_group(step)))
        a_y.wait_recv()
        half_y_a[k] = (half_y_a[k].astype(f32) + half_c[k, place.y, :, a_cols].astype(f32)).astype(bf16)
        a_x = [
            net.send(half_y_a.at[k, rows_of(z, x_other)], half_x_a.at[k, z], place.along_x)
            for z in range(nz)
        ]
        wait_all(b_x)
        for z in range(nz):
            for y in range(2):
                half_x_b[k, y, z] = (
                    half_x_b[k, y, z].astype(f32) + half_c[k, y, rows_of(z, place.x), b_cols].astype(f32)
                ).astype(bf16)
        b_z = [
            net.send(half_x_b.at[k, y, place.z_at(step)], half_z_b.at[k, step - 1, y], place.along_z(step))
            for step in range(1, nz)
            for y in range(2)
        ]
        wait_all(a_x)
        for z in range(nz):
            half_x_a[k, z] = (
                half_x_a[k, z].astype(f32) + half_y_a[k, rows_of(z, place.x)].astype(f32)
            ).astype(bf16)
        a_z = [
            net.send(half_x_a.at[k, place.z_at(step)], half_z_a.at[k, step - 1], place.along_z(step))
            for step in range(1, nz)
        ]
        wait_all(b_z)
        for y in range(2):
            total = half_x_b[k, y, place.z].astype(f32)
            for step in range(nz - 1):
                total += half_z_b[k, step, y].astype(f32)
            half_y_b[k, y] = total.astype(bf16)
        b_y = net.send(half_y_b.at[k, 1 - place.y], half_y_b.at[k, 2], place.along_y)
        wait_all(a_z)
        total = half_x_a[k, place.z].astype(f32)
        for step in range(nz - 1):
            total += half_z_a[k, step].astype(f32)
        sum_ref[k, :, a_cols] = total
        b_y.wait_recv()
        sum_ref[k, :, b_cols] = half_y_b[k, place.y].astype(f32) + half_y_b[k, 2].astype(f32)
    for copy in keeps:
        copy.wait()
    wait_all(row_in)
    net.close()


VMEM_SPEC = pl.BlockSpec(memory_space=pltpu.VMEM)
ANY_SPEC = pl.BlockSpec(memory_space=pl.ANY)
LIMIT = 62 * 1024 * 1024


def gather_all(own, tokens, cotangent, vectors):
    fsdp_size = lax.axis_size("fsdp")
    bf16, f32 = jnp.bfloat16, jnp.float32
    count = 128
    return pl.pallas_call(
        partial(gather_kernel, fsdp_size),
        out_shape=(
            jax.ShapeDtypeStruct((KINDS, 4, WIDTH, WIDTH), bf16),
            jax.ShapeDtypeStruct(tokens.shape, bf16),
            jax.ShapeDtypeStruct(tokens.shape, bf16),
            jax.ShapeDtypeStruct((VECTOR_ROWS, 128), f32),
        ),
        in_specs=[ANY_SPEC, ANY_SPEC, ANY_SPEC, VMEM_SPEC],
        out_specs=(ANY_SPEC, ANY_SPEC, ANY_SPEC, VMEM_SPEC),
        scratch_shapes=[
            pltpu.VMEM((8, VECTOR_ROWS, 128), f32),
            pltpu.SemaphoreType.DMA((count,)),
            pltpu.SemaphoreType.DMA((count,)),
            pltpu.SemaphoreType.DMA((8,)),
        ],
        compiler_params=pltpu.CompilerParams(collective_id=0, has_side_effects=True, vmem_limit_bytes=LIMIT),
        name="gather_all",
    )(own, tokens, cotangent, vectors)


def reduce_all(grads, out, back, vectors):
    fsdp_size = lax.axis_size("fsdp")
    nz = fsdp_size // 2
    part = WIDTH // fsdp_size
    bf16, f32 = jnp.bfloat16, jnp.float32
    count = 128
    return pl.pallas_call(
        partial(reduce_kernel, fsdp_size),
        out_shape=(
            jax.ShapeDtypeStruct((KINDS, part, WIDTH), f32),
            jax.ShapeDtypeStruct(out.shape, bf16),
            jax.ShapeDtypeStruct(back.shape, bf16),
            jax.ShapeDtypeStruct((VECTOR_ROWS, 128), f32),
        ),
        in_specs=[VMEM_SPEC, ANY_SPEC, ANY_SPEC, VMEM_SPEC],
        out_specs=(VMEM_SPEC, ANY_SPEC, ANY_SPEC, VMEM_SPEC),
        scratch_shapes=[
            pltpu.VMEM((KINDS, 2, WIDTH, WIDTH), bf16),
            pltpu.VMEM((KINDS, WIDTH, HALF), bf16),
            pltpu.VMEM((KINDS, nz, part, HALF), bf16),
            pltpu.VMEM((KINDS, nz - 1, part, HALF), bf16),
            pltpu.VMEM((KINDS, 2, nz, part, HALF), bf16),
            pltpu.VMEM((KINDS, nz - 1, 2, part, HALF), bf16),
            pltpu.VMEM((KINDS, 3, part, HALF), bf16),
            pltpu.VMEM((8, VECTOR_ROWS, 128), f32),
            pltpu.SemaphoreType.DMA((count,)),
            pltpu.SemaphoreType.DMA((count,)),
            pltpu.SemaphoreType.DMA((8,)),
        ],
        compiler_params=pltpu.CompilerParams(collective_id=1, has_side_effects=True, vmem_limit_bytes=LIMIT),
        name="reduce_all",
    )(grads, out, back, vectors)


def layer_math(w, rows, back, vectors, length):
    bf16, f32 = jnp.bfloat16, jnp.float32
    seq = rows.shape[0]
    joint_w = w[0]
    inner_w = w[1].transpose(1, 0, 2).reshape(WIDTH, HIDDEN)
    outer_t = w[2].transpose(1, 0, 2).reshape(WIDTH, HIDDEN)
    share = WIDTH // 4
    heads = WIDTH // HEAD

    def full(i):
        return joint_w[:, :, i * share:(i + 1) * share].transpose(1, 0, 2).reshape(WIDTH, WIDTH)

    w_q, w_k, w_v, w_ot = full(0), full(1), full(2), full(3)
    flat = vectors.reshape(-1)
    b_query, b_value, b_output, b_outer, gain_first, shift_first, gain_second, shift_second = [
        flat[i * WIDTH:(i + 1) * WIDTH] for i in range(8)
    ]
    b_inner = flat[8 * WIDTH:]
    index = jnp.arange(seq, dtype=jnp.int32)
    key_valid = index < length
    row_valid = key_valid.astype(f32)[:, None]

    def dot(a, b):
        return jnp.dot(a, b, preferred_element_type=f32)

    q = (dot(rows, w_q) + b_query).astype(bf16).reshape(seq, heads, HEAD)
    k = dot(rows, w_k).astype(bf16).reshape(seq, heads, HEAD)
    v = (dot(rows, w_v) + b_value).astype(bf16).reshape(seq, heads, HEAD)
    context, top, total = attend_forward(k, v, key_valid, q)
    context = context.reshape(seq, WIDTH).astype(bf16)
    attended = dot_back(context, w_ot) + b_output
    normed_first, factor_first = normalize(rows.astype(f32) + attended)
    first = normed_first * gain_first + shift_first
    first_low = first.astype(bf16)
    inner = dot(first_low, inner_w) + b_inner
    active = gelu_value(inner).astype(bf16)
    mixed = dot_back(active, outer_t) + b_outer
    normed_second, factor_second = normalize(first + mixed)
    output = ((normed_second * gain_second + shift_second) * row_valid).astype(bf16)
    out_grad = back.astype(f32) * row_valid
    g_gain_second = column_sum(out_grad * normed_second)
    g_shift_second = column_sum(out_grad)
    sum_grad = normalize_back(out_grad * gain_second, normed_second, factor_second)
    mixed_grad = sum_grad.astype(bf16)
    g_b_outer = column_sum(mixed_grad)
    g_outer_t = dot_rows(mixed_grad, active)
    inner_grad = (dot(mixed_grad, outer_t) * gelu_slope(inner)).astype(bf16)
    g_b_inner = column_sum(inner_grad)
    g_inner = dot_rows(first_low, inner_grad)
    first_grad = sum_grad + dot_back(inner_grad, inner_w)
    g_gain_first = column_sum(first_grad * normed_first)
    g_shift_first = column_sum(first_grad)
    residual_grad = normalize_back(first_grad * gain_first, normed_first, factor_first)
    attended_grad = residual_grad.astype(bf16)
    g_b_output = column_sum(attended_grad)
    g_ot = dot_rows(attended_grad, context)
    context_grad = dot(attended_grad, w_ot).astype(bf16).reshape(seq, heads, HEAD)
    empty = jnp.zeros((seq, heads, HEAD), f32)
    (key_grad, value_grad), query_grad = attend_backward(
        k, v, key_valid, (empty, empty), (q, context_grad, top, total)
    )
    query_grad = query_grad.reshape(seq, WIDTH).astype(bf16)
    key_grad = key_grad.reshape(seq, WIDTH).astype(bf16)
    value_grad = value_grad.reshape(seq, WIDTH).astype(bf16)
    g_b_query = column_sum(query_grad)
    g_b_value = column_sum(value_grad)
    g_q, g_k, g_v = dot_rows(rows, query_grad), dot_rows(rows, key_grad), dot_rows(rows, value_grad)
    input_grad = residual_grad + dot_back(query_grad, w_q) + dot_back(key_grad, w_k) + dot_back(value_grad, w_v)
    g_joint = jnp.concatenate([g.reshape(WIDTH, 4, share) for g in (g_q, g_k, g_v, g_ot)], axis=2)
    grads = jnp.stack([
        g_joint.transpose(1, 0, 2),
        g_inner.reshape(WIDTH, 4, WIDTH).transpose(1, 0, 2),
        g_outer_t.reshape(WIDTH, 4, WIDTH).transpose(1, 0, 2),
    ]).astype(bf16)
    vector_grads = jnp.concatenate([
        g_b_query, g_b_value, g_b_output, g_b_outer, g_gain_first, g_shift_first,
        g_gain_second, g_shift_second, g_b_inner,
    ])
    return output, input_grad.astype(bf16), grads, vector_grads


def local_fast(
    tokens, lengths, cotangent, w_query, w_key, w_value, w_output, w_inner, w_outer,
    b_query, b_value, b_output, b_inner, b_outer, gain_first, shift_first, gain_second, shift_second,
):
    f32 = jnp.float32
    rank = lax.axis_index("fsdp") * 4 + lax.axis_index("tensor")
    own = jnp.stack([
        jnp.concatenate([w_query, w_key, w_value, w_output.T], axis=1),
        w_inner,
        w_outer.T,
    ])
    short = jnp.stack([
        b_query, b_value, b_output, b_outer, gain_first, shift_first, gain_second, shift_second
    ])
    place_short = lax.dynamic_update_slice(jnp.zeros((8, WIDTH), f32), short, (0, rank * short.shape[1]))
    place_long = lax.dynamic_update_slice(jnp.zeros((HIDDEN,), f32), b_inner, (rank * b_inner.shape[0],))
    placed = jnp.concatenate([place_short.reshape(-1), place_long]).reshape(VECTOR_ROWS, 128)
    w, rows, back, vectors = gather_all(own, tokens, cotangent, placed)
    length = lax.dynamic_index_in_dim(lengths, lax.axis_index("tensor"), keepdims=False)
    output, input_grad, grads, vector_grads = layer_math(
        w, rows.reshape(-1, WIDTH), back.reshape(-1, WIDTH), vectors, length
    )
    sums, outs, backs, totals = reduce_all(
        grads, output.reshape(tokens.shape), input_grad.reshape(tokens.shape),
        vector_grads.reshape(VECTOR_ROWS, 128),
    )
    share = w_query.shape[1]
    flat = totals.reshape(-1)
    short_own = lax.dynamic_slice(
        flat[:8 * WIDTH].reshape(8, WIDTH), (0, rank * short.shape[1]), short.shape
    )
    long_own = lax.dynamic_slice(flat, (8 * WIDTH + rank * b_inner.shape[0],), b_inner.shape)
    return (
        outs,
        backs.astype(f32),
        sums[0, :, :share],
        sums[0, :, share:2 * share],
        sums[0, :, 2 * share:3 * share],
        sums[0, :, 3 * share:].T,
        sums[1],
        sums[2].T,
        short_own[0],
        short_own[1],
        short_own[2],
        long_own,
        short_own[3],
        short_own[4],
        short_own[5],
        short_own[6],
        short_own[7],
    )


def solution(mesh):
    placed = (
        P("fsdp", "tensor", None),
        P("fsdp"),
        P("fsdp", "tensor", None),
        P("fsdp", "tensor"),
        P("fsdp", "tensor"),
        P("fsdp", "tensor"),
        P("tensor", "fsdp"),
        P("fsdp", "tensor"),
        P("tensor", "fsdp"),
        P(("fsdp", "tensor")),
        P(("fsdp", "tensor")),
        P(("fsdp", "tensor")),
        P(("fsdp", "tensor")),
        P(("fsdp", "tensor")),
        P(("fsdp", "tensor")),
        P(("fsdp", "tensor")),
        P(("fsdp", "tensor")),
        P(("fsdp", "tensor")),
    )
    return jax.shard_map(
        local_fast if fits(mesh.shape) else local_generic,
        mesh=mesh,
        in_specs=placed,
        out_specs=(
            P("fsdp", "tensor", None),
            P("fsdp", "tensor", None),
            P("fsdp", "tensor"),
            P("fsdp", "tensor"),
            P("fsdp", "tensor"),
            P("tensor", "fsdp"),
            P("fsdp", "tensor"),
            P("tensor", "fsdp"),
            P(("fsdp", "tensor")),
            P(("fsdp", "tensor")),
            P(("fsdp", "tensor")),
            P(("fsdp", "tensor")),
            P(("fsdp", "tensor")),
            P(("fsdp", "tensor")),
            P(("fsdp", "tensor")),
            P(("fsdp", "tensor")),
            P(("fsdp", "tensor")),
        ),
        check_vma=False,
    )
```

```python
from functools import partial

import jax
import jax.numpy as jnp
from jax import lax
from jax.experimental import pallas as pl
from jax.experimental.pallas import tpu as pltpu
from jax.sharding import PartitionSpec as P

FSDP, TENSOR = "fsdp", "tensor"

HEAD = 64


epsilon = 1e-05
root_half = 0.7071067811865476
inverse_root_two_pi = 0.3989422804014327


def gelu_value(inner):
    return 0.5 * inner * (1.0 + jax.scipy.special.erf(inner * root_half))


def gelu_slope(inner):
    return 0.5 * (
        1.0 + jax.scipy.special.erf(inner * root_half)
    ) + inner * inverse_root_two_pi * jnp.exp(-0.5 * inner * inner)


def normalize(rows):
    mean = jnp.mean(rows, axis=1, keepdims=True)
    centered = rows - mean
    variance = jnp.mean(centered * centered, axis=1, keepdims=True)
    factor = lax.rsqrt(variance + epsilon)
    return (centered * factor, factor)


def normalize_back(grad_normed, normed, factor):
    return factor * (
        grad_normed
        - jnp.mean(grad_normed, axis=1, keepdims=True)
        - normed * jnp.mean(grad_normed * normed, axis=1, keepdims=True)
    )


def column_sum(rows):
    return jnp.sum(rows.astype(jnp.float32), axis=0)


def dot_rows(left, right):
    return lax.dot_general(
        left, right, (((0,), (0,)), ((), ())), preferred_element_type=jnp.float32
    )


def dot_back(left, right):
    return lax.dot_general(
        left, right, (((1,), (1,)), ((), ())), preferred_element_type=jnp.float32
    )


def place(values, offset, total_length):
    return lax.dynamic_update_slice(jnp.zeros((total_length,), jnp.float32), values, (offset,))


def block_scores(keys, key_valid, query_block):
    raw = jnp.einsum(
        "qhd,khd->hqk", query_block, keys, preferred_element_type=jnp.float32
    ) * HEAD ** (-0.5)
    return jnp.where(key_valid[None, None, :], raw, -1000000000.0)


def attend_forward(keys, values, key_valid, query_block):
    masked = block_scores(keys, key_valid, query_block)
    top = jnp.max(masked, axis=2, keepdims=True)
    expo = jnp.exp(masked - top)
    total = jnp.sum(expo, axis=2, keepdims=True)
    probs = (expo / total).astype(jnp.bfloat16)
    context = jnp.einsum("hqk,khd->qhd", probs, values, preferred_element_type=jnp.float32)
    return (context, top, total)


def attend_backward(keys, values, key_valid, carry, item):
    key_grad, value_grad = carry
    query_block, context_grad_block, top, total = item
    masked = block_scores(keys, key_valid, query_block)
    probs = jnp.exp(masked - top) / total
    probs_low = probs.astype(jnp.bfloat16)
    prob_grad = jnp.einsum(
        "qhd,khd->hqk", context_grad_block, values, preferred_element_type=jnp.float32
    )
    delta = jnp.sum(prob_grad * probs, axis=2, keepdims=True)
    score_grad = (probs * (prob_grad - delta)).astype(jnp.bfloat16)
    factor = HEAD ** (-0.5)
    query_grad = (
        jnp.einsum("hqk,khd->qhd", score_grad, keys, preferred_element_type=jnp.float32) * factor
    )
    key_grad = (
        key_grad
        + jnp.einsum("hqk,qhd->khd", score_grad, query_block, preferred_element_type=jnp.float32)
        * factor
    )
    value_grad = value_grad + jnp.einsum(
        "hqk,qhd->khd", probs_low, context_grad_block, preferred_element_type=jnp.float32
    )
    return ((key_grad, value_grad), query_grad)


def gather_weights(w_query, w_key, w_value, w_output, w_inner, w_outer):
    return (
        lax.all_gather(w_query, FSDP, axis=0, tiled=True),
        lax.all_gather(w_key, FSDP, axis=0, tiled=True),
        lax.all_gather(w_value, FSDP, axis=0, tiled=True),
        lax.all_gather(w_output, FSDP, axis=1, tiled=True),
        lax.all_gather(w_inner, FSDP, axis=0, tiled=True),
        lax.all_gather(w_outer, FSDP, axis=1, tiled=True),
    )


def split_joint(joint_sum, output_sum, inner_sum, outer_sum, head_width):
    return (
        joint_sum[:, :head_width],
        joint_sum[:, head_width : 2 * head_width],
        joint_sum[:, 2 * head_width :],
        output_sum,
        inner_sum,
        outer_sum,
    )


def add_tuples(left, right):
    return tuple((first_item + second_item for first_item, second_item in zip(left, right)))


def local_generic(
    tokens,
    lengths,
    cotangent,
    w_query,
    w_key,
    w_value,
    w_output,
    w_inner,
    w_outer,
    b_query,
    b_value,
    b_output,
    b_inner,
    b_outer,
    gain_first,
    shift_first,
    gain_second,
    shift_second,
):
    tensor_size = lax.axis_size(TENSOR)
    tensor_rank = lax.axis_index(TENSOR)
    micro_count = tokens.shape[0]
    part_rows = tokens.shape[1]
    width = tokens.shape[2]
    seq_rows = part_rows * tensor_size
    head_width = w_query.shape[1]
    inner_width = w_inner.shape[1]
    local_heads = head_width // HEAD
    block_rows = min(512, seq_rows)
    block_count = seq_rows // block_rows
    vector_full = (
        lax.all_gather(b_query, (FSDP, TENSOR), axis=0, tiled=True),
        lax.all_gather(b_value, (FSDP, TENSOR), axis=0, tiled=True),
        lax.all_gather(b_output, (FSDP, TENSOR), axis=0, tiled=True),
        lax.all_gather(b_inner, (FSDP, TENSOR), axis=0, tiled=True),
        lax.all_gather(b_outer, (FSDP, TENSOR), axis=0, tiled=True),
        lax.all_gather(gain_first, (FSDP, TENSOR), axis=0, tiled=True),
        lax.all_gather(shift_first, (FSDP, TENSOR), axis=0, tiled=True),
        lax.all_gather(gain_second, (FSDP, TENSOR), axis=0, tiled=True),
        lax.all_gather(shift_second, (FSDP, TENSOR), axis=0, tiled=True),
    )
    query_bias = lax.dynamic_slice_in_dim(vector_full[0], tensor_rank * head_width, head_width)
    value_bias = lax.dynamic_slice_in_dim(vector_full[1], tensor_rank * head_width, head_width)
    inner_bias = lax.dynamic_slice_in_dim(vector_full[3], tensor_rank * inner_width, inner_width)
    joint_bias = jnp.concatenate([query_bias, jnp.zeros((head_width,), jnp.float32), value_bias])
    grad_query_bias = jnp.zeros((head_width,), jnp.float32)
    grad_value_bias = jnp.zeros((head_width,), jnp.float32)
    grad_inner_bias = jnp.zeros((inner_width,), jnp.float32)
    grad_output_bias = jnp.zeros((width,), jnp.float32)
    grad_outer_bias = jnp.zeros((width,), jnp.float32)
    grad_gain_one = jnp.zeros((width,), jnp.float32)
    grad_shift_one = jnp.zeros((width,), jnp.float32)
    grad_gain_two = jnp.zeros((width,), jnp.float32)
    grad_shift_two = jnp.zeros((width,), jnp.float32)
    local_totals = None
    shard_totals = None
    outputs = []
    input_grads = []
    slot_index = jnp.arange(seq_rows, dtype=jnp.int32)
    part_index = tensor_rank * part_rows + jnp.arange(part_rows, dtype=jnp.int32)
    for micro_index in range(micro_count):
        forward_weights = gather_weights(w_query, w_key, w_value, w_output, w_inner, w_outer)
        joint_w = jnp.concatenate(
            [forward_weights[0], forward_weights[1], forward_weights[2]], axis=1
        )
        output_w = forward_weights[3]
        inner_w = forward_weights[4]
        outer_w = forward_weights[5]
        length = lengths[micro_index]
        key_valid = slot_index < length
        row_valid = (part_index < length).astype(jnp.float32)[:, None]
        own_rows = tokens[micro_index]
        whole = lax.all_gather(own_rows, TENSOR, axis=0, tiled=True)
        joint = (jnp.dot(whole, joint_w, preferred_element_type=jnp.float32) + joint_bias).astype(
            jnp.bfloat16
        )
        query = joint[:, :head_width].reshape(block_count, block_rows, local_heads, HEAD)
        keys = joint[:, head_width : 2 * head_width].reshape(seq_rows, local_heads, HEAD)
        values = joint[:, 2 * head_width :].reshape(seq_rows, local_heads, HEAD)
        context_blocks, tops, totals = lax.map(
            partial(attend_forward, keys, values, key_valid), query
        )
        context_low = context_blocks.reshape(seq_rows, head_width).astype(jnp.bfloat16)
        attended = (
            lax.psum_scatter(
                jnp.dot(context_low, output_w, preferred_element_type=jnp.float32).astype(
                    jnp.bfloat16
                ),
                TENSOR,
                scatter_dimension=0,
                tiled=True,
            ).astype(jnp.float32)
            + vector_full[2]
        )
        normed_first, factor_first = normalize(own_rows.astype(jnp.float32) + attended)
        first = normed_first * vector_full[5] + vector_full[6]
        first_whole = lax.all_gather(first.astype(jnp.bfloat16), TENSOR, axis=0, tiled=True)
        inner = jnp.dot(first_whole, inner_w, preferred_element_type=jnp.float32) + inner_bias
        active = gelu_value(inner).astype(jnp.bfloat16)
        mixed = (
            lax.psum_scatter(
                jnp.dot(active, outer_w, preferred_element_type=jnp.float32).astype(jnp.bfloat16),
                TENSOR,
                scatter_dimension=0,
                tiled=True,
            ).astype(jnp.float32)
            + vector_full[4]
        )
        normed_second, factor_second = normalize(first + mixed)
        outputs.append(
            ((normed_second * vector_full[7] + vector_full[8]) * row_valid).astype(jnp.bfloat16)
        )
        backward_weights = gather_weights(w_query, w_key, w_value, w_output, w_inner, w_outer)
        joint_w = jnp.concatenate(
            [backward_weights[0], backward_weights[1], backward_weights[2]], axis=1
        )
        output_w = backward_weights[3]
        inner_w = backward_weights[4]
        outer_w = backward_weights[5]
        out_grad = cotangent[micro_index].astype(jnp.float32) * row_valid
        grad_gain_two = grad_gain_two + column_sum(out_grad * normed_second)
        grad_shift_two = grad_shift_two + column_sum(out_grad)
        sum_grad = normalize_back(out_grad * vector_full[7], normed_second, factor_second)
        mixed_grad = sum_grad.astype(jnp.bfloat16)
        grad_outer_bias = grad_outer_bias + column_sum(mixed_grad)
        mixed_whole = lax.all_gather(mixed_grad, TENSOR, axis=0, tiled=True)
        outer_sum = dot_rows(active, mixed_whole)
        inner_grad = (dot_back(mixed_whole, outer_w) * gelu_slope(inner)).astype(jnp.bfloat16)
        grad_inner_bias = grad_inner_bias + column_sum(inner_grad)
        inner_sum = dot_rows(first_whole, inner_grad)
        first_grad = sum_grad + lax.psum_scatter(
            dot_back(inner_grad, inner_w).astype(jnp.bfloat16),
            TENSOR,
            scatter_dimension=0,
            tiled=True,
        ).astype(jnp.float32)
        grad_gain_one = grad_gain_one + column_sum(first_grad * normed_first)
        grad_shift_one = grad_shift_one + column_sum(first_grad)
        residual_grad = normalize_back(first_grad * vector_full[5], normed_first, factor_first)
        attended_grad = residual_grad.astype(jnp.bfloat16)
        grad_output_bias = grad_output_bias + column_sum(attended_grad)
        attended_whole = lax.all_gather(attended_grad, TENSOR, axis=0, tiled=True)
        output_sum = dot_rows(context_low, attended_whole)
        context_grad = (
            dot_back(attended_whole, output_w)
            .astype(jnp.bfloat16)
            .reshape(block_count, block_rows, local_heads, HEAD)
        )
        empty = jnp.zeros((seq_rows, local_heads, HEAD), jnp.float32)
        carried, query_grad = lax.scan(
            partial(attend_backward, keys, values, key_valid),
            (empty, empty),
            (query, context_grad, tops, totals),
        )
        joint_grad = jnp.concatenate(
            [
                query_grad.reshape(seq_rows, head_width),
                carried[0].reshape(seq_rows, head_width),
                carried[1].reshape(seq_rows, head_width),
            ],
            axis=1,
        ).astype(jnp.bfloat16)
        grad_query_bias = grad_query_bias + column_sum(joint_grad[:, :head_width])
        grad_value_bias = grad_value_bias + column_sum(joint_grad[:, 2 * head_width :])
        joint_sum = dot_rows(whole, joint_grad)
        input_grads.append(
            residual_grad
            + lax.psum_scatter(
                dot_back(joint_grad, joint_w).astype(jnp.bfloat16),
                TENSOR,
                scatter_dimension=0,
                tiled=True,
            ).astype(jnp.float32)
        )
        batch_sums = (joint_sum, output_sum, inner_sum, outer_sum)
        local_totals = batch_sums if local_totals is None else add_tuples(local_totals, batch_sums)
    pieces = split_joint(
        local_totals[0], local_totals[1], local_totals[2], local_totals[3], head_width
    )
    shard_totals = (
        lax.psum_scatter(pieces[0], FSDP, scatter_dimension=0, tiled=True),
        lax.psum_scatter(pieces[1], FSDP, scatter_dimension=0, tiled=True),
        lax.psum_scatter(pieces[2], FSDP, scatter_dimension=0, tiled=True),
        lax.psum_scatter(pieces[3], FSDP, scatter_dimension=1, tiled=True),
        lax.psum_scatter(pieces[4], FSDP, scatter_dimension=0, tiled=True),
        lax.psum_scatter(pieces[5], FSDP, scatter_dimension=1, tiled=True),
    )
    vector_grads = (
        lax.psum_scatter(
            place(grad_query_bias, tensor_rank * head_width, width),
            (FSDP, TENSOR),
            scatter_dimension=0,
            tiled=True,
        ),
        lax.psum_scatter(
            place(grad_value_bias, tensor_rank * head_width, width),
            (FSDP, TENSOR),
            scatter_dimension=0,
            tiled=True,
        ),
        lax.psum_scatter(grad_output_bias, (FSDP, TENSOR), scatter_dimension=0, tiled=True),
        lax.psum_scatter(
            place(grad_inner_bias, tensor_rank * inner_width, inner_width * tensor_size),
            (FSDP, TENSOR),
            scatter_dimension=0,
            tiled=True,
        ),
        lax.psum_scatter(grad_outer_bias, (FSDP, TENSOR), scatter_dimension=0, tiled=True),
        lax.psum_scatter(grad_gain_one, (FSDP, TENSOR), scatter_dimension=0, tiled=True),
        lax.psum_scatter(grad_shift_one, (FSDP, TENSOR), scatter_dimension=0, tiled=True),
        lax.psum_scatter(grad_gain_two, (FSDP, TENSOR), scatter_dimension=0, tiled=True),
        lax.psum_scatter(grad_shift_two, (FSDP, TENSOR), scatter_dimension=0, tiled=True),
    )
    return (
        jnp.stack(outputs),
        jnp.stack(input_grads),
        shard_totals[0],
        shard_totals[1],
        shard_totals[2],
        shard_totals[3],
        shard_totals[4],
        shard_totals[5],
        vector_grads[0],
        vector_grads[1],
        vector_grads[2],
        vector_grads[3],
        vector_grads[4],
        vector_grads[5],
        vector_grads[6],
        vector_grads[7],
        vector_grads[8],
    )


MESH = pl.DeviceIdType.MESH
WIDTH = 768
HIDDEN = 3072
HALF = WIDTH // 2
KINDS = 3
VECTOR_ROWS = 16
ROW_OUTPUT, ROW_OUTER, ROW_GAIN1, ROW_SHIFT1, ROW_GAIN2, ROW_SHIFT2, ROW_INNER = 4, 5, 6, 7, 8, 9, 10
BF16 = jnp.bfloat16
F32 = jnp.float32


def fits(sizes):
    fsdp = sizes[FSDP]
    return sizes[TENSOR] == 4 and fsdp % 2 == 0 and WIDTH % (16 * fsdp) == 0


class Place:
    def __init__(self, nz):
        self.f = lax.axis_index(FSDP)
        self.t = lax.axis_index(TENSOR)
        self.nz = nz
        self.z = self.f // 2
        self.x = self.f % 2
        self.y = self.t // 2
        self.c = self.t % 2
        self.core = (self.f, self.t + 1 - 2 * self.c)
        self.along_y = (self.f, self.t + 2 - 4 * self.y)
        self.along_x = (self.f + 1 - 2 * self.x, self.t)

    def z_at(self, step):
        return (self.z + step) % self.nz

    def z_back(self, step):
        return (self.z + self.nz - step) % self.nz

    def along_z(self, step):
        return (self.z_at(step) * 2 + self.x, self.t)

    def in_group(self, step):
        return (self.f, (self.t + step) % 4)


class Net:
    def __init__(self, send_sems, recv_sems):
        self.send_sems = send_sems
        self.recv_sems = recv_sems
        self.count = 0

    def plan(self, source, target, device):
        copy = pltpu.make_async_remote_copy(
            src_ref=source,
            dst_ref=target,
            send_sem=self.send_sems.at[self.count],
            recv_sem=self.recv_sems.at[self.count],
            device_id=device,
            device_id_type=MESH,
        )
        self.count += 1
        return copy

    def keep(self, ref, device):
        return self.plan(ref, ref, device)


def start_all(copies):
    for copy in copies:
        copy.start()


def sent_all(copies):
    for copy in copies:
        copy.wait_send()


def greet(place):
    barrier = pltpu.get_barrier_semaphore()
    peers = [place.in_group(1), place.in_group(2), place.in_group(3), place.along_x]
    peers += [place.along_z(step) for step in range(1, place.nz)]
    for peer in peers:
        pl.semaphore_signal(barrier, inc=1, device_id=peer, device_id_type=MESH)
    pl.semaphore_wait(barrier, len(peers))


def wait_all(copies):
    for copy in copies:
        copy.wait_recv()


def vector_peers(place):
    peers = []
    stride = 1
    while stride < place.nz:
        z = place.z
        other = z + stride - 2 * stride * ((z // stride) % 2)
        peers.append((other * 2 + place.x, place.t))
        stride *= 2
    peers.insert(1, place.core)
    return peers + [place.along_x, place.along_y]


class Exchange:
    def __init__(self, net, place, total, slots):
        self.total, self.slots = total, slots
        self.copies = [net.plan(total, slots.at[i], peer) for i, peer in enumerate(vector_peers(place))]

    def start(self, index):
        self.copies[index].start()

    def finish(self, index):
        self.copies[index].wait()
        self.total[...] += self.slots[index]

    def rest(self, index):
        for later in range(index, len(self.copies)):
            self.start(later)
            self.finish(later)


def dot(left, right):
    return lax.dot_general(left, right, (((1,), (0,)), ((), ())), preferred_element_type=F32)


class Layer:
    def __init__(self, refs, length):
        (
            self.w, self.rows, self.back, self.rows_turned, self.joint, self.probs, self.context, self.acc,
            self.normed, self.factor, self.first_low, self.first_turned, self.active, self.slope, self.grad_low,
            self.grad_turned, self.out, self.vec, self.sums,
        ) = refs
        self.length = length
        self.seq = self.rows.shape[0]
        self.block = 128

    def weight(self, kind, t):
        return self.w[kind, t // 2, t % 2].reshape(WIDTH, WIDTH)

    def output_weight(self, t):
        return self.w[0, t // 2, t % 2, :, :, :, 512:768].reshape(WIDTH, 256)

    def store_grad(self, kind, t, value):
        nz = self.w.shape[3]
        self.w[kind, t // 2, t % 2] = value.astype(BF16).reshape(nz, 2, WIDTH // (2 * nz), WIDTH)

    def row(self, index):
        return self.vec[pl.ds(index, 1), :]

    def blocks(self, body):
        def step(i, carry):
            body(pl.ds(pl.multiple_of(i * self.block, self.block), self.block), i)
            return carry

        lax.fori_loop(0, self.seq // self.block, step, 0)

    def row_valid(self, i):
        index = lax.broadcasted_iota(jnp.int32, (self.block, 1), 0) + i * self.block
        return (index < self.length).astype(F32)

    def lanes(self, low, high, width):
        lane = lax.broadcasted_iota(jnp.int32, (1, width), 1)
        return (lane >= low) & (lane < high)

    def pick(self, value, low, high):
        return jnp.where(self.lanes(low, high, value.shape[1]), value, jnp.zeros_like(value))

    def head_query(self, t, h):
        return self.joint[t, :, 0:128] if h < 2 else self.joint[t, :, 384:512]

    def head_key(self, t, h):
        return self.joint[t, :, 128:256] if h < 2 else self.joint[t, :, 640:768]

    def head_side(self, value, h):
        return self.pick(value, 0, 64) if h == 0 else self.pick(value, 64, 128)

    def head_value(self, t, h):
        return self.pick(self.joint[t, :, 256:512], h * 64, h * 64 + 64)

    def project(self, t):
        self.joint[t] = (dot(self.rows[...], self.weight(0, t)) + self.row(t)).astype(BF16)

    def attend(self, t):
        key_valid = lax.broadcasted_iota(jnp.int32, (1, self.seq), 1) < self.length
        context = None
        for h in range(3):
            raw = dot_back(self.head_query(t, h), self.head_side(self.head_key(t, h), h))
            masked = jnp.where(key_valid, raw * HEAD ** -0.5, -1e9)
            expo = jnp.exp(masked - jnp.max(masked, axis=1, keepdims=True))
            probs = (expo * (1.0 / jnp.sum(expo, axis=1, keepdims=True))).astype(BF16)
            self.probs[t * 3 + h] = probs
            part = dot(probs, self.head_value(t, h))
            context = part if context is None else context + part
        low = context.astype(BF16)
        self.context[t] = low
        self.acc[...] += dot_back(low, self.output_weight(t))

    def start(self):
        def body(rows, i):
            self.acc[rows] = self.rows[rows].astype(F32) + self.row(ROW_OUTPUT)

        self.blocks(body)

    def norm_first(self):
        def body(rows, i):
            normed, factor = normalize(self.acc[rows])
            self.normed[rows] = normed
            self.factor[rows] = jnp.broadcast_to(factor, (self.block, 128))
            first = normed * self.row(ROW_GAIN1) + self.row(ROW_SHIFT1)
            self.first_low[rows] = first.astype(BF16)
            self.acc[rows] = first + self.row(ROW_OUTER)

        self.blocks(body)

    def feed_inner(self, t):
        inner = dot(self.first_low[...], self.weight(1, t)) + self.row(ROW_INNER + t)
        gate = 1.0 + lax.erf(inner * root_half)
        self.active[t] = (0.5 * inner * gate).astype(BF16)
        self.slope[t] = (0.5 * gate + inner * inverse_root_two_pi * jnp.exp(-0.5 * inner * inner)).astype(BF16)

    def feed_outer(self, t):
        self.acc[...] += dot_back(self.active[t], self.weight(2, t))

    def clear_sums(self):
        self.sums[...] = jnp.zeros_like(self.sums)

    def add_sum(self, index, value):
        self.sums[pl.ds(index, 1), :] += jnp.sum(value, axis=0, keepdims=True)

    def norm_second(self):
        def body(rows, i):
            normed, factor = normalize(self.acc[rows])
            valid = self.row_valid(i)
            gain = self.row(ROW_GAIN2)
            self.out[rows] = ((normed * gain + self.row(ROW_SHIFT2)) * valid).astype(BF16)
            out_grad = self.back[rows].astype(F32) * valid
            self.add_sum(ROW_GAIN2, out_grad * normed)
            self.add_sum(ROW_SHIFT2, out_grad)
            sum_grad = normalize_back(out_grad * gain, normed, factor)
            self.acc[rows] = sum_grad
            low = sum_grad.astype(BF16)
            self.grad_low[rows] = low
            self.add_sum(ROW_OUTER, low.astype(F32))

        self.blocks(body)
        self.grad_turned[...] = self.grad_low[...].T

    def outer_back(self, t):
        grad = (dot(self.grad_low[...], self.weight(2, t)) * self.slope[t].astype(F32)).astype(BF16)
        self.slope[t] = grad
        self.add_sum(ROW_INNER + t, grad.astype(F32))
        self.store_grad(2, t, dot(self.grad_turned[...], self.active[t]))

    def inner_back(self, t):
        grad = self.slope[t]
        self.acc[...] += dot_back(grad, self.weight(1, t))
        self.store_grad(1, t, dot(self.first_turned[...], grad))

    def norm_first_back(self):
        def body(rows, i):
            grad = self.acc[rows]
            normed = self.normed[rows]
            self.add_sum(ROW_GAIN1, grad * normed)
            self.add_sum(ROW_SHIFT1, grad)
            residual = normalize_back(grad * self.row(ROW_GAIN1), normed, self.factor[rows][:, 0:1])
            self.acc[rows] = residual
            low = residual.astype(BF16)
            self.grad_low[rows] = low
            self.add_sum(ROW_OUTPUT, low.astype(F32))

        self.blocks(body)
        self.grad_turned[...] = self.grad_low[...].T

    def attend_back(self, t):
        context_grad = self.pick(dot(self.grad_low[...], self.output_weight(t)), 0, 192).astype(BF16)
        query_grads, key_grads, value_grad = [], [], None
        for h in range(3):
            probs = self.probs[t * 3 + h]
            prob_grad = dot_back(context_grad, self.head_value(t, h))
            wide = probs.astype(F32)
            delta = jnp.sum(wide * prob_grad, axis=1, keepdims=True)
            score_grad = (wide * (prob_grad - delta)).astype(BF16)
            query_grads.append(dot(score_grad, self.head_side(self.head_key(t, h), h)) * HEAD ** -0.5)
            key_grads.append(dot_rows(score_grad, self.head_side(self.head_query(t, h), h)) * HEAD ** -0.5)
            part = dot_rows(probs, self.pick(context_grad, h * 64, h * 64 + 64))
            value_grad = part if value_grad is None else value_grad + part
        self.joint[t, :, 0:128] = (query_grads[0] + query_grads[1]).astype(BF16)
        self.joint[t, :, 128:256] = (key_grads[0] + key_grads[1]).astype(BF16)
        self.joint[t, :, 256:384] = value_grad[:, 0:128].astype(BF16)
        self.joint[t, :, 384:512] = (value_grad[:, 128:256] + query_grads[2]).astype(BF16)
        self.joint[t, :, 512:640] = jnp.zeros((self.seq, 128), BF16)
        self.joint[t, :, 640:768] = key_grads[2].astype(BF16)

    def joint_back(self, t):
        joint = self.joint[t]
        self.sums[pl.ds(t, 1), :] = jnp.sum(joint.astype(F32), axis=0, keepdims=True)
        self.acc[...] += dot_back(joint, self.weight(0, t))
        nz = self.w.shape[3]
        shape = (nz, 2, WIDTH // (2 * nz), -1)
        main = dot(self.rows_turned[...], joint[:, 0:512])
        side = dot(self.rows_turned[...], joint[:, 512:768]) + dot(self.grad_turned[...], self.context[t])
        self.w[0, t // 2, t % 2, :, :, :, 0:512] = main.astype(BF16).reshape(shape[:3] + (512,))
        self.w[0, t // 2, t % 2, :, :, :, 512:768] = side.astype(BF16).reshape(shape[:3] + (256,))

    def finish(self):
        def body(rows, i):
            self.back[rows] = self.acc[rows].astype(BF16)

        self.blocks(body)


def each(count, body):
    def step(i, carry):
        body(i)
        return carry

    lax.fori_loop(0, count, step, 0)


BUFFER_COUNT = 19


def buffer_shapes(nz, seq):
    part = WIDTH // (2 * nz)
    low, wide = (seq, WIDTH), (WIDTH, seq)
    shapes = [
        ((KINDS, 2, 2, nz, 2, part, WIDTH), BF16),
        (low, BF16),
        (low, BF16),
        (wide, BF16),
        ((4, seq, WIDTH), BF16),
        ((12, seq, seq), BF16),
        ((4, seq, 256), BF16),
        (low, F32),
        (low, F32),
        ((seq, 128), F32),
        (low, BF16),
        (wide, BF16),
        ((4, seq, WIDTH), BF16),
        ((4, seq, WIDTH), BF16),
        (low, BF16),
        (wide, BF16),
        (low, BF16),
        ((VECTOR_ROWS, WIDTH), F32),
        ((VECTOR_ROWS, WIDTH), F32),
    ]
    return [pltpu.VMEM(*shape) for shape in shapes]


def landing_shapes(nz):
    part = WIDTH // (2 * nz)
    shapes = [
        (KINDS, 2, nz, 2, part, WIDTH),
        (KINDS, nz, 2, part, HALF),
        (KINDS, nz, part, HALF),
        (KINDS, nz - 1, part, HALF),
        (KINDS, 2, nz, part, HALF),
        (KINDS, nz - 1, 2, part, HALF),
        (KINDS, 3, part, HALF),
    ]
    return [pltpu.VMEM(shape, BF16) for shape in shapes]


class Gather:
    def __init__(self, net, place, own, w, k):
        p = place
        a, b = pl.ds(0, HALF), pl.ds(HALF, HALF)
        own_a, own_b = own.at[k, :, a], own.at[k, :, b]
        mine_a, mine_b = (w.at[k, p.y, p.c, p.z, p.x, :, cols] for cols in (a, b))
        steps = range(1, p.nz)
        self.az = [net.plan(own_a, mine_a, p.along_z(step)) for step in steps]
        self.by = [net.plan(own_b, mine_b, p.along_y)]
        self.ax = [net.plan(own_a, mine_a, p.along_x)]
        self.ax += [net.keep(w.at[k, p.y, p.c, p.z_back(step), p.x, :, a], p.along_x) for step in steps]
        self.ay = [net.keep(w.at[k, p.y, p.c, :, x, :, a], p.along_y) for x in (p.x, 1 - p.x)]
        self.ac = [net.keep(w.at[k, y, p.c, :, :, :, a], p.core) for y in (p.y, 1 - p.y)]
        self.bz = [net.keep(w.at[k, :, p.c, p.z, p.x, :, b], p.along_z(step)) for step in steps]
        self.bx = [net.keep(w.at[k, :, p.c, p.z_back(step), p.x, :, b], p.along_x) for step in range(p.nz)]
        self.bc = [net.keep(w.at[k, :, p.c, :, x, :, b], p.core) for x in (p.x, 1 - p.x)]

    def b_y_to_z(self):
        wait_all(self.by)
        start_all(self.bz)
        self.bx[0].start()

    def a_z_to_x(self):
        for arrived, onward in zip(self.az, self.ax[1:]):
            arrived.wait_recv()
            onward.start()
        self.ay[0].start()

    def a_x_to_y(self):
        wait_all(self.ax)
        self.ay[1].start()
        self.ac[0].start()

    def b_z_to_x(self):
        for arrived, onward in zip(self.bz, self.bx[1:]):
            arrived.wait_recv()
            onward.start()
        self.bc[0].start()

    def a_y_to_core(self):
        wait_all(self.ay)
        self.ac[1].start()

    def b_x_to_core(self):
        wait_all(self.bx)
        self.bc[1].start()

    def done(self):
        wait_all(self.ac)
        wait_all(self.bc)

    def sent(self):
        for copies in (self.az, self.ax, self.ay, self.ac, self.by, self.bz, self.bx, self.bc):
            sent_all(copies)


class Reduce:
    def __init__(self, net, place, w, landings, result, k):
        p = self.place = place
        self.core, self.ya, self.xa, self.za, self.xb, self.zb, self.yb = (ref.at[k] for ref in landings)
        self.w, self.result = w.at[k], result.at[k]
        self.a, self.b = pl.ds(0, HALF), pl.ds(HALF, HALF)
        self.ys = ys = (1 - p.y, p.y)
        self.xs = xs = (1 - p.x, p.x)
        self.zs = zs = [p.z_at((step + 1) % p.nz) for step in range(p.nz)]
        self.c = [net.plan(self.w.at[y, 1 - p.c], self.core.at[y], p.core) for y in ys]
        self.ay = [net.plan(self.core.at[ys[0], :, x, :, self.a], self.ya.at[:, x], p.along_y) for x in xs]
        self.bx = [
            [net.plan(self.core.at[y, z, xs[0], :, self.b], self.xb.at[y, z], p.along_x) for z in zs] for y in ys
        ]
        self.bz = [
            [net.plan(self.xb.at[y, zs[i]], self.zb.at[i, y], p.along_z(i + 1)) for i in range(p.nz - 1)] for y in ys
        ]
        self.by = [net.plan(self.yb.at[ys[0]], self.yb.at[2], p.along_y)]
        self.ax = [net.plan(self.ya.at[z, xs[0]], self.xa.at[z], p.along_x) for z in zs]
        self.az = [net.plan(self.xa.at[zs[i]], self.za.at[i], p.along_z(i + 1)) for i in range(p.nz - 1)]

    def add(self, target, source):
        target[...] = (target[...].astype(F32) + source[...].astype(F32)).astype(BF16)

    def core_half(self, half):
        y = self.ys[half]
        self.c[half].wait_recv()

        def body(z):
            self.add(self.core.at[y, z], self.w.at[y, self.place.c, z])

        each(self.place.nz, body)
        if half == 0:
            start_all(self.ay)
        start_all(self.bx[half])

    def a_y(self, index):
        self.ay[index].wait_recv()
        x = self.xs[index]

        def body(z):
            self.add(self.ya.at[z, x], self.core.at[self.ys[1], z, x, :, self.a])

        each(self.place.nz, body)
        if index == 0:
            start_all(self.ax)

    def b_x(self, half):
        y = self.ys[half]
        for i, z in enumerate(self.zs):
            self.bx[half][i].wait_recv()
            self.add(self.xb.at[y, z], self.core.at[y, z, self.xs[1], :, self.b])
            if i < self.place.nz - 1:
                self.bz[half][i].start()

    def a_x(self):
        for i, z in enumerate(self.zs):
            self.ax[i].wait_recv()
            self.add(self.xa.at[z], self.ya.at[z, self.xs[1]])
            if i < self.place.nz - 1:
                self.az[i].start()

    def b_z(self):
        for half, y in enumerate(self.ys):
            wait_all(self.bz[half])
            total = self.xb[y, self.place.z].astype(F32)
            for i in range(self.place.nz - 1):
                total += self.zb[i, y].astype(F32)
            self.yb[y] = total.astype(BF16)
            if half == 0:
                start_all(self.by)

    def a_z(self):
        wait_all(self.az)
        total = self.xa[self.place.z].astype(F32)
        for i in range(self.place.nz - 1):
            total += self.za[i].astype(F32)
        self.result[:, self.a] = total

    def b_y(self):
        wait_all(self.by)
        self.result[:, self.b] = self.yb[self.ys[1]].astype(F32) + self.yb[2].astype(F32)

    def sent(self):
        for copies in (self.c, self.ay, *self.bx, *self.bz, self.by, self.ax, self.az):
            sent_all(copies)


def ticks(i, table):
    for when, actions in table.items():
        @pl.when(i == when)
        def _(actions=actions):
            for action, *given in actions:
                action(*given)


def layer_kernel(nz, *refs):
    own, tokens, cotangent, lengths, vec_in, result, outs, backs, totals = refs[:9]
    rest = list(refs[9:])
    buffers, rest = rest[:BUFFER_COUNT], rest[BUFFER_COUNT:]
    landings, (slots, back_slots, send_sems, recv_sems, local_sems) = rest[:7], rest[7:]
    place = Place(nz)
    net = Net(send_sems, recv_sems)
    t = place.t
    quarter = tokens.shape[1]
    layer = Layer(buffers, lengths[t])
    joint, inner, outer = [Gather(net, place, own, layer.w, k) for k in range(KINDS)]
    to_joint, to_inner, to_outer = [Reduce(net, place, layer.w, landings, result, k) for k in range(KINDS)]

    def quarter_of(ref, index):
        return ref.at[pl.ds(pl.multiple_of(index * quarter, quarter), quarter)]

    def swap_in(source, target):
        return [
            net.plan(source.at[(t + step) % 4], quarter_of(target, t), place.in_group(step)) for step in (2, 1, 3)
        ]

    def swap_out(source, target):
        return [
            net.plan(quarter_of(source, (t + step) % 4), target.at[t], place.in_group(step)) for step in (2, 1, 3)
        ]

    token_in = swap_in(tokens, layer.rows)
    back_in = swap_in(cotangent, layer.back)
    out_out = swap_out(layer.out, outs)
    back_out = swap_out(layer.back, backs)
    vec = Exchange(net, place, layer.vec, slots)
    sums = Exchange(net, place, totals, back_slots)
    pairs = [
        (tokens.at[t], quarter_of(layer.rows, t)),
        (cotangent.at[t], quarter_of(layer.back, t)),
        *[(own.at[k], layer.w.at[k, place.y, place.c, place.z, place.x]) for k in range(KINDS)],
        (quarter_of(layer.out, t), outs.at[t]),
        (quarter_of(layer.back, t), backs.at[t]),
    ]
    local = [pltpu.make_async_copy(*pair, local_sems.at[i]) for i, pair in enumerate(pairs)]

    def order(i):
        return (1 - place.y + i) % 2 * 2 + (1 - place.c + i // 2) % 2

    layer.vec[...] = vec_in[...]
    greet(place)
    vec.start(0)
    start_all(joint.by + inner.by + outer.by)
    start_all(joint.az)
    joint.ax[0].start()
    start_all(token_in)
    start_all(local[:5])
    vec.finish(0)
    vec.start(1)
    vec.finish(1)
    vec.start(2)
    for copy in local[:5]:
        copy.wait()
    joint.b_y_to_z()
    joint.a_z_to_x()
    vec.finish(2)
    vec.start(3)
    start_all(inner.az)
    inner.ax[0].start()
    inner.b_y_to_z()
    vec.finish(3)
    vec.rest(4)
    joint.a_x_to_y()
    joint.b_z_to_x()
    start_all(outer.az)
    outer.ax[0].start()
    outer.b_y_to_z()
    inner.a_z_to_x()
    joint.a_y_to_core()
    joint.b_x_to_core()
    wait_all(token_in)
    layer.start()
    layer.rows_turned[...] = layer.rows[...].T
    layer.clear_sums()
    joint.done()
    each(4, layer.project)
    inner.a_x_to_y()

    def attend(i):
        layer.attend(i)
        ticks(i, {
            0: [(inner.b_z_to_x,)],
            1: [(outer.a_z_to_x,)],
            2: [(inner.a_y_to_core,), (inner.b_x_to_core,)],
            3: [(outer.a_x_to_y,), (start_all, back_in)],
        })

    each(4, attend)
    layer.norm_first()
    layer.first_turned[...] = layer.first_low[...].T
    inner.done()
    outer.b_z_to_x()
    each(4, layer.feed_inner)
    outer.a_y_to_core()
    outer.b_x_to_core()
    outer.done()
    each(4, layer.feed_outer)
    wait_all(back_in)
    layer.norm_second()
    start_all(out_out)
    local[5].start()
    outer.sent()

    def outer_back(i):
        layer.outer_back(order(i))
        ticks(i, {
            0: [(to_outer.c[0].start,)],
            1: [(to_outer.c[1].start,)],
            2: [(to_outer.core_half, 0)],
            3: [(to_outer.core_half, 1)],
        })

    each(4, outer_back)
    inner.sent()

    def inner_back(i):
        layer.inner_back(order(i))
        ticks(i, {
            0: [(to_inner.c[0].start,)],
            1: [(to_inner.c[1].start,)],
            2: [(to_outer.a_y, 0), (to_inner.core_half, 0)],
            3: [(to_inner.core_half, 1)],
        })

    each(4, inner_back)
    to_outer.b_x(0)
    layer.norm_first_back()
    to_outer.a_y(1)
    joint.sent()

    def attend_back(i):
        layer.attend_back(order(i))
        ticks(i, {
            0: [(to_outer.b_x, 1), (to_outer.a_x,)],
            1: [(to_inner.b_x, 1), (to_inner.a_y, 1), (to_inner.a_x,)],
            2: [(to_outer.b_y,), (to_inner.b_z,), (to_inner.a_z,)],
            3: [(to_inner.b_y,)],
        })
        layer.joint_back(order(i))
        ticks(i, {
            0: [(to_joint.c[0].start,), (to_inner.a_y, 0), (to_inner.b_x, 0)],
            1: [(to_joint.c[1].start,), (to_outer.b_z,), (to_outer.a_z,)],
            2: [(to_joint.core_half, 0)],
            3: [(to_joint.core_half, 1)],
        })

    each(4, attend_back)
    wait_all(back_in[:0])
    layer.finish()
    start_all(back_out)
    local[6].start()
    totals[...] = layer.sums[...]
    sums.start(0)
    to_joint.a_y(0)
    to_joint.b_x(0)
    sums.finish(0)
    sums.start(1)
    to_joint.a_y(1)
    to_joint.b_x(1)
    sums.finish(1)
    sums.start(2)
    to_joint.a_x()
    sums.finish(2)
    sums.start(3)
    to_joint.b_z()
    to_joint.a_z()
    sums.finish(3)
    sums.rest(4)
    to_joint.b_y()
    for copy in local[5:]:
        copy.wait()
    wait_all(out_out + back_out)
    for stage in (to_outer, to_inner, to_joint):
        stage.sent()
    sent_all(token_in + back_in + out_out + back_out)


VMEM_SPEC = pl.BlockSpec(memory_space=pltpu.VMEM)
ANY_SPEC = pl.BlockSpec(memory_space=pl.ANY)
LIMIT = 67043328


def whole_layer(own, tokens, cotangent, lengths, vectors):
    nz = lax.axis_size(FSDP) // 2
    part = WIDTH // (2 * nz)
    seq = tokens.shape[1] * 4
    steps = 3 + (nz - 1).bit_length()
    count = 176
    return pl.pallas_call(
        partial(layer_kernel, nz),
        out_shape=(
            jax.ShapeDtypeStruct((KINDS, part, WIDTH), F32),
            jax.ShapeDtypeStruct(tokens.shape, BF16),
            jax.ShapeDtypeStruct(tokens.shape, BF16),
            jax.ShapeDtypeStruct((VECTOR_ROWS, WIDTH), F32),
        ),
        in_specs=[ANY_SPEC, ANY_SPEC, ANY_SPEC, pl.BlockSpec(memory_space=pltpu.SMEM), VMEM_SPEC],
        out_specs=(VMEM_SPEC, ANY_SPEC, ANY_SPEC, VMEM_SPEC),
        scratch_shapes=buffer_shapes(nz, seq) + landing_shapes(nz) + [
            pltpu.VMEM((steps, VECTOR_ROWS, WIDTH), F32),
            pltpu.VMEM((steps, VECTOR_ROWS, WIDTH), F32),
            pltpu.SemaphoreType.DMA((count,)),
            pltpu.SemaphoreType.DMA((count,)),
            pltpu.SemaphoreType.DMA((8,)),
        ],
        compiler_params=pltpu.CompilerParams(collective_id=0, has_side_effects=True, vmem_limit_bytes=LIMIT),
        name="whole_layer",
    )(own, tokens, cotangent, lengths, vectors)


def pack_joint(q, k, v, o):
    return jnp.concatenate(
        [q[:, :128], k[:, :128], v[:, :128], v[:, 128:], q[:, 128:], o[:, :128], o[:, 128:], k[:, 128:]], axis=1
    )


def unpack_joint(joint):
    q = jnp.concatenate([joint[:, 0:128], joint[:, 448:512]], axis=1)
    k = jnp.concatenate([joint[:, 128:256], joint[:, 704:768]], axis=1)
    return q, k, joint[:, 256:448], joint[:, 512:704]


def local_fast(
    tokens, lengths, cotangent, w_query, w_key, w_value, w_output, w_inner, w_outer,
    b_query, b_value, b_output, b_inner, b_outer, gain_first, shift_first, gain_second, shift_second,
):
    tensor_rank = lax.axis_index(TENSOR)
    rank = lax.axis_index(FSDP) * 4 + tensor_rank
    own = jnp.stack([pack_joint(w_query, w_key, w_value, w_output.T), w_inner, w_outer.T])
    size = b_query.shape[0]
    zeros = jnp.zeros((VECTOR_ROWS, WIDTH), F32)
    short = jnp.stack([b_output, b_outer, gain_first, shift_first, gain_second, shift_second])
    placed = lax.dynamic_update_slice(zeros, short, (ROW_OUTPUT, rank * size))
    start = rank * b_inner.shape[0]
    placed = lax.dynamic_update_slice(placed, b_inner[None], (ROW_INNER + start // WIDTH, start % WIDTH))
    start = rank * size
    head_row, within = start // 192, start % 192
    spot = jnp.arange(WIDTH)
    query_spot = jnp.where(spot < 128, spot, jnp.where((spot >= 448) & (spot < 512), spot - 320, -1))
    value_spot = jnp.where((spot >= 256) & (spot < 448), spot - 256, -1)

    def spread(values, spots):
        match = (spots[None, :] == within + jnp.arange(size)[:, None]).astype(F32)
        return jnp.sum(match * values[:, None], axis=0)

    joint_row = spread(b_query, query_spot) + spread(b_value, value_spot)
    placed = lax.dynamic_update_slice(placed, joint_row[None], (head_row, 0))
    sums, outs, backs, totals = whole_layer(own, tokens, cotangent, lengths, placed)
    w_q, w_k, w_v, w_o = unpack_joint(sums[0])
    short_own = lax.dynamic_slice(totals, (ROW_OUTPUT, rank * size), short.shape)
    start = rank * b_inner.shape[0]
    inner_own = lax.dynamic_slice(totals, (ROW_INNER + start // WIDTH, start % WIDTH), (1, b_inner.shape[0]))[0]
    joint_own = lax.dynamic_index_in_dim(totals, head_row, keepdims=False)
    bias_q = jnp.concatenate([joint_own[0:128], joint_own[448:512]])
    query_own = lax.dynamic_slice(bias_q, (within,), (size,))
    value_own = lax.dynamic_slice(joint_own, (256 + within,), (size,))
    return (
        outs,
        backs.astype(F32),
        w_q,
        w_k,
        w_v,
        w_o.T,
        sums[1],
        sums[2].T,
        query_own,
        value_own,
        short_own[0],
        inner_own,
        short_own[1],
        short_own[2],
        short_own[3],
        short_own[4],
        short_own[5],
    )


def solution(mesh):
    placed = (
        P(FSDP, TENSOR, None),
        P(FSDP),
        P(FSDP, TENSOR, None),
        P(FSDP, TENSOR),
        P(FSDP, TENSOR),
        P(FSDP, TENSOR),
        P(TENSOR, FSDP),
        P(FSDP, TENSOR),
        P(TENSOR, FSDP),
        P((FSDP, TENSOR)),
        P((FSDP, TENSOR)),
        P((FSDP, TENSOR)),
        P((FSDP, TENSOR)),
        P((FSDP, TENSOR)),
        P((FSDP, TENSOR)),
        P((FSDP, TENSOR)),
        P((FSDP, TENSOR)),
        P((FSDP, TENSOR)),
    )
    return jax.shard_map(
        local_fast if fits(mesh.shape) else local_generic,
        mesh=mesh,
        in_specs=placed,
        out_specs=(
            P(FSDP, TENSOR, None),
            P(FSDP, TENSOR, None),
            P(FSDP, TENSOR),
            P(FSDP, TENSOR),
            P(FSDP, TENSOR),
            P(TENSOR, FSDP),
            P(FSDP, TENSOR),
            P(TENSOR, FSDP),
            P((FSDP, TENSOR)),
            P((FSDP, TENSOR)),
            P((FSDP, TENSOR)),
            P((FSDP, TENSOR)),
            P((FSDP, TENSOR)),
            P((FSDP, TENSOR)),
            P((FSDP, TENSOR)),
            P((FSDP, TENSOR)),
            P((FSDP, TENSOR)),
        ),
        check_vma=False,
    )
```

```python
from functools import partial

import jax
import jax.numpy as jnp
from jax import lax
from jax.experimental import pallas as pl
from jax.experimental.pallas import tpu as pltpu
from jax.sharding import PartitionSpec as P

FSDP, TENSOR = "fsdp", "tensor"

HEAD = 64


epsilon = 1e-05
root_half = 0.7071067811865476
inverse_root_two_pi = 0.3989422804014327


def gelu_value(inner):
    return 0.5 * inner * (1.0 + jax.scipy.special.erf(inner * root_half))


def gelu_slope(inner):
    return 0.5 * (
        1.0 + jax.scipy.special.erf(inner * root_half)
    ) + inner * inverse_root_two_pi * jnp.exp(-0.5 * inner * inner)


def normalize(rows):
    mean = jnp.mean(rows, axis=1, keepdims=True)
    centered = rows - mean
    variance = jnp.mean(centered * centered, axis=1, keepdims=True)
    factor = lax.rsqrt(variance + epsilon)
    return (centered * factor, factor)


def normalize_back(grad_normed, normed, factor):
    return factor * (
        grad_normed
        - jnp.mean(grad_normed, axis=1, keepdims=True)
        - normed * jnp.mean(grad_normed * normed, axis=1, keepdims=True)
    )


def column_sum(rows):
    return jnp.sum(rows.astype(jnp.float32), axis=0)


def dot_rows(left, right):
    return lax.dot_general(
        left, right, (((0,), (0,)), ((), ())), preferred_element_type=jnp.float32
    )


def dot_back(left, right):
    return lax.dot_general(
        left, right, (((1,), (1,)), ((), ())), preferred_element_type=jnp.float32
    )


def place(values, offset, total_length):
    return lax.dynamic_update_slice(jnp.zeros((total_length,), jnp.float32), values, (offset,))


def block_scores(keys, key_valid, query_block):
    raw = jnp.einsum(
        "qhd,khd->hqk", query_block, keys, preferred_element_type=jnp.float32
    ) * HEAD ** (-0.5)
    return jnp.where(key_valid[None, None, :], raw, -1000000000.0)


def attend_forward(keys, values, key_valid, query_block):
    masked = block_scores(keys, key_valid, query_block)
    top = jnp.max(masked, axis=2, keepdims=True)
    expo = jnp.exp(masked - top)
    total = jnp.sum(expo, axis=2, keepdims=True)
    probs = (expo / total).astype(jnp.bfloat16)
    context = jnp.einsum("hqk,khd->qhd", probs, values, preferred_element_type=jnp.float32)
    return (context, top, total)


def attend_backward(keys, values, key_valid, carry, item):
    key_grad, value_grad = carry
    query_block, context_grad_block, top, total = item
    masked = block_scores(keys, key_valid, query_block)
    probs = jnp.exp(masked - top) / total
    probs_low = probs.astype(jnp.bfloat16)
    prob_grad = jnp.einsum(
        "qhd,khd->hqk", context_grad_block, values, preferred_element_type=jnp.float32
    )
    delta = jnp.sum(prob_grad * probs, axis=2, keepdims=True)
    score_grad = (probs * (prob_grad - delta)).astype(jnp.bfloat16)
    factor = HEAD ** (-0.5)
    query_grad = (
        jnp.einsum("hqk,khd->qhd", score_grad, keys, preferred_element_type=jnp.float32) * factor
    )
    key_grad = (
        key_grad
        + jnp.einsum("hqk,qhd->khd", score_grad, query_block, preferred_element_type=jnp.float32)
        * factor
    )
    value_grad = value_grad + jnp.einsum(
        "hqk,qhd->khd", probs_low, context_grad_block, preferred_element_type=jnp.float32
    )
    return ((key_grad, value_grad), query_grad)


def gather_weights(w_query, w_key, w_value, w_output, w_inner, w_outer):
    return (
        lax.all_gather(w_query, FSDP, axis=0, tiled=True),
        lax.all_gather(w_key, FSDP, axis=0, tiled=True),
        lax.all_gather(w_value, FSDP, axis=0, tiled=True),
        lax.all_gather(w_output, FSDP, axis=1, tiled=True),
        lax.all_gather(w_inner, FSDP, axis=0, tiled=True),
        lax.all_gather(w_outer, FSDP, axis=1, tiled=True),
    )


def split_joint(joint_sum, output_sum, inner_sum, outer_sum, head_width):
    return (
        joint_sum[:, :head_width],
        joint_sum[:, head_width : 2 * head_width],
        joint_sum[:, 2 * head_width :],
        output_sum,
        inner_sum,
        outer_sum,
    )


def add_tuples(left, right):
    return tuple((first_item + second_item for first_item, second_item in zip(left, right)))


def local_generic(
    tokens,
    lengths,
    cotangent,
    w_query,
    w_key,
    w_value,
    w_output,
    w_inner,
    w_outer,
    b_query,
    b_value,
    b_output,
    b_inner,
    b_outer,
    gain_first,
    shift_first,
    gain_second,
    shift_second,
):
    tensor_size = lax.axis_size(TENSOR)
    tensor_rank = lax.axis_index(TENSOR)
    micro_count = tokens.shape[0]
    part_rows = tokens.shape[1]
    width = tokens.shape[2]
    seq_rows = part_rows * tensor_size
    head_width = w_query.shape[1]
    inner_width = w_inner.shape[1]
    local_heads = head_width // HEAD
    block_rows = min(512, seq_rows)
    block_count = seq_rows // block_rows
    vector_full = (
        lax.all_gather(b_query, (FSDP, TENSOR), axis=0, tiled=True),
        lax.all_gather(b_value, (FSDP, TENSOR), axis=0, tiled=True),
        lax.all_gather(b_output, (FSDP, TENSOR), axis=0, tiled=True),
        lax.all_gather(b_inner, (FSDP, TENSOR), axis=0, tiled=True),
        lax.all_gather(b_outer, (FSDP, TENSOR), axis=0, tiled=True),
        lax.all_gather(gain_first, (FSDP, TENSOR), axis=0, tiled=True),
        lax.all_gather(shift_first, (FSDP, TENSOR), axis=0, tiled=True),
        lax.all_gather(gain_second, (FSDP, TENSOR), axis=0, tiled=True),
        lax.all_gather(shift_second, (FSDP, TENSOR), axis=0, tiled=True),
    )
    query_bias = lax.dynamic_slice_in_dim(vector_full[0], tensor_rank * head_width, head_width)
    value_bias = lax.dynamic_slice_in_dim(vector_full[1], tensor_rank * head_width, head_width)
    inner_bias = lax.dynamic_slice_in_dim(vector_full[3], tensor_rank * inner_width, inner_width)
    joint_bias = jnp.concatenate([query_bias, jnp.zeros((head_width,), jnp.float32), value_bias])
    grad_query_bias = jnp.zeros((head_width,), jnp.float32)
    grad_value_bias = jnp.zeros((head_width,), jnp.float32)
    grad_inner_bias = jnp.zeros((inner_width,), jnp.float32)
    grad_output_bias = jnp.zeros((width,), jnp.float32)
    grad_outer_bias = jnp.zeros((width,), jnp.float32)
    grad_gain_one = jnp.zeros((width,), jnp.float32)
    grad_shift_one = jnp.zeros((width,), jnp.float32)
    grad_gain_two = jnp.zeros((width,), jnp.float32)
    grad_shift_two = jnp.zeros((width,), jnp.float32)
    local_totals = None
    shard_totals = None
    outputs = []
    input_grads = []
    slot_index = jnp.arange(seq_rows, dtype=jnp.int32)
    part_index = tensor_rank * part_rows + jnp.arange(part_rows, dtype=jnp.int32)
    for micro_index in range(micro_count):
        forward_weights = gather_weights(w_query, w_key, w_value, w_output, w_inner, w_outer)
        joint_w = jnp.concatenate(
            [forward_weights[0], forward_weights[1], forward_weights[2]], axis=1
        )
        output_w = forward_weights[3]
        inner_w = forward_weights[4]
        outer_w = forward_weights[5]
        length = lengths[micro_index]
        key_valid = slot_index < length
        row_valid = (part_index < length).astype(jnp.float32)[:, None]
        own_rows = tokens[micro_index]
        whole = lax.all_gather(own_rows, TENSOR, axis=0, tiled=True)
        joint = (jnp.dot(whole, joint_w, preferred_element_type=jnp.float32) + joint_bias).astype(
            jnp.bfloat16
        )
        query = joint[:, :head_width].reshape(block_count, block_rows, local_heads, HEAD)
        keys = joint[:, head_width : 2 * head_width].reshape(seq_rows, local_heads, HEAD)
        values = joint[:, 2 * head_width :].reshape(seq_rows, local_heads, HEAD)
        context_blocks, tops, totals = lax.map(
            partial(attend_forward, keys, values, key_valid), query
        )
        context_low = context_blocks.reshape(seq_rows, head_width).astype(jnp.bfloat16)
        attended = (
            lax.psum_scatter(
                jnp.dot(context_low, output_w, preferred_element_type=jnp.float32).astype(
                    jnp.bfloat16
                ),
                TENSOR,
                scatter_dimension=0,
                tiled=True,
            ).astype(jnp.float32)
            + vector_full[2]
        )
        normed_first, factor_first = normalize(own_rows.astype(jnp.float32) + attended)
        first = normed_first * vector_full[5] + vector_full[6]
        first_whole = lax.all_gather(first.astype(jnp.bfloat16), TENSOR, axis=0, tiled=True)
        inner = jnp.dot(first_whole, inner_w, preferred_element_type=jnp.float32) + inner_bias
        active = gelu_value(inner).astype(jnp.bfloat16)
        mixed = (
            lax.psum_scatter(
                jnp.dot(active, outer_w, preferred_element_type=jnp.float32).astype(jnp.bfloat16),
                TENSOR,
                scatter_dimension=0,
                tiled=True,
            ).astype(jnp.float32)
            + vector_full[4]
        )
        normed_second, factor_second = normalize(first + mixed)
        outputs.append(
            ((normed_second * vector_full[7] + vector_full[8]) * row_valid).astype(jnp.bfloat16)
        )
        backward_weights = gather_weights(w_query, w_key, w_value, w_output, w_inner, w_outer)
        joint_w = jnp.concatenate(
            [backward_weights[0], backward_weights[1], backward_weights[2]], axis=1
        )
        output_w = backward_weights[3]
        inner_w = backward_weights[4]
        outer_w = backward_weights[5]
        out_grad = cotangent[micro_index].astype(jnp.float32) * row_valid
        grad_gain_two = grad_gain_two + column_sum(out_grad * normed_second)
        grad_shift_two = grad_shift_two + column_sum(out_grad)
        sum_grad = normalize_back(out_grad * vector_full[7], normed_second, factor_second)
        mixed_grad = sum_grad.astype(jnp.bfloat16)
        grad_outer_bias = grad_outer_bias + column_sum(mixed_grad)
        mixed_whole = lax.all_gather(mixed_grad, TENSOR, axis=0, tiled=True)
        outer_sum = dot_rows(active, mixed_whole)
        inner_grad = (dot_back(mixed_whole, outer_w) * gelu_slope(inner)).astype(jnp.bfloat16)
        grad_inner_bias = grad_inner_bias + column_sum(inner_grad)
        inner_sum = dot_rows(first_whole, inner_grad)
        first_grad = sum_grad + lax.psum_scatter(
            dot_back(inner_grad, inner_w).astype(jnp.bfloat16),
            TENSOR,
            scatter_dimension=0,
            tiled=True,
        ).astype(jnp.float32)
        grad_gain_one = grad_gain_one + column_sum(first_grad * normed_first)
        grad_shift_one = grad_shift_one + column_sum(first_grad)
        residual_grad = normalize_back(first_grad * vector_full[5], normed_first, factor_first)
        attended_grad = residual_grad.astype(jnp.bfloat16)
        grad_output_bias = grad_output_bias + column_sum(attended_grad)
        attended_whole = lax.all_gather(attended_grad, TENSOR, axis=0, tiled=True)
        output_sum = dot_rows(context_low, attended_whole)
        context_grad = (
            dot_back(attended_whole, output_w)
            .astype(jnp.bfloat16)
            .reshape(block_count, block_rows, local_heads, HEAD)
        )
        empty = jnp.zeros((seq_rows, local_heads, HEAD), jnp.float32)
        carried, query_grad = lax.scan(
            partial(attend_backward, keys, values, key_valid),
            (empty, empty),
            (query, context_grad, tops, totals),
        )
        joint_grad = jnp.concatenate(
            [
                query_grad.reshape(seq_rows, head_width),
                carried[0].reshape(seq_rows, head_width),
                carried[1].reshape(seq_rows, head_width),
            ],
            axis=1,
        ).astype(jnp.bfloat16)
        grad_query_bias = grad_query_bias + column_sum(joint_grad[:, :head_width])
        grad_value_bias = grad_value_bias + column_sum(joint_grad[:, 2 * head_width :])
        joint_sum = dot_rows(whole, joint_grad)
        input_grads.append(
            residual_grad
            + lax.psum_scatter(
                dot_back(joint_grad, joint_w).astype(jnp.bfloat16),
                TENSOR,
                scatter_dimension=0,
                tiled=True,
            ).astype(jnp.float32)
        )
        batch_sums = (joint_sum, output_sum, inner_sum, outer_sum)
        local_totals = batch_sums if local_totals is None else add_tuples(local_totals, batch_sums)
    pieces = split_joint(
        local_totals[0], local_totals[1], local_totals[2], local_totals[3], head_width
    )
    shard_totals = (
        lax.psum_scatter(pieces[0], FSDP, scatter_dimension=0, tiled=True),
        lax.psum_scatter(pieces[1], FSDP, scatter_dimension=0, tiled=True),
        lax.psum_scatter(pieces[2], FSDP, scatter_dimension=0, tiled=True),
        lax.psum_scatter(pieces[3], FSDP, scatter_dimension=1, tiled=True),
        lax.psum_scatter(pieces[4], FSDP, scatter_dimension=0, tiled=True),
        lax.psum_scatter(pieces[5], FSDP, scatter_dimension=1, tiled=True),
    )
    vector_grads = (
        lax.psum_scatter(
            place(grad_query_bias, tensor_rank * head_width, width),
            (FSDP, TENSOR),
            scatter_dimension=0,
            tiled=True,
        ),
        lax.psum_scatter(
            place(grad_value_bias, tensor_rank * head_width, width),
            (FSDP, TENSOR),
            scatter_dimension=0,
            tiled=True,
        ),
        lax.psum_scatter(grad_output_bias, (FSDP, TENSOR), scatter_dimension=0, tiled=True),
        lax.psum_scatter(
            place(grad_inner_bias, tensor_rank * inner_width, inner_width * tensor_size),
            (FSDP, TENSOR),
            scatter_dimension=0,
            tiled=True,
        ),
        lax.psum_scatter(grad_outer_bias, (FSDP, TENSOR), scatter_dimension=0, tiled=True),
        lax.psum_scatter(grad_gain_one, (FSDP, TENSOR), scatter_dimension=0, tiled=True),
        lax.psum_scatter(grad_shift_one, (FSDP, TENSOR), scatter_dimension=0, tiled=True),
        lax.psum_scatter(grad_gain_two, (FSDP, TENSOR), scatter_dimension=0, tiled=True),
        lax.psum_scatter(grad_shift_two, (FSDP, TENSOR), scatter_dimension=0, tiled=True),
    )
    return (
        jnp.stack(outputs),
        jnp.stack(input_grads),
        shard_totals[0],
        shard_totals[1],
        shard_totals[2],
        shard_totals[3],
        shard_totals[4],
        shard_totals[5],
        vector_grads[0],
        vector_grads[1],
        vector_grads[2],
        vector_grads[3],
        vector_grads[4],
        vector_grads[5],
        vector_grads[6],
        vector_grads[7],
        vector_grads[8],
    )


MESH = pl.DeviceIdType.MESH
WIDTH = 768
HIDDEN = 3072
HALF = WIDTH // 2
KINDS = 3
VECTOR_ROWS = 16
SHORT, LONG = 24, 96
ROW_OUTPUT, ROW_OUTER, ROW_GAIN1, ROW_SHIFT1, ROW_GAIN2, ROW_SHIFT2, ROW_INNER = 4, 5, 6, 7, 8, 9, 10
BF16 = jnp.bfloat16
F32 = jnp.float32


def fits(sizes):
    fsdp = sizes[FSDP]
    return sizes[TENSOR] == 4 and fsdp == WIDTH // LONG


class Place:
    def __init__(self, nz):
        self.f = lax.axis_index(FSDP)
        self.t = lax.axis_index(TENSOR)
        self.nz = nz
        self.z = self.f // 2
        self.x = self.f % 2
        self.y = self.t // 2
        self.c = self.t % 2
        self.core = (self.f, self.t + 1 - 2 * self.c)
        self.along_y = (self.f, self.t + 2 - 4 * self.y)
        self.along_x = (self.f + 1 - 2 * self.x, self.t)

    def z_at(self, step):
        return (self.z + step) % self.nz

    def z_back(self, step):
        return (self.z + self.nz - step) % self.nz

    def along_z(self, step):
        return (self.z_at(step) * 2 + self.x, self.t)

    def in_group(self, step):
        return (self.f, (self.t + step) % 4)


class Net:
    def __init__(self, send_sems, recv_sems):
        self.send_sems = send_sems
        self.recv_sems = recv_sems
        self.count = 0

    def plan(self, source, target, device):
        copy = pltpu.make_async_remote_copy(
            src_ref=source,
            dst_ref=target,
            send_sem=self.send_sems.at[self.count],
            recv_sem=self.recv_sems.at[self.count],
            device_id=device,
            device_id_type=MESH,
        )
        self.count += 1
        return copy

    def keep(self, ref, device):
        return self.plan(ref, ref, device)


def start_all(copies):
    for copy in copies:
        copy.start()


def sent_all(copies):
    for copy in copies:
        copy.wait_send()


def greet(place):
    barrier = pltpu.get_barrier_semaphore()
    peers = [place.in_group(1), place.in_group(2), place.in_group(3), place.along_x]
    peers += [place.along_z(step) for step in range(1, place.nz)]
    for peer in peers:
        pl.semaphore_signal(barrier, inc=1, device_id=peer, device_id_type=MESH)
    pl.semaphore_wait(barrier, len(peers))


def wait_all(copies):
    for copy in copies:
        copy.wait_recv()


def wait_local(copies):
    for copy in copies:
        copy.wait()


def dot(left, right):
    return lax.dot_general(left, right, (((1,), (0,)), ((), ())), preferred_element_type=F32)


def turn(value, shift):
    shift %= value.shape[1]
    return pltpu.roll(value, shift, 1) if shift else value


class Layer:
    def __init__(self, refs, length):
        (
            self.w, self.rows, self.back, self.rows_turned, self.joint, self.probs, self.context, self.acc,
            self.normed, self.factor, self.first_low, self.first_turned, self.active, self.slope, self.grad_low,
            self.grad_turned, self.out, self.vec, self.sums,
        ) = refs
        self.length = length
        self.seq = self.rows.shape[0]
        self.block = 128

    def weight(self, kind, t):
        return self.w[kind, t // 2, t % 2].reshape(WIDTH, WIDTH)

    def output_weight(self, t):
        return self.w[0, t // 2, t % 2, :, :, :, 512:768].reshape(WIDTH, 256)

    def store_grad(self, kind, t, value):
        nz = self.w.shape[3]
        self.w[kind, t // 2, t % 2] = value.astype(BF16).reshape(nz, 2, WIDTH // (2 * nz), WIDTH)

    def row(self, index):
        return self.vec[pl.ds(index, 1), :]

    def blocks(self, body):
        def step(i, carry):
            body(pl.ds(pl.multiple_of(i * self.block, self.block), self.block), i)
            return carry

        lax.fori_loop(0, self.seq // self.block, step, 0)

    def row_valid(self, i):
        index = lax.broadcasted_iota(jnp.int32, (self.block, 1), 0) + i * self.block
        return (index < self.length).astype(F32)

    def lanes(self, low, high, width):
        lane = lax.broadcasted_iota(jnp.int32, (1, width), 1)
        return (lane >= low) & (lane < high)

    def pick(self, value, low, high):
        return jnp.where(self.lanes(low, high, value.shape[1]), value, jnp.zeros_like(value))

    def head_query(self, t, h):
        return self.joint[t, :, 0:128] if h < 2 else self.joint[t, :, 384:512]

    def head_key(self, t, h):
        return self.joint[t, :, 128:256] if h < 2 else self.joint[t, :, 640:768]

    def head_side(self, value, h):
        return self.pick(value, 0, 64) if h == 0 else self.pick(value, 64, 128)

    def head_value(self, t, h):
        return self.pick(self.joint[t, :, 256:512], h * 64, h * 64 + 64)

    def unpack(self, v):
        nz = v.shape[2]
        short = jnp.zeros((8, WIDTH), F32)
        inner = [jnp.zeros((1, WIDTH), F32) for _ in range(4)]
        for f in range(2 * nz):
            for t in range(4):
                rank = f * 4 + t
                block = v[t // 2, t % 2, f // 2, f % 2]
                wide = jnp.concatenate([self.pick(block, 0, SHORT), jnp.zeros((8, WIDTH - 128), F32)], axis=1)
                short += turn(wide, rank * SHORT)
                wide = jnp.concatenate([self.pick(block[0:1], 32, 128), jnp.zeros((1, WIDTH - 128), F32)], axis=1)
                inner[rank * LONG // WIDTH] += turn(wide, rank * LONG % WIDTH - 32)
        for t in range(4):
            query = self.pick(turn(short[0:1], -192 * t), 0, 128) + self.pick(turn(short[0:1], 320 - 192 * t), 448, 512)
            self.vec[t:t + 1] = query + self.pick(turn(short[1:2], 256 - 192 * t), 256, 448)
            self.vec[ROW_INNER + t:ROW_INNER + t + 1] = inner[t]
        self.vec[ROW_OUTPUT:ROW_INNER] = short[2:8]

    def pack(self, parts):
        nz = parts.shape[2]
        query, value = jnp.zeros((1, WIDTH), F32), jnp.zeros((1, WIDTH), F32)
        for t in range(4):
            row = self.sums[t:t + 1]
            query += turn(self.pick(row, 0, 128), 192 * t) + turn(self.pick(row, 448, 512), 192 * t - 320)
            value += turn(self.pick(row, 256, 448), 192 * t - 256)
        short = jnp.concatenate([query, value, self.sums[ROW_OUTPUT:ROW_INNER]], axis=0)
        top = lax.broadcasted_iota(jnp.int32, (8, 1), 0) == 0
        for f in range(2 * nz):
            for t in range(4):
                rank = f * 4 + t
                block = self.pick(turn(short, -rank * SHORT)[:, 0:128], 0, SHORT)
                index = ROW_INNER + rank * LONG // WIDTH
                inner = turn(self.sums[index:index + 1], 32 - rank * LONG % WIDTH)[:, 0:128]
                inner = jnp.broadcast_to(self.pick(inner, 32, 128), (8, 128))
                parts[t // 2, t % 2, f // 2, f % 2] = block + jnp.where(top, inner, 0.0)

    def project(self, t):
        self.joint[t] = (dot(self.rows[...], self.weight(0, t)) + self.row(t)).astype(BF16)

    def attend(self, t):
        key_valid = lax.broadcasted_iota(jnp.int32, (1, self.seq), 1) < self.length
        context = None
        for h in range(3):
            raw = dot_back(self.head_query(t, h), self.head_side(self.head_key(t, h), h))
            masked = jnp.where(key_valid, raw * HEAD ** -0.5, -1e9)
            expo = jnp.exp(masked - jnp.max(masked, axis=1, keepdims=True))
            probs = (expo * (1.0 / jnp.sum(expo, axis=1, keepdims=True))).astype(BF16)
            self.probs[t * 3 + h] = probs
            part = dot(probs, self.head_value(t, h))
            context = part if context is None else context + part
        low = context.astype(BF16)
        self.context[t] = low
        self.acc[...] += dot_back(low, self.output_weight(t))

    def start(self):
        def body(rows, i):
            self.acc[rows] = self.rows[rows].astype(F32) + self.row(ROW_OUTPUT)

        self.blocks(body)

    def norm_first(self):
        def body(rows, i):
            normed, factor = normalize(self.acc[rows])
            self.normed[rows] = normed
            self.factor[rows] = jnp.broadcast_to(factor, (self.block, 128))
            first = normed * self.row(ROW_GAIN1) + self.row(ROW_SHIFT1)
            self.first_low[rows] = first.astype(BF16)
            self.acc[rows] = first + self.row(ROW_OUTER)

        self.blocks(body)

    def feed_inner(self, t):
        inner = dot(self.first_low[...], self.weight(1, t)) + self.row(ROW_INNER + t)
        gate = 1.0 + lax.erf(inner * root_half)
        self.active[t] = (0.5 * inner * gate).astype(BF16)
        self.slope[t] = (0.5 * gate + inner * inverse_root_two_pi * jnp.exp(-0.5 * inner * inner)).astype(BF16)

    def feed_outer(self, t):
        self.acc[...] += dot_back(self.active[t], self.weight(2, t))

    def clear_sums(self):
        self.sums[...] = jnp.zeros_like(self.sums)

    def add_sum(self, index, value):
        self.sums[pl.ds(index, 1), :] += jnp.sum(value, axis=0, keepdims=True)

    def norm_second(self):
        def body(rows, i):
            normed, factor = normalize(self.acc[rows])
            valid = self.row_valid(i)
            gain = self.row(ROW_GAIN2)
            self.out[rows] = ((normed * gain + self.row(ROW_SHIFT2)) * valid).astype(BF16)
            out_grad = self.back[rows].astype(F32) * valid
            self.add_sum(ROW_GAIN2, out_grad * normed)
            self.add_sum(ROW_SHIFT2, out_grad)
            sum_grad = normalize_back(out_grad * gain, normed, factor)
            self.acc[rows] = sum_grad
            low = sum_grad.astype(BF16)
            self.grad_low[rows] = low
            self.add_sum(ROW_OUTER, low.astype(F32))

        self.blocks(body)
        self.grad_turned[...] = self.grad_low[...].T

    def outer_back(self, t):
        grad = (dot(self.grad_low[...], self.weight(2, t)) * self.slope[t].astype(F32)).astype(BF16)
        self.slope[t] = grad
        self.add_sum(ROW_INNER + t, grad.astype(F32))
        self.store_grad(2, t, dot(self.grad_turned[...], self.active[t]))

    def inner_back(self, t):
        grad = self.slope[t]
        self.acc[...] += dot_back(grad, self.weight(1, t))
        self.store_grad(1, t, dot(self.first_turned[...], grad))

    def norm_first_back(self):
        def body(rows, i):
            grad = self.acc[rows]
            normed = self.normed[rows]
            self.add_sum(ROW_GAIN1, grad * normed)
            self.add_sum(ROW_SHIFT1, grad)
            residual = normalize_back(grad * self.row(ROW_GAIN1), normed, self.factor[rows][:, 0:1])
            self.acc[rows] = residual
            low = residual.astype(BF16)
            self.grad_low[rows] = low
            self.add_sum(ROW_OUTPUT, low.astype(F32))

        self.blocks(body)
        self.grad_turned[...] = self.grad_low[...].T

    def attend_back(self, t):
        context_grad = self.pick(dot(self.grad_low[...], self.output_weight(t)), 0, 192).astype(BF16)
        query_grads, key_grads, value_grad = [], [], None
        for h in range(3):
            probs = self.probs[t * 3 + h]
            prob_grad = dot_back(context_grad, self.head_value(t, h))
            wide = probs.astype(F32)
            delta = jnp.sum(wide * prob_grad, axis=1, keepdims=True)
            score_grad = (wide * (prob_grad - delta)).astype(BF16)
            query_grads.append(dot(score_grad, self.head_side(self.head_key(t, h), h)) * HEAD ** -0.5)
            key_grads.append(dot_rows(score_grad, self.head_side(self.head_query(t, h), h)) * HEAD ** -0.5)
            part = dot_rows(probs, self.pick(context_grad, h * 64, h * 64 + 64))
            value_grad = part if value_grad is None else value_grad + part
        self.joint[t, :, 0:128] = (query_grads[0] + query_grads[1]).astype(BF16)
        self.joint[t, :, 128:256] = (key_grads[0] + key_grads[1]).astype(BF16)
        self.joint[t, :, 256:384] = value_grad[:, 0:128].astype(BF16)
        self.joint[t, :, 384:512] = (value_grad[:, 128:256] + query_grads[2]).astype(BF16)
        self.joint[t, :, 512:640] = jnp.zeros((self.seq, 128), BF16)
        self.joint[t, :, 640:768] = key_grads[2].astype(BF16)

    def joint_back(self, t):
        joint = self.joint[t]
        self.sums[pl.ds(t, 1), :] = jnp.sum(joint.astype(F32), axis=0, keepdims=True)
        self.acc[...] += dot_back(joint, self.weight(0, t))
        nz = self.w.shape[3]
        shape = (nz, 2, WIDTH // (2 * nz), -1)
        main = dot(self.rows_turned[...], joint[:, 0:512])
        side = dot(self.rows_turned[...], joint[:, 512:768]) + dot(self.grad_turned[...], self.context[t])
        self.w[0, t // 2, t % 2, :, :, :, 0:512] = main.astype(BF16).reshape(shape[:3] + (512,))
        self.w[0, t // 2, t % 2, :, :, :, 512:768] = side.astype(BF16).reshape(shape[:3] + (256,))

    def finish(self):
        def body(rows, i):
            self.back[rows] = self.acc[rows].astype(BF16)

        self.blocks(body)


def each(count, body):
    def step(i, carry):
        body(i)
        return carry

    lax.fori_loop(0, count, step, 0)


BUFFER_COUNT = 19


def buffer_shapes(nz, seq):
    part = WIDTH // (2 * nz)
    low, wide = (seq, WIDTH), (WIDTH, seq)
    shapes = [
        ((KINDS, 2, 2, nz, 2, part, WIDTH), BF16),
        (low, BF16),
        (low, BF16),
        (wide, BF16),
        ((4, seq, WIDTH), BF16),
        ((12, seq, seq), BF16),
        ((4, seq, 256), BF16),
        (low, F32),
        (low, F32),
        ((seq, 128), F32),
        (low, BF16),
        (wide, BF16),
        ((4, seq, WIDTH), BF16),
        ((4, seq, WIDTH), BF16),
        (low, BF16),
        (wide, BF16),
        (low, BF16),
        ((VECTOR_ROWS, WIDTH), F32),
        ((VECTOR_ROWS, WIDTH), F32),
    ]
    return [pltpu.VMEM(*shape) for shape in shapes]


def landing_shapes(nz):
    part = WIDTH // (2 * nz)
    shapes = [
        (KINDS, 2, nz, 2, part, WIDTH),
        (KINDS, nz, 2, part, HALF),
        (KINDS, nz, part, HALF),
        (KINDS, nz - 1, part, HALF),
        (KINDS, 2, nz, part, HALF),
        (KINDS, nz - 1, 2, part, HALF),
        (KINDS, 3, part, HALF),
    ]
    return [pltpu.VMEM(shape, BF16) for shape in shapes]


class Gather:
    def __init__(self, net, place, own, w, k, own_v=None, v=None):
        p = place
        a, b = pl.ds(0, HALF), pl.ds(HALF, HALF)
        own_a, own_b = own.at[:, a], own.at[:, b]
        mine_a, mine_b = (w.at[k, p.y, p.c, p.z, p.x, :, cols] for cols in (a, b))
        steps = range(1, p.nz)
        backs = range(p.nz)
        self.az = [net.plan(own_a, mine_a, p.along_z(step)) for step in steps]
        self.by = [net.plan(own_b, mine_b, p.along_y)]
        self.ax = [net.plan(own_a, mine_a, p.along_x)]
        self.ax += [net.keep(w.at[k, p.y, p.c, p.z_back(step), p.x, :, a], p.along_x) for step in steps]
        self.ay = [net.plan(own_a, mine_a, p.along_y)]
        self.ay += [net.keep(w.at[k, p.y, p.c, p.z_back(step), p.x, :, a], p.along_y) for step in steps]
        self.ay += [net.keep(w.at[k, p.y, p.c, p.z_back(step), 1 - p.x, :, a], p.along_y) for step in backs]
        self.ac = [net.keep(w.at[k, y, p.c, :, :, :, a], p.core) for y in (p.y, 1 - p.y)]
        self.bz = [net.keep(w.at[k, :, p.c, p.z, p.x, :, b], p.along_z(step)) for step in steps]
        self.bx = [net.keep(w.at[k, :, p.c, p.z_back(step), p.x, :, b], p.along_x) for step in backs]
        self.bc = [net.keep(w.at[k, :, p.c, :, x, :, b], p.core) for x in (p.x, 1 - p.x)]
        self.vz, self.vx, self.vy, self.vc = [], [], [], []
        if v is not None:
            mine = v.at[p.y, p.c, p.z, p.x]
            self.vz = [net.plan(own_v, mine, p.along_z(step)) for step in steps]
            self.vx = [net.plan(own_v, mine, p.along_x)]
            self.vx += [net.keep(v.at[p.y, p.c, p.z_back(step), p.x], p.along_x) for step in steps]
            self.vy = [net.keep(v.at[p.y, p.c], p.along_y)]
            self.vc = [net.keep(v.at[y, p.c], p.core) for y in (p.y, 1 - p.y)]

    def first(self):
        start_all(self.by + self.vz + self.vx[:1] + self.az)
        self.ax[0].start()
        self.ay[0].start()

    def b_y(self):
        wait_all(self.by)
        start_all(self.bz)
        self.bx[0].start()

    def a_z(self, i):
        if self.vz:
            self.vz[i].wait_recv()
            self.vx[i + 1].start()
        self.az[i].wait_recv()
        self.ax[i + 1].start()
        self.ay[i + 1].start()

    def a_x(self, i):
        self.ax[i].wait_recv()
        self.ay[len(self.ax) + i].start()

    def a_own(self):
        wait_all(self.vx)
        start_all(self.vy + self.vc[:1] + self.ac[:1])

    def a_y(self):
        wait_all(self.vy + self.ay)
        start_all(self.vc[1:] + self.ac[1:])

    def b_z(self, i):
        self.bz[i].wait_recv()
        self.bx[i + 1].start()

    def b_own(self):
        self.bc[0].start()

    def b_x(self):
        wait_all(self.bx)
        self.bc[1].start()

    def done(self):
        wait_all(self.ac + self.bc + self.vc)

    def sent(self):
        sent_all(self.az + self.ax + self.ay + self.ac + self.by + self.bz + self.bx + self.bc)
        sent_all(self.vz + self.vx + self.vy + self.vc)


class Reduce:
    def __init__(self, net, place, w, landings, result, k):
        p = self.place = place
        self.core, self.ya, self.xa, self.za, self.xb, self.zb, self.yb = (ref.at[k] for ref in landings)
        self.w, self.result = w.at[k], result.at[k]
        self.a, self.b = pl.ds(0, HALF), pl.ds(HALF, HALF)
        self.ys = ys = (1 - p.y, p.y)
        self.xs = xs = (1 - p.x, p.x)
        self.zs = zs = [p.z_at((step + 1) % p.nz) for step in range(p.nz)]
        self.c = [net.plan(self.w.at[y, 1 - p.c], self.core.at[y], p.core) for y in ys]
        self.ay = [
            [net.plan(self.core.at[ys[0], z, x, :, self.a], self.ya.at[z, x], p.along_y) for z in zs] for x in xs
        ]
        self.bx = [
            [net.plan(self.core.at[y, z, xs[0], :, self.b], self.xb.at[y, z], p.along_x) for z in zs] for y in ys
        ]
        self.bz = [
            [net.plan(self.xb.at[y, zs[i]], self.zb.at[i, y], p.along_z(i + 1)) for i in range(p.nz - 1)] for y in ys
        ]
        self.by = [net.plan(self.yb.at[ys[0]], self.yb.at[2], p.along_y)]
        self.ax = [net.plan(self.ya.at[z, xs[0]], self.xa.at[z], p.along_x) for z in zs]
        self.az = [net.plan(self.xa.at[zs[i]], self.za.at[i], p.along_z(i + 1)) for i in range(p.nz - 1)]

    def add(self, target, source):
        target[...] = (target[...].astype(F32) + source[...].astype(F32)).astype(BF16)

    def to_core(self, half):
        self.c[half].start()

    def core_half(self, half):
        y = self.ys[half]
        self.c[half].wait_recv()

        def body(z):
            self.add(self.core.at[y, z], self.w.at[y, self.place.c, z])

        each(self.place.nz, body)
        start_all(self.bx[half])
        if half == 0:
            start_all(self.ay[0] + self.ay[1])

    def a_y(self, side, i):
        self.ay[side][i].wait_recv()
        z, x = self.zs[i], self.xs[side]
        self.add(self.ya.at[z, x], self.core.at[self.ys[1], z, x, :, self.a])
        if side == 0:
            self.ax[i].start()

    def b_x(self, half, i):
        y, z = self.ys[half], self.zs[i]
        self.bx[half][i].wait_recv()
        self.add(self.xb.at[y, z], self.core.at[y, z, self.xs[1], :, self.b])
        if i < self.place.nz - 1:
            self.bz[half][i].start()

    def a_x(self, i):
        z = self.zs[i]
        self.ax[i].wait_recv()
        self.add(self.xa.at[z], self.ya.at[z, self.xs[1]])
        if i < self.place.nz - 1:
            self.az[i].start()

    def b_z(self, half):
        y = self.ys[half]
        wait_all(self.bz[half])
        total = self.xb[y, self.place.z].astype(F32)
        for i in range(self.place.nz - 1):
            total += self.zb[i, y].astype(F32)
        self.yb[y] = total.astype(BF16)
        if half == 0:
            start_all(self.by)

    def a_z(self):
        wait_all(self.az)
        total = self.xa[self.place.z].astype(F32)
        for i in range(self.place.nz - 1):
            total += self.za[i].astype(F32)
        self.result[:, self.a] = total

    def b_y(self):
        wait_all(self.by)
        self.result[:, self.b] = self.yb[self.ys[1]].astype(F32) + self.yb[2].astype(F32)

    def sent(self):
        for copies in (self.c, *self.ay, *self.bx, *self.bz, self.by, self.ax, self.az):
            sent_all(copies)


class Back:
    def __init__(self, net, place, parts, landings, result):
        p = self.place = place
        self.parts, self.result = parts, result
        self.core, self.side, self.pair, self.line = landings
        self.c = net.plan(parts.at[:, 1 - p.c], self.core, p.core)
        self.y = net.plan(self.core.at[1 - p.y], self.side, p.along_y)
        self.x = net.plan(self.side.at[:, 1 - p.x], self.pair, p.along_x)
        self.z = [
            net.plan(self.pair.at[p.z_at(step)], self.line.at[step - 1], p.along_z(step)) for step in range(1, p.nz)
        ]

    def first(self):
        self.c.start()

    def core_done(self):
        self.c.wait_recv()
        self.core[...] += self.parts[:, self.place.c]
        self.y.start()

    def y_done(self):
        self.y.wait_recv()
        self.side[...] += self.core[self.place.y]
        self.x.start()

    def x_done(self):
        self.x.wait_recv()
        self.pair[...] += self.side[:, self.place.x]
        start_all(self.z)

    def z_done(self):
        wait_all(self.z)
        total = self.pair[self.place.z]
        for i in range(self.place.nz - 1):
            total += self.line[i]
        self.result[...] = total

    def sent(self):
        sent_all([self.c, self.y, self.x] + self.z)


def ticks(i, table):
    for when, actions in table.items():
        @pl.when(i == when)
        def _(actions=actions):
            for action, *given in actions:
                action(*given)


def layer_kernel(nz, *refs):
    tokens, lengths, cotangent, w_query, w_key, w_value, w_output, w_inner, w_outer = refs[:9]
    short_in, long_in = refs[9:12] + refs[13:18], refs[12]
    result, outs, backs, totals = refs[18:22]
    rest = list(refs[22:])
    buffers, rest = rest[:BUFFER_COUNT], rest[BUFFER_COUNT:]
    landings, back_landings = rest[:7], rest[7:11]
    v, parts, vec_in, raw_query, raw_key, raw_value, raw_output, own_joint = rest[11:19]
    send_sems, recv_sems, local_sems = rest[19:]
    place = Place(nz)
    net = Net(send_sems, recv_sems)
    t = place.t
    quarter = tokens.shape[1]
    layer = Layer(buffers, lengths[t])
    joint = Gather(net, place, own_joint, layer.w, 0, vec_in, v)
    inner = Gather(net, place, w_inner, layer.w, 1)
    outer = Gather(net, place, w_outer, layer.w, 2)
    sums = Back(net, place, parts, back_landings, totals)
    to_joint, to_inner, to_outer = [Reduce(net, place, layer.w, landings, result, k) for k in range(KINDS)]

    def quarter_of(ref, index):
        return ref.at[pl.ds(pl.multiple_of(index * quarter, quarter), quarter)]

    def swap_in(source, target):
        return [
            net.plan(source.at[(t + step) % 4], quarter_of(target, t), place.in_group(step)) for step in (2, 1, 3)
        ]

    def swap_out(source, target):
        return [
            net.plan(quarter_of(source, (t + step) % 4), target.at[t], place.in_group(step)) for step in (2, 1, 3)
        ]

    token_in = swap_in(tokens, layer.rows)
    back_in = swap_in(cotangent, layer.back)
    out_out = swap_out(layer.out, outs)
    back_out = swap_out(layer.back, backs)
    pairs = [
        (tokens.at[t], quarter_of(layer.rows, t)),
        (cotangent.at[t], quarter_of(layer.back, t)),
        *[
            (own, layer.w.at[k, place.y, place.c, place.z, place.x])
            for k, own in enumerate((own_joint, w_inner, w_outer))
        ],
        (vec_in, v.at[place.y, place.c, place.z, place.x]),
        (quarter_of(layer.out, t), outs.at[t]),
        (quarter_of(layer.back, t), backs.at[t]),
        (w_query, raw_query),
        (w_key, raw_key),
        (w_value, raw_value),
        (w_output, raw_output),
    ]
    local = [pltpu.make_async_copy(*pair, local_sems.at[i]) for i, pair in enumerate(pairs)]

    def pack_vectors():
        vec_in[...] = jnp.zeros((8, 128), F32)
        for i, ref in enumerate(short_in):
            vec_in[i:i + 1, 0:SHORT] = ref[...].reshape(1, SHORT)
        vec_in[0:1, 32:128] = long_in[...].reshape(1, LONG)

    def pack_own():
        own_joint[...] = pack_joint(raw_query[...], raw_key[...], raw_value[...], raw_output[...].T)

    def order(i):
        return (1 - place.y + i // 2) % 2 * 2 + (1 - place.c + i) % 2

    start_all(local[8:])
    pack_vectors()
    greet(place)
    wait_local(local[8:12])
    pack_own()
    joint.first()
    start_all(local[0:6])
    wait_local(local[0:6])
    start_all(token_in)
    joint.b_y()
    joint.a_x(0)
    inner.first()
    joint.a_z(0)
    inner.a_x(0)
    joint.a_z(1)
    joint.a_x(1)
    joint.a_z(2)
    wait_all(token_in)
    joint.a_x(2)
    joint.a_x(3)
    joint.a_own()
    inner.b_y()
    outer.first()
    joint.b_z(0)
    outer.a_x(0)
    joint.b_z(1)
    joint.b_z(2)
    joint.b_own()
    joint.a_y()
    outer.b_y()
    inner.a_z(0)
    joint.b_x()
    inner.a_z(1)
    joint.done()
    layer.unpack(v)
    layer.start()
    layer.rows_turned[...] = layer.rows[...].T
    layer.clear_sums()
    def project(i):
        layer.project(i)
        ticks(i, {
            0: [(inner.a_z, 2)],
            1: [(inner.a_x, 1)],
        })

    each(4, project)
    inner.a_x(2)
    def attend(i):
        layer.attend(i)
        ticks(i, {
            0: [(inner.a_x, 3), (inner.a_own,)],
            1: [(inner.b_z, 0)],
            2: [(inner.a_y,)],
        })

    each(4, attend)
    inner.b_z(1)
    layer.norm_first()
    layer.first_turned[...] = layer.first_low[...].T
    inner.b_z(2)
    inner.b_own()
    outer.a_z(0)
    outer.a_z(1)
    inner.b_x()
    outer.a_z(2)
    outer.a_x(1)
    inner.done()
    def feed_inner(i):
        layer.feed_inner(i)
        ticks(i, {
            0: [(outer.a_x, 2), (outer.b_z, 0)],
            1: [(outer.a_x, 3), (outer.a_own,), (start_all, back_in)],
            2: [(outer.b_z, 1)],
        })

    each(4, feed_inner)
    outer.a_y()
    outer.b_z(2)
    outer.b_own()
    outer.b_x()
    outer.done()
    def feed_outer(i):
        layer.feed_outer(i)

    each(4, feed_outer)
    wait_all(back_in)
    layer.norm_second()
    start_all(out_out)
    local[6].start()
    outer.sent()
    def outer_back(i):
        layer.outer_back(order(i))
        ticks(i, {
            0: [(to_outer.to_core, 0)],
            2: [(to_outer.to_core, 1), (to_outer.core_half, 0)],
        })

    each(4, outer_back)
    inner.sent()
    def inner_back(i):
        layer.inner_back(order(i))
        ticks(i, {
            0: [(to_inner.to_core, 0), (to_outer.core_half, 1), (to_outer.b_x, 0, 0)],
            1: [(to_outer.b_x, 0, 1), (to_outer.a_y, 0, 0)],
            2: [(to_inner.to_core, 1), (to_inner.core_half, 0), (to_outer.b_x, 0, 2), (to_outer.a_y, 0, 1), (to_outer.b_x, 0, 3)],
        })

    each(4, inner_back)
    to_outer.a_y(0, 2)
    to_outer.b_x(1, 0)
    layer.norm_first_back()
    to_inner.core_half(1)
    to_outer.a_y(0, 3)
    to_outer.b_x(1, 1)
    to_outer.a_y(1, 0)
    joint.sent()
    def attend_back(i):
        layer.attend_back(order(i))
        ticks(i, {
            0: [(to_outer.b_x, 1, 2), (to_outer.a_y, 1, 1), (to_outer.b_z, 0), (to_outer.b_x, 1, 3), (to_outer.a_y, 1, 2), (to_outer.a_x, 0)],
            1: [(to_inner.a_y, 0, 0), (to_inner.b_x, 0, 1), (to_inner.a_y, 0, 1), (to_inner.b_x, 0, 2)],
            2: [(to_outer.a_x, 1), (to_outer.a_x, 2), (to_inner.a_y, 0, 3), (to_inner.a_y, 1, 0)],
            3: [(to_inner.a_y, 1, 2), (to_inner.b_x, 1, 1), (to_inner.b_z, 0), (to_inner.a_y, 1, 3), (to_inner.b_x, 1, 2)],
        })
        layer.joint_back(order(i))
        ticks(i, {
            0: [(to_joint.to_core, 0), (to_outer.a_y, 1, 3), (to_inner.b_x, 0, 0)],
            1: [(to_joint.core_half, 0), (to_outer.b_z, 1), (to_inner.a_y, 0, 2), (to_inner.b_x, 0, 3)],
            2: [(to_joint.to_core, 1), (to_inner.a_y, 1, 1), (to_inner.b_x, 1, 0)],
        })

    each(4, attend_back)
    to_joint.core_half(1)
    to_outer.b_y()
    to_outer.a_x(3)
    to_inner.b_x(1, 3)
    to_joint.a_y(0, 0)
    layer.pack(parts)
    sums.first()
    to_joint.a_y(0, 1)
    layer.finish()
    start_all(back_out)
    local[7].start()
    to_inner.a_x(0)
    sums.core_done()
    to_outer.a_z()
    to_outer.sent()
    to_joint.a_y(0, 2)
    to_inner.a_x(1)
    to_joint.a_y(0, 3)
    to_joint.b_x(0, 0)
    to_joint.a_y(1, 0)
    to_joint.b_x(0, 1)
    to_joint.a_y(1, 1)
    to_joint.b_x(0, 2)
    to_joint.a_y(1, 2)
    to_joint.b_x(0, 3)
    to_inner.b_z(1)
    to_joint.a_y(1, 3)
    to_inner.a_x(2)
    to_inner.b_y()
    to_inner.a_x(3)
    to_joint.b_x(1, 0)
    to_joint.b_x(1, 1)
    to_joint.b_x(1, 2)
    to_joint.b_x(1, 3)
    to_joint.a_x(0)
    sums.y_done()
    to_joint.a_x(1)
    to_joint.b_z(0)
    to_joint.a_x(2)
    to_inner.a_z()
    to_inner.sent()
    to_joint.a_x(3)
    sums.x_done()
    to_joint.b_z(1)
    to_joint.b_y()
    to_joint.a_z()
    to_joint.sent()
    sums.z_done()
    sums.sent()
    wait_local(local[6:8])
    wait_all(out_out + back_out)
    sent_all(token_in + back_in + out_out + back_out)


VMEM_SPEC = pl.BlockSpec(memory_space=pltpu.VMEM)
ANY_SPEC = pl.BlockSpec(memory_space=pl.ANY)
LIMIT = 67043328


def whole_layer(tokens, *rest):
    nz = lax.axis_size(FSDP) // 2
    part = WIDTH // (2 * nz)
    seq = tokens.shape[1] * 4
    count = 208
    return pl.pallas_call(
        partial(layer_kernel, nz),
        out_shape=(
            jax.ShapeDtypeStruct((KINDS, part, WIDTH), F32),
            jax.ShapeDtypeStruct(tokens.shape, BF16),
            jax.ShapeDtypeStruct(tokens.shape, BF16),
            jax.ShapeDtypeStruct((8, 128), F32),
        ),
        in_specs=[ANY_SPEC, pl.BlockSpec(memory_space=pltpu.SMEM)] + [ANY_SPEC] * 7 + [VMEM_SPEC] * 9,
        out_specs=(VMEM_SPEC, ANY_SPEC, ANY_SPEC, VMEM_SPEC),
        scratch_shapes=buffer_shapes(nz, seq) + landing_shapes(nz) + [
            pltpu.VMEM((2, nz, 2, 8, 128), F32),
            pltpu.VMEM((nz, 2, 8, 128), F32),
            pltpu.VMEM((nz, 8, 128), F32),
            pltpu.VMEM((nz - 1, 8, 128), F32),
            pltpu.VMEM((2, 2, nz, 2, 8, 128), F32),
            pltpu.VMEM((2, 2, nz, 2, 8, 128), F32),
            pltpu.VMEM((8, 128), F32),
            *[pltpu.VMEM((part, WIDTH // 4), BF16)] * 3,
            pltpu.VMEM((WIDTH // 4, part), BF16),
            pltpu.VMEM((part, WIDTH), BF16),
            pltpu.SemaphoreType.DMA((count,)),
            pltpu.SemaphoreType.DMA((count,)),
            pltpu.SemaphoreType.DMA((16,)),
        ],
        compiler_params=pltpu.CompilerParams(collective_id=0, has_side_effects=True, vmem_limit_bytes=LIMIT),
        name="whole_layer",
    )(tokens, *rest)


def finish_kernel(sums, outs, backs, totals, *results):
    output, input_grad, g_query, g_key, g_value, g_output, g_inner, g_outer = results[:8]
    output[...] = outs[...]
    input_grad[...] = backs[...].astype(F32)
    g_query[...], g_key[...], g_value[...], g_turned = unpack_joint(sums[0])
    g_output[...] = g_turned.T
    g_inner[...] = sums[1]
    g_outer[...] = sums[2]
    short = [0, 1, 2, None, 3, 4, 5, 6, 7]
    for row, ref in zip(short, results[8:]):
        ref[...] = (totals[0:1, 32:128] if row is None else totals[row:row + 1, 0:SHORT]).reshape(ref.shape)


def finish_layer(sums, outs, backs, totals):
    part = sums.shape[1]
    share = WIDTH // 4
    shapes = [outs.shape, backs.shape] + [(part, share)] * 3 + [(share, part), (part, WIDTH), (part, WIDTH)]
    shapes += [(SHORT,)] * 3 + [(LONG,)] + [(SHORT,)] * 5
    return pl.pallas_call(
        finish_kernel,
        out_shape=[jax.ShapeDtypeStruct(shape, F32 if i else BF16) for i, shape in enumerate(shapes)],
        in_specs=[VMEM_SPEC] * 4,
        out_specs=[VMEM_SPEC] * len(shapes),
        compiler_params=pltpu.CompilerParams(vmem_limit_bytes=LIMIT // 2),
        name="finish_layer",
    )(sums, outs, backs, totals)


def pack_joint(q, k, v, o):
    return jnp.concatenate(
        [q[:, :128], k[:, :128], v[:, :128], v[:, 128:], q[:, 128:], o[:, :128], o[:, 128:], k[:, 128:]], axis=1
    )


def unpack_joint(joint):
    q = jnp.concatenate([joint[:, 0:128], joint[:, 448:512]], axis=1)
    k = jnp.concatenate([joint[:, 128:256], joint[:, 704:768]], axis=1)
    return q, k, joint[:, 256:448], joint[:, 512:704]


def local_fast(*given):
    given = given[:8] + (given[8].T,) + given[9:]
    results = finish_layer(*whole_layer(*given))
    return (*results[:7], results[7].T, *results[8:])


def solution(mesh):
    placed = (
        P(FSDP, TENSOR, None),
        P(FSDP),
        P(FSDP, TENSOR, None),
        P(FSDP, TENSOR),
        P(FSDP, TENSOR),
        P(FSDP, TENSOR),
        P(TENSOR, FSDP),
        P(FSDP, TENSOR),
        P(TENSOR, FSDP),
        P((FSDP, TENSOR)),
        P((FSDP, TENSOR)),
        P((FSDP, TENSOR)),
        P((FSDP, TENSOR)),
        P((FSDP, TENSOR)),
        P((FSDP, TENSOR)),
        P((FSDP, TENSOR)),
        P((FSDP, TENSOR)),
        P((FSDP, TENSOR)),
    )
    return jax.shard_map(
        local_fast if fits(mesh.shape) else local_generic,
        mesh=mesh,
        in_specs=placed,
        out_specs=(
            P(FSDP, TENSOR, None),
            P(FSDP, TENSOR, None),
            P(FSDP, TENSOR),
            P(FSDP, TENSOR),
            P(FSDP, TENSOR),
            P(TENSOR, FSDP),
            P(FSDP, TENSOR),
            P(TENSOR, FSDP),
            P((FSDP, TENSOR)),
            P((FSDP, TENSOR)),
            P((FSDP, TENSOR)),
            P((FSDP, TENSOR)),
            P((FSDP, TENSOR)),
            P((FSDP, TENSOR)),
            P((FSDP, TENSOR)),
            P((FSDP, TENSOR)),
            P((FSDP, TENSOR)),
        ),
        check_vma=False,
    )
```

```python
from functools import partial

import jax
import jax.numpy as jnp
from jax import lax
from jax.experimental import pallas as pl
from jax.experimental.pallas import tpu as pltpu
from jax.sharding import PartitionSpec as P

FSDP, TENSOR = "fsdp", "tensor"

HEAD = 64


epsilon = 1e-05
root_half = 0.7071067811865476
inverse_root_two_pi = 0.3989422804014327


def gelu_value(inner):
    return 0.5 * inner * (1.0 + jax.scipy.special.erf(inner * root_half))


def gelu_slope(inner):
    return 0.5 * (
        1.0 + jax.scipy.special.erf(inner * root_half)
    ) + inner * inverse_root_two_pi * jnp.exp(-0.5 * inner * inner)


def normalize(rows):
    mean = jnp.mean(rows, axis=1, keepdims=True)
    centered = rows - mean
    variance = jnp.mean(centered * centered, axis=1, keepdims=True)
    factor = lax.rsqrt(variance + epsilon)
    return (centered * factor, factor)


def normalize_back(grad_normed, normed, factor):
    return factor * (
        grad_normed
        - jnp.mean(grad_normed, axis=1, keepdims=True)
        - normed * jnp.mean(grad_normed * normed, axis=1, keepdims=True)
    )


def column_sum(rows):
    return jnp.sum(rows.astype(jnp.float32), axis=0)


def dot_rows(left, right):
    return lax.dot_general(
        left, right, (((0,), (0,)), ((), ())), preferred_element_type=jnp.float32
    )


def dot_back(left, right):
    return lax.dot_general(
        left, right, (((1,), (1,)), ((), ())), preferred_element_type=jnp.float32
    )


def place(values, offset, total_length):
    return lax.dynamic_update_slice(jnp.zeros((total_length,), jnp.float32), values, (offset,))


def block_scores(keys, key_valid, query_block):
    raw = jnp.einsum(
        "qhd,khd->hqk", query_block, keys, preferred_element_type=jnp.float32
    ) * HEAD ** (-0.5)
    return jnp.where(key_valid[None, None, :], raw, -1000000000.0)


def attend_forward(keys, values, key_valid, query_block):
    masked = block_scores(keys, key_valid, query_block)
    top = jnp.max(masked, axis=2, keepdims=True)
    expo = jnp.exp(masked - top)
    total = jnp.sum(expo, axis=2, keepdims=True)
    probs = (expo / total).astype(jnp.bfloat16)
    context = jnp.einsum("hqk,khd->qhd", probs, values, preferred_element_type=jnp.float32)
    return (context, top, total)


def attend_backward(keys, values, key_valid, carry, item):
    key_grad, value_grad = carry
    query_block, context_grad_block, top, total = item
    masked = block_scores(keys, key_valid, query_block)
    probs = jnp.exp(masked - top) / total
    probs_low = probs.astype(jnp.bfloat16)
    prob_grad = jnp.einsum(
        "qhd,khd->hqk", context_grad_block, values, preferred_element_type=jnp.float32
    )
    delta = jnp.sum(prob_grad * probs, axis=2, keepdims=True)
    score_grad = (probs * (prob_grad - delta)).astype(jnp.bfloat16)
    factor = HEAD ** (-0.5)
    query_grad = (
        jnp.einsum("hqk,khd->qhd", score_grad, keys, preferred_element_type=jnp.float32) * factor
    )
    key_grad = (
        key_grad
        + jnp.einsum("hqk,qhd->khd", score_grad, query_block, preferred_element_type=jnp.float32)
        * factor
    )
    value_grad = value_grad + jnp.einsum(
        "hqk,qhd->khd", probs_low, context_grad_block, preferred_element_type=jnp.float32
    )
    return ((key_grad, value_grad), query_grad)


def gather_weights(w_query, w_key, w_value, w_output, w_inner, w_outer):
    return (
        lax.all_gather(w_query, FSDP, axis=0, tiled=True),
        lax.all_gather(w_key, FSDP, axis=0, tiled=True),
        lax.all_gather(w_value, FSDP, axis=0, tiled=True),
        lax.all_gather(w_output, FSDP, axis=1, tiled=True),
        lax.all_gather(w_inner, FSDP, axis=0, tiled=True),
        lax.all_gather(w_outer, FSDP, axis=1, tiled=True),
    )


def split_joint(joint_sum, output_sum, inner_sum, outer_sum, head_width):
    return (
        joint_sum[:, :head_width],
        joint_sum[:, head_width : 2 * head_width],
        joint_sum[:, 2 * head_width :],
        output_sum,
        inner_sum,
        outer_sum,
    )


def add_tuples(left, right):
    return tuple((first_item + second_item for first_item, second_item in zip(left, right)))


def local_generic(
    tokens,
    lengths,
    cotangent,
    w_query,
    w_key,
    w_value,
    w_output,
    w_inner,
    w_outer,
    b_query,
    b_value,
    b_output,
    b_inner,
    b_outer,
    gain_first,
    shift_first,
    gain_second,
    shift_second,
):
    tensor_size = lax.axis_size(TENSOR)
    tensor_rank = lax.axis_index(TENSOR)
    micro_count = tokens.shape[0]
    part_rows = tokens.shape[1]
    width = tokens.shape[2]
    seq_rows = part_rows * tensor_size
    head_width = w_query.shape[1]
    inner_width = w_inner.shape[1]
    local_heads = head_width // HEAD
    block_rows = min(512, seq_rows)
    block_count = seq_rows // block_rows
    vector_full = (
        lax.all_gather(b_query, (FSDP, TENSOR), axis=0, tiled=True),
        lax.all_gather(b_value, (FSDP, TENSOR), axis=0, tiled=True),
        lax.all_gather(b_output, (FSDP, TENSOR), axis=0, tiled=True),
        lax.all_gather(b_inner, (FSDP, TENSOR), axis=0, tiled=True),
        lax.all_gather(b_outer, (FSDP, TENSOR), axis=0, tiled=True),
        lax.all_gather(gain_first, (FSDP, TENSOR), axis=0, tiled=True),
        lax.all_gather(shift_first, (FSDP, TENSOR), axis=0, tiled=True),
        lax.all_gather(gain_second, (FSDP, TENSOR), axis=0, tiled=True),
        lax.all_gather(shift_second, (FSDP, TENSOR), axis=0, tiled=True),
    )
    query_bias = lax.dynamic_slice_in_dim(vector_full[0], tensor_rank * head_width, head_width)
    value_bias = lax.dynamic_slice_in_dim(vector_full[1], tensor_rank * head_width, head_width)
    inner_bias = lax.dynamic_slice_in_dim(vector_full[3], tensor_rank * inner_width, inner_width)
    joint_bias = jnp.concatenate([query_bias, jnp.zeros((head_width,), jnp.float32), value_bias])
    grad_query_bias = jnp.zeros((head_width,), jnp.float32)
    grad_value_bias = jnp.zeros((head_width,), jnp.float32)
    grad_inner_bias = jnp.zeros((inner_width,), jnp.float32)
    grad_output_bias = jnp.zeros((width,), jnp.float32)
    grad_outer_bias = jnp.zeros((width,), jnp.float32)
    grad_gain_one = jnp.zeros((width,), jnp.float32)
    grad_shift_one = jnp.zeros((width,), jnp.float32)
    grad_gain_two = jnp.zeros((width,), jnp.float32)
    grad_shift_two = jnp.zeros((width,), jnp.float32)
    local_totals = None
    shard_totals = None
    outputs = []
    input_grads = []
    slot_index = jnp.arange(seq_rows, dtype=jnp.int32)
    part_index = tensor_rank * part_rows + jnp.arange(part_rows, dtype=jnp.int32)
    for micro_index in range(micro_count):
        forward_weights = gather_weights(w_query, w_key, w_value, w_output, w_inner, w_outer)
        joint_w = jnp.concatenate(
            [forward_weights[0], forward_weights[1], forward_weights[2]], axis=1
        )
        output_w = forward_weights[3]
        inner_w = forward_weights[4]
        outer_w = forward_weights[5]
        length = lengths[micro_index]
        key_valid = slot_index < length
        row_valid = (part_index < length).astype(jnp.float32)[:, None]
        own_rows = tokens[micro_index]
        whole = lax.all_gather(own_rows, TENSOR, axis=0, tiled=True)
        joint = (jnp.dot(whole, joint_w, preferred_element_type=jnp.float32) + joint_bias).astype(
            jnp.bfloat16
        )
        query = joint[:, :head_width].reshape(block_count, block_rows, local_heads, HEAD)
        keys = joint[:, head_width : 2 * head_width].reshape(seq_rows, local_heads, HEAD)
        values = joint[:, 2 * head_width :].reshape(seq_rows, local_heads, HEAD)
        context_blocks, tops, totals = lax.map(
            partial(attend_forward, keys, values, key_valid), query
        )
        context_low = context_blocks.reshape(seq_rows, head_width).astype(jnp.bfloat16)
        attended = (
            lax.psum_scatter(
                jnp.dot(context_low, output_w, preferred_element_type=jnp.float32).astype(
                    jnp.bfloat16
                ),
                TENSOR,
                scatter_dimension=0,
                tiled=True,
            ).astype(jnp.float32)
            + vector_full[2]
        )
        normed_first, factor_first = normalize(own_rows.astype(jnp.float32) + attended)
        first = normed_first * vector_full[5] + vector_full[6]
        first_whole = lax.all_gather(first.astype(jnp.bfloat16), TENSOR, axis=0, tiled=True)
        inner = jnp.dot(first_whole, inner_w, preferred_element_type=jnp.float32) + inner_bias
        active = gelu_value(inner).astype(jnp.bfloat16)
        mixed = (
            lax.psum_scatter(
                jnp.dot(active, outer_w, preferred_element_type=jnp.float32).astype(jnp.bfloat16),
                TENSOR,
                scatter_dimension=0,
                tiled=True,
            ).astype(jnp.float32)
            + vector_full[4]
        )
        normed_second, factor_second = normalize(first + mixed)
        outputs.append(
            ((normed_second * vector_full[7] + vector_full[8]) * row_valid).astype(jnp.bfloat16)
        )
        backward_weights = gather_weights(w_query, w_key, w_value, w_output, w_inner, w_outer)
        joint_w = jnp.concatenate(
            [backward_weights[0], backward_weights[1], backward_weights[2]], axis=1
        )
        output_w = backward_weights[3]
        inner_w = backward_weights[4]
        outer_w = backward_weights[5]
        out_grad = cotangent[micro_index].astype(jnp.float32) * row_valid
        grad_gain_two = grad_gain_two + column_sum(out_grad * normed_second)
        grad_shift_two = grad_shift_two + column_sum(out_grad)
        sum_grad = normalize_back(out_grad * vector_full[7], normed_second, factor_second)
        mixed_grad = sum_grad.astype(jnp.bfloat16)
        grad_outer_bias = grad_outer_bias + column_sum(mixed_grad)
        mixed_whole = lax.all_gather(mixed_grad, TENSOR, axis=0, tiled=True)
        outer_sum = dot_rows(active, mixed_whole)
        inner_grad = (dot_back(mixed_whole, outer_w) * gelu_slope(inner)).astype(jnp.bfloat16)
        grad_inner_bias = grad_inner_bias + column_sum(inner_grad)
        inner_sum = dot_rows(first_whole, inner_grad)
        first_grad = sum_grad + lax.psum_scatter(
            dot_back(inner_grad, inner_w).astype(jnp.bfloat16),
            TENSOR,
            scatter_dimension=0,
            tiled=True,
        ).astype(jnp.float32)
        grad_gain_one = grad_gain_one + column_sum(first_grad * normed_first)
        grad_shift_one = grad_shift_one + column_sum(first_grad)
        residual_grad = normalize_back(first_grad * vector_full[5], normed_first, factor_first)
        attended_grad = residual_grad.astype(jnp.bfloat16)
        grad_output_bias = grad_output_bias + column_sum(attended_grad)
        attended_whole = lax.all_gather(attended_grad, TENSOR, axis=0, tiled=True)
        output_sum = dot_rows(context_low, attended_whole)
        context_grad = (
            dot_back(attended_whole, output_w)
            .astype(jnp.bfloat16)
            .reshape(block_count, block_rows, local_heads, HEAD)
        )
        empty = jnp.zeros((seq_rows, local_heads, HEAD), jnp.float32)
        carried, query_grad = lax.scan(
            partial(attend_backward, keys, values, key_valid),
            (empty, empty),
            (query, context_grad, tops, totals),
        )
        joint_grad = jnp.concatenate(
            [
                query_grad.reshape(seq_rows, head_width),
                carried[0].reshape(seq_rows, head_width),
                carried[1].reshape(seq_rows, head_width),
            ],
            axis=1,
        ).astype(jnp.bfloat16)
        grad_query_bias = grad_query_bias + column_sum(joint_grad[:, :head_width])
        grad_value_bias = grad_value_bias + column_sum(joint_grad[:, 2 * head_width :])
        joint_sum = dot_rows(whole, joint_grad)
        input_grads.append(
            residual_grad
            + lax.psum_scatter(
                dot_back(joint_grad, joint_w).astype(jnp.bfloat16),
                TENSOR,
                scatter_dimension=0,
                tiled=True,
            ).astype(jnp.float32)
        )
        batch_sums = (joint_sum, output_sum, inner_sum, outer_sum)
        local_totals = batch_sums if local_totals is None else add_tuples(local_totals, batch_sums)
    pieces = split_joint(
        local_totals[0], local_totals[1], local_totals[2], local_totals[3], head_width
    )
    shard_totals = (
        lax.psum_scatter(pieces[0], FSDP, scatter_dimension=0, tiled=True),
        lax.psum_scatter(pieces[1], FSDP, scatter_dimension=0, tiled=True),
        lax.psum_scatter(pieces[2], FSDP, scatter_dimension=0, tiled=True),
        lax.psum_scatter(pieces[3], FSDP, scatter_dimension=1, tiled=True),
        lax.psum_scatter(pieces[4], FSDP, scatter_dimension=0, tiled=True),
        lax.psum_scatter(pieces[5], FSDP, scatter_dimension=1, tiled=True),
    )
    vector_grads = (
        lax.psum_scatter(
            place(grad_query_bias, tensor_rank * head_width, width),
            (FSDP, TENSOR),
            scatter_dimension=0,
            tiled=True,
        ),
        lax.psum_scatter(
            place(grad_value_bias, tensor_rank * head_width, width),
            (FSDP, TENSOR),
            scatter_dimension=0,
            tiled=True,
        ),
        lax.psum_scatter(grad_output_bias, (FSDP, TENSOR), scatter_dimension=0, tiled=True),
        lax.psum_scatter(
            place(grad_inner_bias, tensor_rank * inner_width, inner_width * tensor_size),
            (FSDP, TENSOR),
            scatter_dimension=0,
            tiled=True,
        ),
        lax.psum_scatter(grad_outer_bias, (FSDP, TENSOR), scatter_dimension=0, tiled=True),
        lax.psum_scatter(grad_gain_one, (FSDP, TENSOR), scatter_dimension=0, tiled=True),
        lax.psum_scatter(grad_shift_one, (FSDP, TENSOR), scatter_dimension=0, tiled=True),
        lax.psum_scatter(grad_gain_two, (FSDP, TENSOR), scatter_dimension=0, tiled=True),
        lax.psum_scatter(grad_shift_two, (FSDP, TENSOR), scatter_dimension=0, tiled=True),
    )
    return (
        jnp.stack(outputs),
        jnp.stack(input_grads),
        shard_totals[0],
        shard_totals[1],
        shard_totals[2],
        shard_totals[3],
        shard_totals[4],
        shard_totals[5],
        vector_grads[0],
        vector_grads[1],
        vector_grads[2],
        vector_grads[3],
        vector_grads[4],
        vector_grads[5],
        vector_grads[6],
        vector_grads[7],
        vector_grads[8],
    )


MESH = pl.DeviceIdType.MESH
WIDTH = 768
HIDDEN = 3072
HALF = WIDTH // 2
KINDS = 3
FLOWS = (
    (0, 0, 384, "zyx", "yxz"),
    (0, 384, 384, "zyx", "xzy"),
    (1, 0, 512, "zxy", "yxz"),
    (1, 512, 256, "zyx", "xyz"),
    (2, 0, 384, "zxy", "yxz"),
    (2, 384, 384, "yzx", "xzy"),
)
VECTOR_ROWS = 16
SHORT, LONG = 24, 96
ROW_OUTPUT, ROW_OUTER, ROW_GAIN1, ROW_SHIFT1, ROW_GAIN2, ROW_SHIFT2, ROW_INNER = 4, 5, 6, 7, 8, 9, 10
BF16 = jnp.bfloat16
F32 = jnp.float32


def fits(sizes):
    fsdp = sizes[FSDP]
    return sizes[TENSOR] == 4 and fsdp == WIDTH // LONG


class Place:
    def __init__(self, nz):
        self.f = lax.axis_index(FSDP)
        self.t = lax.axis_index(TENSOR)
        self.nz = nz
        self.z = self.f // 2
        self.x = self.f % 2
        self.y = self.t // 2
        self.c = self.t % 2
        self.core = (self.f, self.t + 1 - 2 * self.c)
        self.along_y = (self.f, self.t + 2 - 4 * self.y)
        self.along_x = (self.f + 1 - 2 * self.x, self.t)

    def z_at(self, step):
        return (self.z + step) % self.nz

    def z_back(self, step):
        return (self.z + self.nz - step) % self.nz

    def along_z(self, step):
        return (self.z_at(step) * 2 + self.x, self.t)

    def in_group(self, step):
        return (self.f, (self.t + step) % 4)


class Trip:
    def __init__(self, copy, send_sem, recv_sem):
        self.copy, self.send_sem, self.recv_sem = copy, send_sem, recv_sem

    def start(self):
        self.copy.start()

    def wait_recv(self):
        self.copy.wait_recv()


class Net:
    def __init__(self, send_sems, recv_sems):
        self.send_sems, self.recv_sems = send_sems, recv_sems
        self.sends = self.recvs = 0

    def lane(self):
        self.sends += 1
        return self.send_sems.at[self.sends - 1]

    def door(self):
        self.recvs += 1
        return self.recv_sems.at[self.recvs - 1]

    def plan(self, source, target, device, lane, door=None):
        door = self.door() if door is None else door
        copy = pltpu.make_async_remote_copy(
            src_ref=source, dst_ref=target, send_sem=lane, recv_sem=door, device_id=device, device_id_type=MESH
        )
        return Trip(copy, lane, door)

    def keep(self, ref, device, lane, door=None):
        return self.plan(ref, ref, device, lane, door)


class Meter:
    def __init__(self, low, wide):
        self.low, self.wide = low, wide

    def low_rows(self, rows):
        for count in (1, 2, 3, 4):
            if rows % (16 * count) == 0 and rows // count <= self.low.shape[1]:
                return self.low.at[0:count, 0:rows // count]
        raise ValueError(rows)

    def tiles(self, count):
        return self.wide.at[0:8 * count]


def arrived(trips, size):
    pltpu.make_async_copy(size, size, trips[0].recv_sem).wait()


def departed(trips, size):
    pltpu.make_async_copy(size, size, trips[0].send_sem).wait()


def start_all(copies):
    for copy in copies:
        copy.start()


def greet(place):
    barrier = pltpu.get_barrier_semaphore()
    peers = [place.in_group(1), place.in_group(2), place.in_group(3), place.along_x]
    peers += [place.along_z(step) for step in range(1, place.nz)]
    for peer in peers:
        pl.semaphore_signal(barrier, inc=1, device_id=peer, device_id_type=MESH)
    pl.semaphore_wait(barrier, len(peers))


def wait_local(copies):
    for copy in copies:
        copy.wait()


def dot(left, right):
    return lax.dot_general(left, right, (((1,), (0,)), ((), ())), preferred_element_type=F32)


def turn(value, shift):
    shift %= value.shape[1]
    return pltpu.roll(value, shift, 1) if shift else value


class Layer:
    def __init__(self, refs, length):
        (
            self.w, self.rows, self.back, self.rows_turned, self.joint, self.probs, self.context, self.acc,
            self.normed, self.factor, self.first_low, self.first_turned, self.active, self.slope, self.grad_low,
            self.grad_turned, self.out, self.vec, self.sums,
        ) = refs
        self.length = length
        self.seq = self.rows.shape[0]
        self.block = 128

    def weight(self, kind, t):
        return self.w[kind, t // 2, t % 2].reshape(WIDTH, WIDTH)

    def output_weight(self, t):
        return self.w[0, t // 2, t % 2, :, :, :, 512:768].reshape(WIDTH, 256)

    def store_grad(self, kind, t, value):
        nz = self.w.shape[3]
        self.w[kind, t // 2, t % 2] = value.astype(BF16).reshape(nz, 2, WIDTH // (2 * nz), WIDTH)

    def row(self, index):
        return self.vec[pl.ds(index, 1), :]

    def blocks(self, body):
        def step(i, carry):
            body(pl.ds(pl.multiple_of(i * self.block, self.block), self.block), i)
            return carry

        lax.fori_loop(0, self.seq // self.block, step, 0)

    def row_valid(self, i):
        index = lax.broadcasted_iota(jnp.int32, (self.block, 1), 0) + i * self.block
        return (index < self.length).astype(F32)

    def lanes(self, low, high, width):
        lane = lax.broadcasted_iota(jnp.int32, (1, width), 1)
        return (lane >= low) & (lane < high)

    def pick(self, value, low, high):
        return jnp.where(self.lanes(low, high, value.shape[1]), value, jnp.zeros_like(value))

    def head_query(self, t, h):
        return self.joint[t, :, 0:128] if h < 2 else self.joint[t, :, 384:512]

    def head_key(self, t, h):
        return self.joint[t, :, 128:256] if h < 2 else self.joint[t, :, 640:768]

    def head_side(self, value, h):
        return self.pick(value, 0, 64) if h == 0 else self.pick(value, 64, 128)

    def head_value(self, t, h):
        return self.pick(self.joint[t, :, 256:512], h * 64, h * 64 + 64)

    def unpack(self, v):
        nz = v.shape[2]
        short = jnp.zeros((8, WIDTH), F32)
        inner = [jnp.zeros((1, WIDTH), F32) for _ in range(4)]
        for f in range(2 * nz):
            for t in range(4):
                rank = f * 4 + t
                block = v[t // 2, t % 2, f // 2, f % 2]
                wide = jnp.concatenate([self.pick(block, 0, SHORT), jnp.zeros((8, WIDTH - 128), F32)], axis=1)
                short += turn(wide, rank * SHORT)
                wide = jnp.concatenate([self.pick(block[0:1], 32, 128), jnp.zeros((1, WIDTH - 128), F32)], axis=1)
                inner[rank * LONG // WIDTH] += turn(wide, rank * LONG % WIDTH - 32)
        for t in range(4):
            query = self.pick(turn(short[0:1], -192 * t), 0, 128) + self.pick(turn(short[0:1], 320 - 192 * t), 448, 512)
            self.vec[t:t + 1] = query + self.pick(turn(short[1:2], 256 - 192 * t), 256, 448)
            self.vec[ROW_INNER + t:ROW_INNER + t + 1] = inner[t]
        self.vec[ROW_OUTPUT:ROW_INNER] = short[2:8]

    def pack(self, parts):
        nz = parts.shape[2]
        query, value = jnp.zeros((1, WIDTH), F32), jnp.zeros((1, WIDTH), F32)
        for t in range(4):
            row = self.sums[t:t + 1]
            query += turn(self.pick(row, 0, 128), 192 * t) + turn(self.pick(row, 448, 512), 192 * t - 320)
            value += turn(self.pick(row, 256, 448), 192 * t - 256)
        short = jnp.concatenate([query, value, self.sums[ROW_OUTPUT:ROW_INNER]], axis=0)
        top = lax.broadcasted_iota(jnp.int32, (8, 1), 0) == 0
        for f in range(2 * nz):
            for t in range(4):
                rank = f * 4 + t
                block = self.pick(turn(short, -rank * SHORT)[:, 0:128], 0, SHORT)
                index = ROW_INNER + rank * LONG // WIDTH
                inner = turn(self.sums[index:index + 1], 32 - rank * LONG % WIDTH)[:, 0:128]
                inner = jnp.broadcast_to(self.pick(inner, 32, 128), (8, 128))
                parts[t // 2, t % 2, f // 2, f % 2] = block + jnp.where(top, inner, 0.0)

    def project(self, t):
        self.joint[t] = (dot(self.rows[...], self.weight(0, t)) + self.row(t)).astype(BF16)

    def attend(self, t):
        key_valid = lax.broadcasted_iota(jnp.int32, (1, self.seq), 1) < self.length
        context = None
        for h in range(3):
            raw = dot_back(self.head_query(t, h), self.head_side(self.head_key(t, h), h))
            masked = jnp.where(key_valid, raw * HEAD ** -0.5, -1e9)
            expo = jnp.exp(masked - jnp.max(masked, axis=1, keepdims=True))
            probs = (expo * (1.0 / jnp.sum(expo, axis=1, keepdims=True))).astype(BF16)
            self.probs[t * 3 + h] = probs
            part = dot(probs, self.head_value(t, h))
            context = part if context is None else context + part
        low = context.astype(BF16)
        self.context[t] = low
        self.acc[...] += dot_back(low, self.output_weight(t))

    def start(self):
        def body(rows, i):
            self.acc[rows] = self.rows[rows].astype(F32) + self.row(ROW_OUTPUT)

        self.blocks(body)

    def norm_first(self):
        def body(rows, i):
            normed, factor = normalize(self.acc[rows])
            self.normed[rows] = normed
            self.factor[rows] = jnp.broadcast_to(factor, (self.block, 128))
            first = normed * self.row(ROW_GAIN1) + self.row(ROW_SHIFT1)
            self.first_low[rows] = first.astype(BF16)
            self.acc[rows] = first + self.row(ROW_OUTER)

        self.blocks(body)

    def feed_inner(self, t):
        inner = dot(self.first_low[...], self.weight(1, t)) + self.row(ROW_INNER + t)
        gate = 1.0 + lax.erf(inner * root_half)
        self.active[t] = (0.5 * inner * gate).astype(BF16)
        self.slope[t] = (0.5 * gate + inner * inverse_root_two_pi * jnp.exp(-0.5 * inner * inner)).astype(BF16)

    def feed_outer(self, t):
        self.acc[...] += dot_back(self.active[t], self.weight(2, t))

    def clear_sums(self):
        self.sums[...] = jnp.zeros_like(self.sums)

    def add_sum(self, index, value):
        self.sums[pl.ds(index, 1), :] += jnp.sum(value, axis=0, keepdims=True)

    def norm_second(self):
        def body(rows, i):
            normed, factor = normalize(self.acc[rows])
            valid = self.row_valid(i)
            gain = self.row(ROW_GAIN2)
            self.out[rows] = ((normed * gain + self.row(ROW_SHIFT2)) * valid).astype(BF16)
            out_grad = self.back[rows].astype(F32) * valid
            self.add_sum(ROW_GAIN2, out_grad * normed)
            self.add_sum(ROW_SHIFT2, out_grad)
            sum_grad = normalize_back(out_grad * gain, normed, factor)
            self.acc[rows] = sum_grad
            low = sum_grad.astype(BF16)
            self.grad_low[rows] = low
            self.add_sum(ROW_OUTER, low.astype(F32))

        self.blocks(body)
        self.grad_turned[...] = self.grad_low[...].T

    def outer_back(self, t):
        grad = (dot(self.grad_low[...], self.weight(2, t)) * self.slope[t].astype(F32)).astype(BF16)
        self.slope[t] = grad
        self.add_sum(ROW_INNER + t, grad.astype(F32))
        self.store_grad(2, t, dot(self.grad_turned[...], self.active[t]))

    def inner_back(self, t):
        grad = self.slope[t]
        self.acc[...] += dot_back(grad, self.weight(1, t))
        self.store_grad(1, t, dot(self.first_turned[...], grad))

    def norm_first_back(self):
        def body(rows, i):
            grad = self.acc[rows]
            normed = self.normed[rows]
            self.add_sum(ROW_GAIN1, grad * normed)
            self.add_sum(ROW_SHIFT1, grad)
            residual = normalize_back(grad * self.row(ROW_GAIN1), normed, self.factor[rows][:, 0:1])
            self.acc[rows] = residual
            low = residual.astype(BF16)
            self.grad_low[rows] = low
            self.add_sum(ROW_OUTPUT, low.astype(F32))

        self.blocks(body)
        self.grad_turned[...] = self.grad_low[...].T

    def attend_back(self, t):
        context_grad = self.pick(dot(self.grad_low[...], self.output_weight(t)), 0, 192).astype(BF16)
        query_grads, key_grads, value_grad = [], [], None
        for h in range(3):
            probs = self.probs[t * 3 + h]
            prob_grad = dot_back(context_grad, self.head_value(t, h))
            wide = probs.astype(F32)
            delta = jnp.sum(wide * prob_grad, axis=1, keepdims=True)
            score_grad = (wide * (prob_grad - delta)).astype(BF16)
            query_grads.append(dot(score_grad, self.head_side(self.head_key(t, h), h)) * HEAD ** -0.5)
            key_grads.append(dot_rows(score_grad, self.head_side(self.head_query(t, h), h)) * HEAD ** -0.5)
            part = dot_rows(probs, self.pick(context_grad, h * 64, h * 64 + 64))
            value_grad = part if value_grad is None else value_grad + part
        self.joint[t, :, 0:128] = (query_grads[0] + query_grads[1]).astype(BF16)
        self.joint[t, :, 128:256] = (key_grads[0] + key_grads[1]).astype(BF16)
        self.joint[t, :, 256:384] = value_grad[:, 0:128].astype(BF16)
        self.joint[t, :, 384:512] = (value_grad[:, 128:256] + query_grads[2]).astype(BF16)
        self.joint[t, :, 512:640] = jnp.zeros((self.seq, 128), BF16)
        self.joint[t, :, 640:768] = key_grads[2].astype(BF16)

    def joint_back(self, t):
        joint = self.joint[t]
        self.sums[pl.ds(t, 1), :] = jnp.sum(joint.astype(F32), axis=0, keepdims=True)
        self.acc[...] += dot_back(joint, self.weight(0, t))
        nz = self.w.shape[3]
        shape = (nz, 2, WIDTH // (2 * nz), -1)
        main = dot(self.rows_turned[...], joint[:, 0:512])
        side = dot(self.rows_turned[...], joint[:, 512:768]) + dot(self.grad_turned[...], self.context[t])
        self.w[0, t // 2, t % 2, :, :, :, 0:512] = main.astype(BF16).reshape(shape[:3] + (512,))
        self.w[0, t // 2, t % 2, :, :, :, 512:768] = side.astype(BF16).reshape(shape[:3] + (256,))

    def finish(self):
        def body(rows, i):
            self.back[rows] = self.acc[rows].astype(BF16)

        self.blocks(body)


def each(count, body):
    def step(i, carry):
        body(i)
        return carry

    lax.fori_loop(0, count, step, 0)


BUFFER_COUNT = 19


def buffer_shapes(nz, seq):
    part = WIDTH // (2 * nz)
    low, wide = (seq, WIDTH), (WIDTH, seq)
    shapes = [
        ((KINDS, 2, 2, nz, 2, part, WIDTH), BF16),
        (low, BF16),
        (low, BF16),
        (wide, BF16),
        ((4, seq, WIDTH), BF16),
        ((12, seq, seq), BF16),
        ((4, seq, 256), BF16),
        (low, F32),
        (low, F32),
        ((seq, 128), F32),
        (low, BF16),
        (wide, BF16),
        ((4, seq, WIDTH), BF16),
        ((4, seq, WIDTH), BF16),
        (low, BF16),
        (wide, BF16),
        (low, BF16),
        ((VECTOR_ROWS, WIDTH), F32),
        ((VECTOR_ROWS, WIDTH), F32),
    ]
    return [pltpu.VMEM(*shape) for shape in shapes]


BLOCKS = 15
SEND_COUNT = 15
DOOR_COUNT = 197


def flow_shapes(nz):
    part = WIDTH // (2 * nz)
    shapes = [pltpu.VMEM((KINDS, 2, nz, 2, part, WIDTH), BF16)]
    return shapes + [pltpu.VMEM((BLOCKS, part, flow[2]), BF16) for flow in FLOWS]


def axis_steps(place, axis):
    p = place
    if axis == "x":
        return [(1, 1 - p.x, p.along_x, 1 - p.x)]
    if axis == "y":
        return [(1, 1 - p.y, p.along_y, 1 - p.y)]
    return [(step, p.z_at(step), p.along_z(step), p.z_back(step)) for step in range(1, p.nz)]


class Flow:
    def __init__(self, net, place, order, own, region, lane, core_lane, core_door):
        p = place
        self.pieces = [(None, [])]
        spots = [({"x": p.x, "y": p.y, "z": p.z}, own)]
        for axis in order:
            for index, (spot, source) in enumerate(list(spots)):
                for _, _, device, behind in axis_steps(p, axis):
                    trip = net.plan(region(spot) if source is None else source, region(spot), device, lane)
                    self.pieces[index][1].append(trip)
                    self.pieces.append((trip, []))
                    spots.append(({**spot, axis: behind}, None))
        mine = {"x": p.x, "y": p.y, "z": p.z}[order[2]]
        sides = [mine] + [behind for _, _, _, behind in axis_steps(p, order[2])]
        every = slice(None)
        self.cores = [
            net.keep(region({"x": every, "y": every, "z": every, order[2]: side}), p.core, core_lane, core_door)
            for side in sides
        ]
        self.trips = [trip for _, onward in self.pieces for trip in onward]

    def first(self):
        start_all(self.pieces[0][1])

    def piece(self, index):
        trip, onward = self.pieces[index]
        trip.wait_recv()
        start_all(onward)

    def to_core(self, index):
        self.cores[index].start()


class Cores:
    def __init__(self, net, place, w, core, k):
        self.place = place
        self.w, self.core = w.at[k], core.at[k]
        self.ys = (1 - place.y, place.y)
        lane = net.lane()
        self.c = [net.plan(self.w.at[y, 1 - place.c], self.core.at[y], place.core, lane) for y in self.ys]

    def to_core(self, half):
        self.c[half].start()

    def half(self, half):
        y = self.ys[half]
        self.c[half].wait_recv()

        def body(z):
            target, source = self.core.at[y, z], self.w.at[y, self.place.c, z]
            target[...] = (target[...].astype(F32) + source[...].astype(F32)).astype(BF16)

        each(self.place.nz, body)


class Sink:
    def __init__(self, net, place, order, core, landing, result, cols, lane, meter):
        p = place
        self.meter = meter
        self.core, self.landing, self.result, self.cols = core, landing, result, cols
        here = {"x": p.x, "y": p.y, "z": p.z}
        ahead = {axis: {0: here[axis], **{step: spot for step, spot, _, _ in axis_steps(p, axis)}} for axis in here}
        sizes = {"x": 2, "y": 2, "z": p.nz}
        self.spot = lambda block: tuple(ahead[axis][block[axis]] for axis in ("y", "z", "x"))
        self.order = order
        self.tasks = []
        self.starts = ([], [])
        blocks = [{}]
        for axis in ("y", "z", "x"):
            steps = [i for i in range(1, sizes[axis])] + [0]
            blocks = [{**block, axis: step} for block in blocks for step in steps]
        slot = 0
        self.trips = []
        waits = {}
        for stage, axis in enumerate(order):
            later = order[stage + 1:]
            kept = [block for block in blocks if block[axis] == 0]
            kept.sort(key=lambda block: [block[other] == 0 for other in later])
            devices = {step: device for step, _, device, _ in axis_steps(p, axis)}
            for block in kept:
                arrivals = []
                door = net.door()
                for step in range(1, sizes[axis]):
                    away = {**block, axis: step}
                    copy = net.plan(self.part(away), landing.at[slot], devices[step], lane, door)
                    self.trips.append(copy)
                    if stage == 0:
                        self.starts[0 if away["y"] else 1].append(copy)
                    else:
                        waits[tuple(sorted(away.items()))].append(copy)
                    arrivals.append((copy, slot))
                    slot += 1
                onward = []
                waits[tuple(sorted(block.items()))] = onward
                self.tasks.append((block, arrivals, onward))
            blocks = kept

    def part(self, block):
        return self.core.at[(*self.spot(block), slice(None), self.cols)]

    def start(self, half):
        start_all(self.starts[half])

    def add(self, index):
        block, arrivals, onward = self.tasks[index]
        target = self.part(block)
        total = target[...].astype(F32)
        rows = self.landing.shape[1] * self.landing.shape[2] // WIDTH
        arrived([trip for trip, _ in arrivals], self.meter.low_rows(rows * len(arrivals)))
        for _, slot in arrivals:
            total += self.landing[slot].astype(F32)
        if index < len(self.tasks) - 1:
            target[...] = total.astype(BF16)
            start_all(onward)
        else:
            self.result[:, self.cols] = total


class Back:
    def __init__(self, net, place, parts, landings, result, meter):
        p = self.place = place
        self.parts, self.result, self.meter = parts, result, meter
        self.core, self.side, self.pair, self.line = landings
        lane = net.lane()
        self.c = net.plan(parts.at[:, 1 - p.c], self.core, p.core, lane)
        self.y = net.plan(self.core.at[1 - p.y], self.side, p.along_y, lane)
        self.x = net.plan(self.side.at[:, 1 - p.x], self.pair, p.along_x, lane)
        door = net.door()
        self.z = [
            net.plan(self.pair.at[p.z_at(step)], self.line.at[step - 1], p.along_z(step), lane, door)
            for step in range(1, p.nz)
        ]

    def first(self):
        self.c.start()

    def core_done(self):
        self.c.wait_recv()
        self.core[...] += self.parts[:, self.place.c]
        self.y.start()

    def y_done(self):
        self.y.wait_recv()
        self.side[...] += self.core[self.place.y]
        self.x.start()

    def x_done(self):
        self.x.wait_recv()
        self.pair[...] += self.side[:, self.place.x]
        start_all(self.z)

    def z_done(self):
        arrived(self.z, self.meter.tiles(len(self.z)))
        total = self.pair[self.place.z]
        for i in range(self.place.nz - 1):
            total += self.line[i]
        self.result[...] = total

    def sent(self):
        departed([self.c, self.y, self.x] + self.z, self.meter.tiles(8 * self.place.nz - 1))


def ticks(i, table):
    for when, actions in table.items():
        @pl.when(i == when)
        def _(actions=actions):
            for action, *given in actions:
                action(*given)


def layer_kernel(nz, *refs):
    tokens, lengths, cotangent, w_query, w_key, w_value, w_output, w_inner, w_outer = refs[:9]
    short_in, long_in = refs[9:12] + refs[13:18], refs[12]
    result, outs, backs, totals = refs[18:22]
    rest = list(refs[22:])
    buffers, rest = rest[:BUFFER_COUNT], rest[BUFFER_COUNT:]
    core_landing, landings, rest = rest[0], rest[1:1 + len(FLOWS)], rest[1 + len(FLOWS):]
    back_landings = rest[:4]
    v, parts, vec_in, raw_query, raw_key, raw_value, raw_output, own_joint = rest[4:12]
    raw_short, raw_long = rest[12:20], rest[20]
    send_sems, recv_sems, local_sems = rest[21:]
    place = Place(nz)
    net = Net(send_sems, recv_sems)
    t = place.t
    quarter = tokens.shape[1]
    layer = Layer(buffers, lengths[t])
    owns = (own_joint, w_inner, w_outer)
    g, r = [], []
    meter = Meter(layer.joint, layer.factor)
    cores = [Cores(net, place, layer.w, core_landing, k) for k in range(KINDS)]
    lanes = [[net.lane() for k in range(KINDS)] for _ in range(3)]
    doors = [net.door() for k in range(KINDS)]
    for (k, first, width, order_in, order_out), landing in zip(FLOWS, landings):
        cols = pl.ds(first, width)

        def region(spot, k=k, cols=cols):
            return layer.w.at[k, spot["y"], place.c, spot["z"], spot["x"], :, cols]

        g.append(Flow(net, place, order_in, owns[k].at[:, cols], region, lanes[0][k], lanes[1][k], doors[k]))
        sink = (core_landing.at[k], landing, result.at[k], cols, lanes[2][k], meter)
        r.append(Sink(net, place, order_out, *sink))
    one = net.lane()
    vecs = Flow(
        net, place, FLOWS[0][3], vec_in, lambda spot: v.at[spot["y"], place.c, spot["z"], spot["x"]],
        one, one, net.door(),
    )
    sums = Back(net, place, parts, back_landings, totals, meter)

    def of_kind(flows, k):
        return [flow for flow, row in zip(flows, FLOWS) if row[0] == k]

    def trips_of(flows):
        return [trip for flow in flows for trip in flow.trips]

    def cores_of(flows):
        return [trip for flow in flows for trip in flow.cores]

    def gathered(k):
        arrived(cores_of(of_kind(g, k)), meter.low_rows(2 * WIDTH))

    def passed_on(k):
        flows = of_kind(g, k)
        departed(trips_of(flows), meter.low_rows(2 * WIDTH - own_joint.shape[0]))
        departed(cores_of(flows), meter.low_rows(2 * WIDTH))

    def reduced(k):
        departed(trips_of(of_kind(r, k)), meter.low_rows(2 * WIDTH - own_joint.shape[0]))
        departed(cores[k].c, meter.low_rows(2 * WIDTH))

    def vectors_in():
        arrived(vecs.cores, meter.tiles(4 * nz))

    def vectors_sent():
        departed(vecs.trips + vecs.cores, meter.tiles(8 * nz - 1))

    def quarter_of(ref, index):
        return ref.at[pl.ds(pl.multiple_of(index * quarter, quarter), quarter)]

    swap_lane = net.lane()

    def swap(source, target):
        door = net.door()
        return [net.plan(source(step), target, place.in_group(step), swap_lane, door) for step in (2, 1, 3)]

    def swapped(trips):
        arrived(trips, meter.low_rows(3 * quarter))

    token_in = swap(lambda step: tokens.at[(t + step) % 4], quarter_of(layer.rows, t))
    back_in = swap(lambda step: cotangent.at[(t + step) % 4], quarter_of(layer.back, t))
    out_out = swap(lambda step: quarter_of(layer.out, (t + step) % 4), outs.at[t])
    back_out = swap(lambda step: quarter_of(layer.back, (t + step) % 4), backs.at[t])

    def swaps_sent():
        departed(token_in + back_in + out_out + back_out, meter.low_rows(12 * quarter))

    pairs = [
        (tokens.at[t], quarter_of(layer.rows, t)),
        (cotangent.at[t], quarter_of(layer.back, t)),
        *[
            (own, layer.w.at[k, place.y, place.c, place.z, place.x])
            for k, own in enumerate(owns)
        ],
        (vec_in, v.at[place.y, place.c, place.z, place.x]),
        (quarter_of(layer.out, t), outs.at[t]),
        (quarter_of(layer.back, t), backs.at[t]),
        (w_query, raw_query),
        (w_key, raw_key),
        (w_value, raw_value),
        (w_output, raw_output),
        *zip(short_in, raw_short),
        (long_in, raw_long),
    ]
    local = [pltpu.make_async_copy(*pair, local_sems.at[i]) for i, pair in enumerate(pairs)]

    def pack_vectors():
        vec_in[...] = jnp.zeros((8, 128), F32)
        for i, ref in enumerate(raw_short):
            vec_in[i:i + 1, 0:SHORT] = ref[...].reshape(1, SHORT)
        vec_in[0:1, 32:128] = raw_long[...].reshape(1, LONG)

    def pack_own():
        own_joint[...] = pack_joint(raw_query[...], raw_key[...], raw_value[...], raw_output[...].T)

    def near(i):
        return (place.y + i) % 2 * 2 + (place.c + i // 2) % 2

    def order(i):
        return (1 - place.y + i // 2) % 2 * 2 + (1 - place.c + i) % 2

    start_all(local[8:])
    greet(place)
    wait_local(local[8:])
    pack_vectors()
    pack_own()
    vecs.first()
    g[0].first()
    start_all(local[:6])
    wait_local(local[:6])
    g[1].first()
    start_all(token_in)
    g[2].first()
    g[3].first()
    g[4].first()
    g[5].first()
    vecs.piece(4)
    vecs.piece(8)
    vecs.piece(2)
    g[0].piece(4)
    vecs.piece(1)
    vecs.piece(3)
    g[0].piece(8)
    g[1].piece(4)
    g[1].piece(8)
    g[2].piece(4)
    g[3].piece(8)
    g[0].piece(1)
    g[4].piece(4)
    g[0].piece(2)
    g[5].piece(8)
    vecs.piece(12)
    vecs.piece(10)
    g[0].piece(3)
    g[0].piece(12)
    vecs.piece(9)
    vecs.piece(11)
    swapped(token_in)
    g[1].piece(12)
    g[2].piece(8)
    g[0].piece(9)
    g[3].piece(4)
    g[1].piece(1)
    g[0].piece(10)
    g[4].piece(8)
    g[1].piece(2)
    vecs.piece(6)
    vecs.piece(5)
    vecs.piece(7)
    vecs.to_core(0)
    g[0].piece(11)
    g[5].piece(1)
    g[1].piece(3)
    g[3].piece(12)
    g[2].piece(12)
    g[1].piece(9)
    g[0].piece(5)
    vecs.piece(14)
    vecs.piece(13)
    vecs.piece(15)
    vecs.to_core(1)
    g[1].piece(10)
    vectors_in()
    g[4].piece(12)
    layer.unpack(v)
    layer.start()
    layer.rows_turned[...] = layer.rows[...].T
    layer.clear_sums()
    g[0].piece(6)
    g[2].piece(1)
    g[5].piece(9)
    g[1].piece(11)
    g[0].piece(7)
    g[0].to_core(0)
    g[0].piece(13)
    g[2].piece(2)
    g[1].piece(5)
    g[0].piece(14)
    g[2].piece(3)
    g[1].piece(6)
    g[2].piece(5)
    g[1].piece(7)
    g[1].to_core(0)
    g[0].piece(15)
    g[0].to_core(1)
    g[3].piece(1)
    g[2].piece(9)
    g[2].piece(6)
    g[3].piece(2)
    g[3].piece(3)
    g[2].piece(10)
    g[1].piece(13)
    g[2].piece(11)
    g[2].piece(7)
    g[2].to_core(0)
    g[4].piece(1)
    g[1].piece(14)
    g[2].piece(13)
    g[3].piece(5)
    g[1].piece(15)
    g[1].to_core(1)
    def project(i):
        layer.project(near(i))
        ticks(i, {
            0: [(g[3].piece, 9), (g[4].piece, 2)],
            1: [(g[2].piece, 14), (g[3].piece, 10), (g[4].piece, 3), (gathered, 0)],
            2: [(g[3].piece, 6), (g[3].piece, 11)],
        })

    each(4, project)
    g[3].piece(7)
    g[3].to_core(0)
    def attend(i):
        layer.attend(i)
        ticks(i, {
            0: [(g[3].piece, 13), (g[2].piece, 15), (g[2].to_core, 1), (g[5].piece, 2), (g[4].piece, 5), (g[5].piece, 3), (g[5].piece, 4)],
            1: [(g[4].piece, 6), (g[4].piece, 9)],
            2: [(g[3].piece, 14), (g[4].piece, 7), (g[4].to_core, 0), (g[4].piece, 10), (g[5].piece, 5), (g[5].piece, 6), (g[4].piece, 11), (g[5].piece, 7), (g[3].piece, 15), (g[3].to_core, 1), (g[5].to_core, 0), (start_all, back_in)],
        })

    each(4, attend)
    g[4].piece(13)
    g[5].piece(10)
    layer.norm_first()
    layer.first_turned[...] = layer.first_low[...].T
    g[4].piece(14)
    g[5].piece(11)
    def feed_inner(i):
        layer.feed_inner(near(i))
        ticks(i, {
            0: [(g[4].piece, 15), (g[4].to_core, 1)],
            1: [(g[5].piece, 12), (gathered, 1)],
            2: [(g[5].piece, 13)],
        })

    each(4, feed_inner)
    g[5].piece(14)
    g[5].piece(15)
    g[5].to_core(1)
    def feed_outer(i):
        layer.feed_outer(near(i))
        ticks(i, {
            1: [(gathered, 2)],
        })

    each(4, feed_outer)
    swapped(back_in)
    layer.norm_second()
    start_all(out_out)
    local[6].start()
    passed_on(2)
    def outer_back(i):
        layer.outer_back(order(i))
        ticks(i, {
            0: [(cores[2].to_core, 0)],
            2: [(cores[2].to_core, 1), (cores[2].half, 0), (r[4].start, 0), (r[5].start, 0)],
        })

    each(4, outer_back)
    passed_on(1)
    def inner_back(i):
        layer.inner_back(order(i))
        ticks(i, {
            0: [(cores[1].to_core, 0), (cores[2].half, 1), (r[4].start, 1), (r[5].start, 1), (r[5].add, 0)],
            1: [(r[5].add, 1), (r[4].add, 0)],
            2: [(cores[1].to_core, 1), (cores[1].half, 0), (r[3].start, 0), (r[2].start, 0), (r[5].add, 2), (r[4].add, 1), (r[5].add, 6)],
        })

    each(4, inner_back)
    r[4].add(2)
    r[5].add(3)
    layer.norm_first_back()
    cores[1].half(1)
    r[3].start(1)
    r[2].start(1)
    r[4].add(3)
    r[5].add(4)
    r[4].add(4)
    vectors_sent()
    passed_on(0)
    def attend_back(i):
        layer.attend_back(order(i))
        ticks(i, {
            0: [(r[5].add, 5), (r[4].add, 5), (r[5].add, 8), (r[5].add, 7), (r[4].add, 6), (r[4].add, 8)],
            1: [(r[3].add, 1), (r[3].add, 2), (r[2].add, 0), (r[3].add, 3)],
            2: [(r[4].add, 10), (r[2].add, 2), (r[3].add, 4), (r[3].add, 5), (r[2].add, 3), (r[3].add, 6)],
            3: [(r[4].add, 11), (r[2].add, 5), (r[4].add, 12), (r[2].add, 8)],
        })
        layer.joint_back(order(i))
        ticks(i, {
            0: [(cores[0].to_core, 0), (r[3].add, 0), (r[4].add, 7)],
            1: [(cores[0].half, 0), (r[0].start, 0), (r[1].start, 0), (r[5].add, 9), (r[2].add, 1), (r[4].add, 9)],
            2: [(cores[0].to_core, 1), (r[3].add, 7), (r[2].add, 4)],
        })

    each(4, attend_back)
    cores[0].half(1)
    r[0].start(1)
    r[1].start(1)
    r[1].add(0)
    r[2].add(6)
    layer.pack(parts)
    sums.first()
    r[1].add(1)
    r[2].add(7)
    layer.finish()
    start_all(back_out)
    local[7].start()
    sums.core_done()
    r[5].add(10)
    reduced(2)
    r[1].add(2)
    r[3].add(8)
    r[1].add(6)
    r[3].add(9)
    r[3].add(10)
    r[2].add(9)
    r[3].add(11)
    r[0].add(0)
    r[2].add(10)
    r[0].add(1)
    r[2].add(11)
    r[0].add(2)
    r[1].add(8)
    r[1].add(3)
    r[0].add(3)
    r[1].add(4)
    r[0].add(4)
    r[1].add(5)
    r[0].add(5)
    r[3].add(12)
    r[1].add(7)
    r[0].add(6)
    r[0].add(8)
    r[0].add(7)
    r[0].add(9)
    r[0].add(10)
    r[0].add(11)
    r[2].add(12)
    reduced(1)
    sums.y_done()
    r[1].add(9)
    sums.x_done()
    r[1].add(10)
    r[0].add(12)
    sums.z_done()
    reduced(0)
    sums.sent()
    wait_local(local[6:8])
    swapped(out_out)
    swapped(back_out)
    swaps_sent()


VMEM_SPEC = pl.BlockSpec(memory_space=pltpu.VMEM)
ANY_SPEC = pl.BlockSpec(memory_space=pl.ANY)
LIMIT = 67043328


def whole_layer(tokens, *rest):
    nz = lax.axis_size(FSDP) // 2
    part = WIDTH // (2 * nz)
    seq = tokens.shape[1] * 4
    return pl.pallas_call(
        partial(layer_kernel, nz),
        out_shape=(
            jax.ShapeDtypeStruct((KINDS, part, WIDTH), F32),
            jax.ShapeDtypeStruct(tokens.shape, BF16),
            jax.ShapeDtypeStruct(tokens.shape, BF16),
            jax.ShapeDtypeStruct((8, 128), F32),
        ),
        in_specs=[ANY_SPEC, pl.BlockSpec(memory_space=pltpu.SMEM)] + [ANY_SPEC] * 16,
        out_specs=(VMEM_SPEC, ANY_SPEC, ANY_SPEC, VMEM_SPEC),
        scratch_shapes=buffer_shapes(nz, seq) + flow_shapes(nz) + [
            pltpu.VMEM((2, nz, 2, 8, 128), F32),
            pltpu.VMEM((nz, 2, 8, 128), F32),
            pltpu.VMEM((nz, 8, 128), F32),
            pltpu.VMEM((nz - 1, 8, 128), F32),
            pltpu.VMEM((2, 2, nz, 2, 8, 128), F32),
            pltpu.VMEM((2, 2, nz, 2, 8, 128), F32),
            pltpu.VMEM((8, 128), F32),
            *[pltpu.VMEM((part, WIDTH // 4), BF16)] * 3,
            pltpu.VMEM((WIDTH // 4, part), BF16),
            pltpu.VMEM((part, WIDTH), BF16),
            *[pltpu.VMEM((SHORT,), F32)] * 8,
            pltpu.VMEM((LONG,), F32),
            pltpu.SemaphoreType.DMA((SEND_COUNT,)),
            pltpu.SemaphoreType.DMA((DOOR_COUNT,)),
            pltpu.SemaphoreType.DMA((24,)),
        ],
        compiler_params=pltpu.CompilerParams(collective_id=0, has_side_effects=True, vmem_limit_bytes=LIMIT),
        name="whole_layer",
    )(tokens, *rest)


def finish_kernel(count, *refs):
    given, results, rest = refs[:4], refs[4:4 + count], refs[4 + count:]
    (sums, outs, backs, totals), made, (sems, sent) = rest[:4], rest[4:-2], rest[-2:]
    arrivals = [pltpu.make_async_copy(ref, spot, sems.at[i]) for i, (ref, spot) in enumerate(zip(given, rest))]
    start_all(arrivals)
    input_grad, g_query, g_key, g_value, g_output, g_inner, g_outer = made[:7]
    copies = [pltpu.make_async_copy(outs, results[0], sent.at[0])]
    copies += [pltpu.make_async_copy(*pair, sent.at[i + 1]) for i, pair in enumerate(zip(made, results[1:]))]
    arrivals[2].wait()
    input_grad[...] = backs[...].astype(F32)
    copies[1].start()
    arrivals[1].wait()
    copies[0].start()
    arrivals[0].wait()
    g_inner[...] = sums[1]
    g_outer[...] = sums[2]
    g_query[...], g_key[...], g_value[...], g_turned = unpack_joint(sums[0])
    g_output[...] = g_turned.T
    start_all(copies[2:8])
    arrivals[3].wait()
    short = [0, 1, 2, None, 3, 4, 5, 6, 7]
    for row, ref in zip(short, made[7:]):
        ref[...] = (totals[0:1, 32:128] if row is None else totals[row:row + 1, 0:SHORT]).reshape(ref.shape)
    start_all(copies[8:])
    wait_local(copies)


def finish_layer(sums, outs, backs, totals):
    part = sums.shape[1]
    share = WIDTH // 4
    shapes = [outs.shape, backs.shape] + [(part, share)] * 3 + [(share, part), (part, WIDTH), (part, WIDTH)]
    shapes += [(SHORT,)] * 3 + [(LONG,)] + [(SHORT,)] * 5
    given = (sums, outs, backs, totals)
    return pl.pallas_call(
        partial(finish_kernel, len(shapes)),
        out_shape=[jax.ShapeDtypeStruct(shape, F32 if i else BF16) for i, shape in enumerate(shapes)],
        in_specs=[ANY_SPEC] * 4,
        out_specs=[ANY_SPEC] * len(shapes),
        scratch_shapes=[pltpu.VMEM(ref.shape, ref.dtype) for ref in given]
        + [pltpu.VMEM(shape, F32) for shape in shapes[1:]]
        + [pltpu.SemaphoreType.DMA((4,)), pltpu.SemaphoreType.DMA((len(shapes),))],
        compiler_params=pltpu.CompilerParams(vmem_limit_bytes=LIMIT),
        name="finish_layer",
    )(*given)


def pack_joint(q, k, v, o):
    return jnp.concatenate(
        [q[:, :128], k[:, :128], v[:, :128], v[:, 128:], q[:, 128:], o[:, :128], o[:, 128:], k[:, 128:]], axis=1
    )


def unpack_joint(joint):
    q = jnp.concatenate([joint[:, 0:128], joint[:, 448:512]], axis=1)
    k = jnp.concatenate([joint[:, 128:256], joint[:, 704:768]], axis=1)
    return q, k, joint[:, 256:448], joint[:, 512:704]


def local_fast(*given):
    given = given[:8] + (given[8].T,) + given[9:]
    results = finish_layer(*whole_layer(*given))
    return (*results[:7], results[7].T, *results[8:])


def solution(mesh):
    placed = (
        P(FSDP, TENSOR, None),
        P(FSDP),
        P(FSDP, TENSOR, None),
        P(FSDP, TENSOR),
        P(FSDP, TENSOR),
        P(FSDP, TENSOR),
        P(TENSOR, FSDP),
        P(FSDP, TENSOR),
        P(TENSOR, FSDP),
        P((FSDP, TENSOR)),
        P((FSDP, TENSOR)),
        P((FSDP, TENSOR)),
        P((FSDP, TENSOR)),
        P((FSDP, TENSOR)),
        P((FSDP, TENSOR)),
        P((FSDP, TENSOR)),
        P((FSDP, TENSOR)),
        P((FSDP, TENSOR)),
    )
    return jax.shard_map(
        local_fast if fits(mesh.shape) else local_generic,
        mesh=mesh,
        in_specs=placed,
        out_specs=(
            P(FSDP, TENSOR, None),
            P(FSDP, TENSOR, None),
            P(FSDP, TENSOR),
            P(FSDP, TENSOR),
            P(FSDP, TENSOR),
            P(TENSOR, FSDP),
            P(FSDP, TENSOR),
            P(TENSOR, FSDP),
            P((FSDP, TENSOR)),
            P((FSDP, TENSOR)),
            P((FSDP, TENSOR)),
            P((FSDP, TENSOR)),
            P((FSDP, TENSOR)),
            P((FSDP, TENSOR)),
            P((FSDP, TENSOR)),
            P((FSDP, TENSOR)),
            P((FSDP, TENSOR)),
        ),
        check_vma=False,
    )
```

```python
from functools import partial

import jax
import jax.numpy as jnp
from jax import lax
from jax.experimental import pallas as pl
from jax.experimental.pallas import tpu as pltpu
from jax.sharding import PartitionSpec as P

FSDP, TENSOR = "fsdp", "tensor"

HEAD = 64


epsilon = 1e-05
root_half = 0.7071067811865476
inverse_root_two_pi = 0.3989422804014327


def gelu_value(inner):
    return 0.5 * inner * (1.0 + jax.scipy.special.erf(inner * root_half))


def gelu_slope(inner):
    return 0.5 * (
        1.0 + jax.scipy.special.erf(inner * root_half)
    ) + inner * inverse_root_two_pi * jnp.exp(-0.5 * inner * inner)


def normalize(rows):
    mean = jnp.mean(rows, axis=1, keepdims=True)
    centered = rows - mean
    variance = jnp.mean(centered * centered, axis=1, keepdims=True)
    factor = lax.rsqrt(variance + epsilon)
    return (centered * factor, factor)


def normalize_back(grad_normed, normed, factor):
    return factor * (
        grad_normed
        - jnp.mean(grad_normed, axis=1, keepdims=True)
        - normed * jnp.mean(grad_normed * normed, axis=1, keepdims=True)
    )


def column_sum(rows):
    return jnp.sum(rows.astype(jnp.float32), axis=0)


def dot_rows(left, right):
    return lax.dot_general(
        left, right, (((0,), (0,)), ((), ())), preferred_element_type=jnp.float32
    )


def dot_back(left, right):
    return lax.dot_general(
        left, right, (((1,), (1,)), ((), ())), preferred_element_type=jnp.float32
    )


def place(values, offset, total_length):
    return lax.dynamic_update_slice(jnp.zeros((total_length,), jnp.float32), values, (offset,))


def block_scores(keys, key_valid, query_block):
    raw = jnp.einsum(
        "qhd,khd->hqk", query_block, keys, preferred_element_type=jnp.float32
    ) * HEAD ** (-0.5)
    return jnp.where(key_valid[None, None, :], raw, -1000000000.0)


def attend_forward(keys, values, key_valid, query_block):
    masked = block_scores(keys, key_valid, query_block)
    top = jnp.max(masked, axis=2, keepdims=True)
    expo = jnp.exp(masked - top)
    total = jnp.sum(expo, axis=2, keepdims=True)
    probs = (expo / total).astype(jnp.bfloat16)
    context = jnp.einsum("hqk,khd->qhd", probs, values, preferred_element_type=jnp.float32)
    return (context, top, total)


def attend_backward(keys, values, key_valid, carry, item):
    key_grad, value_grad = carry
    query_block, context_grad_block, top, total = item
    masked = block_scores(keys, key_valid, query_block)
    probs = jnp.exp(masked - top) / total
    probs_low = probs.astype(jnp.bfloat16)
    prob_grad = jnp.einsum(
        "qhd,khd->hqk", context_grad_block, values, preferred_element_type=jnp.float32
    )
    delta = jnp.sum(prob_grad * probs, axis=2, keepdims=True)
    score_grad = (probs * (prob_grad - delta)).astype(jnp.bfloat16)
    factor = HEAD ** (-0.5)
    query_grad = (
        jnp.einsum("hqk,khd->qhd", score_grad, keys, preferred_element_type=jnp.float32) * factor
    )
    key_grad = (
        key_grad
        + jnp.einsum("hqk,qhd->khd", score_grad, query_block, preferred_element_type=jnp.float32)
        * factor
    )
    value_grad = value_grad + jnp.einsum(
        "hqk,qhd->khd", probs_low, context_grad_block, preferred_element_type=jnp.float32
    )
    return ((key_grad, value_grad), query_grad)


def gather_weights(w_query, w_key, w_value, w_output, w_inner, w_outer):
    return (
        lax.all_gather(w_query, FSDP, axis=0, tiled=True),
        lax.all_gather(w_key, FSDP, axis=0, tiled=True),
        lax.all_gather(w_value, FSDP, axis=0, tiled=True),
        lax.all_gather(w_output, FSDP, axis=1, tiled=True),
        lax.all_gather(w_inner, FSDP, axis=0, tiled=True),
        lax.all_gather(w_outer, FSDP, axis=1, tiled=True),
    )


def split_joint(joint_sum, output_sum, inner_sum, outer_sum, head_width):
    return (
        joint_sum[:, :head_width],
        joint_sum[:, head_width : 2 * head_width],
        joint_sum[:, 2 * head_width :],
        output_sum,
        inner_sum,
        outer_sum,
    )


def add_tuples(left, right):
    return tuple((first_item + second_item for first_item, second_item in zip(left, right)))


def local_generic(
    tokens,
    lengths,
    cotangent,
    w_query,
    w_key,
    w_value,
    w_output,
    w_inner,
    w_outer,
    b_query,
    b_value,
    b_output,
    b_inner,
    b_outer,
    gain_first,
    shift_first,
    gain_second,
    shift_second,
):
    tensor_size = lax.axis_size(TENSOR)
    tensor_rank = lax.axis_index(TENSOR)
    micro_count = tokens.shape[0]
    part_rows = tokens.shape[1]
    width = tokens.shape[2]
    seq_rows = part_rows * tensor_size
    head_width = w_query.shape[1]
    inner_width = w_inner.shape[1]
    local_heads = head_width // HEAD
    block_rows = min(512, seq_rows)
    block_count = seq_rows // block_rows
    vector_full = (
        lax.all_gather(b_query, (FSDP, TENSOR), axis=0, tiled=True),
        lax.all_gather(b_value, (FSDP, TENSOR), axis=0, tiled=True),
        lax.all_gather(b_output, (FSDP, TENSOR), axis=0, tiled=True),
        lax.all_gather(b_inner, (FSDP, TENSOR), axis=0, tiled=True),
        lax.all_gather(b_outer, (FSDP, TENSOR), axis=0, tiled=True),
        lax.all_gather(gain_first, (FSDP, TENSOR), axis=0, tiled=True),
        lax.all_gather(shift_first, (FSDP, TENSOR), axis=0, tiled=True),
        lax.all_gather(gain_second, (FSDP, TENSOR), axis=0, tiled=True),
        lax.all_gather(shift_second, (FSDP, TENSOR), axis=0, tiled=True),
    )
    query_bias = lax.dynamic_slice_in_dim(vector_full[0], tensor_rank * head_width, head_width)
    value_bias = lax.dynamic_slice_in_dim(vector_full[1], tensor_rank * head_width, head_width)
    inner_bias = lax.dynamic_slice_in_dim(vector_full[3], tensor_rank * inner_width, inner_width)
    joint_bias = jnp.concatenate([query_bias, jnp.zeros((head_width,), jnp.float32), value_bias])
    grad_query_bias = jnp.zeros((head_width,), jnp.float32)
    grad_value_bias = jnp.zeros((head_width,), jnp.float32)
    grad_inner_bias = jnp.zeros((inner_width,), jnp.float32)
    grad_output_bias = jnp.zeros((width,), jnp.float32)
    grad_outer_bias = jnp.zeros((width,), jnp.float32)
    grad_gain_one = jnp.zeros((width,), jnp.float32)
    grad_shift_one = jnp.zeros((width,), jnp.float32)
    grad_gain_two = jnp.zeros((width,), jnp.float32)
    grad_shift_two = jnp.zeros((width,), jnp.float32)
    local_totals = None
    shard_totals = None
    outputs = []
    input_grads = []
    slot_index = jnp.arange(seq_rows, dtype=jnp.int32)
    part_index = tensor_rank * part_rows + jnp.arange(part_rows, dtype=jnp.int32)
    for micro_index in range(micro_count):
        forward_weights = gather_weights(w_query, w_key, w_value, w_output, w_inner, w_outer)
        joint_w = jnp.concatenate(
            [forward_weights[0], forward_weights[1], forward_weights[2]], axis=1
        )
        output_w = forward_weights[3]
        inner_w = forward_weights[4]
        outer_w = forward_weights[5]
        length = lengths[micro_index]
        key_valid = slot_index < length
        row_valid = (part_index < length).astype(jnp.float32)[:, None]
        own_rows = tokens[micro_index]
        whole = lax.all_gather(own_rows, TENSOR, axis=0, tiled=True)
        joint = (jnp.dot(whole, joint_w, preferred_element_type=jnp.float32) + joint_bias).astype(
            jnp.bfloat16
        )
        query = joint[:, :head_width].reshape(block_count, block_rows, local_heads, HEAD)
        keys = joint[:, head_width : 2 * head_width].reshape(seq_rows, local_heads, HEAD)
        values = joint[:, 2 * head_width :].reshape(seq_rows, local_heads, HEAD)
        context_blocks, tops, totals = lax.map(
            partial(attend_forward, keys, values, key_valid), query
        )
        context_low = context_blocks.reshape(seq_rows, head_width).astype(jnp.bfloat16)
        attended = (
            lax.psum_scatter(
                jnp.dot(context_low, output_w, preferred_element_type=jnp.float32).astype(
                    jnp.bfloat16
                ),
                TENSOR,
                scatter_dimension=0,
                tiled=True,
            ).astype(jnp.float32)
            + vector_full[2]
        )
        normed_first, factor_first = normalize(own_rows.astype(jnp.float32) + attended)
        first = normed_first * vector_full[5] + vector_full[6]
        first_whole = lax.all_gather(first.astype(jnp.bfloat16), TENSOR, axis=0, tiled=True)
        inner = jnp.dot(first_whole, inner_w, preferred_element_type=jnp.float32) + inner_bias
        active = gelu_value(inner).astype(jnp.bfloat16)
        mixed = (
            lax.psum_scatter(
                jnp.dot(active, outer_w, preferred_element_type=jnp.float32).astype(jnp.bfloat16),
                TENSOR,
                scatter_dimension=0,
                tiled=True,
            ).astype(jnp.float32)
            + vector_full[4]
        )
        normed_second, factor_second = normalize(first + mixed)
        outputs.append(
            ((normed_second * vector_full[7] + vector_full[8]) * row_valid).astype(jnp.bfloat16)
        )
        backward_weights = gather_weights(w_query, w_key, w_value, w_output, w_inner, w_outer)
        joint_w = jnp.concatenate(
            [backward_weights[0], backward_weights[1], backward_weights[2]], axis=1
        )
        output_w = backward_weights[3]
        inner_w = backward_weights[4]
        outer_w = backward_weights[5]
        out_grad = cotangent[micro_index].astype(jnp.float32) * row_valid
        grad_gain_two = grad_gain_two + column_sum(out_grad * normed_second)
        grad_shift_two = grad_shift_two + column_sum(out_grad)
        sum_grad = normalize_back(out_grad * vector_full[7], normed_second, factor_second)
        mixed_grad = sum_grad.astype(jnp.bfloat16)
        grad_outer_bias = grad_outer_bias + column_sum(mixed_grad)
        mixed_whole = lax.all_gather(mixed_grad, TENSOR, axis=0, tiled=True)
        outer_sum = dot_rows(active, mixed_whole)
        inner_grad = (dot_back(mixed_whole, outer_w) * gelu_slope(inner)).astype(jnp.bfloat16)
        grad_inner_bias = grad_inner_bias + column_sum(inner_grad)
        inner_sum = dot_rows(first_whole, inner_grad)
        first_grad = sum_grad + lax.psum_scatter(
            dot_back(inner_grad, inner_w).astype(jnp.bfloat16),
            TENSOR,
            scatter_dimension=0,
            tiled=True,
        ).astype(jnp.float32)
        grad_gain_one = grad_gain_one + column_sum(first_grad * normed_first)
        grad_shift_one = grad_shift_one + column_sum(first_grad)
        residual_grad = normalize_back(first_grad * vector_full[5], normed_first, factor_first)
        attended_grad = residual_grad.astype(jnp.bfloat16)
        grad_output_bias = grad_output_bias + column_sum(attended_grad)
        attended_whole = lax.all_gather(attended_grad, TENSOR, axis=0, tiled=True)
        output_sum = dot_rows(context_low, attended_whole)
        context_grad = (
            dot_back(attended_whole, output_w)
            .astype(jnp.bfloat16)
            .reshape(block_count, block_rows, local_heads, HEAD)
        )
        empty = jnp.zeros((seq_rows, local_heads, HEAD), jnp.float32)
        carried, query_grad = lax.scan(
            partial(attend_backward, keys, values, key_valid),
            (empty, empty),
            (query, context_grad, tops, totals),
        )
        joint_grad = jnp.concatenate(
            [
                query_grad.reshape(seq_rows, head_width),
                carried[0].reshape(seq_rows, head_width),
                carried[1].reshape(seq_rows, head_width),
            ],
            axis=1,
        ).astype(jnp.bfloat16)
        grad_query_bias = grad_query_bias + column_sum(joint_grad[:, :head_width])
        grad_value_bias = grad_value_bias + column_sum(joint_grad[:, 2 * head_width :])
        joint_sum = dot_rows(whole, joint_grad)
        input_grads.append(
            residual_grad
            + lax.psum_scatter(
                dot_back(joint_grad, joint_w).astype(jnp.bfloat16),
                TENSOR,
                scatter_dimension=0,
                tiled=True,
            ).astype(jnp.float32)
        )
        batch_sums = (joint_sum, output_sum, inner_sum, outer_sum)
        local_totals = batch_sums if local_totals is None else add_tuples(local_totals, batch_sums)
    pieces = split_joint(
        local_totals[0], local_totals[1], local_totals[2], local_totals[3], head_width
    )
    shard_totals = (
        lax.psum_scatter(pieces[0], FSDP, scatter_dimension=0, tiled=True),
        lax.psum_scatter(pieces[1], FSDP, scatter_dimension=0, tiled=True),
        lax.psum_scatter(pieces[2], FSDP, scatter_dimension=0, tiled=True),
        lax.psum_scatter(pieces[3], FSDP, scatter_dimension=1, tiled=True),
        lax.psum_scatter(pieces[4], FSDP, scatter_dimension=0, tiled=True),
        lax.psum_scatter(pieces[5], FSDP, scatter_dimension=1, tiled=True),
    )
    vector_grads = (
        lax.psum_scatter(
            place(grad_query_bias, tensor_rank * head_width, width),
            (FSDP, TENSOR),
            scatter_dimension=0,
            tiled=True,
        ),
        lax.psum_scatter(
            place(grad_value_bias, tensor_rank * head_width, width),
            (FSDP, TENSOR),
            scatter_dimension=0,
            tiled=True,
        ),
        lax.psum_scatter(grad_output_bias, (FSDP, TENSOR), scatter_dimension=0, tiled=True),
        lax.psum_scatter(
            place(grad_inner_bias, tensor_rank * inner_width, inner_width * tensor_size),
            (FSDP, TENSOR),
            scatter_dimension=0,
            tiled=True,
        ),
        lax.psum_scatter(grad_outer_bias, (FSDP, TENSOR), scatter_dimension=0, tiled=True),
        lax.psum_scatter(grad_gain_one, (FSDP, TENSOR), scatter_dimension=0, tiled=True),
        lax.psum_scatter(grad_shift_one, (FSDP, TENSOR), scatter_dimension=0, tiled=True),
        lax.psum_scatter(grad_gain_two, (FSDP, TENSOR), scatter_dimension=0, tiled=True),
        lax.psum_scatter(grad_shift_two, (FSDP, TENSOR), scatter_dimension=0, tiled=True),
    )
    return (
        jnp.stack(outputs),
        jnp.stack(input_grads),
        shard_totals[0],
        shard_totals[1],
        shard_totals[2],
        shard_totals[3],
        shard_totals[4],
        shard_totals[5],
        vector_grads[0],
        vector_grads[1],
        vector_grads[2],
        vector_grads[3],
        vector_grads[4],
        vector_grads[5],
        vector_grads[6],
        vector_grads[7],
        vector_grads[8],
    )


MESH = pl.DeviceIdType.MESH
WIDTH = 768
HIDDEN = 3072
HALF = WIDTH // 2
KINDS = 3
FLOWS = (
    (0, 0, 512, "zyx", "xyz"),
    (0, 512, 256, "zyx", "xyz"),
    (1, 0, 256, "zxy", "xyz"),
    (1, 256, 512, "zxy", "yxz"),
    (2, 0, 256, "zyx", "yxz"),
    (2, 256, 256, "zyx", "zxy"),
    (2, 512, 256, "yxz", "xzy"),
)
VECTOR_ROWS = 16
SHORT, LONG = 24, 96
ROW_OUTPUT, ROW_OUTER, ROW_GAIN1, ROW_SHIFT1, ROW_GAIN2, ROW_SHIFT2, ROW_INNER = 4, 5, 6, 7, 8, 9, 10
BF16 = jnp.bfloat16
F32 = jnp.float32


def fits(sizes):
    fsdp = sizes[FSDP]
    return sizes[TENSOR] == 4 and fsdp == WIDTH // LONG


class Place:
    def __init__(self, nz):
        self.f = lax.axis_index(FSDP)
        self.t = lax.axis_index(TENSOR)
        self.nz = nz
        self.z = self.f // 2
        self.x = self.f % 2
        self.y = self.t // 2
        self.c = self.t % 2
        self.core = (self.f, self.t + 1 - 2 * self.c)
        self.along_y = (self.f, self.t + 2 - 4 * self.y)
        self.along_x = (self.f + 1 - 2 * self.x, self.t)

    def z_at(self, step):
        return (self.z + step) % self.nz

    def z_back(self, step):
        return (self.z + self.nz - step) % self.nz

    def along_z(self, step):
        return (self.z_at(step) * 2 + self.x, self.t)

    def in_group(self, step):
        return (self.f, (self.t + step) % 4)


class Trip:
    def __init__(self, copy, send_sem, recv_sem):
        self.copy, self.send_sem, self.recv_sem = copy, send_sem, recv_sem

    def start(self):
        self.copy.start()

    def wait_recv(self):
        self.copy.wait_recv()


class Net:
    def __init__(self, send_sems, recv_sems):
        self.send_sems, self.recv_sems = send_sems, recv_sems
        self.sends = self.recvs = 0

    def lane(self):
        self.sends += 1
        return self.send_sems.at[self.sends - 1]

    def door(self):
        self.recvs += 1
        return self.recv_sems.at[self.recvs - 1]

    def plan(self, source, target, device, lane, door=None):
        door = self.door() if door is None else door
        copy = pltpu.make_async_remote_copy(
            src_ref=source, dst_ref=target, send_sem=lane, recv_sem=door, device_id=device, device_id_type=MESH
        )
        return Trip(copy, lane, door)

    def keep(self, ref, device, lane, door=None):
        return self.plan(ref, ref, device, lane, door)


class Meter:
    def __init__(self, low, wide):
        self.low, self.wide = low, wide

    def low_rows(self, rows):
        for count in (1, 2, 3, 4):
            if rows % (16 * count) == 0 and rows // count <= self.low.shape[1]:
                return self.low.at[0:count, 0:rows // count]
        raise ValueError(rows)

    def tiles(self, count):
        return self.wide.at[0:8 * count]


def arrived(trips, size):
    pltpu.make_async_copy(size, size, trips[0].recv_sem).wait()


def departed(trips, size):
    pltpu.make_async_copy(size, size, trips[0].send_sem).wait()


def start_all(copies):
    for copy in copies:
        copy.start()


def greet(place):
    barrier = pltpu.get_barrier_semaphore()
    peers = [place.in_group(1), place.in_group(2), place.in_group(3), place.along_x]
    peers += [place.along_z(step) for step in range(1, place.nz)]
    for peer in peers:
        pl.semaphore_signal(barrier, inc=1, device_id=peer, device_id_type=MESH)
    pl.semaphore_wait(barrier, len(peers))


def wait_local(copies):
    for copy in copies:
        copy.wait()


def dot(left, right):
    return lax.dot_general(left, right, (((1,), (0,)), ((), ())), preferred_element_type=F32)


def turn(value, shift):
    shift %= value.shape[1]
    return pltpu.roll(value, shift, 1) if shift else value


class Layer:
    def __init__(self, refs, length):
        (
            self.w, self.rows, self.back, self.rows_turned, self.joint, self.probs, self.context, self.acc,
            self.normed, self.factor, self.first_low, self.first_turned, self.active, self.slope, self.grad_low,
            self.grad_turned, self.out, self.vec, self.sums,
        ) = refs
        self.length = length
        self.seq = self.rows.shape[0]
        self.block = 128

    def weight(self, kind, t):
        return self.w[kind, t // 2, t % 2].reshape(WIDTH, WIDTH)

    def output_weight(self, t):
        return self.w[0, t // 2, t % 2, :, :, :, 512:768].reshape(WIDTH, 256)

    def store_grad(self, kind, t, value):
        nz = self.w.shape[3]
        self.w[kind, t // 2, t % 2] = value.astype(BF16).reshape(nz, 2, WIDTH // (2 * nz), WIDTH)

    def row(self, index):
        return self.vec[pl.ds(index, 1), :]

    def blocks(self, body):
        def step(i, carry):
            body(pl.ds(pl.multiple_of(i * self.block, self.block), self.block), i)
            return carry

        lax.fori_loop(0, self.seq // self.block, step, 0)

    def row_valid(self, i):
        index = lax.broadcasted_iota(jnp.int32, (self.block, 1), 0) + i * self.block
        return (index < self.length).astype(F32)

    def lanes(self, low, high, width):
        lane = lax.broadcasted_iota(jnp.int32, (1, width), 1)
        return (lane >= low) & (lane < high)

    def pick(self, value, low, high):
        return jnp.where(self.lanes(low, high, value.shape[1]), value, jnp.zeros_like(value))

    def head_query(self, t, h):
        return self.joint[t, :, 0:128] if h < 2 else self.joint[t, :, 384:512]

    def head_key(self, t, h):
        return self.joint[t, :, 128:256] if h < 2 else self.joint[t, :, 640:768]

    def head_side(self, value, h):
        return self.pick(value, 0, 64) if h == 0 else self.pick(value, 64, 128)

    def head_value(self, t, h):
        return self.pick(self.joint[t, :, 256:512], h * 64, h * 64 + 64)

    def unpack(self, v):
        nz = v.shape[2]
        short = jnp.zeros((8, WIDTH), F32)
        inner = [jnp.zeros((1, WIDTH), F32) for _ in range(4)]
        for f in range(2 * nz):
            for t in range(4):
                rank = f * 4 + t
                block = v[t // 2, t % 2, f // 2, f % 2]
                wide = jnp.concatenate([self.pick(block, 0, SHORT), jnp.zeros((8, WIDTH - 128), F32)], axis=1)
                short += turn(wide, rank * SHORT)
                wide = jnp.concatenate([self.pick(block[0:1], 32, 128), jnp.zeros((1, WIDTH - 128), F32)], axis=1)
                inner[rank * LONG // WIDTH] += turn(wide, rank * LONG % WIDTH - 32)
        for t in range(4):
            query = self.pick(turn(short[0:1], -192 * t), 0, 128) + self.pick(turn(short[0:1], 320 - 192 * t), 448, 512)
            self.vec[t:t + 1] = query + self.pick(turn(short[1:2], 256 - 192 * t), 256, 448)
            self.vec[ROW_INNER + t:ROW_INNER + t + 1] = inner[t]
        self.vec[ROW_OUTPUT:ROW_INNER] = short[2:8]

    def pack(self, parts):
        nz = parts.shape[2]
        query, value = jnp.zeros((1, WIDTH), F32), jnp.zeros((1, WIDTH), F32)
        for t in range(4):
            row = self.sums[t:t + 1]
            query += turn(self.pick(row, 0, 128), 192 * t) + turn(self.pick(row, 448, 512), 192 * t - 320)
            value += turn(self.pick(row, 256, 448), 192 * t - 256)
        short = jnp.concatenate([query, value, self.sums[ROW_OUTPUT:ROW_INNER]], axis=0)
        top = lax.broadcasted_iota(jnp.int32, (8, 1), 0) == 0
        for f in range(2 * nz):
            for t in range(4):
                rank = f * 4 + t
                block = self.pick(turn(short, -rank * SHORT)[:, 0:128], 0, SHORT)
                index = ROW_INNER + rank * LONG // WIDTH
                inner = turn(self.sums[index:index + 1], 32 - rank * LONG % WIDTH)[:, 0:128]
                inner = jnp.broadcast_to(self.pick(inner, 32, 128), (8, 128))
                parts[t // 2, t % 2, f // 2, f % 2] = block + jnp.where(top, inner, 0.0)

    def project(self, t):
        self.joint[t] = (dot(self.rows[...], self.weight(0, t)) + self.row(t)).astype(BF16)

    def attend(self, t):
        key_valid = lax.broadcasted_iota(jnp.int32, (1, self.seq), 1) < self.length
        context = None
        for h in range(3):
            raw = dot_back(self.head_query(t, h), self.head_side(self.head_key(t, h), h))
            masked = jnp.where(key_valid, raw * HEAD ** -0.5, -1e9)
            expo = jnp.exp(masked - jnp.max(masked, axis=1, keepdims=True))
            probs = (expo * (1.0 / jnp.sum(expo, axis=1, keepdims=True))).astype(BF16)
            self.probs[t * 3 + h] = probs
            part = dot(probs, self.head_value(t, h))
            context = part if context is None else context + part
        low = context.astype(BF16)
        self.context[t] = low
        self.acc[...] += dot_back(low, self.output_weight(t))

    def start(self):
        def body(rows, i):
            self.acc[rows] = self.rows[rows].astype(F32) + self.row(ROW_OUTPUT)

        self.blocks(body)

    def norm_first(self):
        def body(rows, i):
            normed, factor = normalize(self.acc[rows])
            self.normed[rows] = normed
            self.factor[rows] = jnp.broadcast_to(factor, (self.block, 128))
            first = normed * self.row(ROW_GAIN1) + self.row(ROW_SHIFT1)
            self.first_low[rows] = first.astype(BF16)
            self.acc[rows] = first + self.row(ROW_OUTER)

        self.blocks(body)

    def feed_inner(self, t):
        inner = dot(self.first_low[...], self.weight(1, t)) + self.row(ROW_INNER + t)
        gate = 1.0 + lax.erf(inner * root_half)
        self.active[t] = (0.5 * inner * gate).astype(BF16)
        self.slope[t] = (0.5 * gate + inner * inverse_root_two_pi * jnp.exp(-0.5 * inner * inner)).astype(BF16)

    def feed_outer(self, t):
        self.acc[...] += dot_back(self.active[t], self.weight(2, t))

    def clear_sums(self):
        self.sums[...] = jnp.zeros_like(self.sums)

    def add_sum(self, index, value):
        self.sums[pl.ds(index, 1), :] += jnp.sum(value, axis=0, keepdims=True)

    def norm_second(self):
        def body(rows, i):
            normed, factor = normalize(self.acc[rows])
            valid = self.row_valid(i)
            gain = self.row(ROW_GAIN2)
            self.out[rows] = ((normed * gain + self.row(ROW_SHIFT2)) * valid).astype(BF16)
            out_grad = self.back[rows].astype(F32) * valid
            self.add_sum(ROW_GAIN2, out_grad * normed)
            self.add_sum(ROW_SHIFT2, out_grad)
            sum_grad = normalize_back(out_grad * gain, normed, factor)
            self.acc[rows] = sum_grad
            low = sum_grad.astype(BF16)
            self.grad_low[rows] = low
            self.add_sum(ROW_OUTER, low.astype(F32))

        self.blocks(body)
        self.grad_turned[...] = self.grad_low[...].T

    def outer_back(self, t):
        grad = (dot(self.grad_low[...], self.weight(2, t)) * self.slope[t].astype(F32)).astype(BF16)
        self.slope[t] = grad
        self.add_sum(ROW_INNER + t, grad.astype(F32))
        self.store_grad(2, t, dot(self.grad_turned[...], self.active[t]))

    def inner_back(self, t):
        grad = self.slope[t]
        self.acc[...] += dot_back(grad, self.weight(1, t))
        self.store_grad(1, t, dot(self.first_turned[...], grad))

    def norm_first_back(self):
        def body(rows, i):
            grad = self.acc[rows]
            normed = self.normed[rows]
            self.add_sum(ROW_GAIN1, grad * normed)
            self.add_sum(ROW_SHIFT1, grad)
            residual = normalize_back(grad * self.row(ROW_GAIN1), normed, self.factor[rows][:, 0:1])
            self.acc[rows] = residual
            low = residual.astype(BF16)
            self.grad_low[rows] = low
            self.add_sum(ROW_OUTPUT, low.astype(F32))

        self.blocks(body)
        self.grad_turned[...] = self.grad_low[...].T

    def attend_back(self, t):
        context_grad = self.pick(dot(self.grad_low[...], self.output_weight(t)), 0, 192).astype(BF16)
        query_grads, key_grads, value_grad = [], [], None
        for h in range(3):
            probs = self.probs[t * 3 + h]
            prob_grad = dot_back(context_grad, self.head_value(t, h))
            wide = probs.astype(F32)
            delta = jnp.sum(wide * prob_grad, axis=1, keepdims=True)
            score_grad = (wide * (prob_grad - delta)).astype(BF16)
            query_grads.append(dot(score_grad, self.head_side(self.head_key(t, h), h)) * HEAD ** -0.5)
            key_grads.append(dot_rows(score_grad, self.head_side(self.head_query(t, h), h)) * HEAD ** -0.5)
            part = dot_rows(probs, self.pick(context_grad, h * 64, h * 64 + 64))
            value_grad = part if value_grad is None else value_grad + part
        self.joint[t, :, 0:128] = (query_grads[0] + query_grads[1]).astype(BF16)
        self.joint[t, :, 128:256] = (key_grads[0] + key_grads[1]).astype(BF16)
        self.joint[t, :, 256:384] = value_grad[:, 0:128].astype(BF16)
        self.joint[t, :, 384:512] = (value_grad[:, 128:256] + query_grads[2]).astype(BF16)
        self.joint[t, :, 512:640] = jnp.zeros((self.seq, 128), BF16)
        self.joint[t, :, 640:768] = key_grads[2].astype(BF16)

    def joint_back(self, t):
        joint = self.joint[t]
        self.sums[pl.ds(t, 1), :] = jnp.sum(joint.astype(F32), axis=0, keepdims=True)
        self.acc[...] += dot_back(joint, self.weight(0, t))
        nz = self.w.shape[3]
        shape = (nz, 2, WIDTH // (2 * nz), -1)
        main = dot(self.rows_turned[...], joint[:, 0:512])
        side = dot(self.rows_turned[...], joint[:, 512:768]) + dot(self.grad_turned[...], self.context[t])
        self.w[0, t // 2, t % 2, :, :, :, 0:512] = main.astype(BF16).reshape(shape[:3] + (512,))
        self.w[0, t // 2, t % 2, :, :, :, 512:768] = side.astype(BF16).reshape(shape[:3] + (256,))

    def finish(self):
        def body(rows, i):
            self.back[rows] = self.acc[rows].astype(BF16)

        self.blocks(body)


def each(count, body):
    def step(i, carry):
        body(i)
        return carry

    lax.fori_loop(0, count, step, 0)


BUFFER_COUNT = 19


def buffer_shapes(nz, seq):
    part = WIDTH // (2 * nz)
    low, wide = (seq, WIDTH), (WIDTH, seq)
    shapes = [
        ((KINDS, 2, 2, nz, 2, part, WIDTH), BF16),
        (low, BF16),
        (low, BF16),
        (wide, BF16),
        ((4, seq, WIDTH), BF16),
        ((12, seq, seq), BF16),
        ((4, seq, 256), BF16),
        (low, F32),
        (low, F32),
        ((seq, 128), F32),
        (low, BF16),
        (wide, BF16),
        ((4, seq, WIDTH), BF16),
        ((4, seq, WIDTH), BF16),
        (low, BF16),
        (wide, BF16),
        (low, BF16),
        ((VECTOR_ROWS, WIDTH), F32),
        ((VECTOR_ROWS, WIDTH), F32),
    ]
    return [pltpu.VMEM(*shape) for shape in shapes]


BLOCKS = 15
SEND_COUNT = 15
DOOR_COUNT = 227


def flow_shapes(nz):
    part = WIDTH // (2 * nz)
    shapes = [pltpu.VMEM((KINDS, 2, nz, 2, part, WIDTH), BF16)]
    return shapes + [pltpu.VMEM((BLOCKS, part, flow[2]), BF16) for flow in FLOWS]


def axis_steps(place, axis):
    p = place
    if axis == "x":
        return [(1, 1 - p.x, p.along_x, 1 - p.x)]
    if axis == "y":
        return [(1, 1 - p.y, p.along_y, 1 - p.y)]
    return [(step, p.z_at(step), p.along_z(step), p.z_back(step)) for step in range(1, p.nz)]


class Flow:
    def __init__(self, net, place, order, own, region, lane, core_lane, core_door):
        p = place
        self.pieces = [(None, [])]
        spots = [({"x": p.x, "y": p.y, "z": p.z}, own)]
        for axis in order:
            for index, (spot, source) in enumerate(list(spots)):
                for _, _, device, behind in axis_steps(p, axis):
                    trip = net.plan(region(spot) if source is None else source, region(spot), device, lane)
                    self.pieces[index][1].append(trip)
                    self.pieces.append((trip, []))
                    spots.append(({**spot, axis: behind}, None))
        mine = {"x": p.x, "y": p.y, "z": p.z}[order[2]]
        sides = [mine] + [behind for _, _, _, behind in axis_steps(p, order[2])]
        every = slice(None)
        self.cores = [
            net.keep(region({"x": every, "y": every, "z": every, order[2]: side}), p.core, core_lane, core_door)
            for side in sides
        ]
        self.trips = [trip for _, onward in self.pieces for trip in onward]

    def first(self):
        start_all(self.pieces[0][1])

    def piece(self, index):
        trip, onward = self.pieces[index]
        trip.wait_recv()
        start_all(onward)

    def to_core(self, index):
        self.cores[index].start()


class Cores:
    def __init__(self, net, place, w, core, k, meter):
        self.place, self.meter = place, meter
        self.w, self.core = w.at[k], core.at[k]
        self.ys = (1 - place.y, place.y)
        steps = list(range(1, place.nz)) + [0]
        self.parts = steps[:place.nz // 2], steps[place.nz // 2:]
        self.c = []
        lane = net.lane()
        for y in self.ys:
            for part in self.parts:
                door = net.door()
                spots = [place.z_at(step) for step in part]
                self.c.append([
                    net.plan(self.w.at[y, 1 - place.c, z], self.core.at[y, z], place.core, lane, door) for z in spots
                ])
        self.trips = [trip for trips in self.c for trip in trips]

    def to_core(self, half):
        start_all(self.c[2 * half] + self.c[2 * half + 1])

    def half(self, half, part):
        y = self.ys[half]
        trips = self.c[2 * half + part]
        arrived(trips, self.meter.low_rows(2 * self.core.shape[-2] * len(trips)))
        for step in self.parts[part]:
            z = self.place.z_at(step)
            target, source = self.core.at[y, z], self.w.at[y, self.place.c, z]
            target[...] = (target[...].astype(F32) + source[...].astype(F32)).astype(BF16)


class Sink:
    def __init__(self, net, place, order, core, landing, result, cols, lane, meter):
        p = place
        self.meter = meter
        self.core, self.landing, self.result, self.cols = core, landing, result, cols
        here = {"x": p.x, "y": p.y, "z": p.z}
        ahead = {axis: {0: here[axis], **{step: spot for step, spot, _, _ in axis_steps(p, axis)}} for axis in here}
        sizes = {"x": 2, "y": 2, "z": p.nz}
        self.spot = lambda block: tuple(ahead[axis][block[axis]] for axis in ("y", "z", "x"))
        self.order = order
        self.tasks = []
        self.starts = [[], [], [], []]
        blocks = [{}]
        for axis in ("y", "z", "x"):
            steps = [i for i in range(1, sizes[axis])] + [0]
            blocks = [{**block, axis: step} for block in blocks for step in steps]
        slot = 0
        self.trips = []
        waits = {}
        for stage, axis in enumerate(order):
            later = order[stage + 1:]
            kept = [block for block in blocks if block[axis] == 0]
            kept.sort(key=lambda block: [block[other] == 0 for other in later])
            devices = {step: device for step, _, device, _ in axis_steps(p, axis)}
            for block in kept:
                arrivals = []
                door = net.door()
                for step in range(1, sizes[axis]):
                    away = {**block, axis: step}
                    copy = net.plan(self.part(away), landing.at[slot], devices[step], lane, door)
                    self.trips.append(copy)
                    if stage == 0:
                        soon = 0 < away["z"] <= p.nz // 2
                        self.starts[(0 if away["y"] else 2) + (0 if soon else 1)].append(copy)
                    else:
                        waits[tuple(sorted(away.items()))].append(copy)
                    arrivals.append((copy, slot))
                    slot += 1
                onward = []
                waits[tuple(sorted(block.items()))] = onward
                self.tasks.append((block, arrivals, onward))
            blocks = kept

    def part(self, block):
        return self.core.at[(*self.spot(block), slice(None), self.cols)]

    def start(self, half, part):
        start_all(self.starts[2 * half + part])

    def add(self, index):
        block, arrivals, onward = self.tasks[index]
        target = self.part(block)
        total = target[...].astype(F32)
        rows = self.landing.shape[1] * self.landing.shape[2] // WIDTH
        arrived([trip for trip, _ in arrivals], self.meter.low_rows(rows * len(arrivals)))
        for _, slot in arrivals:
            total += self.landing[slot].astype(F32)
        if index < len(self.tasks) - 1:
            target[...] = total.astype(BF16)
            start_all(onward)
        else:
            self.result[:, self.cols] = total


class Back:
    def __init__(self, net, place, parts, landings, result, meter):
        p = self.place = place
        self.parts, self.result, self.meter = parts, result, meter
        self.core, self.side, self.pair, self.line = landings
        lane = net.lane()
        self.c = net.plan(parts.at[:, 1 - p.c], self.core, p.core, lane)
        self.y = net.plan(self.core.at[1 - p.y], self.side, p.along_y, lane)
        self.x = net.plan(self.side.at[:, 1 - p.x], self.pair, p.along_x, lane)
        door = net.door()
        self.z = [
            net.plan(self.pair.at[p.z_at(step)], self.line.at[step - 1], p.along_z(step), lane, door)
            for step in range(1, p.nz)
        ]

    def first(self):
        self.c.start()

    def core_done(self):
        self.c.wait_recv()
        self.core[...] += self.parts[:, self.place.c]
        self.y.start()

    def y_done(self):
        self.y.wait_recv()
        self.side[...] += self.core[self.place.y]
        self.x.start()

    def x_done(self):
        self.x.wait_recv()
        self.pair[...] += self.side[:, self.place.x]
        start_all(self.z)

    def z_done(self):
        arrived(self.z, self.meter.tiles(len(self.z)))
        total = self.pair[self.place.z]
        for i in range(self.place.nz - 1):
            total += self.line[i]
        self.result[...] = total

    def sent(self):
        departed([self.c, self.y, self.x] + self.z, self.meter.tiles(8 * self.place.nz - 1))


def ticks(i, table):
    for when, actions in table.items():
        @pl.when(i == when)
        def _(actions=actions):
            for action, *given in actions:
                action(*given)


def layer_kernel(nz, *refs):
    tokens, lengths, cotangent, w_query, w_key, w_value, w_output, w_inner, w_outer = refs[:9]
    short_in, long_in = refs[9:12] + refs[13:18], refs[12]
    result_out, outs, backs, totals_out = refs[18:22]
    rest = list(refs[22:])
    buffers, rest = rest[:BUFFER_COUNT], rest[BUFFER_COUNT:]
    core_landing, landings, rest = rest[0], rest[1:1 + len(FLOWS)], rest[1 + len(FLOWS):]
    back_landings = rest[:4]
    v, parts, vec_in, raw_query, raw_key, raw_value, raw_output, own_joint = rest[4:12]
    raw_short, raw_long, result, totals = rest[12:20], rest[20], rest[21], rest[22]
    send_sems, recv_sems, local_sems = rest[23:]
    place = Place(nz)
    net = Net(send_sems, recv_sems)
    t = place.t
    quarter = tokens.shape[1]
    layer = Layer(buffers, lengths[t])
    owns = (own_joint, w_inner, w_outer)
    g, r = [], []
    meter = Meter(layer.joint, layer.factor)
    cores = [Cores(net, place, layer.w, core_landing, k, meter) for k in range(KINDS)]
    lanes = [[net.lane() for k in range(KINDS)] for _ in range(3)]
    doors = [net.door() for k in range(KINDS)]
    for (k, first, width, order_in, order_out), landing in zip(FLOWS, landings):
        cols = pl.ds(first, width)

        def region(spot, k=k, cols=cols):
            return layer.w.at[k, spot["y"], place.c, spot["z"], spot["x"], :, cols]

        g.append(Flow(net, place, order_in, owns[k].at[:, cols], region, lanes[0][k], lanes[1][k], doors[k]))
        sink = (core_landing.at[k], landing, result.at[k], cols, lanes[2][k], meter)
        r.append(Sink(net, place, order_out, *sink))
    one = net.lane()
    vecs = Flow(
        net, place, FLOWS[0][3], vec_in, lambda spot: v.at[spot["y"], place.c, spot["z"], spot["x"]],
        one, one, net.door(),
    )
    sums = Back(net, place, parts, back_landings, totals, meter)

    def of_kind(flows, k):
        return [flow for flow, row in zip(flows, FLOWS) if row[0] == k]

    def trips_of(flows):
        return [trip for flow in flows for trip in flow.trips]

    def cores_of(flows):
        return [trip for flow in flows for trip in flow.cores]

    def gathered(k):
        arrived(cores_of(of_kind(g, k)), meter.low_rows(2 * WIDTH))

    def passed_on(k):
        flows = of_kind(g, k)
        departed(trips_of(flows), meter.low_rows(2 * WIDTH - own_joint.shape[0]))
        departed(cores_of(flows), meter.low_rows(2 * WIDTH))

    def reduced(k):
        departed(trips_of(of_kind(r, k)), meter.low_rows(2 * WIDTH - own_joint.shape[0]))
        departed(cores[k].trips, meter.low_rows(2 * WIDTH))

    def vectors_in():
        arrived(vecs.cores, meter.tiles(4 * nz))

    def vectors_sent():
        departed(vecs.trips + vecs.cores, meter.tiles(8 * nz - 1))

    def quarter_of(ref, index):
        return ref.at[pl.ds(pl.multiple_of(index * quarter, quarter), quarter)]

    swap_lane = net.lane()

    def swap(source, target):
        door = net.door()
        return [net.plan(source(step), target, place.in_group(step), swap_lane, door) for step in (2, 1, 3)]

    def swapped(trips):
        arrived(trips, meter.low_rows(3 * quarter))

    token_in = swap(lambda step: tokens.at[(t + step) % 4], quarter_of(layer.rows, t))
    back_in = swap(lambda step: cotangent.at[(t + step) % 4], quarter_of(layer.back, t))
    out_out = swap(lambda step: quarter_of(layer.out, (t + step) % 4), outs.at[t])
    back_out = swap(lambda step: quarter_of(layer.back, (t + step) % 4), backs.at[t])

    def swaps_sent():
        departed(token_in + back_in + out_out + back_out, meter.low_rows(12 * quarter))

    pairs = [
        (tokens.at[t], quarter_of(layer.rows, t)),
        (cotangent.at[t], quarter_of(layer.back, t)),
        *[
            (own, layer.w.at[k, place.y, place.c, place.z, place.x])
            for k, own in enumerate(owns)
        ],
        (vec_in, v.at[place.y, place.c, place.z, place.x]),
        (quarter_of(layer.out, t), outs.at[t]),
        (quarter_of(layer.back, t), backs.at[t]),
        *[(result.at[k], result_out.at[k]) for k in range(KINDS)],
        (totals, totals_out),
        (w_query, raw_query),
        (w_key, raw_key),
        (w_value, raw_value),
        (w_output, raw_output),
        *zip(short_in, raw_short),
        (long_in, raw_long),
    ]
    local = [pltpu.make_async_copy(*pair, local_sems.at[i]) for i, pair in enumerate(pairs)]

    def pack_vectors():
        vec_in[...] = jnp.zeros((8, 128), F32)
        for i, ref in enumerate(raw_short):
            vec_in[i:i + 1, 0:SHORT] = ref[...].reshape(1, SHORT)
        vec_in[0:1, 32:128] = raw_long[...].reshape(1, LONG)

    def pack_own():
        own_joint[...] = pack_joint(raw_query[...], raw_key[...], raw_value[...], raw_output[...].T)

    def near(i):
        return (place.y + i) % 2 * 2 + (place.c + i // 2) % 2

    def order(i):
        return (1 - place.y + i // 2) % 2 * 2 + (1 - place.c + i) % 2

    start_all(local[12:])
    greet(place)
    wait_local(local[12:])
    pack_vectors()
    pack_own()
    vecs.first()
    g[1].first()
    g[0].first()
    start_all(local[:6])
    wait_local(local[:6])
    start_all(token_in)
    vecs.piece(4)
    vecs.piece(8)
    g[1].piece(4)
    g[1].piece(8)
    vecs.piece(2)
    vecs.piece(1)
    vecs.piece(3)
    g[0].piece(4)
    vecs.piece(12)
    g[0].piece(8)
    g[1].piece(12)
    vecs.piece(10)
    vecs.piece(9)
    vecs.piece(11)
    g[1].piece(1)
    g[1].piece(2)
    g[0].piece(12)
    g[1].piece(3)
    g[1].piece(9)
    g[1].piece(10)
    g[1].piece(11)
    swapped(token_in)
    vecs.piece(6)
    vecs.piece(5)
    vecs.piece(7)
    vecs.to_core(0)
    g[0].piece(1)
    g[2].first()
    g[3].first()
    g[1].piece(5)
    vecs.piece(14)
    vecs.piece(13)
    vecs.piece(15)
    vecs.to_core(1)
    g[1].piece(6)
    vectors_in()
    layer.unpack(v)
    layer.start()
    layer.rows_turned[...] = layer.rows[...].T
    layer.clear_sums()
    g[1].piece(7)
    g[1].to_core(0)
    g[0].piece(2)
    g[0].piece(9)
    g[0].piece(3)
    g[0].piece(5)
    g[2].piece(4)
    g[2].piece(8)
    g[3].piece(4)
    g[2].piece(1)
    g[3].piece(8)
    g[1].piece(13)
    g[2].piece(2)
    g[1].piece(14)
    g[2].piece(3)
    g[0].piece(6)
    g[1].piece(15)
    g[1].to_core(1)
    g[0].piece(7)
    g[0].to_core(0)
    g[0].piece(10)
    g[2].piece(12)
    g[0].piece(11)
    g[3].piece(1)
    g[4].first()
    g[5].first()
    g[6].first()
    g[3].piece(12)
    g[3].piece(2)
    g[2].piece(9)
    g[0].piece(13)
    g[2].piece(10)
    g[2].piece(5)
    g[3].piece(3)
    g[2].piece(11)
    g[2].piece(6)
    g[2].piece(7)
    g[2].to_core(0)
    g[3].piece(9)
    g[4].piece(4)
    g[0].piece(14)
    g[4].piece(1)
    g[5].piece(4)
    g[4].piece(2)
    g[4].piece(3)
    g[6].piece(1)
    g[0].piece(15)
    g[0].to_core(1)
    def project(i):
        layer.project(near(i))
        ticks(i, {
            1: [(g[3].piece, 10), (g[3].piece, 5), (gathered, 0)],
            2: [(g[2].piece, 13), (g[5].piece, 1), (g[4].piece, 8)],
        })

    each(4, project)
    g[5].piece(8)
    g[5].piece(2)
    def attend(i):
        layer.attend(i)
        ticks(i, {
            0: [(g[3].piece, 11), (g[2].piece, 14), (g[6].piece, 2), (g[5].piece, 3)],
            1: [(g[2].piece, 15), (g[2].to_core, 1), (g[3].piece, 6), (g[4].piece, 5), (g[6].piece, 4)],
            2: [(g[3].piece, 7), (g[3].to_core, 0), (g[6].piece, 5), (g[4].piece, 6), (g[6].piece, 6), (g[4].piece, 7), (g[4].to_core, 0), (g[4].piece, 12)],
        })

    each(4, attend)
    g[3].piece(13)
    g[4].piece(9)
    g[5].piece(12)
    g[5].piece(5)
    g[6].piece(7)
    g[4].piece(10)
    layer.norm_first()
    layer.first_turned[...] = layer.first_low[...].T
    g[6].piece(8)
    g[5].piece(6)
    g[6].piece(9)
    g[4].piece(11)
    g[5].piece(7)
    g[5].to_core(0)
    g[6].piece(3)
    g[6].to_core(0)
    start_all(back_in)
    g[5].piece(9)
    g[6].piece(10)
    g[6].piece(11)
    g[3].piece(14)
    g[6].piece(12)
    g[5].piece(10)
    g[5].piece(11)
    g[3].piece(15)
    g[3].to_core(1)
    g[4].piece(13)
    def feed_inner(i):
        layer.feed_inner(near(i))
        ticks(i, {
            0: [(g[4].piece, 14)],
            1: [(g[4].piece, 15), (g[4].to_core, 1), (g[6].piece, 13), (g[6].to_core, 1), (gathered, 1)],
            2: [(g[5].piece, 13), (g[6].piece, 14), (g[6].to_core, 2), (g[6].piece, 15), (g[6].to_core, 3)],
        })

    each(4, feed_inner)
    g[5].piece(14)
    g[5].piece(15)
    g[5].to_core(1)
    def feed_outer(i):
        layer.feed_outer(near(i))
        ticks(i, {
            1: [(gathered, 2)],
        })

    each(4, feed_outer)
    swapped(back_in)
    layer.norm_second()
    start_all(out_out)
    local[6].start()
    passed_on(2)
    def outer_back(i):
        layer.outer_back(order(i))
        ticks(i, {
            0: [(cores[2].to_core, 0)],
            1: [(cores[2].half, 0, 0), (r[6].start, 0, 0), (r[5].start, 0, 0), (r[4].start, 0, 0)],
            2: [(cores[2].to_core, 1), (cores[2].half, 0, 1), (r[6].start, 0, 1), (r[5].start, 0, 1), (r[4].start, 0, 1)],
        })

    each(4, outer_back)
    cores[2].half(1, 0)
    r[6].start(1, 0)
    r[5].start(1, 0)
    r[4].start(1, 0)
    r[6].add(0)
    r[6].add(1)
    passed_on(1)
    def inner_back(i):
        layer.inner_back(order(i))
        ticks(i, {
            0: [(cores[1].to_core, 0), (cores[2].half, 1, 1), (r[6].start, 1, 1), (r[5].start, 1, 1), (r[4].start, 1, 1), (r[6].add, 2), (r[6].add, 6)],
            1: [(cores[1].half, 0, 0), (r[2].start, 0, 0), (r[3].start, 0, 0), (r[6].add, 3), (r[4].add, 0), (r[6].add, 4), (r[4].add, 1)],
            2: [(cores[1].to_core, 1), (cores[1].half, 0, 1), (r[2].start, 0, 1), (r[3].start, 0, 1), (r[6].add, 5), (r[4].add, 4), (r[6].add, 7), (r[4].add, 5)],
        })

    each(4, inner_back)
    cores[1].half(1, 0)
    r[2].start(1, 0)
    r[3].start(1, 0)
    r[2].add(0)
    r[2].add(1)
    r[4].add(2)
    r[5].add(0)
    r[4].add(3)
    layer.norm_first_back()
    cores[1].half(1, 1)
    r[2].start(1, 1)
    r[3].start(1, 1)
    r[4].add(8)
    r[4].add(6)
    r[4].add(9)
    r[4].add(7)
    r[5].add(2)
    vectors_sent()
    passed_on(0)
    def attend_back(i):
        layer.attend_back(order(i))
        ticks(i, {
            0: [(r[2].add, 2), (r[2].add, 3), (r[2].add, 4), (r[3].add, 0)],
            1: [(r[2].add, 6), (r[5].add, 4), (r[4].add, 11), (r[3].add, 4), (r[3].add, 5)],
            2: [(r[5].add, 1), (r[5].add, 3), (r[3].add, 8), (r[3].add, 3), (r[3].add, 9)],
            3: [(r[2].add, 8), (r[2].add, 9), (r[0].add, 0), (r[6].add, 9), (r[3].add, 7)],
        })
        layer.joint_back(order(i))
        ticks(i, {
            0: [(cores[0].to_core, 0), (r[2].add, 5), (r[4].add, 10), (r[3].add, 1)],
            1: [(cores[0].half, 0, 0), (r[1].start, 0, 0), (r[0].start, 0, 0), (cores[0].half, 0, 1), (r[1].start, 0, 1), (r[0].start, 0, 1), (r[2].add, 7), (r[3].add, 2)],
            2: [(cores[0].to_core, 1), (r[1].add, 0), (r[6].add, 8), (r[1].add, 1), (r[3].add, 6)],
        })

    each(4, attend_back)
    cores[0].half(1, 0)
    r[1].start(1, 0)
    r[0].start(1, 0)
    cores[0].half(1, 1)
    r[1].start(1, 1)
    r[0].start(1, 1)
    r[2].add(10)
    r[2].add(11)
    r[0].add(1)
    r[1].add(2)
    layer.pack(parts)
    sums.first()
    r[1].add(3)
    layer.finish()
    start_all(back_out)
    local[7].start()
    sums.core_done()
    r[0].add(2)
    r[6].add(10)
    r[4].add(12)
    r[0].add(3)
    r[3].add(10)
    r[5].add(5)
    r[5].add(6)
    local[10].start()
    reduced(2)
    r[3].add(11)
    r[1].add(4)
    r[1].add(8)
    r[2].add(12)
    r[1].add(5)
    r[1].add(9)
    r[3].add(12)
    local[9].start()
    reduced(1)
    r[0].add(4)
    r[0].add(8)
    r[0].add(5)
    r[0].add(9)
    r[1].add(6)
    r[1].add(10)
    r[1].add(7)
    r[1].add(11)
    sums.y_done()
    r[0].add(6)
    r[0].add(10)
    r[0].add(7)
    sums.x_done()
    r[0].add(11)
    r[1].add(12)
    r[0].add(12)
    sums.z_done()
    local[11].start()
    local[8].start()
    reduced(0)
    sums.sent()
    wait_local(local[6:12])
    swapped(out_out)
    swapped(back_out)
    swaps_sent()


ANY_SPEC = pl.BlockSpec(memory_space=pl.ANY)
LIMIT = 67043328


def whole_layer(tokens, *rest):
    nz = lax.axis_size(FSDP) // 2
    part = WIDTH // (2 * nz)
    seq = tokens.shape[1] * 4
    return pl.pallas_call(
        partial(layer_kernel, nz),
        out_shape=(
            jax.ShapeDtypeStruct((KINDS, part, WIDTH), F32),
            jax.ShapeDtypeStruct(tokens.shape, BF16),
            jax.ShapeDtypeStruct(tokens.shape, BF16),
            jax.ShapeDtypeStruct((8, 128), F32),
        ),
        in_specs=[ANY_SPEC, pl.BlockSpec(memory_space=pltpu.SMEM)] + [ANY_SPEC] * 16,
        out_specs=(ANY_SPEC,) * 4,
        scratch_shapes=buffer_shapes(nz, seq) + flow_shapes(nz) + [
            pltpu.VMEM((2, nz, 2, 8, 128), F32),
            pltpu.VMEM((nz, 2, 8, 128), F32),
            pltpu.VMEM((nz, 8, 128), F32),
            pltpu.VMEM((nz - 1, 8, 128), F32),
            pltpu.VMEM((2, 2, nz, 2, 8, 128), F32),
            pltpu.VMEM((2, 2, nz, 2, 8, 128), F32),
            pltpu.VMEM((8, 128), F32),
            *[pltpu.VMEM((part, WIDTH // 4), BF16)] * 3,
            pltpu.VMEM((WIDTH // 4, part), BF16),
            pltpu.VMEM((part, WIDTH), BF16),
            *[pltpu.VMEM((SHORT,), F32)] * 8,
            pltpu.VMEM((LONG,), F32),
            pltpu.VMEM((KINDS, part, WIDTH), F32),
            pltpu.VMEM((8, 128), F32),
            pltpu.SemaphoreType.DMA((SEND_COUNT,)),
            pltpu.SemaphoreType.DMA((DOOR_COUNT,)),
            pltpu.SemaphoreType.DMA((25,)),
        ],
        compiler_params=pltpu.CompilerParams(collective_id=0, has_side_effects=True, vmem_limit_bytes=LIMIT),
        name="whole_layer",
    )(tokens, *rest)


def finish_kernel(count, *refs):
    given, results, rest = refs[:4], refs[4:4 + count], refs[4 + count:]
    (sums, outs, backs, totals), made, (sems, sent) = rest[:4], rest[4:-2], rest[-2:]
    arrivals = [pltpu.make_async_copy(ref, spot, sems.at[i]) for i, (ref, spot) in enumerate(zip(given, rest))]
    start_all(arrivals)
    input_grad, g_query, g_key, g_value, g_output, g_inner, g_outer = made[:7]
    copies = [pltpu.make_async_copy(outs, results[0], sent.at[0])]
    copies += [pltpu.make_async_copy(*pair, sent.at[i + 1]) for i, pair in enumerate(zip(made, results[1:]))]
    arrivals[2].wait()
    input_grad[...] = backs[...].astype(F32)
    copies[1].start()
    arrivals[1].wait()
    copies[0].start()
    arrivals[0].wait()
    g_inner[...] = sums[1]
    g_outer[...] = sums[2]
    g_query[...], g_key[...], g_value[...], g_turned = unpack_joint(sums[0])
    g_output[...] = g_turned.T
    start_all(copies[2:8])
    arrivals[3].wait()
    short = [0, 1, 2, None, 3, 4, 5, 6, 7]
    for row, ref in zip(short, made[7:]):
        ref[...] = (totals[0:1, 32:128] if row is None else totals[row:row + 1, 0:SHORT]).reshape(ref.shape)
    start_all(copies[8:])
    wait_local(copies)


def finish_layer(sums, outs, backs, totals):
    part = sums.shape[1]
    share = WIDTH // 4
    shapes = [outs.shape, backs.shape] + [(part, share)] * 3 + [(share, part), (part, WIDTH), (part, WIDTH)]
    shapes += [(SHORT,)] * 3 + [(LONG,)] + [(SHORT,)] * 5
    given = (sums, outs, backs, totals)
    return pl.pallas_call(
        partial(finish_kernel, len(shapes)),
        out_shape=[jax.ShapeDtypeStruct(shape, F32 if i else BF16) for i, shape in enumerate(shapes)],
        in_specs=[ANY_SPEC] * 4,
        out_specs=[ANY_SPEC] * len(shapes),
        scratch_shapes=[pltpu.VMEM(ref.shape, ref.dtype) for ref in given]
        + [pltpu.VMEM(shape, F32) for shape in shapes[1:]]
        + [pltpu.SemaphoreType.DMA((4,)), pltpu.SemaphoreType.DMA((len(shapes),))],
        compiler_params=pltpu.CompilerParams(vmem_limit_bytes=LIMIT),
        name="finish_layer",
    )(*given)


def pack_joint(q, k, v, o):
    return jnp.concatenate(
        [q[:, :128], k[:, :128], v[:, :128], v[:, 128:], q[:, 128:], o[:, :128], o[:, 128:], k[:, 128:]], axis=1
    )


def unpack_joint(joint):
    q = jnp.concatenate([joint[:, 0:128], joint[:, 448:512]], axis=1)
    k = jnp.concatenate([joint[:, 128:256], joint[:, 704:768]], axis=1)
    return q, k, joint[:, 256:448], joint[:, 512:704]


def local_fast(*given):
    given = given[:8] + (given[8].T,) + given[9:]
    results = finish_layer(*whole_layer(*given))
    return (*results[:7], results[7].T, *results[8:])


def solution(mesh):
    placed = (
        P(FSDP, TENSOR, None),
        P(FSDP),
        P(FSDP, TENSOR, None),
        P(FSDP, TENSOR),
        P(FSDP, TENSOR),
        P(FSDP, TENSOR),
        P(TENSOR, FSDP),
        P(FSDP, TENSOR),
        P(TENSOR, FSDP),
        P((FSDP, TENSOR)),
        P((FSDP, TENSOR)),
        P((FSDP, TENSOR)),
        P((FSDP, TENSOR)),
        P((FSDP, TENSOR)),
        P((FSDP, TENSOR)),
        P((FSDP, TENSOR)),
        P((FSDP, TENSOR)),
        P((FSDP, TENSOR)),
    )
    return jax.shard_map(
        local_fast if fits(mesh.shape) else local_generic,
        mesh=mesh,
        in_specs=placed,
        out_specs=(
            P(FSDP, TENSOR, None),
            P(FSDP, TENSOR, None),
            P(FSDP, TENSOR),
            P(FSDP, TENSOR),
            P(FSDP, TENSOR),
            P(TENSOR, FSDP),
            P(FSDP, TENSOR),
            P(TENSOR, FSDP),
            P((FSDP, TENSOR)),
            P((FSDP, TENSOR)),
            P((FSDP, TENSOR)),
            P((FSDP, TENSOR)),
            P((FSDP, TENSOR)),
            P((FSDP, TENSOR)),
            P((FSDP, TENSOR)),
            P((FSDP, TENSOR)),
            P((FSDP, TENSOR)),
        ),
        check_vma=False,
    )
```

```python
from functools import partial

import jax
import jax.numpy as jnp
from jax import lax
from jax.experimental import pallas as pl
from jax.experimental.pallas import tpu as pltpu
from jax.sharding import PartitionSpec as P

FSDP, TENSOR = "fsdp", "tensor"

HEAD = 64


epsilon = 1e-05
root_half = 0.7071067811865476
inverse_root_two_pi = 0.3989422804014327


def gelu_value(inner):
    return 0.5 * inner * (1.0 + jax.scipy.special.erf(inner * root_half))


def gelu_slope(inner):
    return 0.5 * (
        1.0 + jax.scipy.special.erf(inner * root_half)
    ) + inner * inverse_root_two_pi * jnp.exp(-0.5 * inner * inner)


def normalize(rows):
    mean = jnp.mean(rows, axis=1, keepdims=True)
    centered = rows - mean
    variance = jnp.mean(centered * centered, axis=1, keepdims=True)
    factor = lax.rsqrt(variance + epsilon)
    return (centered * factor, factor)


def normalize_back(grad_normed, normed, factor):
    return factor * (
        grad_normed
        - jnp.mean(grad_normed, axis=1, keepdims=True)
        - normed * jnp.mean(grad_normed * normed, axis=1, keepdims=True)
    )


def column_sum(rows):
    return jnp.sum(rows.astype(jnp.float32), axis=0)


def dot_rows(left, right):
    return lax.dot_general(
        left, right, (((0,), (0,)), ((), ())), preferred_element_type=jnp.float32
    )


def dot_back(left, right):
    return lax.dot_general(
        left, right, (((1,), (1,)), ((), ())), preferred_element_type=jnp.float32
    )


def place(values, offset, total_length):
    return lax.dynamic_update_slice(jnp.zeros((total_length,), jnp.float32), values, (offset,))


def block_scores(keys, key_valid, query_block):
    raw = jnp.einsum(
        "qhd,khd->hqk", query_block, keys, preferred_element_type=jnp.float32
    ) * HEAD ** (-0.5)
    return jnp.where(key_valid[None, None, :], raw, -1000000000.0)


def attend_forward(keys, values, key_valid, query_block):
    masked = block_scores(keys, key_valid, query_block)
    top = jnp.max(masked, axis=2, keepdims=True)
    expo = jnp.exp(masked - top)
    total = jnp.sum(expo, axis=2, keepdims=True)
    probs = (expo / total).astype(jnp.bfloat16)
    context = jnp.einsum("hqk,khd->qhd", probs, values, preferred_element_type=jnp.float32)
    return (context, top, total)


def attend_backward(keys, values, key_valid, carry, item):
    key_grad, value_grad = carry
    query_block, context_grad_block, top, total = item
    masked = block_scores(keys, key_valid, query_block)
    probs = jnp.exp(masked - top) / total
    probs_low = probs.astype(jnp.bfloat16)
    prob_grad = jnp.einsum(
        "qhd,khd->hqk", context_grad_block, values, preferred_element_type=jnp.float32
    )
    delta = jnp.sum(prob_grad * probs, axis=2, keepdims=True)
    score_grad = (probs * (prob_grad - delta)).astype(jnp.bfloat16)
    factor = HEAD ** (-0.5)
    query_grad = (
        jnp.einsum("hqk,khd->qhd", score_grad, keys, preferred_element_type=jnp.float32) * factor
    )
    key_grad = (
        key_grad
        + jnp.einsum("hqk,qhd->khd", score_grad, query_block, preferred_element_type=jnp.float32)
        * factor
    )
    value_grad = value_grad + jnp.einsum(
        "hqk,qhd->khd", probs_low, context_grad_block, preferred_element_type=jnp.float32
    )
    return ((key_grad, value_grad), query_grad)


def gather_weights(w_query, w_key, w_value, w_output, w_inner, w_outer):
    return (
        lax.all_gather(w_query, FSDP, axis=0, tiled=True),
        lax.all_gather(w_key, FSDP, axis=0, tiled=True),
        lax.all_gather(w_value, FSDP, axis=0, tiled=True),
        lax.all_gather(w_output, FSDP, axis=1, tiled=True),
        lax.all_gather(w_inner, FSDP, axis=0, tiled=True),
        lax.all_gather(w_outer, FSDP, axis=1, tiled=True),
    )


def split_joint(joint_sum, output_sum, inner_sum, outer_sum, head_width):
    return (
        joint_sum[:, :head_width],
        joint_sum[:, head_width : 2 * head_width],
        joint_sum[:, 2 * head_width :],
        output_sum,
        inner_sum,
        outer_sum,
    )


def add_tuples(left, right):
    return tuple((first_item + second_item for first_item, second_item in zip(left, right)))


def local_generic(
    tokens,
    lengths,
    cotangent,
    w_query,
    w_key,
    w_value,
    w_output,
    w_inner,
    w_outer,
    b_query,
    b_value,
    b_output,
    b_inner,
    b_outer,
    gain_first,
    shift_first,
    gain_second,
    shift_second,
):
    tensor_size = lax.axis_size(TENSOR)
    tensor_rank = lax.axis_index(TENSOR)
    micro_count = tokens.shape[0]
    part_rows = tokens.shape[1]
    width = tokens.shape[2]
    seq_rows = part_rows * tensor_size
    head_width = w_query.shape[1]
    inner_width = w_inner.shape[1]
    local_heads = head_width // HEAD
    block_rows = min(512, seq_rows)
    block_count = seq_rows // block_rows
    vector_full = (
        lax.all_gather(b_query, (FSDP, TENSOR), axis=0, tiled=True),
        lax.all_gather(b_value, (FSDP, TENSOR), axis=0, tiled=True),
        lax.all_gather(b_output, (FSDP, TENSOR), axis=0, tiled=True),
        lax.all_gather(b_inner, (FSDP, TENSOR), axis=0, tiled=True),
        lax.all_gather(b_outer, (FSDP, TENSOR), axis=0, tiled=True),
        lax.all_gather(gain_first, (FSDP, TENSOR), axis=0, tiled=True),
        lax.all_gather(shift_first, (FSDP, TENSOR), axis=0, tiled=True),
        lax.all_gather(gain_second, (FSDP, TENSOR), axis=0, tiled=True),
        lax.all_gather(shift_second, (FSDP, TENSOR), axis=0, tiled=True),
    )
    query_bias = lax.dynamic_slice_in_dim(vector_full[0], tensor_rank * head_width, head_width)
    value_bias = lax.dynamic_slice_in_dim(vector_full[1], tensor_rank * head_width, head_width)
    inner_bias = lax.dynamic_slice_in_dim(vector_full[3], tensor_rank * inner_width, inner_width)
    joint_bias = jnp.concatenate([query_bias, jnp.zeros((head_width,), jnp.float32), value_bias])
    grad_query_bias = jnp.zeros((head_width,), jnp.float32)
    grad_value_bias = jnp.zeros((head_width,), jnp.float32)
    grad_inner_bias = jnp.zeros((inner_width,), jnp.float32)
    grad_output_bias = jnp.zeros((width,), jnp.float32)
    grad_outer_bias = jnp.zeros((width,), jnp.float32)
    grad_gain_one = jnp.zeros((width,), jnp.float32)
    grad_shift_one = jnp.zeros((width,), jnp.float32)
    grad_gain_two = jnp.zeros((width,), jnp.float32)
    grad_shift_two = jnp.zeros((width,), jnp.float32)
    local_totals = None
    shard_totals = None
    outputs = []
    input_grads = []
    slot_index = jnp.arange(seq_rows, dtype=jnp.int32)
    part_index = tensor_rank * part_rows + jnp.arange(part_rows, dtype=jnp.int32)
    for micro_index in range(micro_count):
        forward_weights = gather_weights(w_query, w_key, w_value, w_output, w_inner, w_outer)
        joint_w = jnp.concatenate(
            [forward_weights[0], forward_weights[1], forward_weights[2]], axis=1
        )
        output_w = forward_weights[3]
        inner_w = forward_weights[4]
        outer_w = forward_weights[5]
        length = lengths[micro_index]
        key_valid = slot_index < length
        row_valid = (part_index < length).astype(jnp.float32)[:, None]
        own_rows = tokens[micro_index]
        whole = lax.all_gather(own_rows, TENSOR, axis=0, tiled=True)
        joint = (jnp.dot(whole, joint_w, preferred_element_type=jnp.float32) + joint_bias).astype(
            jnp.bfloat16
        )
        query = joint[:, :head_width].reshape(block_count, block_rows, local_heads, HEAD)
        keys = joint[:, head_width : 2 * head_width].reshape(seq_rows, local_heads, HEAD)
        values = joint[:, 2 * head_width :].reshape(seq_rows, local_heads, HEAD)
        context_blocks, tops, totals = lax.map(
            partial(attend_forward, keys, values, key_valid), query
        )
        context_low = context_blocks.reshape(seq_rows, head_width).astype(jnp.bfloat16)
        attended = (
            lax.psum_scatter(
                jnp.dot(context_low, output_w, preferred_element_type=jnp.float32).astype(
                    jnp.bfloat16
                ),
                TENSOR,
                scatter_dimension=0,
                tiled=True,
            ).astype(jnp.float32)
            + vector_full[2]
        )
        normed_first, factor_first = normalize(own_rows.astype(jnp.float32) + attended)
        first = normed_first * vector_full[5] + vector_full[6]
        first_whole = lax.all_gather(first.astype(jnp.bfloat16), TENSOR, axis=0, tiled=True)
        inner = jnp.dot(first_whole, inner_w, preferred_element_type=jnp.float32) + inner_bias
        active = gelu_value(inner).astype(jnp.bfloat16)
        mixed = (
            lax.psum_scatter(
                jnp.dot(active, outer_w, preferred_element_type=jnp.float32).astype(jnp.bfloat16),
                TENSOR,
                scatter_dimension=0,
                tiled=True,
            ).astype(jnp.float32)
            + vector_full[4]
        )
        normed_second, factor_second = normalize(first + mixed)
        outputs.append(
            ((normed_second * vector_full[7] + vector_full[8]) * row_valid).astype(jnp.bfloat16)
        )
        backward_weights = gather_weights(w_query, w_key, w_value, w_output, w_inner, w_outer)
        joint_w = jnp.concatenate(
            [backward_weights[0], backward_weights[1], backward_weights[2]], axis=1
        )
        output_w = backward_weights[3]
        inner_w = backward_weights[4]
        outer_w = backward_weights[5]
        out_grad = cotangent[micro_index].astype(jnp.float32) * row_valid
        grad_gain_two = grad_gain_two + column_sum(out_grad * normed_second)
        grad_shift_two = grad_shift_two + column_sum(out_grad)
        sum_grad = normalize_back(out_grad * vector_full[7], normed_second, factor_second)
        mixed_grad = sum_grad.astype(jnp.bfloat16)
        grad_outer_bias = grad_outer_bias + column_sum(mixed_grad)
        mixed_whole = lax.all_gather(mixed_grad, TENSOR, axis=0, tiled=True)
        outer_sum = dot_rows(active, mixed_whole)
        inner_grad = (dot_back(mixed_whole, outer_w) * gelu_slope(inner)).astype(jnp.bfloat16)
        grad_inner_bias = grad_inner_bias + column_sum(inner_grad)
        inner_sum = dot_rows(first_whole, inner_grad)
        first_grad = sum_grad + lax.psum_scatter(
            dot_back(inner_grad, inner_w).astype(jnp.bfloat16),
            TENSOR,
            scatter_dimension=0,
            tiled=True,
        ).astype(jnp.float32)
        grad_gain_one = grad_gain_one + column_sum(first_grad * normed_first)
        grad_shift_one = grad_shift_one + column_sum(first_grad)
        residual_grad = normalize_back(first_grad * vector_full[5], normed_first, factor_first)
        attended_grad = residual_grad.astype(jnp.bfloat16)
        grad_output_bias = grad_output_bias + column_sum(attended_grad)
        attended_whole = lax.all_gather(attended_grad, TENSOR, axis=0, tiled=True)
        output_sum = dot_rows(context_low, attended_whole)
        context_grad = (
            dot_back(attended_whole, output_w)
            .astype(jnp.bfloat16)
            .reshape(block_count, block_rows, local_heads, HEAD)
        )
        empty = jnp.zeros((seq_rows, local_heads, HEAD), jnp.float32)
        carried, query_grad = lax.scan(
            partial(attend_backward, keys, values, key_valid),
            (empty, empty),
            (query, context_grad, tops, totals),
        )
        joint_grad = jnp.concatenate(
            [
                query_grad.reshape(seq_rows, head_width),
                carried[0].reshape(seq_rows, head_width),
                carried[1].reshape(seq_rows, head_width),
            ],
            axis=1,
        ).astype(jnp.bfloat16)
        grad_query_bias = grad_query_bias + column_sum(joint_grad[:, :head_width])
        grad_value_bias = grad_value_bias + column_sum(joint_grad[:, 2 * head_width :])
        joint_sum = dot_rows(whole, joint_grad)
        input_grads.append(
            residual_grad
            + lax.psum_scatter(
                dot_back(joint_grad, joint_w).astype(jnp.bfloat16),
                TENSOR,
                scatter_dimension=0,
                tiled=True,
            ).astype(jnp.float32)
        )
        batch_sums = (joint_sum, output_sum, inner_sum, outer_sum)
        local_totals = batch_sums if local_totals is None else add_tuples(local_totals, batch_sums)
    pieces = split_joint(
        local_totals[0], local_totals[1], local_totals[2], local_totals[3], head_width
    )
    shard_totals = (
        lax.psum_scatter(pieces[0], FSDP, scatter_dimension=0, tiled=True),
        lax.psum_scatter(pieces[1], FSDP, scatter_dimension=0, tiled=True),
        lax.psum_scatter(pieces[2], FSDP, scatter_dimension=0, tiled=True),
        lax.psum_scatter(pieces[3], FSDP, scatter_dimension=1, tiled=True),
        lax.psum_scatter(pieces[4], FSDP, scatter_dimension=0, tiled=True),
        lax.psum_scatter(pieces[5], FSDP, scatter_dimension=1, tiled=True),
    )
    vector_grads = (
        lax.psum_scatter(
            place(grad_query_bias, tensor_rank * head_width, width),
            (FSDP, TENSOR),
            scatter_dimension=0,
            tiled=True,
        ),
        lax.psum_scatter(
            place(grad_value_bias, tensor_rank * head_width, width),
            (FSDP, TENSOR),
            scatter_dimension=0,
            tiled=True,
        ),
        lax.psum_scatter(grad_output_bias, (FSDP, TENSOR), scatter_dimension=0, tiled=True),
        lax.psum_scatter(
            place(grad_inner_bias, tensor_rank * inner_width, inner_width * tensor_size),
            (FSDP, TENSOR),
            scatter_dimension=0,
            tiled=True,
        ),
        lax.psum_scatter(grad_outer_bias, (FSDP, TENSOR), scatter_dimension=0, tiled=True),
        lax.psum_scatter(grad_gain_one, (FSDP, TENSOR), scatter_dimension=0, tiled=True),
        lax.psum_scatter(grad_shift_one, (FSDP, TENSOR), scatter_dimension=0, tiled=True),
        lax.psum_scatter(grad_gain_two, (FSDP, TENSOR), scatter_dimension=0, tiled=True),
        lax.psum_scatter(grad_shift_two, (FSDP, TENSOR), scatter_dimension=0, tiled=True),
    )
    return (
        jnp.stack(outputs),
        jnp.stack(input_grads),
        shard_totals[0],
        shard_totals[1],
        shard_totals[2],
        shard_totals[3],
        shard_totals[4],
        shard_totals[5],
        vector_grads[0],
        vector_grads[1],
        vector_grads[2],
        vector_grads[3],
        vector_grads[4],
        vector_grads[5],
        vector_grads[6],
        vector_grads[7],
        vector_grads[8],
    )


MESH = pl.DeviceIdType.MESH
WIDTH = 768
HIDDEN = 3072
HALF = WIDTH // 2
KINDS = 3
FLOWS = (
    (0, 0, 512, "zyx", "xyz"),
    (0, 512, 256, "zyx", "xyz"),
    (1, 0, 256, "zxy", "xyz"),
    (1, 256, 512, "zxy", "yxz"),
    (2, 0, 256, "zyx", "zxy"),
    (2, 256, 256, "zyx", "yxz"),
    (2, 512, 256, "yxz", "xzy"),
)
VECTOR_ROWS = 16
SHORT, LONG = 24, 96
ROW_OUTPUT, ROW_OUTER, ROW_GAIN1, ROW_SHIFT1, ROW_GAIN2, ROW_SHIFT2, ROW_INNER = 4, 5, 6, 7, 8, 9, 10
BF16 = jnp.bfloat16
F32 = jnp.float32


def fits(sizes):
    fsdp = sizes[FSDP]
    return sizes[TENSOR] == 4 and fsdp == WIDTH // LONG


class Place:
    def __init__(self, nz):
        self.f = lax.axis_index(FSDP)
        self.t = lax.axis_index(TENSOR)
        self.nz = nz
        self.z = self.f // 2
        self.x = self.f % 2
        self.y = self.t // 2
        self.c = self.t % 2
        self.core = (self.f, self.t + 1 - 2 * self.c)
        self.along_y = (self.f, self.t + 2 - 4 * self.y)
        self.along_x = (self.f + 1 - 2 * self.x, self.t)

    def z_at(self, step):
        return (self.z + step) % self.nz

    def z_back(self, step):
        return (self.z + self.nz - step) % self.nz

    def along_z(self, step):
        return (self.z_at(step) * 2 + self.x, self.t)

    def in_group(self, step):
        return (self.f, (self.t + step) % 4)


class Trip:
    def __init__(self, copy, send_sem, recv_sem):
        self.copy, self.send_sem, self.recv_sem = copy, send_sem, recv_sem

    def start(self):
        self.copy.start()

    def wait_recv(self):
        self.copy.wait_recv()


class Net:
    def __init__(self, send_sems, recv_sems):
        self.send_sems, self.recv_sems = send_sems, recv_sems
        self.sends = self.recvs = 0

    def lane(self):
        self.sends += 1
        return self.send_sems.at[self.sends - 1]

    def door(self):
        self.recvs += 1
        return self.recv_sems.at[self.recvs - 1]

    def plan(self, source, target, device, lane, door=None):
        door = self.door() if door is None else door
        copy = pltpu.make_async_remote_copy(
            src_ref=source, dst_ref=target, send_sem=lane, recv_sem=door, device_id=device, device_id_type=MESH
        )
        return Trip(copy, lane, door)

    def keep(self, ref, device, lane, door=None):
        return self.plan(ref, ref, device, lane, door)


class Meter:
    def __init__(self, low, wide):
        self.low, self.wide = low, wide

    def low_rows(self, rows):
        for count in (1, 2, 3, 4):
            if rows % (16 * count) == 0 and rows // count <= self.low.shape[1]:
                return self.low.at[0:count, 0:rows // count]
        raise ValueError(rows)

    def tiles(self, count):
        return self.wide.at[0:8 * count]


def arrived(trips, size):
    pltpu.make_async_copy(size, size, trips[0].recv_sem).wait()


def departed(trips, size):
    pltpu.make_async_copy(size, size, trips[0].send_sem).wait()


def start_all(copies):
    for copy in copies:
        copy.start()


def greet(place):
    barrier = pltpu.get_barrier_semaphore()
    peers = [place.in_group(1), place.in_group(2), place.in_group(3), place.along_x]
    peers += [place.along_z(step) for step in range(1, place.nz)]
    for peer in peers:
        pl.semaphore_signal(barrier, inc=1, device_id=peer, device_id_type=MESH)
    pl.semaphore_wait(barrier, len(peers))


def wait_local(copies):
    for copy in copies:
        copy.wait()


def dot(left, right):
    return lax.dot_general(left, right, (((1,), (0,)), ((), ())), preferred_element_type=F32)


def turn(value, shift):
    shift %= value.shape[1]
    return pltpu.roll(value, shift, 1) if shift else value


class Layer:
    def __init__(self, refs, length):
        (
            self.w, self.rows, self.back, self.rows_turned, self.joint, self.probs, self.context, self.acc,
            self.normed, self.factor, self.first_low, self.first_turned, self.active, self.slope, self.grad_low,
            self.grad_turned, self.out, self.vec, self.sums, self.early,
        ) = refs
        self.length = length
        self.seq = self.rows.shape[0]
        self.block = self.seq

    def weight(self, kind, t):
        return self.w[kind, t // 2, t % 2].reshape(WIDTH, WIDTH)

    def output_weight(self, t):
        return self.w[0, t // 2, t % 2, :, :, :, 512:768].reshape(WIDTH, 256)

    def store_grad(self, kind, t, value):
        nz = self.w.shape[3]
        self.w[kind, t // 2, t % 2] = value.astype(BF16).reshape(nz, 2, WIDTH // (2 * nz), WIDTH)

    def row(self, index):
        return self.vec[pl.ds(index, 1), :]

    def blocks(self, body):
        def step(i, carry):
            body(pl.ds(pl.multiple_of(i * self.block, self.block), self.block), i)
            return carry

        lax.fori_loop(0, self.seq // self.block, step, 0)

    def row_valid(self, i):
        index = lax.broadcasted_iota(jnp.int32, (self.block, 1), 0) + i * self.block
        return (index < self.length).astype(F32)

    def lanes(self, low, high, width):
        lane = lax.broadcasted_iota(jnp.int32, (1, width), 1)
        return (lane >= low) & (lane < high)

    def pick(self, value, low, high):
        return jnp.where(self.lanes(low, high, value.shape[1]), value, jnp.zeros_like(value))

    def head_query(self, t, h):
        return self.joint[t, :, 0:128] if h < 2 else self.joint[t, :, 384:512]

    def head_key(self, t, h):
        return self.joint[t, :, 128:256] if h < 2 else self.joint[t, :, 640:768]

    def head_side(self, value, h):
        return self.pick(value, 0, 64) if h == 0 else self.pick(value, 64, 128)

    def head_value(self, t, h):
        return self.pick(self.joint[t, :, 256:512], h * 64, h * 64 + 64)

    def unpack(self, v):
        nz = v.shape[2]
        short = jnp.zeros((8, WIDTH), F32)
        inner = [jnp.zeros((1, WIDTH), F32) for _ in range(4)]
        for f in range(2 * nz):
            for t in range(4):
                rank = f * 4 + t
                block = v[t // 2, t % 2, f // 2, f % 2]
                wide = jnp.concatenate([self.pick(block, 0, SHORT), jnp.zeros((8, WIDTH - 128), F32)], axis=1)
                short += turn(wide, rank * SHORT)
                wide = jnp.concatenate([self.pick(block[0:1], 32, 128), jnp.zeros((1, WIDTH - 128), F32)], axis=1)
                inner[rank * LONG // WIDTH] += turn(wide, rank * LONG % WIDTH - 32)
        for t in range(4):
            query = self.pick(turn(short[0:1], -192 * t), 0, 128) + self.pick(turn(short[0:1], 320 - 192 * t), 448, 512)
            self.vec[t:t + 1] = query + self.pick(turn(short[1:2], 256 - 192 * t), 256, 448)
            self.vec[ROW_INNER + t:ROW_INNER + t + 1] = inner[t]
        self.vec[ROW_OUTPUT:ROW_INNER] = short[2:8]

    def pack(self, parts):
        nz = parts.shape[2]
        query, value = jnp.zeros((1, WIDTH), F32), jnp.zeros((1, WIDTH), F32)
        for t in range(4):
            row = self.sums[t:t + 1]
            query += turn(self.pick(row, 0, 128), 192 * t) + turn(self.pick(row, 448, 512), 192 * t - 320)
            value += turn(self.pick(row, 256, 448), 192 * t - 256)
        short = jnp.concatenate([query, value, self.sums[ROW_OUTPUT:ROW_INNER]], axis=0)
        top = lax.broadcasted_iota(jnp.int32, (8, 1), 0) == 0
        for f in range(2 * nz):
            for t in range(4):
                rank = f * 4 + t
                block = self.pick(turn(short, -rank * SHORT)[:, 0:128], 0, SHORT)
                index = ROW_INNER + rank * LONG // WIDTH
                inner = turn(self.sums[index:index + 1], 32 - rank * LONG % WIDTH)[:, 0:128]
                inner = jnp.broadcast_to(self.pick(inner, 32, 128), (8, 128))
                parts[t // 2, t % 2, f // 2, f % 2] = block + jnp.where(top, inner, 0.0)

    def project(self, t):
        self.joint[t] = (dot(self.rows[...], self.weight(0, t)) + self.row(t)).astype(BF16)

    def attend(self, t):
        key_valid = lax.broadcasted_iota(jnp.int32, (1, self.seq), 1) < self.length
        context = None
        for h in range(3):
            raw = dot_back(self.head_query(t, h), self.head_side(self.head_key(t, h), h))
            masked = jnp.where(key_valid, raw * HEAD ** -0.5, -1e9)
            expo = jnp.exp(masked - jnp.max(masked, axis=1, keepdims=True))
            probs = (expo * (1.0 / jnp.sum(expo, axis=1, keepdims=True))).astype(BF16)
            self.probs[t * 3 + h] = probs
            part = dot(probs, self.head_value(t, h))
            context = part if context is None else context + part
        low = context.astype(BF16)
        self.context[t] = low
        self.acc[...] += dot_back(low, self.output_weight(t))

    def start(self):
        def body(rows, i):
            self.acc[rows] = self.rows[rows].astype(F32) + self.row(ROW_OUTPUT)

        self.blocks(body)

    def norm_first(self):
        def body(rows, i):
            normed, factor = normalize(self.acc[rows])
            self.normed[rows] = normed
            self.factor[rows] = jnp.broadcast_to(factor, (self.block, 128))
            first = normed * self.row(ROW_GAIN1) + self.row(ROW_SHIFT1)
            self.first_low[rows] = first.astype(BF16)
            self.acc[rows] = first + self.row(ROW_OUTER)

        self.blocks(body)

    def feed_inner(self, t):
        inner = dot(self.first_low[...], self.weight(1, t)) + self.row(ROW_INNER + t)
        gate = 1.0 + lax.erf(inner * root_half)
        self.active[t] = (0.5 * inner * gate).astype(BF16)
        self.slope[t] = (0.5 * gate + inner * inverse_root_two_pi * jnp.exp(-0.5 * inner * inner)).astype(BF16)

    def feed_outer(self, t):
        self.acc[...] += dot_back(self.active[t], self.weight(2, t))

    def clear_sums(self):
        self.sums[...] = jnp.zeros_like(self.sums)

    def add_sum(self, index, value):
        self.sums[pl.ds(index, 1), :] += jnp.sum(value, axis=0, keepdims=True)

    def norm_second(self):
        def body(rows, i):
            normed, factor = normalize(self.acc[rows])
            valid = self.row_valid(i)
            gain = self.row(ROW_GAIN2)
            self.first_low[rows] = normed.astype(BF16)
            self.out[rows] = ((normed * gain + self.row(ROW_SHIFT2)) * valid).astype(BF16)
            out_grad = self.back[rows].astype(F32) * valid
            sum_grad = normalize_back(out_grad * gain, normed, factor)
            self.acc[rows] = sum_grad
            self.grad_low[rows] = sum_grad.astype(BF16)

        self.blocks(body)

    def second_sums(self):
        def body(rows, i):
            out_grad = self.back[rows].astype(F32) * self.row_valid(i)
            self.add_sum(ROW_GAIN2, out_grad * self.first_low[rows].astype(F32))
            self.add_sum(ROW_SHIFT2, out_grad)
            self.add_sum(ROW_OUTER, self.grad_low[rows].astype(F32))

        self.blocks(body)

    def outer_slope(self, t):
        grad = (dot(self.grad_low[...], self.weight(2, t)) * self.slope[t].astype(F32)).astype(BF16)
        self.slope[t] = grad
        self.add_sum(ROW_INNER + t, grad.astype(F32))

    def outer_back(self, t):
        self.outer_slope(t)
        self.store_grad(2, t, dot_rows(self.grad_low[...], self.active[t]))

    def outer_early(self, t):
        value = dot_rows(self.grad_low[...], self.active[t])
        self.early[...] = value.astype(BF16).reshape(self.early.shape)

    def inner_back(self, t):
        grad = self.slope[t]
        self.acc[...] += dot_back(grad, self.weight(1, t))
        self.store_grad(1, t, dot(self.first_turned[...], grad))

    def norm_first_back(self):
        def body(rows, i):
            grad = self.acc[rows]
            normed = self.normed[rows]
            self.add_sum(ROW_GAIN1, grad * normed)
            self.add_sum(ROW_SHIFT1, grad)
            residual = normalize_back(grad * self.row(ROW_GAIN1), normed, self.factor[rows][:, 0:1])
            self.acc[rows] = residual
            low = residual.astype(BF16)
            self.grad_low[rows] = low
            self.add_sum(ROW_OUTPUT, low.astype(F32))

        self.blocks(body)
        self.grad_turned[...] = self.grad_low[...].T

    def attend_back(self, t):
        context_grad = self.pick(dot(self.grad_low[...], self.output_weight(t)), 0, 192).astype(BF16)
        query_grads, key_grads, value_grad = [], [], None
        for h in range(3):
            probs = self.probs[t * 3 + h]
            prob_grad = dot_back(context_grad, self.head_value(t, h))
            wide = probs.astype(F32)
            delta = jnp.sum(wide * prob_grad, axis=1, keepdims=True)
            score_grad = (wide * (prob_grad - delta)).astype(BF16)
            query_grads.append(dot(score_grad, self.head_side(self.head_key(t, h), h)) * HEAD ** -0.5)
            key_grads.append(dot_rows(score_grad, self.head_side(self.head_query(t, h), h)) * HEAD ** -0.5)
            part = dot_rows(probs, self.pick(context_grad, h * 64, h * 64 + 64))
            value_grad = part if value_grad is None else value_grad + part
        self.joint[t, :, 0:128] = (query_grads[0] + query_grads[1]).astype(BF16)
        self.joint[t, :, 128:256] = (key_grads[0] + key_grads[1]).astype(BF16)
        self.joint[t, :, 256:384] = value_grad[:, 0:128].astype(BF16)
        self.joint[t, :, 384:512] = (value_grad[:, 128:256] + query_grads[2]).astype(BF16)
        self.joint[t, :, 512:640] = jnp.zeros((self.seq, 128), BF16)
        self.joint[t, :, 640:768] = key_grads[2].astype(BF16)

    def joint_back(self, t):
        joint = self.joint[t]
        self.sums[pl.ds(t, 1), :] = jnp.sum(joint.astype(F32), axis=0, keepdims=True)
        self.acc[...] += dot_back(joint, self.weight(0, t))
        nz = self.w.shape[3]
        shape = (nz, 2, WIDTH // (2 * nz), -1)
        main = dot(self.rows_turned[...], joint[:, 0:512])
        side = dot(self.rows_turned[...], joint[:, 512:768]) + dot(self.grad_turned[...], self.context[t])
        self.w[0, t // 2, t % 2, :, :, :, 0:512] = main.astype(BF16).reshape(shape[:3] + (512,))
        self.w[0, t // 2, t % 2, :, :, :, 512:768] = side.astype(BF16).reshape(shape[:3] + (256,))

    def finish(self):
        def body(rows, i):
            self.back[rows] = self.acc[rows].astype(BF16)

        self.blocks(body)


def each(count, body):
    def step(i, carry):
        body(i)
        return carry

    lax.fori_loop(0, count, step, 0)


BUFFER_COUNT = 20


def buffer_shapes(nz, seq):
    part = WIDTH // (2 * nz)
    low, wide = (seq, WIDTH), (WIDTH, seq)
    shapes = [
        ((KINDS, 2, 2, nz, 2, part, WIDTH), BF16),
        (low, BF16),
        (low, BF16),
        (wide, BF16),
        ((4, seq, WIDTH), BF16),
        ((12, seq, seq), BF16),
        ((4, seq, 256), BF16),
        (low, F32),
        (low, F32),
        ((seq, 128), F32),
        (low, BF16),
        (wide, BF16),
        ((4, seq, WIDTH), BF16),
        ((4, seq, WIDTH), BF16),
        (low, BF16),
        (wide, BF16),
        (low, BF16),
        ((VECTOR_ROWS, WIDTH), F32),
        ((VECTOR_ROWS, WIDTH), F32),
        ((nz, 2, part, WIDTH), BF16),
    ]
    return [pltpu.VMEM(*shape) for shape in shapes]


BLOCKS = 15
SEND_COUNT = 15
DOOR_COUNT = 227


def flow_shapes(nz):
    part = WIDTH // (2 * nz)
    shapes = [pltpu.VMEM((KINDS, 2, nz, 2, part, WIDTH), BF16)]
    return shapes + [pltpu.VMEM((BLOCKS, part, flow[2]), BF16) for flow in FLOWS]


def axis_steps(place, axis):
    p = place
    if axis == "x":
        return [(1, 1 - p.x, p.along_x, 1 - p.x)]
    if axis == "y":
        return [(1, 1 - p.y, p.along_y, 1 - p.y)]
    return [(step, p.z_at(step), p.along_z(step), p.z_back(step)) for step in range(1, p.nz)]


class Flow:
    def __init__(self, net, place, order, own, region, lane, core_lane, core_door):
        p = place
        self.pieces = [(None, [])]
        spots = [({"x": p.x, "y": p.y, "z": p.z}, own)]
        for axis in order:
            for index, (spot, source) in enumerate(list(spots)):
                for _, _, device, behind in axis_steps(p, axis):
                    trip = net.plan(region(spot) if source is None else source, region(spot), device, lane)
                    self.pieces[index][1].append(trip)
                    self.pieces.append((trip, []))
                    spots.append(({**spot, axis: behind}, None))
        mine = {"x": p.x, "y": p.y, "z": p.z}[order[2]]
        sides = [mine] + [behind for _, _, _, behind in axis_steps(p, order[2])]
        every = slice(None)
        self.cores = [
            net.keep(region({"x": every, "y": every, "z": every, order[2]: side}), p.core, core_lane, core_door)
            for side in sides
        ]
        self.trips = [trip for _, onward in self.pieces for trip in onward]

    def first(self):
        start_all(self.pieces[0][1])

    def piece(self, index):
        trip, onward = self.pieces[index]
        trip.wait_recv()
        start_all(onward)

    def to_core(self, index):
        self.cores[index].start()


class Cores:
    def __init__(self, net, place, w, core, k, meter, early=None):
        self.place, self.meter = place, meter
        self.w, self.core = w.at[k], core.at[k]
        self.ys = (1 - place.y, place.y)
        steps = list(range(1, place.nz)) + [0]
        self.parts = steps[:place.nz // 2], steps[place.nz // 2:]
        self.c = []
        lane = net.lane()
        for y in self.ys:
            for part in self.parts:
                door = net.door()
                spots = [place.z_at(step) for step in part]
                source = self.w.at[y, 1 - place.c] if early is None or self.c[1:] else early
                self.c.append([net.plan(source.at[z], self.core.at[y, z], place.core, lane, door) for z in spots])
        self.trips = [trip for trips in self.c for trip in trips]

    def to_core(self, half):
        start_all(self.c[2 * half] + self.c[2 * half + 1])

    def half(self, half, part):
        y = self.ys[half]
        trips = self.c[2 * half + part]
        arrived(trips, self.meter.low_rows(2 * self.core.shape[-2] * len(trips)))
        for step in self.parts[part]:
            z = self.place.z_at(step)
            target, source = self.core.at[y, z], self.w.at[y, self.place.c, z]
            target[...] = (target[...].astype(F32) + source[...].astype(F32)).astype(BF16)


class Sink:
    def __init__(self, net, place, order, core, landing, result, cols, lane, meter):
        p = place
        self.meter = meter
        self.core, self.landing, self.result, self.cols = core, landing, result, cols
        here = {"x": p.x, "y": p.y, "z": p.z}
        ahead = {axis: {0: here[axis], **{step: spot for step, spot, _, _ in axis_steps(p, axis)}} for axis in here}
        sizes = {"x": 2, "y": 2, "z": p.nz}
        self.spot = lambda block: tuple(ahead[axis][block[axis]] for axis in ("y", "z", "x"))
        self.order = order
        self.tasks = []
        self.starts = [[], [], [], []]
        blocks = [{}]
        for axis in ("y", "z", "x"):
            steps = [i for i in range(1, sizes[axis])] + [0]
            blocks = [{**block, axis: step} for block in blocks for step in steps]
        slot = 0
        self.trips = []
        waits = {}
        for stage, axis in enumerate(order):
            later = order[stage + 1:]
            kept = [block for block in blocks if block[axis] == 0]
            kept.sort(key=lambda block: [block[other] == 0 for other in later])
            devices = {step: device for step, _, device, _ in axis_steps(p, axis)}
            for block in kept:
                arrivals = []
                door = net.door()
                for step in range(1, sizes[axis]):
                    away = {**block, axis: step}
                    copy = net.plan(self.part(away), landing.at[slot], devices[step], lane, door)
                    self.trips.append(copy)
                    if stage == 0:
                        soon = 0 < away["z"] <= p.nz // 2
                        self.starts[(0 if away["y"] else 2) + (0 if soon else 1)].append(copy)
                    else:
                        waits[tuple(sorted(away.items()))].append(copy)
                    arrivals.append((copy, slot))
                    slot += 1
                onward = []
                waits[tuple(sorted(block.items()))] = onward
                self.tasks.append((block, arrivals, onward))
            blocks = kept

    def part(self, block):
        return self.core.at[(*self.spot(block), slice(None), self.cols)]

    def start(self, half, part):
        start_all(self.starts[2 * half + part])

    def add(self, index):
        block, arrivals, onward = self.tasks[index]
        target = self.part(block)
        total = target[...].astype(F32)
        rows = self.landing.shape[1] * self.landing.shape[2] // WIDTH
        arrived([trip for trip, _ in arrivals], self.meter.low_rows(rows * len(arrivals)))
        for _, slot in arrivals:
            total += self.landing[slot].astype(F32)
        if index < len(self.tasks) - 1:
            target[...] = total.astype(BF16)
            start_all(onward)
        else:
            self.result[:, self.cols] = total


class Back:
    def __init__(self, net, place, parts, landings, result, meter):
        p = self.place = place
        self.parts, self.result, self.meter = parts, result, meter
        self.core, self.side, self.pair, self.line = landings
        lane = net.lane()
        self.c = net.plan(parts.at[:, 1 - p.c], self.core, p.core, lane)
        self.y = net.plan(self.core.at[1 - p.y], self.side, p.along_y, lane)
        self.x = net.plan(self.side.at[:, 1 - p.x], self.pair, p.along_x, lane)
        door = net.door()
        self.z = [
            net.plan(self.pair.at[p.z_at(step)], self.line.at[step - 1], p.along_z(step), lane, door)
            for step in range(1, p.nz)
        ]

    def first(self):
        self.c.start()

    def core_done(self):
        self.c.wait_recv()
        self.core[...] += self.parts[:, self.place.c]
        self.y.start()

    def y_done(self):
        self.y.wait_recv()
        self.side[...] += self.core[self.place.y]
        self.x.start()

    def x_done(self):
        self.x.wait_recv()
        self.pair[...] += self.side[:, self.place.x]
        start_all(self.z)

    def z_done(self):
        arrived(self.z, self.meter.tiles(len(self.z)))
        total = self.pair[self.place.z]
        for i in range(self.place.nz - 1):
            total += self.line[i]
        self.result[...] = total

    def sent(self):
        departed([self.c, self.y, self.x] + self.z, self.meter.tiles(8 * self.place.nz - 1))


def ticks(i, table):
    for when, actions in table.items():
        @pl.when(i == when)
        def _(actions=actions):
            for action, *given in actions:
                action(*given)


def layer_kernel(nz, *refs):
    tokens, lengths, cotangent, w_query, w_key, w_value, w_output, w_inner, w_outer = refs[:9]
    short_in, long_in = refs[9:12] + refs[13:18], refs[12]
    result_out, outs, backs, totals_out = refs[18:22]
    rest = list(refs[22:])
    buffers, rest = rest[:BUFFER_COUNT], rest[BUFFER_COUNT:]
    core_landing, landings, rest = rest[0], rest[1:1 + len(FLOWS)], rest[1 + len(FLOWS):]
    back_landings = rest[:4]
    v, parts, vec_in, raw_query, raw_key, raw_value, raw_output, own_joint = rest[4:12]
    raw_short, raw_long, result, totals = rest[12:20], rest[20], rest[21], rest[22]
    send_sems, recv_sems, local_sems = rest[23:]
    place = Place(nz)
    net = Net(send_sems, recv_sems)
    t = place.t
    quarter = tokens.shape[1]
    layer = Layer(buffers, lengths[t])
    owns = (own_joint, w_inner, w_outer)
    g, r = [], []
    meter = Meter(layer.joint, layer.factor)
    cores = [Cores(net, place, layer.w, core_landing, k, meter) for k in (0, 1)]
    cores.append(Cores(net, place, layer.w, core_landing, 2, meter, layer.early))
    lanes = [[net.lane() for k in range(KINDS)] for _ in range(3)]
    doors = [net.door() for k in range(KINDS)]
    for (k, first, width, order_in, order_out), landing in zip(FLOWS, landings):
        cols = pl.ds(first, width)

        def region(spot, k=k, cols=cols):
            return layer.w.at[k, spot["y"], place.c, spot["z"], spot["x"], :, cols]

        g.append(Flow(net, place, order_in, owns[k].at[:, cols], region, lanes[0][k], lanes[1][k], doors[k]))
        sink = (core_landing.at[k], landing, result.at[k], cols, lanes[2][k], meter)
        r.append(Sink(net, place, order_out, *sink))
    one = net.lane()
    vecs = Flow(
        net, place, FLOWS[0][3], vec_in, lambda spot: v.at[spot["y"], place.c, spot["z"], spot["x"]],
        one, one, net.door(),
    )
    sums = Back(net, place, parts, back_landings, totals, meter)

    def of_kind(flows, k):
        return [flow for flow, row in zip(flows, FLOWS) if row[0] == k]

    def trips_of(flows):
        return [trip for flow in flows for trip in flow.trips]

    def cores_of(flows):
        return [trip for flow in flows for trip in flow.cores]

    def gathered(k):
        arrived(cores_of(of_kind(g, k)), meter.low_rows(2 * WIDTH))

    def passed_on(k):
        flows = of_kind(g, k)
        departed(trips_of(flows), meter.low_rows(2 * WIDTH - own_joint.shape[0]))
        departed(cores_of(flows), meter.low_rows(2 * WIDTH))

    def reduced(k):
        departed(trips_of(of_kind(r, k)), meter.low_rows(2 * WIDTH - own_joint.shape[0]))
        departed(cores[k].trips, meter.low_rows(2 * WIDTH))

    def vectors_in():
        arrived(vecs.cores, meter.tiles(4 * nz))

    def vectors_sent():
        departed(vecs.trips + vecs.cores, meter.tiles(8 * nz - 1))

    def quarter_of(ref, index):
        return ref.at[pl.ds(pl.multiple_of(index * quarter, quarter), quarter)]

    swap_lane = net.lane()

    def swap(source, target):
        door = net.door()
        return [net.plan(source(step), target, place.in_group(step), swap_lane, door) for step in (2, 1, 3)]

    def swapped(trips):
        arrived(trips, meter.low_rows(3 * quarter))

    token_in = swap(lambda step: tokens.at[(t + step) % 4], quarter_of(layer.rows, t))
    back_in = swap(lambda step: cotangent.at[(t + step) % 4], quarter_of(layer.back, t))
    out_out = swap(lambda step: quarter_of(layer.out, (t + step) % 4), outs.at[t])
    back_out = swap(lambda step: quarter_of(layer.back, (t + step) % 4), backs.at[t])

    def swaps_sent():
        departed(token_in + back_in + out_out + back_out, meter.low_rows(12 * quarter))

    pairs = [
        (tokens.at[t], quarter_of(layer.rows, t)),
        (cotangent.at[t], quarter_of(layer.back, t)),
        *[
            (own, layer.w.at[k, place.y, place.c, place.z, place.x])
            for k, own in enumerate(owns)
        ],
        (vec_in, v.at[place.y, place.c, place.z, place.x]),
        (quarter_of(layer.out, t), outs.at[t]),
        (quarter_of(layer.back, t), backs.at[t]),
        *[(result.at[k], result_out.at[k]) for k in range(KINDS)],
        (totals, totals_out),
        (w_query, raw_query),
        (w_key, raw_key),
        (w_value, raw_value),
        (w_output, raw_output),
        *zip(short_in, raw_short),
        (long_in, raw_long),
    ]
    local = [pltpu.make_async_copy(*pair, local_sems.at[i]) for i, pair in enumerate(pairs)]

    def pack_vectors():
        vec_in[...] = jnp.zeros((8, 128), F32)
        for i, ref in enumerate(raw_short):
            vec_in[i:i + 1, 0:SHORT] = ref[...].reshape(1, SHORT)
        vec_in[0:1, 32:128] = raw_long[...].reshape(1, LONG)

    def pack_own():
        own_joint[...] = pack_joint(raw_query[...], raw_key[...], raw_value[...], raw_output[...].T)

    def near(i):
        return (place.y + i) % 2 * 2 + (place.c + i // 2) % 2

    def order(i):
        return (1 - place.y + i // 2) % 2 * 2 + (1 - place.c + i) % 2

    start_all(local[12:])
    greet(place)
    wait_local(local[12:])
    pack_vectors()
    pack_own()
    vecs.first()
    g[1].first()
    g[0].first()
    g[2].first()
    g[1].piece(4)
    start_all(token_in)
    vecs.piece(2)
    start_all(local[:6])
    wait_local(local[:6])
    g[1].piece(8)
    g[3].first()
    g[5].first()
    g[4].first()
    g[0].piece(8)
    vecs.piece(1)
    g[1].piece(2)
    g[6].first()
    vecs.piece(3)
    vecs.piece(8)
    g[3].piece(4)
    g[1].piece(1)
    g[1].piece(3)
    g[5].piece(8)
    vecs.piece(11)
    vecs.piece(4)
    g[0].piece(4)
    g[2].piece(4)
    g[4].piece(8)
    g[1].piece(12)
    vecs.piece(12)
    g[2].piece(8)
    g[6].piece(2)
    vecs.piece(9)
    g[1].piece(11)
    vecs.piece(6)
    g[0].piece(1)
    g[0].piece(12)
    g[5].piece(4)
    g[0].piece(2)
    g[6].piece(1)
    vecs.piece(5)
    vecs.piece(7)
    g[5].piece(12)
    g[4].piece(4)
    g[1].piece(9)
    g[3].piece(12)
    vecs.piece(10)
    g[6].piece(3)
    swapped(token_in)
    vecs.piece(14)
    g[2].piece(1)
    g[1].piece(5)
    g[1].piece(7)
    g[1].piece(10)
    g[0].piece(9)
    g[0].piece(10)
    vecs.piece(15)
    vecs.piece(13)
    vecs.to_core(0)
    g[0].piece(3)
    g[3].piece(8)
    g[6].to_core(0)
    g[2].piece(12)
    vecs.to_core(1)
    g[2].piece(2)
    g[4].piece(12)
    g[1].piece(6)
    vectors_in()
    g[2].piece(5)
    layer.unpack(v)
    layer.start()
    layer.rows_turned[...] = layer.rows[...].T
    layer.clear_sums()
    g[2].piece(3)
    g[1].piece(13)
    g[2].piece(6)
    g[1].piece(15)
    g[0].piece(7)
    g[0].piece(5)
    g[1].piece(14)
    g[1].to_core(1)
    g[0].piece(6)
    g[2].piece(7)
    g[2].piece(9)
    g[3].piece(1)
    g[0].piece(11)
    g[2].to_core(0)
    g[2].piece(10)
    g[0].piece(13)
    g[0].to_core(0)
    g[1].to_core(0)
    g[3].piece(3)
    g[0].piece(14)
    g[2].piece(11)
    g[0].piece(15)
    g[2].piece(15)
    g[3].piece(2)
    g[0].to_core(1)
    g[5].piece(3)
    def project(i):
        layer.project(near(i))
        ticks(i, {
            1: [(g[2].piece, 14), (g[2].piece, 13), (gathered, 0), (g[3].piece, 9), (g[5].piece, 1)],
            2: [(g[3].piece, 5), (g[3].piece, 11)],
        })

    each(4, project)
    g[5].piece(2)
    g[3].piece(10)
    g[3].piece(7)
    def attend(i):
        layer.attend(i)
        ticks(i, {
            0: [(g[3].piece, 13), (g[4].piece, 1), (g[3].piece, 6), (g[3].to_core, 0), (g[5].piece, 7), (g[4].piece, 2)],
            1: [(g[5].piece, 6), (g[2].to_core, 1), (g[5].piece, 5), (g[6].piece, 6), (g[4].piece, 3), (start_all, back_in), (g[6].piece, 4), (g[5].piece, 9), (g[5].to_core, 0)],
            2: [(g[5].piece, 11)],
        })

    each(4, attend)
    g[6].piece(10)
    g[3].piece(15)
    g[4].piece(10)
    layer.norm_first()
    layer.first_turned[...] = layer.first_low[...].T
    g[6].piece(5)
    g[4].piece(6)
    g[3].piece(14)
    g[5].piece(13)
    g[4].piece(5)
    g[5].piece(10)
    g[3].to_core(1)
    def feed_inner(i):
        layer.feed_inner(near(i))
        ticks(i, {
            0: [(g[5].piece, 14), (g[5].piece, 15), (g[5].to_core, 1), (g[4].piece, 9)],
            1: [(g[4].piece, 7), (gathered, 1)],
            2: [(g[4].to_core, 0), (g[4].piece, 11), (g[6].piece, 7)],
        })

    each(4, feed_inner)
    g[6].piece(9)
    g[6].piece(12)
    g[6].piece(13)
    g[6].to_core(1)
    g[6].piece(15)
    g[6].to_core(3)
    g[6].piece(14)
    g[4].piece(15)
    g[6].piece(11)
    g[6].piece(8)
    g[6].to_core(2)
    g[4].piece(13)
    g[4].piece(14)
    g[4].to_core(1)
    def feed_outer(i):
        layer.feed_outer(near(i))
        ticks(i, {
            1: [(gathered, 2)],
        })

    each(4, feed_outer)
    swapped(back_in)
    layer.norm_second()
    start_all(out_out)
    local[6].start()
    layer.outer_early(order(0))
    passed_on(2)
    cores[2].to_core(0)
    def outer_back(i):
        layer.outer_back(order(i + 1))
        ticks(i, {
            0: [(cores[2].half, 0, 0), (r[6].start, 0, 0), (r[5].start, 0, 0), (r[4].start, 0, 0)],
            1: [(passed_on, 1), (cores[2].to_core, 1), (cores[2].half, 0, 1), (r[6].start, 0, 1), (r[5].start, 0, 1), (r[4].start, 0, 1)],
        })

    each(3, outer_back)
    cores[2].half(1, 0)
    r[6].start(1, 0)
    r[5].start(1, 0)
    r[4].start(1, 0)
    layer.outer_slope(order(0))
    def inner_back(i):
        layer.inner_back(order(i))
        ticks(i, {
            0: [(cores[1].to_core, 0), (cores[2].half, 1, 1), (r[6].start, 1, 1), (r[5].start, 1, 1), (r[4].start, 1, 1), (r[6].add, 2), (r[6].add, 0)],
            1: [(cores[1].half, 0, 0), (r[2].start, 0, 0), (r[3].start, 0, 0)],
            2: [(cores[1].to_core, 1), (r[6].add, 1), (r[5].add, 4), (cores[1].half, 0, 1), (r[2].start, 0, 1), (r[3].start, 0, 1), (r[2].add, 0), (r[5].add, 1), (r[6].add, 6)],
        })

    each(4, inner_back)
    r[5].add(0)
    r[6].add(3)
    r[5].add(5)
    r[5].add(3)
    vectors_sent()
    r[6].add(4)
    r[6].add(5)
    layer.second_sums()
    r[5].add(2)
    cores[1].half(1, 0)
    r[2].start(1, 0)
    r[3].start(1, 0)
    cores[1].half(1, 1)
    r[2].start(1, 1)
    r[3].start(1, 1)
    layer.norm_first_back()
    r[2].add(1)
    passed_on(0)
    r[5].add(7)
    r[5].add(8)
    r[4].add(0)
    r[5].add(9)
    def attend_back(i):
        layer.attend_back(order(i))
        ticks(i, {
            2: [(r[4].add, 1), (r[4].add, 2), (r[6].add, 8), (r[2].add, 3), (r[2].add, 6), (r[3].add, 2), (cores[0].half, 0, 1), (r[1].start, 0, 1), (r[0].start, 0, 1), (r[5].add, 10), (r[4].add, 4)],
            3: [(cores[0].to_core, 1), (r[3].add, 6), (r[3].add, 3), (r[3].add, 7), (r[3].add, 9), (r[1].add, 1), (r[5].add, 11), (r[0].add, 0)],
        })
        layer.joint_back(order(i))
        ticks(i, {
            0: [(r[3].add, 0), (r[2].add, 4), (cores[0].to_core, 0), (r[3].add, 1), (r[2].add, 5), (r[2].add, 2), (r[5].add, 6)],
            1: [(cores[0].half, 0, 0), (r[1].start, 0, 0), (r[0].start, 0, 0), (r[2].add, 7), (r[6].add, 7), (r[3].add, 4), (r[3].add, 5)],
            2: [(r[4].add, 3), (r[3].add, 8)],
        })

    each(4, attend_back)
    cores[0].half(1, 0)
    r[1].start(1, 0)
    r[0].start(1, 0)
    r[2].add(10)
    r[1].add(0)
    r[1].add(3)
    layer.pack(parts)
    r[2].add(9)
    r[6].add(9)
    r[1].add(2)
    sums.first()
    r[0].add(1)
    r[2].add(8)
    layer.finish()
    r[0].add(2)
    r[4].add(5)
    r[4].add(6)
    r[6].add(10)
    r[2].add(11)
    sums.core_done()
    start_all(back_out)
    local[7].start()
    r[5].add(12)
    local[10].start()
    cores[0].half(1, 1)
    r[1].start(1, 1)
    r[0].start(1, 1)
    r[0].add(3)
    reduced(2)
    r[3].add(10)
    r[3].add(11)
    r[1].add(4)
    r[1].add(8)
    r[2].add(12)
    r[1].add(5)
    r[1].add(9)
    r[3].add(12)
    local[9].start()
    reduced(1)
    r[0].add(4)
    r[0].add(8)
    r[0].add(5)
    r[0].add(9)
    r[1].add(6)
    r[1].add(10)
    r[1].add(7)
    r[1].add(11)
    sums.y_done()
    r[0].add(6)
    r[0].add(10)
    r[0].add(7)
    sums.x_done()
    r[0].add(11)
    r[1].add(12)
    r[0].add(12)
    sums.z_done()
    local[11].start()
    local[8].start()
    reduced(0)
    sums.sent()
    wait_local(local[6:12])
    swapped(out_out)
    swapped(back_out)
    swaps_sent()


ANY_SPEC = pl.BlockSpec(memory_space=pl.ANY)
LIMIT = 67043328


def whole_layer(tokens, *rest):
    nz = lax.axis_size(FSDP) // 2
    part = WIDTH // (2 * nz)
    seq = tokens.shape[1] * 4
    return pl.pallas_call(
        partial(layer_kernel, nz),
        out_shape=(
            jax.ShapeDtypeStruct((KINDS, part, WIDTH), F32),
            jax.ShapeDtypeStruct(tokens.shape, BF16),
            jax.ShapeDtypeStruct(tokens.shape, BF16),
            jax.ShapeDtypeStruct((8, 128), F32),
        ),
        in_specs=[ANY_SPEC, pl.BlockSpec(memory_space=pltpu.SMEM)] + [ANY_SPEC] * 16,
        out_specs=(ANY_SPEC,) * 4,
        scratch_shapes=buffer_shapes(nz, seq) + flow_shapes(nz) + [
            pltpu.VMEM((2, nz, 2, 8, 128), F32),
            pltpu.VMEM((nz, 2, 8, 128), F32),
            pltpu.VMEM((nz, 8, 128), F32),
            pltpu.VMEM((nz - 1, 8, 128), F32),
            pltpu.VMEM((2, 2, nz, 2, 8, 128), F32),
            pltpu.VMEM((2, 2, nz, 2, 8, 128), F32),
            pltpu.VMEM((8, 128), F32),
            *[pltpu.VMEM((part, WIDTH // 4), BF16)] * 3,
            pltpu.VMEM((WIDTH // 4, part), BF16),
            pltpu.VMEM((part, WIDTH), BF16),
            *[pltpu.VMEM((SHORT,), F32)] * 8,
            pltpu.VMEM((LONG,), F32),
            pltpu.VMEM((KINDS, part, WIDTH), F32),
            pltpu.VMEM((8, 128), F32),
            pltpu.SemaphoreType.DMA((SEND_COUNT,)),
            pltpu.SemaphoreType.DMA((DOOR_COUNT,)),
            pltpu.SemaphoreType.DMA((25,)),
        ],
        compiler_params=pltpu.CompilerParams(collective_id=0, has_side_effects=True, vmem_limit_bytes=LIMIT),
        name="whole_layer",
    )(tokens, *rest)


def finish_kernel(count, *refs):
    sums_in, outs_in, backs_in, totals_in = refs[:4]
    results, rest = refs[4:4 + count], refs[4 + count:]
    sums, outs, backs, totals, input_grad, g_query, g_key, g_value, g_output = rest[:9]
    vectors, (sems, sent) = rest[9:-2], rest[-2:]
    quarters = range(backs.shape[0])
    pairs = [(backs_in.at[i], backs.at[i]) for i in quarters] + [(sums_in.at[k], sums.at[k]) for k in range(KINDS)]
    pairs += [(totals_in, totals), (outs_in, outs)]
    reads = [pltpu.make_async_copy(*pair, sems.at[i]) for i, pair in enumerate(pairs)]
    start_all(reads)
    writes = []

    def write(source, target):
        writes.append(pltpu.make_async_copy(source, target, sent.at[len(writes)]))
        writes[-1].start()

    for i in quarters:
        reads[i].wait()
        input_grad[i] = backs[i].astype(F32)
        write(input_grad.at[i], results[1].at[i])
    joint_read, inner_read, outer_read, totals_read, outs_read = reads[len(quarters):]
    joint_read.wait()
    g_query[...], g_key[...], g_value[...], g_turned = unpack_joint(sums[0])
    g_output[...] = g_turned.T
    for ref, target in zip((g_query, g_key, g_value, g_output), results[2:6]):
        write(ref, target)
    inner_read.wait()
    write(sums.at[1], results[6])
    outer_read.wait()
    write(sums.at[2], results[7])
    totals_read.wait()
    short = [0, 1, 2, None, 3, 4, 5, 6, 7]
    for row, ref, target in zip(short, vectors, results[8:]):
        ref[...] = (totals[0:1, 32:128] if row is None else totals[row:row + 1, 0:SHORT]).reshape(ref.shape)
        write(ref, target)
    outs_read.wait()
    write(outs, results[0])
    wait_local(writes)


def finish_layer(sums, outs, backs, totals):
    part = sums.shape[1]
    share = WIDTH // 4
    shapes = [outs.shape, backs.shape] + [(part, share)] * 3 + [(share, part), (part, WIDTH), (part, WIDTH)]
    shapes += [(SHORT,)] * 3 + [(LONG,)] + [(SHORT,)] * 5
    given = (sums, outs, backs, totals)
    reads, writes = backs.shape[0] + KINDS + 2, backs.shape[0] + len(shapes) - 1
    return pl.pallas_call(
        partial(finish_kernel, len(shapes)),
        out_shape=[jax.ShapeDtypeStruct(shape, F32 if i else BF16) for i, shape in enumerate(shapes)],
        in_specs=[ANY_SPEC] * len(given),
        out_specs=[ANY_SPEC] * len(shapes),
        scratch_shapes=[pltpu.VMEM(ref.shape, ref.dtype) for ref in given]
        + [pltpu.VMEM(shape, F32) for shape in shapes[1:6] + shapes[8:]]
        + [pltpu.SemaphoreType.DMA((reads,)), pltpu.SemaphoreType.DMA((writes,))],
        compiler_params=pltpu.CompilerParams(vmem_limit_bytes=LIMIT),
        name="finish_layer",
    )(*given)


def pack_joint(q, k, v, o):
    return jnp.concatenate(
        [q[:, :128], k[:, :128], v[:, :128], v[:, 128:], q[:, 128:], o[:, :128], o[:, 128:], k[:, 128:]], axis=1
    )


def unpack_joint(joint):
    q = jnp.concatenate([joint[:, 0:128], joint[:, 448:512]], axis=1)
    k = jnp.concatenate([joint[:, 128:256], joint[:, 704:768]], axis=1)
    return q, k, joint[:, 256:448], joint[:, 512:704]


def local_fast(*given):
    given = given[:8] + (given[8].T,) + given[9:]
    results = finish_layer(*whole_layer(*given))
    return (*results[:7], results[7].T, *results[8:])


def solution(mesh):
    placed = (
        P(FSDP, TENSOR, None),
        P(FSDP),
        P(FSDP, TENSOR, None),
        P(FSDP, TENSOR),
        P(FSDP, TENSOR),
        P(FSDP, TENSOR),
        P(TENSOR, FSDP),
        P(FSDP, TENSOR),
        P(TENSOR, FSDP),
        P((FSDP, TENSOR)),
        P((FSDP, TENSOR)),
        P((FSDP, TENSOR)),
        P((FSDP, TENSOR)),
        P((FSDP, TENSOR)),
        P((FSDP, TENSOR)),
        P((FSDP, TENSOR)),
        P((FSDP, TENSOR)),
        P((FSDP, TENSOR)),
    )
    return jax.shard_map(
        local_fast if fits(mesh.shape) else local_generic,
        mesh=mesh,
        in_specs=placed,
        out_specs=(
            P(FSDP, TENSOR, None),
            P(FSDP, TENSOR, None),
            P(FSDP, TENSOR),
            P(FSDP, TENSOR),
            P(FSDP, TENSOR),
            P(TENSOR, FSDP),
            P(FSDP, TENSOR),
            P(TENSOR, FSDP),
            P((FSDP, TENSOR)),
            P((FSDP, TENSOR)),
            P((FSDP, TENSOR)),
            P((FSDP, TENSOR)),
            P((FSDP, TENSOR)),
            P((FSDP, TENSOR)),
            P((FSDP, TENSOR)),
            P((FSDP, TENSOR)),
            P((FSDP, TENSOR)),
        ),
        check_vma=False,
    )
```

```python
from functools import partial

import jax
import jax.numpy as jnp
from jax import lax
from jax.experimental import pallas as pl
from jax.experimental.pallas import tpu as pltpu
from jax.sharding import PartitionSpec as P

FSDP, TENSOR = "fsdp", "tensor"

HEAD = 64


epsilon = 1e-05
root_half = 0.7071067811865476
inverse_root_two_pi = 0.3989422804014327


def gelu_value(inner):
    return 0.5 * inner * (1.0 + jax.scipy.special.erf(inner * root_half))


def gelu_slope(inner):
    return 0.5 * (
        1.0 + jax.scipy.special.erf(inner * root_half)
    ) + inner * inverse_root_two_pi * jnp.exp(-0.5 * inner * inner)


def normalize(rows):
    mean = jnp.mean(rows, axis=1, keepdims=True)
    centered = rows - mean
    variance = jnp.mean(centered * centered, axis=1, keepdims=True)
    factor = lax.rsqrt(variance + epsilon)
    return (centered * factor, factor)


def normalize_back(grad_normed, normed, factor):
    return factor * (
        grad_normed
        - jnp.mean(grad_normed, axis=1, keepdims=True)
        - normed * jnp.mean(grad_normed * normed, axis=1, keepdims=True)
    )


def column_sum(rows):
    return jnp.sum(rows.astype(jnp.float32), axis=0)


def dot_rows(left, right):
    return lax.dot_general(
        left, right, (((0,), (0,)), ((), ())), preferred_element_type=jnp.float32
    )


def dot_back(left, right):
    return lax.dot_general(
        left, right, (((1,), (1,)), ((), ())), preferred_element_type=jnp.float32
    )


def place(values, offset, total_length):
    return lax.dynamic_update_slice(jnp.zeros((total_length,), jnp.float32), values, (offset,))


def block_scores(keys, key_valid, query_block):
    raw = jnp.einsum(
        "qhd,khd->hqk", query_block, keys, preferred_element_type=jnp.float32
    ) * HEAD ** (-0.5)
    return jnp.where(key_valid[None, None, :], raw, -1000000000.0)


def attend_forward(keys, values, key_valid, query_block):
    masked = block_scores(keys, key_valid, query_block)
    top = jnp.max(masked, axis=2, keepdims=True)
    expo = jnp.exp(masked - top)
    total = jnp.sum(expo, axis=2, keepdims=True)
    probs = (expo / total).astype(jnp.bfloat16)
    context = jnp.einsum("hqk,khd->qhd", probs, values, preferred_element_type=jnp.float32)
    return (context, top, total)


def attend_backward(keys, values, key_valid, carry, item):
    key_grad, value_grad = carry
    query_block, context_grad_block, top, total = item
    masked = block_scores(keys, key_valid, query_block)
    probs = jnp.exp(masked - top) / total
    probs_low = probs.astype(jnp.bfloat16)
    prob_grad = jnp.einsum(
        "qhd,khd->hqk", context_grad_block, values, preferred_element_type=jnp.float32
    )
    delta = jnp.sum(prob_grad * probs, axis=2, keepdims=True)
    score_grad = (probs * (prob_grad - delta)).astype(jnp.bfloat16)
    factor = HEAD ** (-0.5)
    query_grad = (
        jnp.einsum("hqk,khd->qhd", score_grad, keys, preferred_element_type=jnp.float32) * factor
    )
    key_grad = (
        key_grad
        + jnp.einsum("hqk,qhd->khd", score_grad, query_block, preferred_element_type=jnp.float32)
        * factor
    )
    value_grad = value_grad + jnp.einsum(
        "hqk,qhd->khd", probs_low, context_grad_block, preferred_element_type=jnp.float32
    )
    return ((key_grad, value_grad), query_grad)


def gather_weights(w_query, w_key, w_value, w_output, w_inner, w_outer):
    return (
        lax.all_gather(w_query, FSDP, axis=0, tiled=True),
        lax.all_gather(w_key, FSDP, axis=0, tiled=True),
        lax.all_gather(w_value, FSDP, axis=0, tiled=True),
        lax.all_gather(w_output, FSDP, axis=1, tiled=True),
        lax.all_gather(w_inner, FSDP, axis=0, tiled=True),
        lax.all_gather(w_outer, FSDP, axis=1, tiled=True),
    )


def split_joint(joint_sum, output_sum, inner_sum, outer_sum, head_width):
    return (
        joint_sum[:, :head_width],
        joint_sum[:, head_width : 2 * head_width],
        joint_sum[:, 2 * head_width :],
        output_sum,
        inner_sum,
        outer_sum,
    )


def add_tuples(left, right):
    return tuple((first_item + second_item for first_item, second_item in zip(left, right)))


def local_generic(
    tokens,
    lengths,
    cotangent,
    w_query,
    w_key,
    w_value,
    w_output,
    w_inner,
    w_outer,
    b_query,
    b_value,
    b_output,
    b_inner,
    b_outer,
    gain_first,
    shift_first,
    gain_second,
    shift_second,
):
    tensor_size = lax.axis_size(TENSOR)
    tensor_rank = lax.axis_index(TENSOR)
    micro_count = tokens.shape[0]
    part_rows = tokens.shape[1]
    width = tokens.shape[2]
    seq_rows = part_rows * tensor_size
    head_width = w_query.shape[1]
    inner_width = w_inner.shape[1]
    local_heads = head_width // HEAD
    block_rows = min(512, seq_rows)
    block_count = seq_rows // block_rows
    vector_full = (
        lax.all_gather(b_query, (FSDP, TENSOR), axis=0, tiled=True),
        lax.all_gather(b_value, (FSDP, TENSOR), axis=0, tiled=True),
        lax.all_gather(b_output, (FSDP, TENSOR), axis=0, tiled=True),
        lax.all_gather(b_inner, (FSDP, TENSOR), axis=0, tiled=True),
        lax.all_gather(b_outer, (FSDP, TENSOR), axis=0, tiled=True),
        lax.all_gather(gain_first, (FSDP, TENSOR), axis=0, tiled=True),
        lax.all_gather(shift_first, (FSDP, TENSOR), axis=0, tiled=True),
        lax.all_gather(gain_second, (FSDP, TENSOR), axis=0, tiled=True),
        lax.all_gather(shift_second, (FSDP, TENSOR), axis=0, tiled=True),
    )
    query_bias = lax.dynamic_slice_in_dim(vector_full[0], tensor_rank * head_width, head_width)
    value_bias = lax.dynamic_slice_in_dim(vector_full[1], tensor_rank * head_width, head_width)
    inner_bias = lax.dynamic_slice_in_dim(vector_full[3], tensor_rank * inner_width, inner_width)
    joint_bias = jnp.concatenate([query_bias, jnp.zeros((head_width,), jnp.float32), value_bias])
    grad_query_bias = jnp.zeros((head_width,), jnp.float32)
    grad_value_bias = jnp.zeros((head_width,), jnp.float32)
    grad_inner_bias = jnp.zeros((inner_width,), jnp.float32)
    grad_output_bias = jnp.zeros((width,), jnp.float32)
    grad_outer_bias = jnp.zeros((width,), jnp.float32)
    grad_gain_one = jnp.zeros((width,), jnp.float32)
    grad_shift_one = jnp.zeros((width,), jnp.float32)
    grad_gain_two = jnp.zeros((width,), jnp.float32)
    grad_shift_two = jnp.zeros((width,), jnp.float32)
    local_totals = None
    shard_totals = None
    outputs = []
    input_grads = []
    slot_index = jnp.arange(seq_rows, dtype=jnp.int32)
    part_index = tensor_rank * part_rows + jnp.arange(part_rows, dtype=jnp.int32)
    for micro_index in range(micro_count):
        forward_weights = gather_weights(w_query, w_key, w_value, w_output, w_inner, w_outer)
        joint_w = jnp.concatenate(
            [forward_weights[0], forward_weights[1], forward_weights[2]], axis=1
        )
        output_w = forward_weights[3]
        inner_w = forward_weights[4]
        outer_w = forward_weights[5]
        length = lengths[micro_index]
        key_valid = slot_index < length
        row_valid = (part_index < length).astype(jnp.float32)[:, None]
        own_rows = tokens[micro_index]
        whole = lax.all_gather(own_rows, TENSOR, axis=0, tiled=True)
        joint = (jnp.dot(whole, joint_w, preferred_element_type=jnp.float32) + joint_bias).astype(
            jnp.bfloat16
        )
        query = joint[:, :head_width].reshape(block_count, block_rows, local_heads, HEAD)
        keys = joint[:, head_width : 2 * head_width].reshape(seq_rows, local_heads, HEAD)
        values = joint[:, 2 * head_width :].reshape(seq_rows, local_heads, HEAD)
        context_blocks, tops, totals = lax.map(
            partial(attend_forward, keys, values, key_valid), query
        )
        context_low = context_blocks.reshape(seq_rows, head_width).astype(jnp.bfloat16)
        attended = (
            lax.psum_scatter(
                jnp.dot(context_low, output_w, preferred_element_type=jnp.float32).astype(
                    jnp.bfloat16
                ),
                TENSOR,
                scatter_dimension=0,
                tiled=True,
            ).astype(jnp.float32)
            + vector_full[2]
        )
        normed_first, factor_first = normalize(own_rows.astype(jnp.float32) + attended)
        first = normed_first * vector_full[5] + vector_full[6]
        first_whole = lax.all_gather(first.astype(jnp.bfloat16), TENSOR, axis=0, tiled=True)
        inner = jnp.dot(first_whole, inner_w, preferred_element_type=jnp.float32) + inner_bias
        active = gelu_value(inner).astype(jnp.bfloat16)
        mixed = (
            lax.psum_scatter(
                jnp.dot(active, outer_w, preferred_element_type=jnp.float32).astype(jnp.bfloat16),
                TENSOR,
                scatter_dimension=0,
                tiled=True,
            ).astype(jnp.float32)
            + vector_full[4]
        )
        normed_second, factor_second = normalize(first + mixed)
        outputs.append(
            ((normed_second * vector_full[7] + vector_full[8]) * row_valid).astype(jnp.bfloat16)
        )
        backward_weights = gather_weights(w_query, w_key, w_value, w_output, w_inner, w_outer)
        joint_w = jnp.concatenate(
            [backward_weights[0], backward_weights[1], backward_weights[2]], axis=1
        )
        output_w = backward_weights[3]
        inner_w = backward_weights[4]
        outer_w = backward_weights[5]
        out_grad = cotangent[micro_index].astype(jnp.float32) * row_valid
        grad_gain_two = grad_gain_two + column_sum(out_grad * normed_second)
        grad_shift_two = grad_shift_two + column_sum(out_grad)
        sum_grad = normalize_back(out_grad * vector_full[7], normed_second, factor_second)
        mixed_grad = sum_grad.astype(jnp.bfloat16)
        grad_outer_bias = grad_outer_bias + column_sum(mixed_grad)
        mixed_whole = lax.all_gather(mixed_grad, TENSOR, axis=0, tiled=True)
        outer_sum = dot_rows(active, mixed_whole)
        inner_grad = (dot_back(mixed_whole, outer_w) * gelu_slope(inner)).astype(jnp.bfloat16)
        grad_inner_bias = grad_inner_bias + column_sum(inner_grad)
        inner_sum = dot_rows(first_whole, inner_grad)
        first_grad = sum_grad + lax.psum_scatter(
            dot_back(inner_grad, inner_w).astype(jnp.bfloat16),
            TENSOR,
            scatter_dimension=0,
            tiled=True,
        ).astype(jnp.float32)
        grad_gain_one = grad_gain_one + column_sum(first_grad * normed_first)
        grad_shift_one = grad_shift_one + column_sum(first_grad)
        residual_grad = normalize_back(first_grad * vector_full[5], normed_first, factor_first)
        attended_grad = residual_grad.astype(jnp.bfloat16)
        grad_output_bias = grad_output_bias + column_sum(attended_grad)
        attended_whole = lax.all_gather(attended_grad, TENSOR, axis=0, tiled=True)
        output_sum = dot_rows(context_low, attended_whole)
        context_grad = (
            dot_back(attended_whole, output_w)
            .astype(jnp.bfloat16)
            .reshape(block_count, block_rows, local_heads, HEAD)
        )
        empty = jnp.zeros((seq_rows, local_heads, HEAD), jnp.float32)
        carried, query_grad = lax.scan(
            partial(attend_backward, keys, values, key_valid),
            (empty, empty),
            (query, context_grad, tops, totals),
        )
        joint_grad = jnp.concatenate(
            [
                query_grad.reshape(seq_rows, head_width),
                carried[0].reshape(seq_rows, head_width),
                carried[1].reshape(seq_rows, head_width),
            ],
            axis=1,
        ).astype(jnp.bfloat16)
        grad_query_bias = grad_query_bias + column_sum(joint_grad[:, :head_width])
        grad_value_bias = grad_value_bias + column_sum(joint_grad[:, 2 * head_width :])
        joint_sum = dot_rows(whole, joint_grad)
        input_grads.append(
            residual_grad
            + lax.psum_scatter(
                dot_back(joint_grad, joint_w).astype(jnp.bfloat16),
                TENSOR,
                scatter_dimension=0,
                tiled=True,
            ).astype(jnp.float32)
        )
        batch_sums = (joint_sum, output_sum, inner_sum, outer_sum)
        local_totals = batch_sums if local_totals is None else add_tuples(local_totals, batch_sums)
    pieces = split_joint(
        local_totals[0], local_totals[1], local_totals[2], local_totals[3], head_width
    )
    shard_totals = (
        lax.psum_scatter(pieces[0], FSDP, scatter_dimension=0, tiled=True),
        lax.psum_scatter(pieces[1], FSDP, scatter_dimension=0, tiled=True),
        lax.psum_scatter(pieces[2], FSDP, scatter_dimension=0, tiled=True),
        lax.psum_scatter(pieces[3], FSDP, scatter_dimension=1, tiled=True),
        lax.psum_scatter(pieces[4], FSDP, scatter_dimension=0, tiled=True),
        lax.psum_scatter(pieces[5], FSDP, scatter_dimension=1, tiled=True),
    )
    vector_grads = (
        lax.psum_scatter(
            place(grad_query_bias, tensor_rank * head_width, width),
            (FSDP, TENSOR),
            scatter_dimension=0,
            tiled=True,
        ),
        lax.psum_scatter(
            place(grad_value_bias, tensor_rank * head_width, width),
            (FSDP, TENSOR),
            scatter_dimension=0,
            tiled=True,
        ),
        lax.psum_scatter(grad_output_bias, (FSDP, TENSOR), scatter_dimension=0, tiled=True),
        lax.psum_scatter(
            place(grad_inner_bias, tensor_rank * inner_width, inner_width * tensor_size),
            (FSDP, TENSOR),
            scatter_dimension=0,
            tiled=True,
        ),
        lax.psum_scatter(grad_outer_bias, (FSDP, TENSOR), scatter_dimension=0, tiled=True),
        lax.psum_scatter(grad_gain_one, (FSDP, TENSOR), scatter_dimension=0, tiled=True),
        lax.psum_scatter(grad_shift_one, (FSDP, TENSOR), scatter_dimension=0, tiled=True),
        lax.psum_scatter(grad_gain_two, (FSDP, TENSOR), scatter_dimension=0, tiled=True),
        lax.psum_scatter(grad_shift_two, (FSDP, TENSOR), scatter_dimension=0, tiled=True),
    )
    return (
        jnp.stack(outputs),
        jnp.stack(input_grads),
        shard_totals[0],
        shard_totals[1],
        shard_totals[2],
        shard_totals[3],
        shard_totals[4],
        shard_totals[5],
        vector_grads[0],
        vector_grads[1],
        vector_grads[2],
        vector_grads[3],
        vector_grads[4],
        vector_grads[5],
        vector_grads[6],
        vector_grads[7],
        vector_grads[8],
    )


MESH = pl.DeviceIdType.MESH
WIDTH = 768
HIDDEN = 3072
HALF = WIDTH // 2
KINDS = 3
FLOWS = (
    (0, 0, 512, "zyx", "xyz"),
    (0, 512, 256, "zyx", "xyz"),
    (1, 0, 256, "zxy", "xyz"),
    (1, 256, 512, "zxy", "yxz"),
    (2, 0, 256, "zyx", "zxy"),
    (2, 256, 256, "zyx", "yxz"),
    (2, 512, 256, "yxz", "xzy"),
)
VECTOR_ROWS = 16
SHORT, LONG = 24, 96
ROW_OUTPUT, ROW_OUTER, ROW_GAIN1, ROW_SHIFT1, ROW_GAIN2, ROW_SHIFT2, ROW_INNER = 4, 5, 6, 7, 8, 9, 10
BF16 = jnp.bfloat16
F32 = jnp.float32


def fits(sizes):
    fsdp = sizes[FSDP]
    return sizes[TENSOR] == 4 and fsdp == WIDTH // LONG


class Place:
    def __init__(self, nz):
        self.f = lax.axis_index(FSDP)
        self.t = lax.axis_index(TENSOR)
        self.nz = nz
        self.z = self.f // 2
        self.x = self.f % 2
        self.y = self.t // 2
        self.c = self.t % 2
        self.core = (self.f, self.t + 1 - 2 * self.c)
        self.along_y = (self.f, self.t + 2 - 4 * self.y)
        self.along_x = (self.f + 1 - 2 * self.x, self.t)

    def z_at(self, step):
        return (self.z + step) % self.nz

    def z_back(self, step):
        return (self.z + self.nz - step) % self.nz

    def along_z(self, step):
        return (self.z_at(step) * 2 + self.x, self.t)

    def in_group(self, step):
        return (self.f, (self.t + step) % 4)


class Trip:
    def __init__(self, copy, send_sem, recv_sem):
        self.copy, self.send_sem, self.recv_sem = copy, send_sem, recv_sem

    def start(self):
        self.copy.start()

    def wait_recv(self):
        self.copy.wait_recv()


class Net:
    def __init__(self, send_sems, recv_sems):
        self.send_sems, self.recv_sems = send_sems, recv_sems
        self.sends = self.recvs = 0

    def lane(self):
        self.sends += 1
        return self.send_sems.at[self.sends - 1]

    def door(self):
        self.recvs += 1
        return self.recv_sems.at[self.recvs - 1]

    def plan(self, source, target, device, lane, door=None):
        door = self.door() if door is None else door
        copy = pltpu.make_async_remote_copy(
            src_ref=source, dst_ref=target, send_sem=lane, recv_sem=door, device_id=device, device_id_type=MESH
        )
        return Trip(copy, lane, door)

    def keep(self, ref, device, lane, door=None):
        return self.plan(ref, ref, device, lane, door)


class Meter:
    def __init__(self, low, wide):
        self.low, self.wide = low, wide

    def low_rows(self, rows):
        for count in (1, 2, 3, 4):
            if rows % (16 * count) == 0 and rows // count <= self.low.shape[1]:
                return self.low.at[0:count, 0:rows // count]
        raise ValueError(rows)

    def tiles(self, count):
        return self.wide.at[0:8 * count]


def arrived(trips, size):
    pltpu.make_async_copy(size, size, trips[0].recv_sem).wait()


def departed(trips, size):
    pltpu.make_async_copy(size, size, trips[0].send_sem).wait()


def start_all(copies):
    for copy in copies:
        copy.start()


def greet(place):
    barrier = pltpu.get_barrier_semaphore()
    peers = [place.in_group(1), place.in_group(2), place.in_group(3), place.along_x]
    peers += [place.along_z(step) for step in range(1, place.nz)]
    for peer in peers:
        pl.semaphore_signal(barrier, inc=1, device_id=peer, device_id_type=MESH)
    pl.semaphore_wait(barrier, len(peers))


def wait_local(copies):
    for copy in copies:
        copy.wait()


def dot(left, right):
    return lax.dot_general(left, right, (((1,), (0,)), ((), ())), preferred_element_type=F32)


def turn(value, shift):
    shift %= value.shape[1]
    return pltpu.roll(value, shift, 1) if shift else value


class Layer:
    def __init__(self, refs, length):
        (
            self.w, self.rows, self.back, self.rows_turned, self.joint, self.probs, self.context, self.acc,
            self.normed, self.factor, self.first_low, self.first_turned, self.active, self.slope, self.grad_low,
            self.grad_turned, self.out, self.vec, self.sums, self.early,
        ) = refs
        self.length = length
        self.seq = self.rows.shape[0]
        self.block = self.seq

    def weight(self, kind, t):
        return self.w[kind, t // 2, t % 2].reshape(WIDTH, WIDTH)

    def output_weight(self, t):
        return self.w[0, t // 2, t % 2, :, :, :, 512:768].reshape(WIDTH, 256)

    def store_grad(self, kind, t, value):
        nz = self.w.shape[3]
        self.w[kind, t // 2, t % 2] = value.astype(BF16).reshape(nz, 2, WIDTH // (2 * nz), WIDTH)

    def row(self, index):
        return self.vec[pl.ds(index, 1), :]

    def blocks(self, body):
        def step(i, carry):
            body(pl.ds(pl.multiple_of(i * self.block, self.block), self.block), i)
            return carry

        lax.fori_loop(0, self.seq // self.block, step, 0)

    def row_valid(self, i):
        index = lax.broadcasted_iota(jnp.int32, (self.block, 1), 0) + i * self.block
        return (index < self.length).astype(F32)

    def lanes(self, low, high, width):
        lane = lax.broadcasted_iota(jnp.int32, (1, width), 1)
        return (lane >= low) & (lane < high)

    def pick(self, value, low, high):
        return jnp.where(self.lanes(low, high, value.shape[1]), value, jnp.zeros_like(value))

    def head_query(self, t, h):
        return self.joint[t, :, 0:128] if h < 2 else self.joint[t, :, 384:512]

    def head_key(self, t, h):
        return self.joint[t, :, 128:256] if h < 2 else self.joint[t, :, 640:768]

    def head_side(self, value, h):
        return self.pick(value, 0, 64) if h == 0 else self.pick(value, 64, 128)

    def head_value(self, t, h):
        return self.pick(self.joint[t, :, 256:512], h * 64, h * 64 + 64)

    def unpack(self, v):
        nz = v.shape[2]
        short = jnp.zeros((8, WIDTH), F32)
        inner = [jnp.zeros((1, WIDTH), F32) for _ in range(4)]
        for f in range(2 * nz):
            for t in range(4):
                rank = f * 4 + t
                block = v[t // 2, t % 2, f // 2, f % 2]
                wide = jnp.concatenate([self.pick(block, 0, SHORT), jnp.zeros((8, WIDTH - 128), F32)], axis=1)
                short += turn(wide, rank * SHORT)
                wide = jnp.concatenate([self.pick(block[0:1], 32, 128), jnp.zeros((1, WIDTH - 128), F32)], axis=1)
                inner[rank * LONG // WIDTH] += turn(wide, rank * LONG % WIDTH - 32)
        for t in range(4):
            query = self.pick(turn(short[0:1], -192 * t), 0, 128) + self.pick(turn(short[0:1], 320 - 192 * t), 448, 512)
            self.vec[t:t + 1] = query + self.pick(turn(short[1:2], 256 - 192 * t), 256, 448)
            self.vec[ROW_INNER + t:ROW_INNER + t + 1] = inner[t]
        self.vec[ROW_OUTPUT:ROW_INNER] = short[2:8]

    def pack(self, parts):
        nz = parts.shape[2]
        query, value = jnp.zeros((1, WIDTH), F32), jnp.zeros((1, WIDTH), F32)
        for t in range(4):
            row = self.sums[t:t + 1]
            query += turn(self.pick(row, 0, 128), 192 * t) + turn(self.pick(row, 448, 512), 192 * t - 320)
            value += turn(self.pick(row, 256, 448), 192 * t - 256)
        short = jnp.concatenate([query, value, self.sums[ROW_OUTPUT:ROW_INNER]], axis=0)
        top = lax.broadcasted_iota(jnp.int32, (8, 1), 0) == 0
        for f in range(2 * nz):
            for t in range(4):
                rank = f * 4 + t
                block = self.pick(turn(short, -rank * SHORT)[:, 0:128], 0, SHORT)
                index = ROW_INNER + rank * LONG // WIDTH
                inner = turn(self.sums[index:index + 1], 32 - rank * LONG % WIDTH)[:, 0:128]
                inner = jnp.broadcast_to(self.pick(inner, 32, 128), (8, 128))
                parts[t // 2, t % 2, f // 2, f % 2] = block + jnp.where(top, inner, 0.0)

    def project(self, t):
        self.joint[t] = (dot(self.rows[...], self.weight(0, t)) + self.row(t)).astype(BF16)

    def attend(self, t):
        key_valid = lax.broadcasted_iota(jnp.int32, (1, self.seq), 1) < self.length
        context = None
        for h in range(3):
            raw = dot_back(self.head_query(t, h), self.head_side(self.head_key(t, h), h))
            masked = jnp.where(key_valid, raw * HEAD ** -0.5, -1e9)
            expo = jnp.exp(masked - jnp.max(masked, axis=1, keepdims=True))
            probs = (expo * (1.0 / jnp.sum(expo, axis=1, keepdims=True))).astype(BF16)
            self.probs[t * 3 + h] = probs
            part = dot(probs, self.head_value(t, h))
            context = part if context is None else context + part
        low = context.astype(BF16)
        self.context[t] = low
        self.acc[...] += dot_back(low, self.output_weight(t))

    def start(self):
        def body(rows, i):
            self.acc[rows] = self.rows[rows].astype(F32) + self.row(ROW_OUTPUT)

        self.blocks(body)

    def norm_first(self):
        def body(rows, i):
            normed, factor = normalize(self.acc[rows])
            self.normed[rows] = normed
            self.factor[rows] = jnp.broadcast_to(factor, (self.block, 128))
            first = normed * self.row(ROW_GAIN1) + self.row(ROW_SHIFT1)
            self.first_low[rows] = first.astype(BF16)
            self.acc[rows] = first + self.row(ROW_OUTER)

        self.blocks(body)

    def feed_inner(self, t):
        inner = dot(self.first_low[...], self.weight(1, t)) + self.row(ROW_INNER + t)
        gate = 1.0 + lax.erf(inner * root_half)
        self.active[t] = (0.5 * inner * gate).astype(BF16)
        self.slope[t] = (0.5 * gate + inner * inverse_root_two_pi * jnp.exp(-0.5 * inner * inner)).astype(BF16)

    def feed_outer(self, t):
        self.acc[...] += dot_back(self.active[t], self.weight(2, t))

    def clear_sums(self):
        self.sums[...] = jnp.zeros_like(self.sums)

    def add_sum(self, index, value):
        self.sums[pl.ds(index, 1), :] += jnp.sum(value, axis=0, keepdims=True)

    def norm_second(self):
        def body(rows, i):
            normed, factor = normalize(self.acc[rows])
            valid = self.row_valid(i)
            gain = self.row(ROW_GAIN2)
            self.first_low[rows] = normed.astype(BF16)
            self.out[rows] = ((normed * gain + self.row(ROW_SHIFT2)) * valid).astype(BF16)
            out_grad = self.back[rows].astype(F32) * valid
            sum_grad = normalize_back(out_grad * gain, normed, factor)
            self.acc[rows] = sum_grad
            self.grad_low[rows] = sum_grad.astype(BF16)

        self.blocks(body)

    def second_sums(self):
        def body(rows, i):
            out_grad = self.back[rows].astype(F32) * self.row_valid(i)
            self.add_sum(ROW_GAIN2, out_grad * self.first_low[rows].astype(F32))
            self.add_sum(ROW_SHIFT2, out_grad)
            self.add_sum(ROW_OUTER, self.grad_low[rows].astype(F32))

        self.blocks(body)

    def outer_slope(self, t):
        grad = (dot(self.grad_low[...], self.weight(2, t)) * self.slope[t].astype(F32)).astype(BF16)
        self.slope[t] = grad
        self.add_sum(ROW_INNER + t, grad.astype(F32))

    def outer_back(self, t):
        self.outer_slope(t)
        self.store_grad(2, t, dot_rows(self.grad_low[...], self.active[t]))

    def outer_early(self, t):
        value = dot_rows(self.grad_low[...], self.active[t])
        self.early[...] = value.astype(BF16).reshape(self.early.shape)

    def inner_back(self, t):
        grad = self.slope[t]
        self.acc[...] += dot_back(grad, self.weight(1, t))
        self.store_grad(1, t, dot(self.first_turned[...], grad))

    def norm_first_back(self):
        def body(rows, i):
            grad = self.acc[rows]
            normed = self.normed[rows]
            self.add_sum(ROW_GAIN1, grad * normed)
            self.add_sum(ROW_SHIFT1, grad)
            residual = normalize_back(grad * self.row(ROW_GAIN1), normed, self.factor[rows][:, 0:1])
            self.acc[rows] = residual
            low = residual.astype(BF16)
            self.grad_low[rows] = low
            self.add_sum(ROW_OUTPUT, low.astype(F32))

        self.blocks(body)
        self.grad_turned[...] = self.grad_low[...].T

    def attend_back(self, t):
        context_grad = self.pick(dot(self.grad_low[...], self.output_weight(t)), 0, 192).astype(BF16)
        query_grads, key_grads, value_grad = [], [], None
        for h in range(3):
            probs = self.probs[t * 3 + h]
            prob_grad = dot_back(context_grad, self.head_value(t, h))
            wide = probs.astype(F32)
            delta = jnp.sum(wide * prob_grad, axis=1, keepdims=True)
            score_grad = (wide * (prob_grad - delta)).astype(BF16)
            query_grads.append(dot(score_grad, self.head_side(self.head_key(t, h), h)) * HEAD ** -0.5)
            key_grads.append(dot_rows(score_grad, self.head_side(self.head_query(t, h), h)) * HEAD ** -0.5)
            part = dot_rows(probs, self.pick(context_grad, h * 64, h * 64 + 64))
            value_grad = part if value_grad is None else value_grad + part
        self.joint[t, :, 0:128] = (query_grads[0] + query_grads[1]).astype(BF16)
        self.joint[t, :, 128:256] = (key_grads[0] + key_grads[1]).astype(BF16)
        self.joint[t, :, 256:384] = value_grad[:, 0:128].astype(BF16)
        self.joint[t, :, 384:512] = (value_grad[:, 128:256] + query_grads[2]).astype(BF16)
        self.joint[t, :, 512:640] = jnp.zeros((self.seq, 128), BF16)
        self.joint[t, :, 640:768] = key_grads[2].astype(BF16)

    def joint_back(self, t):
        joint = self.joint[t]
        self.sums[pl.ds(t, 1), :] = jnp.sum(joint.astype(F32), axis=0, keepdims=True)
        self.acc[...] += dot_back(joint, self.weight(0, t))
        nz = self.w.shape[3]
        shape = (nz, 2, WIDTH // (2 * nz), -1)
        main = dot(self.rows_turned[...], joint[:, 0:512])
        side = dot(self.rows_turned[...], joint[:, 512:768]) + dot(self.grad_turned[...], self.context[t])
        self.w[0, t // 2, t % 2, :, :, :, 0:512] = main.astype(BF16).reshape(shape[:3] + (512,))
        self.w[0, t // 2, t % 2, :, :, :, 512:768] = side.astype(BF16).reshape(shape[:3] + (256,))

    def finish(self):
        def body(rows, i):
            self.back[rows] = self.acc[rows].astype(BF16)

        self.blocks(body)


def each(count, body):
    def step(i, carry):
        body(i)
        return carry

    lax.fori_loop(0, count, step, 0)


BUFFER_COUNT = 20


def buffer_shapes(nz, seq):
    part = WIDTH // (2 * nz)
    low, wide = (seq, WIDTH), (WIDTH, seq)
    shapes = [
        ((KINDS, 2, 2, nz, 2, part, WIDTH), BF16),
        (low, BF16),
        (low, BF16),
        (wide, BF16),
        ((4, seq, WIDTH), BF16),
        ((12, seq, seq), BF16),
        ((4, seq, 256), BF16),
        (low, F32),
        (low, F32),
        ((seq, 128), F32),
        (low, BF16),
        (wide, BF16),
        ((4, seq, WIDTH), BF16),
        ((4, seq, WIDTH), BF16),
        (low, BF16),
        (wide, BF16),
        (low, BF16),
        ((VECTOR_ROWS, WIDTH), F32),
        ((VECTOR_ROWS, WIDTH), F32),
        ((nz, 2, part, WIDTH), BF16),
    ]
    return [pltpu.VMEM(*shape) for shape in shapes]


BLOCKS = 15
SEND_COUNT = 15
DOOR_COUNT = 227


def flow_shapes(nz):
    part = WIDTH // (2 * nz)
    shapes = [pltpu.VMEM((KINDS, 2, nz, 2, part, WIDTH), BF16)]
    return shapes + [pltpu.VMEM((BLOCKS, part, flow[2]), BF16) for flow in FLOWS]


def axis_steps(place, axis):
    p = place
    if axis == "x":
        return [(1, 1 - p.x, p.along_x, 1 - p.x)]
    if axis == "y":
        return [(1, 1 - p.y, p.along_y, 1 - p.y)]
    return [(step, p.z_at(step), p.along_z(step), p.z_back(step)) for step in range(1, p.nz)]


class Flow:
    def __init__(self, net, place, order, own, region, lane, core_lane, core_door):
        p = place
        self.pieces = [(None, [])]
        spots = [({"x": p.x, "y": p.y, "z": p.z}, own)]
        for axis in order:
            for index, (spot, source) in enumerate(list(spots)):
                for _, _, device, behind in axis_steps(p, axis):
                    trip = net.plan(region(spot) if source is None else source, region(spot), device, lane)
                    self.pieces[index][1].append(trip)
                    self.pieces.append((trip, []))
                    spots.append(({**spot, axis: behind}, None))
        mine = {"x": p.x, "y": p.y, "z": p.z}[order[2]]
        sides = [mine] + [behind for _, _, _, behind in axis_steps(p, order[2])]
        every = slice(None)
        self.cores = [
            net.keep(region({"x": every, "y": every, "z": every, order[2]: side}), p.core, core_lane, core_door)
            for side in sides
        ]
        self.trips = [trip for _, onward in self.pieces for trip in onward]

    def first(self):
        start_all(self.pieces[0][1])

    def piece(self, index):
        trip, onward = self.pieces[index]
        trip.wait_recv()
        start_all(onward)

    def to_core(self, index):
        self.cores[index].start()


class Cores:
    def __init__(self, net, place, w, core, k, meter, early=None):
        self.place, self.meter = place, meter
        self.w, self.core = w.at[k], core.at[k]
        self.ys = (1 - place.y, place.y)
        steps = list(range(1, place.nz)) + [0]
        self.parts = steps[:place.nz // 2], steps[place.nz // 2:]
        self.c = []
        lane = net.lane()
        for y in self.ys:
            for part in self.parts:
                door = net.door()
                spots = [place.z_at(step) for step in part]
                source = self.w.at[y, 1 - place.c] if early is None or self.c[1:] else early
                self.c.append([net.plan(source.at[z], self.core.at[y, z], place.core, lane, door) for z in spots])
        self.trips = [trip for trips in self.c for trip in trips]

    def to_core(self, half):
        start_all(self.c[2 * half] + self.c[2 * half + 1])

    def half(self, half, part):
        y = self.ys[half]
        trips = self.c[2 * half + part]
        arrived(trips, self.meter.low_rows(2 * self.core.shape[-2] * len(trips)))
        for step in self.parts[part]:
            z = self.place.z_at(step)
            target, source = self.core.at[y, z], self.w.at[y, self.place.c, z]
            target[...] = (target[...].astype(F32) + source[...].astype(F32)).astype(BF16)


class Sink:
    def __init__(self, net, place, order, core, landing, result, cols, lane, meter):
        p = place
        self.meter = meter
        self.core, self.landing, self.result, self.cols = core, landing, result, cols
        here = {"x": p.x, "y": p.y, "z": p.z}
        ahead = {axis: {0: here[axis], **{step: spot for step, spot, _, _ in axis_steps(p, axis)}} for axis in here}
        sizes = {"x": 2, "y": 2, "z": p.nz}
        self.spot = lambda block: tuple(ahead[axis][block[axis]] for axis in ("y", "z", "x"))
        self.order = order
        self.tasks = []
        self.starts = [[], [], [], []]
        blocks = [{}]
        for axis in ("y", "z", "x"):
            steps = [i for i in range(1, sizes[axis])] + [0]
            blocks = [{**block, axis: step} for block in blocks for step in steps]
        slot = 0
        self.trips = []
        waits = {}
        for stage, axis in enumerate(order):
            later = order[stage + 1:]
            kept = [block for block in blocks if block[axis] == 0]
            kept.sort(key=lambda block: [block[other] == 0 for other in later])
            devices = {step: device for step, _, device, _ in axis_steps(p, axis)}
            for block in kept:
                arrivals = []
                door = net.door()
                for step in range(1, sizes[axis]):
                    away = {**block, axis: step}
                    copy = net.plan(self.part(away), landing.at[slot], devices[step], lane, door)
                    self.trips.append(copy)
                    if stage == 0:
                        soon = 0 < away["z"] <= p.nz // 2
                        self.starts[(0 if away["y"] else 2) + (0 if soon else 1)].append(copy)
                    else:
                        waits[tuple(sorted(away.items()))].append(copy)
                    arrivals.append((copy, slot))
                    slot += 1
                onward = []
                waits[tuple(sorted(block.items()))] = onward
                self.tasks.append((block, arrivals, onward))
            blocks = kept

    def part(self, block):
        return self.core.at[(*self.spot(block), slice(None), self.cols)]

    def start(self, half, part):
        start_all(self.starts[2 * half + part])

    def add(self, index):
        block, arrivals, onward = self.tasks[index]
        target = self.part(block)
        total = target[...].astype(F32)
        rows = self.landing.shape[1] * self.landing.shape[2] // WIDTH
        arrived([trip for trip, _ in arrivals], self.meter.low_rows(rows * len(arrivals)))
        for _, slot in arrivals:
            total += self.landing[slot].astype(F32)
        if index < len(self.tasks) - 1:
            target[...] = total.astype(BF16)
            start_all(onward)
        else:
            self.result[:, self.cols] = total


class Back:
    def __init__(self, net, place, parts, landings, result, meter):
        p = self.place = place
        self.parts, self.result, self.meter = parts, result, meter
        self.core, self.side, self.pair, self.line = landings
        lane = net.lane()
        self.c = net.plan(parts.at[:, 1 - p.c], self.core, p.core, lane)
        self.y = net.plan(self.core.at[1 - p.y], self.side, p.along_y, lane)
        self.x = net.plan(self.side.at[:, 1 - p.x], self.pair, p.along_x, lane)
        door = net.door()
        self.z = [
            net.plan(self.pair.at[p.z_at(step)], self.line.at[step - 1], p.along_z(step), lane, door)
            for step in range(1, p.nz)
        ]

    def first(self):
        self.c.start()

    def core_done(self):
        self.c.wait_recv()
        self.core[...] += self.parts[:, self.place.c]
        self.y.start()

    def y_done(self):
        self.y.wait_recv()
        self.side[...] += self.core[self.place.y]
        self.x.start()

    def x_done(self):
        self.x.wait_recv()
        self.pair[...] += self.side[:, self.place.x]
        start_all(self.z)

    def z_done(self):
        arrived(self.z, self.meter.tiles(len(self.z)))
        total = self.pair[self.place.z]
        for i in range(self.place.nz - 1):
            total += self.line[i]
        self.result[...] = total

    def sent(self):
        departed([self.c, self.y, self.x] + self.z, self.meter.tiles(8 * self.place.nz - 1))


def ticks(i, table):
    for when, actions in table.items():
        @pl.when(i == when)
        def _(actions=actions):
            for action, *given in actions:
                action(*given)


def layer_kernel(nz, *refs):
    tokens, lengths, cotangent, w_query, w_key, w_value, w_output, w_inner, w_outer = refs[:9]
    short_in, long_in = refs[9:12] + refs[13:18], refs[12]
    result_out, outs, backs, totals_out = refs[18:22]
    rest = list(refs[22:])
    buffers, rest = rest[:BUFFER_COUNT], rest[BUFFER_COUNT:]
    core_landing, landings, rest = rest[0], rest[1:1 + len(FLOWS)], rest[1 + len(FLOWS):]
    back_landings = rest[:4]
    v, parts, vec_in, raw_query, raw_key, raw_value, raw_output, own_joint = rest[4:12]
    raw_short, raw_long, result, totals = rest[12:20], rest[20], rest[21], rest[22]
    send_sems, recv_sems, local_sems = rest[23:]
    place = Place(nz)
    net = Net(send_sems, recv_sems)
    t = place.t
    quarter = tokens.shape[1]
    layer = Layer(buffers, lengths[t])
    owns = (own_joint, w_inner, w_outer)
    g, r = [], []
    meter = Meter(layer.joint, layer.factor)
    cores = [Cores(net, place, layer.w, core_landing, k, meter) for k in (0, 1)]
    cores.append(Cores(net, place, layer.w, core_landing, 2, meter, layer.early))
    lanes = [[net.lane() for k in range(KINDS)] for _ in range(3)]
    doors = [net.door() for k in range(KINDS)]
    for (k, first, width, order_in, order_out), landing in zip(FLOWS, landings):
        cols = pl.ds(first, width)

        def region(spot, k=k, cols=cols):
            return layer.w.at[k, spot["y"], place.c, spot["z"], spot["x"], :, cols]

        g.append(Flow(net, place, order_in, owns[k].at[:, cols], region, lanes[0][k], lanes[1][k], doors[k]))
        sink = (core_landing.at[k], landing, result.at[k], cols, lanes[2][k], meter)
        r.append(Sink(net, place, order_out, *sink))
    one = net.lane()
    vecs = Flow(
        net, place, FLOWS[0][3], vec_in, lambda spot: v.at[spot["y"], place.c, spot["z"], spot["x"]],
        one, one, net.door(),
    )
    sums = Back(net, place, parts, back_landings, totals, meter)

    def of_kind(flows, k):
        return [flow for flow, row in zip(flows, FLOWS) if row[0] == k]

    def trips_of(flows):
        return [trip for flow in flows for trip in flow.trips]

    def cores_of(flows):
        return [trip for flow in flows for trip in flow.cores]

    def gathered(k):
        arrived(cores_of(of_kind(g, k)), meter.low_rows(2 * WIDTH))

    def passed_on(k):
        flows = of_kind(g, k)
        departed(trips_of(flows), meter.low_rows(2 * WIDTH - own_joint.shape[0]))
        departed(cores_of(flows), meter.low_rows(2 * WIDTH))

    def reduced(k):
        departed(trips_of(of_kind(r, k)), meter.low_rows(2 * WIDTH - own_joint.shape[0]))
        departed(cores[k].trips, meter.low_rows(2 * WIDTH))

    def vectors_in():
        arrived(vecs.cores, meter.tiles(4 * nz))

    def vectors_sent():
        departed(vecs.trips + vecs.cores, meter.tiles(8 * nz - 1))

    def quarter_of(ref, index):
        return ref.at[pl.ds(pl.multiple_of(index * quarter, quarter), quarter)]

    swap_lane = net.lane()

    def swap(source, target):
        door = net.door()
        return [net.plan(source(step), target, place.in_group(step), swap_lane, door) for step in (2, 1, 3)]

    def swapped(trips):
        arrived(trips, meter.low_rows(3 * quarter))

    token_in = swap(lambda step: tokens.at[(t + step) % 4], quarter_of(layer.rows, t))
    back_in = swap(lambda step: cotangent.at[(t + step) % 4], quarter_of(layer.back, t))
    out_out = swap(lambda step: quarter_of(layer.out, (t + step) % 4), outs.at[t])
    back_out = swap(lambda step: quarter_of(layer.back, (t + step) % 4), backs.at[t])

    def swaps_sent():
        departed(token_in + back_in + out_out + back_out, meter.low_rows(12 * quarter))

    pairs = [
        (tokens.at[t], quarter_of(layer.rows, t)),
        (cotangent.at[t], quarter_of(layer.back, t)),
        *[
            (own, layer.w.at[k, place.y, place.c, place.z, place.x])
            for k, own in enumerate(owns)
        ],
        (vec_in, v.at[place.y, place.c, place.z, place.x]),
        (quarter_of(layer.out, t), outs.at[t]),
        (quarter_of(layer.back, t), backs.at[t]),
        *[(result.at[k], result_out.at[k]) for k in range(KINDS)],
        (totals, totals_out),
        (w_query, raw_query),
        (w_key, raw_key),
        (w_value, raw_value),
        (w_output, raw_output),
        *zip(short_in, raw_short),
        (long_in, raw_long),
    ]
    local = [pltpu.make_async_copy(*pair, local_sems.at[i]) for i, pair in enumerate(pairs)]

    def pack_vectors():
        vec_in[...] = jnp.zeros((8, 128), F32)
        for i, ref in enumerate(raw_short):
            vec_in[i:i + 1, 0:SHORT] = ref[...].reshape(1, SHORT)
        vec_in[0:1, 32:128] = raw_long[...].reshape(1, LONG)

    def pack_own():
        own_joint[...] = pack_joint(raw_query[...], raw_key[...], raw_value[...], raw_output[...].T)

    def near(i):
        return (place.y + i) % 2 * 2 + (place.c + i // 2) % 2

    def order(i):
        return (1 - place.y + i // 2) % 2 * 2 + (1 - place.c + i) % 2

    start_all(local[12:])
    greet(place)
    wait_local(local[12:])
    pack_vectors()
    pack_own()
    vecs.first()
    g[1].first()
    g[0].first()
    g[2].first()
    g[1].piece(4)
    vecs.piece(2)
    g[1].piece(8)
    g[3].first()
    start_all(local[:6])
    wait_local(local[:6])
    start_all(token_in)
    g[5].first()
    g[4].first()
    g[0].piece(8)
    vecs.piece(1)
    g[1].piece(2)
    g[6].first()
    vecs.piece(3)
    vecs.piece(8)
    g[1].piece(1)
    g[3].piece(4)
    g[1].piece(3)
    g[5].piece(8)
    vecs.piece(11)
    vecs.piece(4)
    g[0].piece(4)
    g[4].piece(8)
    g[2].piece(4)
    g[1].piece(12)
    vecs.piece(12)
    g[2].piece(8)
    g[6].piece(2)
    vecs.piece(9)
    g[1].piece(11)
    vecs.piece(6)
    g[0].piece(1)
    g[0].piece(12)
    g[5].piece(4)
    g[0].piece(2)
    g[6].piece(1)
    vecs.piece(5)
    vecs.piece(7)
    g[5].piece(12)
    g[4].piece(4)
    g[3].piece(12)
    g[1].piece(9)
    vecs.piece(10)
    swapped(token_in)
    vecs.piece(14)
    g[2].piece(1)
    g[1].piece(5)
    g[1].piece(10)
    g[1].piece(7)
    g[0].piece(10)
    g[0].piece(9)
    vecs.piece(15)
    vecs.piece(13)
    vecs.to_core(0)
    g[0].piece(3)
    g[6].piece(3)
    g[6].to_core(0)
    g[4].piece(12)
    g[3].piece(8)
    g[2].piece(12)
    g[2].piece(2)
    g[1].piece(6)
    vecs.to_core(1)
    g[2].piece(5)
    vectors_in()
    layer.unpack(v)
    layer.start()
    layer.rows_turned[...] = layer.rows[...].T
    layer.clear_sums()
    g[2].piece(3)
    g[1].piece(15)
    g[1].piece(13)
    g[2].piece(6)
    g[0].piece(5)
    g[1].piece(14)
    g[1].to_core(1)
    g[0].piece(7)
    g[0].piece(6)
    g[2].piece(7)
    g[3].piece(1)
    g[2].piece(9)
    g[0].piece(11)
    g[2].to_core(0)
    g[0].piece(13)
    g[0].to_core(0)
    g[0].piece(15)
    g[2].piece(10)
    g[3].piece(3)
    g[0].piece(14)
    g[2].piece(11)
    g[2].piece(15)
    g[1].to_core(0)
    g[3].piece(2)
    g[5].piece(3)
    g[0].to_core(1)
    def project(i):
        layer.project(near(i))
        ticks(i, {
            1: [(g[2].piece, 14), (gathered, 0), (g[2].piece, 13), (g[5].piece, 1), (g[3].piece, 9)],
            2: [(g[3].piece, 5), (g[3].piece, 11)],
        })

    each(4, project)
    g[5].piece(2)
    g[3].piece(10)
    def attend(i):
        layer.attend(i)
        ticks(i, {
            0: [(g[3].piece, 7), (g[3].piece, 6), (g[3].to_core, 0), (g[5].piece, 7), (g[4].piece, 2)],
            1: [(g[4].piece, 1), (g[5].piece, 6), (g[2].to_core, 1), (g[5].piece, 5), (g[3].piece, 13), (g[6].piece, 6), (g[4].piece, 3), (g[5].to_core, 0), (g[5].piece, 9), (start_all, back_in)],
        })

    each(4, attend)
    g[6].piece(4)
    g[6].piece(10)
    g[5].piece(11)
    g[3].piece(15)
    g[4].piece(10)
    layer.norm_first()
    layer.first_turned[...] = layer.first_low[...].T
    g[6].piece(5)
    g[4].piece(6)
    g[3].piece(14)
    g[5].piece(13)
    g[4].piece(5)
    g[5].piece(10)
    g[3].to_core(1)
    def feed_inner(i):
        layer.feed_inner(near(i))
        ticks(i, {
            0: [(g[5].piece, 15), (g[5].piece, 14), (g[5].to_core, 1), (g[4].piece, 9)],
            1: [(g[4].piece, 7), (gathered, 1)],
            2: [(g[4].to_core, 0), (g[4].piece, 11), (g[6].piece, 7)],
        })

    each(4, feed_inner)
    g[6].piece(12)
    g[6].piece(13)
    g[6].to_core(1)
    g[6].piece(9)
    g[6].piece(15)
    g[6].to_core(3)
    g[4].piece(13)
    g[6].piece(14)
    g[6].piece(11)
    g[6].piece(8)
    g[6].to_core(2)
    g[4].piece(14)
    g[4].piece(15)
    g[4].to_core(1)
    def feed_outer(i):
        layer.feed_outer(near(i))
        ticks(i, {
            1: [(gathered, 2)],
        })

    each(4, feed_outer)
    swapped(back_in)
    layer.norm_second()
    start_all(out_out)
    local[6].start()
    layer.outer_early(order(0))
    passed_on(2)
    cores[2].to_core(0)
    def outer_back(i):
        layer.outer_back(order(i + 1))
        ticks(i, {
            0: [(cores[2].half, 0, 0), (r[6].start, 0, 0), (r[5].start, 0, 0), (r[4].start, 0, 0)],
            1: [(passed_on, 1), (cores[2].to_core, 1), (cores[2].half, 0, 1), (r[6].start, 0, 1), (r[5].start, 0, 1), (r[4].start, 0, 1)],
        })

    each(3, outer_back)
    cores[2].half(1, 0)
    r[6].start(1, 0)
    r[5].start(1, 0)
    r[4].start(1, 0)
    layer.outer_slope(order(0))
    def inner_back(i):
        layer.inner_back(order(i))
        ticks(i, {
            0: [(cores[1].to_core, 0), (cores[2].half, 1, 1), (r[6].start, 1, 1), (r[5].start, 1, 1), (r[4].start, 1, 1), (r[6].add, 2), (r[6].add, 0)],
            1: [(cores[1].half, 0, 0), (r[2].start, 0, 0), (r[3].start, 0, 0)],
            2: [(cores[1].to_core, 1), (r[6].add, 1), (r[5].add, 4), (cores[1].half, 0, 1), (r[2].start, 0, 1), (r[3].start, 0, 1), (r[2].add, 0), (r[5].add, 1), (r[6].add, 6), (r[5].add, 0)],
        })

    each(4, inner_back)
    r[6].add(3)
    r[5].add(5)
    r[5].add(3)
    vectors_sent()
    r[6].add(4)
    r[6].add(5)
    layer.second_sums()
    r[5].add(2)
    cores[1].half(1, 0)
    r[2].start(1, 0)
    r[3].start(1, 0)
    cores[1].half(1, 1)
    r[2].start(1, 1)
    r[3].start(1, 1)
    passed_on(0)
    layer.norm_first_back()
    r[2].add(1)
    r[5].add(7)
    r[5].add(8)
    r[4].add(0)
    r[5].add(9)
    def attend_back(i):
        layer.attend_back(order(i))
        ticks(i, {
            1: [(r[2].add, 7), (r[3].add, 4)],
            2: [(r[4].add, 1), (r[4].add, 2), (r[2].add, 3), (r[6].add, 8), (r[2].add, 6), (r[4].add, 4), (r[3].add, 2), (cores[0].half, 0, 1), (r[1].start, 0, 1), (r[0].start, 0, 1)],
            3: [(cores[0].to_core, 1), (r[3].add, 6), (r[3].add, 3), (r[3].add, 7), (r[3].add, 9), (r[1].add, 1), (r[5].add, 11), (r[0].add, 0)],
        })
        layer.joint_back(order(i))
        ticks(i, {
            0: [(r[2].add, 4), (r[3].add, 0), (r[3].add, 1), (cores[0].to_core, 0), (r[2].add, 5), (r[5].add, 6)],
            1: [(r[2].add, 2), (cores[0].half, 0, 0), (r[1].start, 0, 0), (r[0].start, 0, 0), (r[6].add, 7), (r[5].add, 10), (r[3].add, 5)],
            2: [(r[4].add, 3), (r[3].add, 8)],
        })

    each(4, attend_back)
    cores[0].half(1, 0)
    r[1].start(1, 0)
    r[0].start(1, 0)
    r[1].add(3)
    r[2].add(10)
    r[1].add(0)
    layer.pack(parts)
    r[2].add(9)
    r[1].add(2)
    r[6].add(9)
    r[0].add(1)
    r[2].add(8)
    sums.first()
    layer.finish()
    r[0].add(2)
    r[4].add(5)
    r[6].add(10)
    r[4].add(6)
    r[2].add(11)
    sums.core_done()
    start_all(back_out)
    local[7].start()
    r[5].add(12)
    local[10].start()
    r[0].add(3)
    cores[0].half(1, 1)
    r[1].start(1, 1)
    r[0].start(1, 1)
    reduced(2)
    r[3].add(10)
    r[3].add(11)
    r[1].add(4)
    r[1].add(8)
    r[2].add(12)
    r[1].add(5)
    r[1].add(9)
    r[3].add(12)
    local[9].start()
    reduced(1)
    r[0].add(4)
    r[0].add(8)
    r[0].add(5)
    r[0].add(9)
    r[1].add(6)
    r[1].add(10)
    r[1].add(7)
    r[1].add(11)
    sums.y_done()
    r[0].add(6)
    r[0].add(10)
    r[0].add(7)
    sums.x_done()
    r[0].add(11)
    r[1].add(12)
    r[0].add(12)
    sums.z_done()
    local[11].start()
    local[8].start()
    reduced(0)
    sums.sent()
    wait_local(local[6:12])
    swapped(out_out)
    swapped(back_out)
    swaps_sent()


ANY_SPEC = pl.BlockSpec(memory_space=pl.ANY)
LIMIT = 67043328


def whole_layer(tokens, *rest):
    nz = lax.axis_size(FSDP) // 2
    part = WIDTH // (2 * nz)
    seq = tokens.shape[1] * 4
    return pl.pallas_call(
        partial(layer_kernel, nz),
        out_shape=(
            jax.ShapeDtypeStruct((KINDS, part, WIDTH), F32),
            jax.ShapeDtypeStruct(tokens.shape, BF16),
            jax.ShapeDtypeStruct(tokens.shape, BF16),
            jax.ShapeDtypeStruct((8, 128), F32),
        ),
        in_specs=[ANY_SPEC, pl.BlockSpec(memory_space=pltpu.SMEM)] + [ANY_SPEC] * 16,
        out_specs=(ANY_SPEC,) * 4,
        scratch_shapes=buffer_shapes(nz, seq) + flow_shapes(nz) + [
            pltpu.VMEM((2, nz, 2, 8, 128), F32),
            pltpu.VMEM((nz, 2, 8, 128), F32),
            pltpu.VMEM((nz, 8, 128), F32),
            pltpu.VMEM((nz - 1, 8, 128), F32),
            pltpu.VMEM((2, 2, nz, 2, 8, 128), F32),
            pltpu.VMEM((2, 2, nz, 2, 8, 128), F32),
            pltpu.VMEM((8, 128), F32),
            *[pltpu.VMEM((part, WIDTH // 4), BF16)] * 3,
            pltpu.VMEM((WIDTH // 4, part), BF16),
            pltpu.VMEM((part, WIDTH), BF16),
            *[pltpu.VMEM((SHORT,), F32)] * 8,
            pltpu.VMEM((LONG,), F32),
            pltpu.VMEM((KINDS, part, WIDTH), F32),
            pltpu.VMEM((8, 128), F32),
            pltpu.SemaphoreType.DMA((SEND_COUNT,)),
            pltpu.SemaphoreType.DMA((DOOR_COUNT,)),
            pltpu.SemaphoreType.DMA((25,)),
        ],
        compiler_params=pltpu.CompilerParams(collective_id=0, has_side_effects=True, vmem_limit_bytes=LIMIT),
        name="whole_layer",
    )(tokens, *rest)


def finish_kernel(count, *refs):
    sums_in, outs_in, backs_in, totals_in = refs[:4]
    results, rest = refs[4:4 + count], refs[4 + count:]
    sums, outs, backs, totals, input_grad, g_query, g_key, g_value, g_output = rest[:9]
    vectors, (sems, sent) = rest[9:-2], rest[-2:]
    quarters = range(backs.shape[0])
    pairs = [(backs_in.at[i], backs.at[i]) for i in quarters] + [(sums_in.at[k], sums.at[k]) for k in range(KINDS)]
    pairs += [(totals_in, totals), (outs_in, outs)]
    reads = [pltpu.make_async_copy(*pair, sems.at[i]) for i, pair in enumerate(pairs)]
    start_all(reads)
    writes = []

    def write(source, target):
        writes.append(pltpu.make_async_copy(source, target, sent.at[len(writes)]))
        writes[-1].start()

    for i in quarters:
        reads[i].wait()
        input_grad[i] = backs[i].astype(F32)
        write(input_grad.at[i], results[1].at[i])
    joint_read, inner_read, outer_read, totals_read, outs_read = reads[len(quarters):]
    joint_read.wait()
    g_query[...], g_key[...], g_value[...], g_turned = unpack_joint(sums[0])
    g_output[...] = g_turned.T
    for ref, target in zip((g_query, g_key, g_value, g_output), results[2:6]):
        write(ref, target)
    inner_read.wait()
    write(sums.at[1], results[6])
    outer_read.wait()
    write(sums.at[2], results[7])
    totals_read.wait()
    short = [0, 1, 2, None, 3, 4, 5, 6, 7]
    for row, ref, target in zip(short, vectors, results[8:]):
        ref[...] = (totals[0:1, 32:128] if row is None else totals[row:row + 1, 0:SHORT]).reshape(ref.shape)
        write(ref, target)
    outs_read.wait()
    write(outs, results[0])
    wait_local(writes)


def finish_layer(sums, outs, backs, totals):
    part = sums.shape[1]
    share = WIDTH // 4
    shapes = [outs.shape, backs.shape] + [(part, share)] * 3 + [(share, part), (part, WIDTH), (part, WIDTH)]
    shapes += [(SHORT,)] * 3 + [(LONG,)] + [(SHORT,)] * 5
    given = (sums, outs, backs, totals)
    reads, writes = backs.shape[0] + KINDS + 2, backs.shape[0] + len(shapes) - 1
    return pl.pallas_call(
        partial(finish_kernel, len(shapes)),
        out_shape=[jax.ShapeDtypeStruct(shape, F32 if i else BF16) for i, shape in enumerate(shapes)],
        in_specs=[ANY_SPEC] * len(given),
        out_specs=[ANY_SPEC] * len(shapes),
        scratch_shapes=[pltpu.VMEM(ref.shape, ref.dtype) for ref in given]
        + [pltpu.VMEM(shape, F32) for shape in shapes[1:6] + shapes[8:]]
        + [pltpu.SemaphoreType.DMA((reads,)), pltpu.SemaphoreType.DMA((writes,))],
        compiler_params=pltpu.CompilerParams(vmem_limit_bytes=LIMIT),
        name="finish_layer",
    )(*given)


def pack_joint(q, k, v, o):
    return jnp.concatenate(
        [q[:, :128], k[:, :128], v[:, :128], v[:, 128:], q[:, 128:], o[:, :128], o[:, 128:], k[:, 128:]], axis=1
    )


def unpack_joint(joint):
    q = jnp.concatenate([joint[:, 0:128], joint[:, 448:512]], axis=1)
    k = jnp.concatenate([joint[:, 128:256], joint[:, 704:768]], axis=1)
    return q, k, joint[:, 256:448], joint[:, 512:704]


def local_fast(*given):
    given = given[:8] + (given[8].T,) + given[9:]
    results = finish_layer(*whole_layer(*given))
    return (*results[:7], results[7].T, *results[8:])


def solution(mesh):
    placed = (
        P(FSDP, TENSOR, None),
        P(FSDP),
        P(FSDP, TENSOR, None),
        P(FSDP, TENSOR),
        P(FSDP, TENSOR),
        P(FSDP, TENSOR),
        P(TENSOR, FSDP),
        P(FSDP, TENSOR),
        P(TENSOR, FSDP),
        P((FSDP, TENSOR)),
        P((FSDP, TENSOR)),
        P((FSDP, TENSOR)),
        P((FSDP, TENSOR)),
        P((FSDP, TENSOR)),
        P((FSDP, TENSOR)),
        P((FSDP, TENSOR)),
        P((FSDP, TENSOR)),
        P((FSDP, TENSOR)),
    )
    return jax.shard_map(
        local_fast if fits(mesh.shape) else local_generic,
        mesh=mesh,
        in_specs=placed,
        out_specs=(
            P(FSDP, TENSOR, None),
            P(FSDP, TENSOR, None),
            P(FSDP, TENSOR),
            P(FSDP, TENSOR),
            P(FSDP, TENSOR),
            P(TENSOR, FSDP),
            P(FSDP, TENSOR),
            P(TENSOR, FSDP),
            P((FSDP, TENSOR)),
            P((FSDP, TENSOR)),
            P((FSDP, TENSOR)),
            P((FSDP, TENSOR)),
            P((FSDP, TENSOR)),
            P((FSDP, TENSOR)),
            P((FSDP, TENSOR)),
            P((FSDP, TENSOR)),
            P((FSDP, TENSOR)),
        ),
        check_vma=False,
    )
```

```python
from functools import partial

import jax
import jax.numpy as jnp
from jax import lax
from jax.experimental import pallas as pl
from jax.experimental.pallas import tpu as pltpu
from jax.sharding import PartitionSpec as P

FSDP, TENSOR = "fsdp", "tensor"

HEAD = 64


epsilon = 1e-05
root_half = 0.7071067811865476
inverse_root_two_pi = 0.3989422804014327


def gelu_value(inner):
    return 0.5 * inner * (1.0 + jax.scipy.special.erf(inner * root_half))


def gelu_slope(inner):
    return 0.5 * (
        1.0 + jax.scipy.special.erf(inner * root_half)
    ) + inner * inverse_root_two_pi * jnp.exp(-0.5 * inner * inner)


def normalize(rows):
    mean = jnp.mean(rows, axis=1, keepdims=True)
    centered = rows - mean
    variance = jnp.mean(centered * centered, axis=1, keepdims=True)
    factor = lax.rsqrt(variance + epsilon)
    return (centered * factor, factor)


def normalize_back(grad_normed, normed, factor):
    return factor * (
        grad_normed
        - jnp.mean(grad_normed, axis=1, keepdims=True)
        - normed * jnp.mean(grad_normed * normed, axis=1, keepdims=True)
    )


def column_sum(rows):
    return jnp.sum(rows.astype(jnp.float32), axis=0)


def dot_rows(left, right):
    return lax.dot_general(
        left, right, (((0,), (0,)), ((), ())), preferred_element_type=jnp.float32
    )


def dot_back(left, right):
    return lax.dot_general(
        left, right, (((1,), (1,)), ((), ())), preferred_element_type=jnp.float32
    )


def place(values, offset, total_length):
    return lax.dynamic_update_slice(jnp.zeros((total_length,), jnp.float32), values, (offset,))


def block_scores(keys, key_valid, query_block):
    raw = jnp.einsum(
        "qhd,khd->hqk", query_block, keys, preferred_element_type=jnp.float32
    ) * HEAD ** (-0.5)
    return jnp.where(key_valid[None, None, :], raw, -1000000000.0)


def attend_forward(keys, values, key_valid, query_block):
    masked = block_scores(keys, key_valid, query_block)
    top = jnp.max(masked, axis=2, keepdims=True)
    expo = jnp.exp(masked - top)
    total = jnp.sum(expo, axis=2, keepdims=True)
    probs = (expo / total).astype(jnp.bfloat16)
    context = jnp.einsum("hqk,khd->qhd", probs, values, preferred_element_type=jnp.float32)
    return (context, top, total)


def attend_backward(keys, values, key_valid, carry, item):
    key_grad, value_grad = carry
    query_block, context_grad_block, top, total = item
    masked = block_scores(keys, key_valid, query_block)
    probs = jnp.exp(masked - top) / total
    probs_low = probs.astype(jnp.bfloat16)
    prob_grad = jnp.einsum(
        "qhd,khd->hqk", context_grad_block, values, preferred_element_type=jnp.float32
    )
    delta = jnp.sum(prob_grad * probs, axis=2, keepdims=True)
    score_grad = (probs * (prob_grad - delta)).astype(jnp.bfloat16)
    factor = HEAD ** (-0.5)
    query_grad = (
        jnp.einsum("hqk,khd->qhd", score_grad, keys, preferred_element_type=jnp.float32) * factor
    )
    key_grad = (
        key_grad
        + jnp.einsum("hqk,qhd->khd", score_grad, query_block, preferred_element_type=jnp.float32)
        * factor
    )
    value_grad = value_grad + jnp.einsum(
        "hqk,qhd->khd", probs_low, context_grad_block, preferred_element_type=jnp.float32
    )
    return ((key_grad, value_grad), query_grad)


def gather_weights(w_query, w_key, w_value, w_output, w_inner, w_outer):
    return (
        lax.all_gather(w_query, FSDP, axis=0, tiled=True),
        lax.all_gather(w_key, FSDP, axis=0, tiled=True),
        lax.all_gather(w_value, FSDP, axis=0, tiled=True),
        lax.all_gather(w_output, FSDP, axis=1, tiled=True),
        lax.all_gather(w_inner, FSDP, axis=0, tiled=True),
        lax.all_gather(w_outer, FSDP, axis=1, tiled=True),
    )


def split_joint(joint_sum, output_sum, inner_sum, outer_sum, head_width):
    return (
        joint_sum[:, :head_width],
        joint_sum[:, head_width : 2 * head_width],
        joint_sum[:, 2 * head_width :],
        output_sum,
        inner_sum,
        outer_sum,
    )


def add_tuples(left, right):
    return tuple((first_item + second_item for first_item, second_item in zip(left, right)))


def local_generic(
    tokens,
    lengths,
    cotangent,
    w_query,
    w_key,
    w_value,
    w_output,
    w_inner,
    w_outer,
    b_query,
    b_value,
    b_output,
    b_inner,
    b_outer,
    gain_first,
    shift_first,
    gain_second,
    shift_second,
):
    tensor_size = lax.axis_size(TENSOR)
    tensor_rank = lax.axis_index(TENSOR)
    micro_count = tokens.shape[0]
    part_rows = tokens.shape[1]
    width = tokens.shape[2]
    seq_rows = part_rows * tensor_size
    head_width = w_query.shape[1]
    inner_width = w_inner.shape[1]
    local_heads = head_width // HEAD
    block_rows = min(512, seq_rows)
    block_count = seq_rows // block_rows
    vector_full = (
        lax.all_gather(b_query, (FSDP, TENSOR), axis=0, tiled=True),
        lax.all_gather(b_value, (FSDP, TENSOR), axis=0, tiled=True),
        lax.all_gather(b_output, (FSDP, TENSOR), axis=0, tiled=True),
        lax.all_gather(b_inner, (FSDP, TENSOR), axis=0, tiled=True),
        lax.all_gather(b_outer, (FSDP, TENSOR), axis=0, tiled=True),
        lax.all_gather(gain_first, (FSDP, TENSOR), axis=0, tiled=True),
        lax.all_gather(shift_first, (FSDP, TENSOR), axis=0, tiled=True),
        lax.all_gather(gain_second, (FSDP, TENSOR), axis=0, tiled=True),
        lax.all_gather(shift_second, (FSDP, TENSOR), axis=0, tiled=True),
    )
    query_bias = lax.dynamic_slice_in_dim(vector_full[0], tensor_rank * head_width, head_width)
    value_bias = lax.dynamic_slice_in_dim(vector_full[1], tensor_rank * head_width, head_width)
    inner_bias = lax.dynamic_slice_in_dim(vector_full[3], tensor_rank * inner_width, inner_width)
    joint_bias = jnp.concatenate([query_bias, jnp.zeros((head_width,), jnp.float32), value_bias])
    grad_query_bias = jnp.zeros((head_width,), jnp.float32)
    grad_value_bias = jnp.zeros((head_width,), jnp.float32)
    grad_inner_bias = jnp.zeros((inner_width,), jnp.float32)
    grad_output_bias = jnp.zeros((width,), jnp.float32)
    grad_outer_bias = jnp.zeros((width,), jnp.float32)
    grad_gain_one = jnp.zeros((width,), jnp.float32)
    grad_shift_one = jnp.zeros((width,), jnp.float32)
    grad_gain_two = jnp.zeros((width,), jnp.float32)
    grad_shift_two = jnp.zeros((width,), jnp.float32)
    local_totals = None
    shard_totals = None
    outputs = []
    input_grads = []
    slot_index = jnp.arange(seq_rows, dtype=jnp.int32)
    part_index = tensor_rank * part_rows + jnp.arange(part_rows, dtype=jnp.int32)
    for micro_index in range(micro_count):
        forward_weights = gather_weights(w_query, w_key, w_value, w_output, w_inner, w_outer)
        joint_w = jnp.concatenate(
            [forward_weights[0], forward_weights[1], forward_weights[2]], axis=1
        )
        output_w = forward_weights[3]
        inner_w = forward_weights[4]
        outer_w = forward_weights[5]
        length = lengths[micro_index]
        key_valid = slot_index < length
        row_valid = (part_index < length).astype(jnp.float32)[:, None]
        own_rows = tokens[micro_index]
        whole = lax.all_gather(own_rows, TENSOR, axis=0, tiled=True)
        joint = (jnp.dot(whole, joint_w, preferred_element_type=jnp.float32) + joint_bias).astype(
            jnp.bfloat16
        )
        query = joint[:, :head_width].reshape(block_count, block_rows, local_heads, HEAD)
        keys = joint[:, head_width : 2 * head_width].reshape(seq_rows, local_heads, HEAD)
        values = joint[:, 2 * head_width :].reshape(seq_rows, local_heads, HEAD)
        context_blocks, tops, totals = lax.map(
            partial(attend_forward, keys, values, key_valid), query
        )
        context_low = context_blocks.reshape(seq_rows, head_width).astype(jnp.bfloat16)
        attended = (
            lax.psum_scatter(
                jnp.dot(context_low, output_w, preferred_element_type=jnp.float32).astype(
                    jnp.bfloat16
                ),
                TENSOR,
                scatter_dimension=0,
                tiled=True,
            ).astype(jnp.float32)
            + vector_full[2]
        )
        normed_first, factor_first = normalize(own_rows.astype(jnp.float32) + attended)
        first = normed_first * vector_full[5] + vector_full[6]
        first_whole = lax.all_gather(first.astype(jnp.bfloat16), TENSOR, axis=0, tiled=True)
        inner = jnp.dot(first_whole, inner_w, preferred_element_type=jnp.float32) + inner_bias
        active = gelu_value(inner).astype(jnp.bfloat16)
        mixed = (
            lax.psum_scatter(
                jnp.dot(active, outer_w, preferred_element_type=jnp.float32).astype(jnp.bfloat16),
                TENSOR,
                scatter_dimension=0,
                tiled=True,
            ).astype(jnp.float32)
            + vector_full[4]
        )
        normed_second, factor_second = normalize(first + mixed)
        outputs.append(
            ((normed_second * vector_full[7] + vector_full[8]) * row_valid).astype(jnp.bfloat16)
        )
        backward_weights = gather_weights(w_query, w_key, w_value, w_output, w_inner, w_outer)
        joint_w = jnp.concatenate(
            [backward_weights[0], backward_weights[1], backward_weights[2]], axis=1
        )
        output_w = backward_weights[3]
        inner_w = backward_weights[4]
        outer_w = backward_weights[5]
        out_grad = cotangent[micro_index].astype(jnp.float32) * row_valid
        grad_gain_two = grad_gain_two + column_sum(out_grad * normed_second)
        grad_shift_two = grad_shift_two + column_sum(out_grad)
        sum_grad = normalize_back(out_grad * vector_full[7], normed_second, factor_second)
        mixed_grad = sum_grad.astype(jnp.bfloat16)
        grad_outer_bias = grad_outer_bias + column_sum(mixed_grad)
        mixed_whole = lax.all_gather(mixed_grad, TENSOR, axis=0, tiled=True)
        outer_sum = dot_rows(active, mixed_whole)
        inner_grad = (dot_back(mixed_whole, outer_w) * gelu_slope(inner)).astype(jnp.bfloat16)
        grad_inner_bias = grad_inner_bias + column_sum(inner_grad)
        inner_sum = dot_rows(first_whole, inner_grad)
        first_grad = sum_grad + lax.psum_scatter(
            dot_back(inner_grad, inner_w).astype(jnp.bfloat16),
            TENSOR,
            scatter_dimension=0,
            tiled=True,
        ).astype(jnp.float32)
        grad_gain_one = grad_gain_one + column_sum(first_grad * normed_first)
        grad_shift_one = grad_shift_one + column_sum(first_grad)
        residual_grad = normalize_back(first_grad * vector_full[5], normed_first, factor_first)
        attended_grad = residual_grad.astype(jnp.bfloat16)
        grad_output_bias = grad_output_bias + column_sum(attended_grad)
        attended_whole = lax.all_gather(attended_grad, TENSOR, axis=0, tiled=True)
        output_sum = dot_rows(context_low, attended_whole)
        context_grad = (
            dot_back(attended_whole, output_w)
            .astype(jnp.bfloat16)
            .reshape(block_count, block_rows, local_heads, HEAD)
        )
        empty = jnp.zeros((seq_rows, local_heads, HEAD), jnp.float32)
        carried, query_grad = lax.scan(
            partial(attend_backward, keys, values, key_valid),
            (empty, empty),
            (query, context_grad, tops, totals),
        )
        joint_grad = jnp.concatenate(
            [
                query_grad.reshape(seq_rows, head_width),
                carried[0].reshape(seq_rows, head_width),
                carried[1].reshape(seq_rows, head_width),
            ],
            axis=1,
        ).astype(jnp.bfloat16)
        grad_query_bias = grad_query_bias + column_sum(joint_grad[:, :head_width])
        grad_value_bias = grad_value_bias + column_sum(joint_grad[:, 2 * head_width :])
        joint_sum = dot_rows(whole, joint_grad)
        input_grads.append(
            residual_grad
            + lax.psum_scatter(
                dot_back(joint_grad, joint_w).astype(jnp.bfloat16),
                TENSOR,
                scatter_dimension=0,
                tiled=True,
            ).astype(jnp.float32)
        )
        batch_sums = (joint_sum, output_sum, inner_sum, outer_sum)
        local_totals = batch_sums if local_totals is None else add_tuples(local_totals, batch_sums)
    pieces = split_joint(
        local_totals[0], local_totals[1], local_totals[2], local_totals[3], head_width
    )
    shard_totals = (
        lax.psum_scatter(pieces[0], FSDP, scatter_dimension=0, tiled=True),
        lax.psum_scatter(pieces[1], FSDP, scatter_dimension=0, tiled=True),
        lax.psum_scatter(pieces[2], FSDP, scatter_dimension=0, tiled=True),
        lax.psum_scatter(pieces[3], FSDP, scatter_dimension=1, tiled=True),
        lax.psum_scatter(pieces[4], FSDP, scatter_dimension=0, tiled=True),
        lax.psum_scatter(pieces[5], FSDP, scatter_dimension=1, tiled=True),
    )
    vector_grads = (
        lax.psum_scatter(
            place(grad_query_bias, tensor_rank * head_width, width),
            (FSDP, TENSOR),
            scatter_dimension=0,
            tiled=True,
        ),
        lax.psum_scatter(
            place(grad_value_bias, tensor_rank * head_width, width),
            (FSDP, TENSOR),
            scatter_dimension=0,
            tiled=True,
        ),
        lax.psum_scatter(grad_output_bias, (FSDP, TENSOR), scatter_dimension=0, tiled=True),
        lax.psum_scatter(
            place(grad_inner_bias, tensor_rank * inner_width, inner_width * tensor_size),
            (FSDP, TENSOR),
            scatter_dimension=0,
            tiled=True,
        ),
        lax.psum_scatter(grad_outer_bias, (FSDP, TENSOR), scatter_dimension=0, tiled=True),
        lax.psum_scatter(grad_gain_one, (FSDP, TENSOR), scatter_dimension=0, tiled=True),
        lax.psum_scatter(grad_shift_one, (FSDP, TENSOR), scatter_dimension=0, tiled=True),
        lax.psum_scatter(grad_gain_two, (FSDP, TENSOR), scatter_dimension=0, tiled=True),
        lax.psum_scatter(grad_shift_two, (FSDP, TENSOR), scatter_dimension=0, tiled=True),
    )
    return (
        jnp.stack(outputs),
        jnp.stack(input_grads),
        shard_totals[0],
        shard_totals[1],
        shard_totals[2],
        shard_totals[3],
        shard_totals[4],
        shard_totals[5],
        vector_grads[0],
        vector_grads[1],
        vector_grads[2],
        vector_grads[3],
        vector_grads[4],
        vector_grads[5],
        vector_grads[6],
        vector_grads[7],
        vector_grads[8],
    )


MESH = pl.DeviceIdType.MESH
WIDTH = 768
HIDDEN = 3072
HALF = WIDTH // 2
KINDS = 3
FLOWS = (
    (0, 0, 512, "zyx", "xyz"),
    (0, 512, 256, "zyx", "xyz"),
    (1, 0, 256, "zxy", "xyz"),
    (1, 256, 512, "zxy", "yxz"),
    (2, 0, 256, "zyx", "zxy"),
    (2, 256, 256, "zyx", "yxz"),
    (2, 512, 256, "yxz", "xzy"),
)
VECTOR_ROWS = 16
SHORT, LONG = 24, 96
ROW_OUTPUT, ROW_OUTER, ROW_GAIN1, ROW_SHIFT1, ROW_GAIN2, ROW_SHIFT2, ROW_INNER = 4, 5, 6, 7, 8, 9, 10
BF16 = jnp.bfloat16
F32 = jnp.float32


def fits(sizes):
    fsdp = sizes[FSDP]
    return sizes[TENSOR] == 4 and fsdp == WIDTH // LONG


class Place:
    def __init__(self, nz):
        self.f = lax.axis_index(FSDP)
        self.t = lax.axis_index(TENSOR)
        self.nz = nz
        self.z = self.f // 2
        self.x = self.f % 2
        self.y = self.t // 2
        self.c = self.t % 2
        self.core = (self.f, self.t + 1 - 2 * self.c)
        self.along_y = (self.f, self.t + 2 - 4 * self.y)
        self.along_x = (self.f + 1 - 2 * self.x, self.t)

    def z_at(self, step):
        return (self.z + step) % self.nz

    def z_back(self, step):
        return (self.z + self.nz - step) % self.nz

    def along_z(self, step):
        return (self.z_at(step) * 2 + self.x, self.t)

    def in_group(self, step):
        return (self.f, (self.t + step) % 4)


class Trip:
    def __init__(self, copy, send_sem, recv_sem):
        self.copy, self.send_sem, self.recv_sem = copy, send_sem, recv_sem

    def start(self):
        self.copy.start()

    def wait_recv(self):
        self.copy.wait_recv()


class Net:
    def __init__(self, send_sems, recv_sems):
        self.send_sems, self.recv_sems = send_sems, recv_sems
        self.sends = self.recvs = 0

    def lane(self):
        self.sends += 1
        return self.send_sems.at[self.sends - 1]

    def door(self):
        self.recvs += 1
        return self.recv_sems.at[self.recvs - 1]

    def plan(self, source, target, device, lane, door=None):
        door = self.door() if door is None else door
        copy = pltpu.make_async_remote_copy(
            src_ref=source, dst_ref=target, send_sem=lane, recv_sem=door, device_id=device, device_id_type=MESH
        )
        return Trip(copy, lane, door)

    def keep(self, ref, device, lane, door=None):
        return self.plan(ref, ref, device, lane, door)


class Meter:
    def __init__(self, low, wide):
        self.low, self.wide = low, wide

    def low_rows(self, rows):
        for count in (1, 2, 3, 4):
            if rows % (16 * count) == 0 and rows // count <= self.low.shape[1]:
                return self.low.at[0:count, 0:rows // count]
        raise ValueError(rows)

    def tiles(self, count):
        return self.wide.at[0:8 * count]


def arrived(trips, size):
    pltpu.make_async_copy(size, size, trips[0].recv_sem).wait()


def departed(trips, size):
    pltpu.make_async_copy(size, size, trips[0].send_sem).wait()


def start_all(copies):
    for copy in copies:
        copy.start()


def greet(place):
    barrier = pltpu.get_barrier_semaphore()
    peers = [place.in_group(1), place.in_group(2), place.in_group(3), place.along_x]
    peers += [place.along_z(step) for step in range(1, place.nz)]
    for peer in peers:
        pl.semaphore_signal(barrier, inc=1, device_id=peer, device_id_type=MESH)
    pl.semaphore_wait(barrier, len(peers))


def wait_local(copies):
    for copy in copies:
        copy.wait()


def dot(left, right):
    return lax.dot_general(left, right, (((1,), (0,)), ((), ())), preferred_element_type=F32)


def turn(value, shift):
    shift %= value.shape[1]
    return pltpu.roll(value, shift, 1) if shift else value


class Layer:
    def __init__(self, refs, length):
        (
            self.w, self.rows, self.back, self.rows_turned, self.joint, self.probs, self.context, self.acc,
            self.normed, self.factor, self.first_low, self.first_turned, self.active, self.slope, self.grad_low,
            self.grad_turned, self.out, self.vec, self.sums, self.early,
        ) = refs
        self.length = length
        self.seq = self.rows.shape[0]
        self.block = self.seq

    def weight(self, kind, t):
        return self.w[kind, t // 2, t % 2].reshape(WIDTH, WIDTH)

    def output_weight(self, t):
        return self.w[0, t // 2, t % 2, :, :, :, 512:768].reshape(WIDTH, 256)

    def store_grad(self, kind, t, value):
        nz = self.w.shape[3]
        self.w[kind, t // 2, t % 2] = value.astype(BF16).reshape(nz, 2, WIDTH // (2 * nz), WIDTH)

    def row(self, index):
        return self.vec[pl.ds(index, 1), :]

    def blocks(self, body):
        def step(i, carry):
            body(pl.ds(pl.multiple_of(i * self.block, self.block), self.block), i)
            return carry

        lax.fori_loop(0, self.seq // self.block, step, 0)

    def row_valid(self, i):
        index = lax.broadcasted_iota(jnp.int32, (self.block, 1), 0) + i * self.block
        return (index < self.length).astype(F32)

    def lanes(self, low, high, width):
        lane = lax.broadcasted_iota(jnp.int32, (1, width), 1)
        return (lane >= low) & (lane < high)

    def pick(self, value, low, high):
        return jnp.where(self.lanes(low, high, value.shape[1]), value, jnp.zeros_like(value))

    def head_query(self, t, h):
        return self.joint[t, :, 0:128] if h < 2 else self.joint[t, :, 384:512]

    def head_key(self, t, h):
        return self.joint[t, :, 128:256] if h < 2 else self.joint[t, :, 640:768]

    def head_side(self, value, h):
        return self.pick(value, 0, 64) if h == 0 else self.pick(value, 64, 128)

    def head_value(self, t, h):
        return self.pick(self.joint[t, :, 256:512], h * 64, h * 64 + 64)

    def unpack(self, v):
        nz = v.shape[2]
        short = jnp.zeros((8, WIDTH), F32)
        inner = [jnp.zeros((1, WIDTH), F32) for _ in range(4)]
        for f in range(2 * nz):
            for t in range(4):
                rank = f * 4 + t
                block = v[t // 2, t % 2, f // 2, f % 2]
                wide = jnp.concatenate([self.pick(block, 0, SHORT), jnp.zeros((8, WIDTH - 128), F32)], axis=1)
                short += turn(wide, rank * SHORT)
                wide = jnp.concatenate([self.pick(block[0:1], 32, 128), jnp.zeros((1, WIDTH - 128), F32)], axis=1)
                inner[rank * LONG // WIDTH] += turn(wide, rank * LONG % WIDTH - 32)
        for t in range(4):
            query = self.pick(turn(short[0:1], -192 * t), 0, 128) + self.pick(turn(short[0:1], 320 - 192 * t), 448, 512)
            self.vec[t:t + 1] = query + self.pick(turn(short[1:2], 256 - 192 * t), 256, 448)
            self.vec[ROW_INNER + t:ROW_INNER + t + 1] = inner[t]
        self.vec[ROW_OUTPUT:ROW_INNER] = short[2:8]

    def pack(self, parts):
        nz = parts.shape[2]
        query, value = jnp.zeros((1, WIDTH), F32), jnp.zeros((1, WIDTH), F32)
        for t in range(4):
            row = self.sums[t:t + 1]
            query += turn(self.pick(row, 0, 128), 192 * t) + turn(self.pick(row, 448, 512), 192 * t - 320)
            value += turn(self.pick(row, 256, 448), 192 * t - 256)
        short = jnp.concatenate([query, value, self.sums[ROW_OUTPUT:ROW_INNER]], axis=0)
        top = lax.broadcasted_iota(jnp.int32, (8, 1), 0) == 0
        for f in range(2 * nz):
            for t in range(4):
                rank = f * 4 + t
                block = self.pick(turn(short, -rank * SHORT)[:, 0:128], 0, SHORT)
                index = ROW_INNER + rank * LONG // WIDTH
                inner = turn(self.sums[index:index + 1], 32 - rank * LONG % WIDTH)[:, 0:128]
                inner = jnp.broadcast_to(self.pick(inner, 32, 128), (8, 128))
                parts[t // 2, t % 2, f // 2, f % 2] = block + jnp.where(top, inner, 0.0)

    def project(self, t):
        self.joint[t] = (dot(self.rows[...], self.weight(0, t)) + self.row(t)).astype(BF16)

    def attend(self, t):
        key_valid = lax.broadcasted_iota(jnp.int32, (1, self.seq), 1) < self.length
        context = None
        for h in range(3):
            raw = dot_back(self.head_query(t, h), self.head_side(self.head_key(t, h), h))
            masked = jnp.where(key_valid, raw * HEAD ** -0.5, -1e9)
            expo = jnp.exp(masked - jnp.max(masked, axis=1, keepdims=True))
            probs = (expo * (1.0 / jnp.sum(expo, axis=1, keepdims=True))).astype(BF16)
            self.probs[t * 3 + h] = probs
            part = dot(probs, self.head_value(t, h))
            context = part if context is None else context + part
        low = context.astype(BF16)
        self.context[t] = low
        self.acc[...] += dot_back(low, self.output_weight(t))

    def start(self):
        def body(rows, i):
            self.acc[rows] = self.rows[rows].astype(F32) + self.row(ROW_OUTPUT)

        self.blocks(body)

    def norm_first(self):
        def body(rows, i):
            normed, factor = normalize(self.acc[rows])
            self.normed[rows] = normed
            self.factor[rows] = jnp.broadcast_to(factor, (self.block, 128))
            first = normed * self.row(ROW_GAIN1) + self.row(ROW_SHIFT1)
            self.first_low[rows] = first.astype(BF16)
            self.acc[rows] = first + self.row(ROW_OUTER)

        self.blocks(body)

    def feed_inner(self, t):
        inner = dot(self.first_low[...], self.weight(1, t)) + self.row(ROW_INNER + t)
        gate = 1.0 + lax.erf(inner * root_half)
        self.active[t] = (0.5 * inner * gate).astype(BF16)
        self.slope[t] = (0.5 * gate + inner * inverse_root_two_pi * jnp.exp(-0.5 * inner * inner)).astype(BF16)

    def feed_outer(self, t):
        self.acc[...] += dot_back(self.active[t], self.weight(2, t))

    def clear_sums(self):
        self.sums[...] = jnp.zeros_like(self.sums)

    def add_sum(self, index, value):
        self.sums[pl.ds(index, 1), :] += jnp.sum(value, axis=0, keepdims=True)

    def norm_second(self):
        def body(rows, i):
            normed, factor = normalize(self.acc[rows])
            valid = self.row_valid(i)
            gain = self.row(ROW_GAIN2)
            self.first_low[rows] = normed.astype(BF16)
            self.out[rows] = ((normed * gain + self.row(ROW_SHIFT2)) * valid).astype(BF16)
            out_grad = self.back[rows].astype(F32) * valid
            sum_grad = normalize_back(out_grad * gain, normed, factor)
            self.acc[rows] = sum_grad
            self.grad_low[rows] = sum_grad.astype(BF16)

        self.blocks(body)

    def second_sums(self):
        def body(rows, i):
            out_grad = self.back[rows].astype(F32) * self.row_valid(i)
            self.add_sum(ROW_GAIN2, out_grad * self.first_low[rows].astype(F32))
            self.add_sum(ROW_SHIFT2, out_grad)
            self.add_sum(ROW_OUTER, self.grad_low[rows].astype(F32))

        self.blocks(body)

    def outer_slope(self, t):
        grad = (dot(self.grad_low[...], self.weight(2, t)) * self.slope[t].astype(F32)).astype(BF16)
        self.slope[t] = grad
        self.add_sum(ROW_INNER + t, grad.astype(F32))

    def outer_back(self, t):
        self.outer_slope(t)
        self.store_grad(2, t, dot_rows(self.grad_low[...], self.active[t]))

    def outer_early(self, t):
        value = dot_rows(self.grad_low[...], self.active[t])
        self.early[...] = value.astype(BF16).reshape(self.early.shape)

    def inner_back(self, t):
        grad = self.slope[t]
        self.acc[...] += dot_back(grad, self.weight(1, t))
        self.store_grad(1, t, dot(self.first_turned[...], grad))

    def norm_first_back(self):
        def body(rows, i):
            grad = self.acc[rows]
            normed = self.normed[rows]
            self.add_sum(ROW_GAIN1, grad * normed)
            self.add_sum(ROW_SHIFT1, grad)
            residual = normalize_back(grad * self.row(ROW_GAIN1), normed, self.factor[rows][:, 0:1])
            self.acc[rows] = residual
            low = residual.astype(BF16)
            self.grad_low[rows] = low
            self.add_sum(ROW_OUTPUT, low.astype(F32))

        self.blocks(body)
        self.grad_turned[...] = self.grad_low[...].T

    def attend_back(self, t):
        context_grad = self.pick(dot(self.grad_low[...], self.output_weight(t)), 0, 192).astype(BF16)
        query_grads, key_grads, value_grad = [], [], None
        for h in range(3):
            probs = self.probs[t * 3 + h]
            prob_grad = dot_back(context_grad, self.head_value(t, h))
            wide = probs.astype(F32)
            delta = jnp.sum(wide * prob_grad, axis=1, keepdims=True)
            score_grad = (wide * (prob_grad - delta)).astype(BF16)
            query_grads.append(dot(score_grad, self.head_side(self.head_key(t, h), h)) * HEAD ** -0.5)
            key_grads.append(dot_rows(score_grad, self.head_side(self.head_query(t, h), h)) * HEAD ** -0.5)
            part = dot_rows(probs, self.pick(context_grad, h * 64, h * 64 + 64))
            value_grad = part if value_grad is None else value_grad + part
        self.joint[t, :, 0:128] = (query_grads[0] + query_grads[1]).astype(BF16)
        self.joint[t, :, 128:256] = (key_grads[0] + key_grads[1]).astype(BF16)
        self.joint[t, :, 256:384] = value_grad[:, 0:128].astype(BF16)
        self.joint[t, :, 384:512] = (value_grad[:, 128:256] + query_grads[2]).astype(BF16)
        self.joint[t, :, 512:640] = jnp.zeros((self.seq, 128), BF16)
        self.joint[t, :, 640:768] = key_grads[2].astype(BF16)

    def joint_back(self, t):
        joint = self.joint[t]
        self.sums[pl.ds(t, 1), :] = jnp.sum(joint.astype(F32), axis=0, keepdims=True)
        self.acc[...] += dot_back(joint, self.weight(0, t))
        nz = self.w.shape[3]
        shape = (nz, 2, WIDTH // (2 * nz), -1)
        main = dot(self.rows_turned[...], joint[:, 0:512])
        side = dot(self.rows_turned[...], joint[:, 512:768]) + dot(self.grad_turned[...], self.context[t])
        self.w[0, t // 2, t % 2, :, :, :, 0:512] = main.astype(BF16).reshape(shape[:3] + (512,))
        self.w[0, t // 2, t % 2, :, :, :, 512:768] = side.astype(BF16).reshape(shape[:3] + (256,))

    def finish(self):
        def body(rows, i):
            self.back[rows] = self.acc[rows].astype(BF16)

        self.blocks(body)


def each(count, body):
    def step(i, carry):
        body(i)
        return carry

    lax.fori_loop(0, count, step, 0)


BUFFER_COUNT = 20


def buffer_shapes(nz, seq):
    part = WIDTH // (2 * nz)
    low, wide = (seq, WIDTH), (WIDTH, seq)
    shapes = [
        ((KINDS, 2, 2, nz, 2, part, WIDTH), BF16),
        (low, BF16),
        (low, BF16),
        (wide, BF16),
        ((4, seq, WIDTH), BF16),
        ((12, seq, seq), BF16),
        ((4, seq, 256), BF16),
        (low, F32),
        (low, F32),
        ((seq, 128), F32),
        (low, BF16),
        (wide, BF16),
        ((4, seq, WIDTH), BF16),
        ((4, seq, WIDTH), BF16),
        (low, BF16),
        (wide, BF16),
        (low, BF16),
        ((VECTOR_ROWS, WIDTH), F32),
        ((VECTOR_ROWS, WIDTH), F32),
        ((nz, 2, part, WIDTH), BF16),
    ]
    return [pltpu.VMEM(*shape) for shape in shapes]


BLOCKS = 15
SEND_COUNT = 15
DOOR_COUNT = 227


def flow_shapes(nz):
    part = WIDTH // (2 * nz)
    shapes = [pltpu.VMEM((KINDS, 2, nz, 2, part, WIDTH), BF16)]
    return shapes + [pltpu.VMEM((BLOCKS, part, flow[2]), BF16) for flow in FLOWS]


def axis_steps(place, axis):
    p = place
    if axis == "x":
        return [(1, 1 - p.x, p.along_x, 1 - p.x)]
    if axis == "y":
        return [(1, 1 - p.y, p.along_y, 1 - p.y)]
    return [(step, p.z_at(step), p.along_z(step), p.z_back(step)) for step in range(1, p.nz)]


class Flow:
    def __init__(self, net, place, order, own, region, lane, core_lane, core_door):
        p = place
        self.pieces = [(None, [])]
        spots = [({"x": p.x, "y": p.y, "z": p.z}, own)]
        for axis in order:
            for index, (spot, source) in enumerate(list(spots)):
                for _, _, device, behind in axis_steps(p, axis):
                    trip = net.plan(region(spot) if source is None else source, region(spot), device, lane)
                    self.pieces[index][1].append(trip)
                    self.pieces.append((trip, []))
                    spots.append(({**spot, axis: behind}, None))
        mine = {"x": p.x, "y": p.y, "z": p.z}[order[2]]
        sides = [mine] + [behind for _, _, _, behind in axis_steps(p, order[2])]
        every = slice(None)
        self.cores = [
            net.keep(region({"x": every, "y": every, "z": every, order[2]: side}), p.core, core_lane, core_door)
            for side in sides
        ]
        self.trips = [trip for _, onward in self.pieces for trip in onward]

    def first(self):
        start_all(self.pieces[0][1])

    def piece(self, index):
        trip, onward = self.pieces[index]
        trip.wait_recv()
        start_all(onward)

    def to_core(self, index):
        self.cores[index].start()


class Cores:
    def __init__(self, net, place, w, core, k, meter, early=None):
        self.place, self.meter = place, meter
        self.w, self.core = w.at[k], core.at[k]
        self.ys = (1 - place.y, place.y)
        steps = list(range(1, place.nz)) + [0]
        self.parts = steps[:place.nz // 2], steps[place.nz // 2:]
        self.c = []
        lane = net.lane()
        for y in self.ys:
            for part in self.parts:
                door = net.door()
                spots = [place.z_at(step) for step in part]
                source = self.w.at[y, 1 - place.c] if early is None or self.c[1:] else early
                self.c.append([net.plan(source.at[z], self.core.at[y, z], place.core, lane, door) for z in spots])
        self.trips = [trip for trips in self.c for trip in trips]

    def to_core(self, half):
        start_all(self.c[2 * half] + self.c[2 * half + 1])

    def half(self, half, part):
        y = self.ys[half]
        trips = self.c[2 * half + part]
        arrived(trips, self.meter.low_rows(2 * self.core.shape[-2] * len(trips)))
        for step in self.parts[part]:
            z = self.place.z_at(step)
            target, source = self.core.at[y, z], self.w.at[y, self.place.c, z]
            target[...] = (target[...].astype(F32) + source[...].astype(F32)).astype(BF16)


class Sink:
    def __init__(self, net, place, order, core, landing, result, cols, lane, meter):
        p = place
        self.meter = meter
        self.core, self.landing, self.result, self.cols = core, landing, result, cols
        here = {"x": p.x, "y": p.y, "z": p.z}
        ahead = {axis: {0: here[axis], **{step: spot for step, spot, _, _ in axis_steps(p, axis)}} for axis in here}
        sizes = {"x": 2, "y": 2, "z": p.nz}
        self.spot = lambda block: tuple(ahead[axis][block[axis]] for axis in ("y", "z", "x"))
        self.order = order
        self.tasks = []
        self.starts = [[], [], [], []]
        blocks = [{}]
        for axis in ("y", "z", "x"):
            steps = [i for i in range(1, sizes[axis])] + [0]
            blocks = [{**block, axis: step} for block in blocks for step in steps]
        slot = 0
        self.trips = []
        waits = {}
        for stage, axis in enumerate(order):
            later = order[stage + 1:]
            kept = [block for block in blocks if block[axis] == 0]
            kept.sort(key=lambda block: [block[other] == 0 for other in later])
            devices = {step: device for step, _, device, _ in axis_steps(p, axis)}
            for block in kept:
                arrivals = []
                door = net.door()
                for step in range(1, sizes[axis]):
                    away = {**block, axis: step}
                    copy = net.plan(self.part(away), landing.at[slot], devices[step], lane, door)
                    self.trips.append(copy)
                    if stage == 0:
                        soon = 0 < away["z"] <= p.nz // 2
                        self.starts[(0 if away["y"] else 2) + (0 if soon else 1)].append(copy)
                    else:
                        waits[tuple(sorted(away.items()))].append(copy)
                    arrivals.append((copy, slot))
                    slot += 1
                onward = []
                waits[tuple(sorted(block.items()))] = onward
                self.tasks.append((block, arrivals, onward))
            blocks = kept

    def part(self, block):
        return self.core.at[(*self.spot(block), slice(None), self.cols)]

    def start(self, half, part):
        start_all(self.starts[2 * half + part])

    def add(self, index):
        block, arrivals, onward = self.tasks[index]
        target = self.part(block)
        total = target[...].astype(F32)
        rows = self.landing.shape[1] * self.landing.shape[2] // WIDTH
        arrived([trip for trip, _ in arrivals], self.meter.low_rows(rows * len(arrivals)))
        for _, slot in arrivals:
            total += self.landing[slot].astype(F32)
        if index < len(self.tasks) - 1:
            target[...] = total.astype(BF16)
            start_all(onward)
        else:
            self.result[:, self.cols] = total


class Back:
    def __init__(self, net, place, parts, landings, result, meter):
        p = self.place = place
        self.parts, self.result, self.meter = parts, result, meter
        self.core, self.side, self.pair, self.line = landings
        lane = net.lane()
        self.c = net.plan(parts.at[:, 1 - p.c], self.core, p.core, lane)
        self.y = net.plan(self.core.at[1 - p.y], self.side, p.along_y, lane)
        self.x = net.plan(self.side.at[:, 1 - p.x], self.pair, p.along_x, lane)
        door = net.door()
        self.z = [
            net.plan(self.pair.at[p.z_at(step)], self.line.at[step - 1], p.along_z(step), lane, door)
            for step in range(1, p.nz)
        ]

    def first(self):
        self.c.start()

    def core_done(self):
        self.c.wait_recv()
        self.core[...] += self.parts[:, self.place.c]
        self.y.start()

    def y_done(self):
        self.y.wait_recv()
        self.side[...] += self.core[self.place.y]
        self.x.start()

    def x_done(self):
        self.x.wait_recv()
        self.pair[...] += self.side[:, self.place.x]
        start_all(self.z)

    def z_done(self):
        arrived(self.z, self.meter.tiles(len(self.z)))
        total = self.pair[self.place.z]
        for i in range(self.place.nz - 1):
            total += self.line[i]
        self.result[...] = total

    def sent(self):
        departed([self.c, self.y, self.x] + self.z, self.meter.tiles(8 * self.place.nz - 1))


def ticks(i, table):
    for when, actions in table.items():
        @pl.when(i == when)
        def _(actions=actions):
            for action, *given in actions:
                action(*given)


def layer_kernel(nz, *refs):
    tokens, lengths, cotangent, w_query, w_key, w_value, w_output, w_inner, w_outer = refs[:9]
    short_in, long_in = refs[9:12] + refs[13:18], refs[12]
    result_out, outs, backs, totals_out = refs[18:22]
    rest = list(refs[22:])
    buffers, rest = rest[:BUFFER_COUNT], rest[BUFFER_COUNT:]
    core_landing, landings, rest = rest[0], rest[1:1 + len(FLOWS)], rest[1 + len(FLOWS):]
    back_landings = rest[:4]
    v, parts, vec_in, raw_query, raw_key, raw_value, raw_output, own_joint = rest[4:12]
    raw_short, raw_long, result, totals = rest[12:20], rest[20], rest[21], rest[22]
    send_sems, recv_sems, local_sems = rest[23:]
    place = Place(nz)
    net = Net(send_sems, recv_sems)
    t = place.t
    quarter = tokens.shape[1]
    layer = Layer(buffers, lengths[t])
    owns = (own_joint, w_inner, w_outer)
    g, r = [], []
    meter = Meter(layer.joint, layer.factor)
    cores = [Cores(net, place, layer.w, core_landing, k, meter) for k in (0, 1)]
    cores.append(Cores(net, place, layer.w, core_landing, 2, meter, layer.early))
    lanes = [[net.lane() for k in range(KINDS)] for _ in range(3)]
    doors = [net.door() for k in range(KINDS)]
    for (k, first, width, order_in, order_out), landing in zip(FLOWS, landings):
        cols = pl.ds(first, width)

        def region(spot, k=k, cols=cols):
            return layer.w.at[k, spot["y"], place.c, spot["z"], spot["x"], :, cols]

        g.append(Flow(net, place, order_in, owns[k].at[:, cols], region, lanes[0][k], lanes[1][k], doors[k]))
        sink = (core_landing.at[k], landing, result.at[k], cols, lanes[2][k], meter)
        r.append(Sink(net, place, order_out, *sink))
    one = net.lane()
    vecs = Flow(
        net, place, FLOWS[0][3], vec_in, lambda spot: v.at[spot["y"], place.c, spot["z"], spot["x"]],
        one, one, net.door(),
    )
    sums = Back(net, place, parts, back_landings, totals, meter)

    def of_kind(flows, k):
        return [flow for flow, row in zip(flows, FLOWS) if row[0] == k]

    def trips_of(flows):
        return [trip for flow in flows for trip in flow.trips]

    def cores_of(flows):
        return [trip for flow in flows for trip in flow.cores]

    def gathered(k):
        arrived(cores_of(of_kind(g, k)), meter.low_rows(2 * WIDTH))

    def passed_on(k):
        flows = of_kind(g, k)
        departed(trips_of(flows), meter.low_rows(2 * WIDTH - own_joint.shape[0]))
        departed(cores_of(flows), meter.low_rows(2 * WIDTH))

    def reduced(k):
        departed(trips_of(of_kind(r, k)), meter.low_rows(2 * WIDTH - own_joint.shape[0]))
        departed(cores[k].trips, meter.low_rows(2 * WIDTH))

    def vectors_in():
        arrived(vecs.cores, meter.tiles(4 * nz))

    def vectors_sent():
        departed(vecs.trips + vecs.cores, meter.tiles(8 * nz - 1))

    def quarter_of(ref, index):
        return ref.at[pl.ds(pl.multiple_of(index * quarter, quarter), quarter)]

    swap_lane = net.lane()

    def swap(source, target):
        door = net.door()
        return [net.plan(source(step), target, place.in_group(step), swap_lane, door) for step in (2, 1, 3)]

    def swapped(trips):
        arrived(trips, meter.low_rows(3 * quarter))

    token_in = swap(lambda step: tokens.at[(t + step) % 4], quarter_of(layer.rows, t))
    back_in = swap(lambda step: cotangent.at[(t + step) % 4], quarter_of(layer.back, t))
    out_out = swap(lambda step: quarter_of(layer.out, (t + step) % 4), outs.at[t])
    back_out = swap(lambda step: quarter_of(layer.back, (t + step) % 4), backs.at[t])

    def swaps_sent():
        departed(token_in + back_in + out_out + back_out, meter.low_rows(12 * quarter))

    pairs = [
        (tokens.at[t], quarter_of(layer.rows, t)),
        (cotangent.at[t], quarter_of(layer.back, t)),
        *[
            (own, layer.w.at[k, place.y, place.c, place.z, place.x])
            for k, own in enumerate(owns)
        ],
        (vec_in, v.at[place.y, place.c, place.z, place.x]),
        (quarter_of(layer.out, t), outs.at[t]),
        (quarter_of(layer.back, t), backs.at[t]),
        *[(result.at[k], result_out.at[k]) for k in range(KINDS)],
        (totals, totals_out),
        (w_query, raw_query),
        (w_key, raw_key),
        (w_value, raw_value),
        (w_output, raw_output),
        *zip(short_in, raw_short),
        (long_in, raw_long),
    ]
    local = [pltpu.make_async_copy(*pair, local_sems.at[i]) for i, pair in enumerate(pairs)]

    def pack_vectors():
        vec_in[...] = jnp.zeros((8, 128), F32)
        for i, ref in enumerate(raw_short):
            vec_in[i:i + 1, 0:SHORT] = ref[...].reshape(1, SHORT)
        vec_in[0:1, 32:128] = raw_long[...].reshape(1, LONG)

    def pack_own():
        own_joint[...] = pack_joint(raw_query[...], raw_key[...], raw_value[...], raw_output[...].T)

    def near(i):
        return (place.y + i) % 2 * 2 + (place.c + i // 2) % 2

    def order(i):
        return (1 - place.y + i // 2) % 2 * 2 + (1 - place.c + i) % 2

    start_all(local[12:])
    greet(place)
    wait_local(local[12:])
    pack_vectors()
    pack_own()
    vecs.first()
    g[1].first()
    g[0].first()
    start_all(token_in)
    g[1].piece(4)
    vecs.piece(2)
    g[2].first()
    g[1].piece(8)
    g[0].piece(8)
    start_all(local[:6])
    wait_local(local[:6])
    g[3].first()
    g[5].first()
    vecs.piece(1)
    g[4].first()
    vecs.piece(3)
    g[1].piece(2)
    g[6].first()
    g[3].piece(4)
    g[1].piece(1)
    g[1].piece(3)
    g[5].piece(8)
    vecs.piece(11)
    vecs.piece(4)
    g[0].piece(4)
    g[4].piece(8)
    g[1].piece(12)
    vecs.piece(12)
    vecs.piece(8)
    g[6].piece(2)
    vecs.piece(6)
    g[2].piece(8)
    g[2].piece(4)
    g[1].piece(11)
    vecs.piece(9)
    g[0].piece(1)
    g[5].piece(4)
    g[0].piece(2)
    g[6].piece(1)
    vecs.piece(5)
    g[0].piece(12)
    vecs.piece(7)
    g[5].piece(12)
    g[4].piece(4)
    g[6].piece(3)
    g[1].piece(9)
    swapped(token_in)
    g[0].piece(10)
    g[3].piece(12)
    vecs.piece(10)
    vecs.piece(14)
    g[0].piece(9)
    g[1].piece(5)
    g[2].piece(1)
    g[1].piece(7)
    g[1].piece(10)
    vecs.piece(13)
    vecs.piece(15)
    vecs.to_core(0)
    g[0].piece(3)
    g[3].piece(8)
    g[6].to_core(0)
    g[2].piece(12)
    vecs.to_core(1)
    g[2].piece(2)
    g[4].piece(12)
    g[2].piece(5)
    g[1].piece(6)
    vectors_in()
    layer.unpack(v)
    layer.start()
    layer.rows_turned[...] = layer.rows[...].T
    layer.clear_sums()
    g[1].piece(13)
    g[2].piece(3)
    g[2].piece(6)
    g[1].piece(15)
    g[0].piece(5)
    g[0].piece(7)
    g[2].piece(10)
    g[1].piece(14)
    g[1].to_core(1)
    g[0].piece(6)
    g[3].piece(1)
    g[2].piece(9)
    g[0].piece(11)
    g[2].piece(7)
    g[2].to_core(0)
    g[1].to_core(0)
    g[0].to_core(0)
    g[3].piece(3)
    g[2].piece(11)
    g[0].piece(14)
    g[0].piece(15)
    g[3].piece(2)
    g[2].piece(15)
    g[0].piece(13)
    g[5].piece(3)
    g[0].to_core(1)
    def project(i):
        layer.project(near(i))
        ticks(i, {
            1: [(g[2].piece, 13), (g[2].piece, 14), (gathered, 0), (g[3].piece, 9), (g[5].piece, 1)],
            2: [(g[3].piece, 5)],
        })

    each(4, project)
    g[3].piece(11)
    g[3].piece(10)
    g[5].piece(2)
    g[3].piece(7)
    def attend(i):
        layer.attend(i)
        ticks(i, {
            0: [(g[3].piece, 13), (g[4].piece, 1), (g[3].piece, 6), (g[5].piece, 7), (g[3].to_core, 0), (g[4].piece, 2)],
            1: [(g[5].piece, 5), (g[2].to_core, 1), (g[6].piece, 6), (g[6].piece, 4), (g[4].piece, 3), (g[5].piece, 9), (g[5].piece, 6), (g[5].to_core, 0)],
            2: [(g[5].piece, 11)],
        })

    each(4, attend)
    g[6].piece(10)
    g[3].piece(15)
    start_all(back_in)
    g[4].piece(10)
    layer.norm_first()
    layer.first_turned[...] = layer.first_low[...].T
    g[6].piece(5)
    g[4].piece(5)
    g[4].piece(6)
    g[3].piece(14)
    g[5].piece(13)
    g[5].piece(10)
    g[3].to_core(1)
    def feed_inner(i):
        layer.feed_inner(near(i))
        ticks(i, {
            0: [(g[5].piece, 14), (g[5].piece, 15), (g[5].to_core, 1), (g[4].piece, 9)],
            1: [(g[4].piece, 7), (gathered, 1)],
            2: [(g[4].to_core, 0), (g[4].piece, 11), (g[6].piece, 7)],
        })

    each(4, feed_inner)
    g[6].piece(9)
    g[6].piece(13)
    g[6].piece(12)
    g[6].to_core(1)
    g[6].piece(15)
    g[6].to_core(3)
    g[4].piece(15)
    g[6].piece(11)
    g[6].piece(8)
    g[6].piece(14)
    g[6].to_core(2)
    g[4].piece(13)
    g[4].piece(14)
    g[4].to_core(1)
    def feed_outer(i):
        layer.feed_outer(near(i))
        ticks(i, {
            1: [(gathered, 2), (passed_on, 2)],
        })

    each(4, feed_outer)
    swapped(back_in)
    layer.norm_second()
    start_all(out_out)
    local[6].start()
    layer.outer_early(order(0))
    cores[2].to_core(0)
    def outer_back(i):
        layer.outer_back(order(i + 1))
        ticks(i, {
            0: [(cores[2].half, 0, 0), (r[6].start, 0, 0), (r[5].start, 0, 0), (r[4].start, 0, 0)],
            1: [(cores[2].to_core, 1), (passed_on, 1), (cores[2].half, 0, 1), (r[6].start, 0, 1), (r[5].start, 0, 1), (r[4].start, 0, 1)],
        })

    each(3, outer_back)
    cores[2].half(1, 0)
    r[6].start(1, 0)
    r[5].start(1, 0)
    r[4].start(1, 0)
    layer.outer_slope(order(0))
    def inner_back(i):
        layer.inner_back(order(i))
        ticks(i, {
            0: [(cores[1].to_core, 0), (cores[2].half, 1, 1), (r[6].start, 1, 1), (r[5].start, 1, 1), (r[4].start, 1, 1), (r[6].add, 2), (r[6].add, 0)],
            1: [(cores[1].half, 0, 0), (r[2].start, 0, 0), (r[3].start, 0, 0)],
            2: [(cores[1].to_core, 1), (r[5].add, 4), (r[6].add, 1), (cores[1].half, 0, 1), (r[2].start, 0, 1), (r[3].start, 0, 1), (r[2].add, 0), (r[5].add, 1), (r[6].add, 6), (r[5].add, 0)],
        })

    each(4, inner_back)
    r[6].add(3)
    r[5].add(5)
    r[5].add(3)
    r[6].add(4)
    r[6].add(5)
    layer.second_sums()
    r[5].add(2)
    cores[1].half(1, 0)
    r[2].start(1, 0)
    r[3].start(1, 0)
    layer.norm_first_back()
    cores[1].half(1, 1)
    r[2].start(1, 1)
    r[3].start(1, 1)
    r[2].add(1)
    r[5].add(7)
    passed_on(0)
    r[5].add(8)
    r[4].add(0)
    r[5].add(9)
    vectors_sent()
    def attend_back(i):
        layer.attend_back(order(i))
        ticks(i, {
            0: [(r[3].add, 0)],
            1: [(r[5].add, 10)],
            2: [(r[2].add, 7), (r[4].add, 2), (r[2].add, 3), (r[4].add, 1), (r[4].add, 3), (r[2].add, 6), (r[6].add, 8), (r[3].add, 2), (cores[0].half, 0, 1), (r[1].start, 0, 1), (r[0].start, 0, 1), (r[4].add, 4)],
            3: [(cores[0].to_core, 1), (r[3].add, 3), (r[3].add, 7), (r[3].add, 9), (r[1].add, 1), (r[5].add, 11), (r[1].add, 0), (r[0].add, 0)],
        })
        layer.joint_back(order(i))
        ticks(i, {
            0: [(cores[0].to_core, 0), (r[2].add, 4), (r[3].add, 1), (r[2].add, 5), (r[6].add, 7), (r[5].add, 6), (r[2].add, 2)],
            1: [(cores[0].half, 0, 0), (r[1].start, 0, 0), (r[0].start, 0, 0), (r[3].add, 4), (r[3].add, 5)],
            2: [(r[3].add, 8), (r[3].add, 6)],
        })

    each(4, attend_back)
    cores[0].half(1, 0)
    r[1].start(1, 0)
    r[0].start(1, 0)
    r[2].add(10)
    r[1].add(3)
    layer.pack(parts)
    sums.first()
    r[2].add(9)
    r[6].add(9)
    r[1].add(2)
    r[0].add(1)
    r[2].add(8)
    layer.finish()
    r[0].add(2)
    r[4].add(5)
    r[4].add(6)
    r[2].add(11)
    sums.core_done()
    start_all(back_out)
    local[7].start()
    r[5].add(12)
    r[6].add(10)
    cores[0].half(1, 1)
    r[1].start(1, 1)
    r[0].start(1, 1)
    r[0].add(3)
    local[10].start()
    reduced(2)
    r[3].add(10)
    r[3].add(11)
    r[1].add(4)
    r[1].add(8)
    r[2].add(12)
    r[1].add(5)
    r[1].add(9)
    r[3].add(12)
    local[9].start()
    reduced(1)
    r[0].add(4)
    r[0].add(8)
    r[0].add(5)
    r[0].add(9)
    r[1].add(6)
    r[1].add(10)
    r[1].add(7)
    r[1].add(11)
    sums.y_done()
    r[0].add(6)
    r[0].add(10)
    r[0].add(7)
    sums.x_done()
    r[0].add(11)
    r[1].add(12)
    r[0].add(12)
    sums.z_done()
    local[11].start()
    local[8].start()
    reduced(0)
    sums.sent()
    wait_local(local[6:12])
    swapped(out_out)
    swapped(back_out)
    swaps_sent()


ANY_SPEC = pl.BlockSpec(memory_space=pl.ANY)
LIMIT = 67043328


def whole_layer(tokens, *rest):
    nz = lax.axis_size(FSDP) // 2
    part = WIDTH // (2 * nz)
    seq = tokens.shape[1] * 4
    return pl.pallas_call(
        partial(layer_kernel, nz),
        out_shape=(
            jax.ShapeDtypeStruct((KINDS, part, WIDTH), F32),
            jax.ShapeDtypeStruct(tokens.shape, BF16),
            jax.ShapeDtypeStruct(tokens.shape, BF16),
            jax.ShapeDtypeStruct((8, 128), F32),
        ),
        in_specs=[ANY_SPEC, pl.BlockSpec(memory_space=pltpu.SMEM)] + [ANY_SPEC] * 16,
        out_specs=(ANY_SPEC,) * 4,
        scratch_shapes=buffer_shapes(nz, seq) + flow_shapes(nz) + [
            pltpu.VMEM((2, nz, 2, 8, 128), F32),
            pltpu.VMEM((nz, 2, 8, 128), F32),
            pltpu.VMEM((nz, 8, 128), F32),
            pltpu.VMEM((nz - 1, 8, 128), F32),
            pltpu.VMEM((2, 2, nz, 2, 8, 128), F32),
            pltpu.VMEM((2, 2, nz, 2, 8, 128), F32),
            pltpu.VMEM((8, 128), F32),
            *[pltpu.VMEM((part, WIDTH // 4), BF16)] * 3,
            pltpu.VMEM((WIDTH // 4, part), BF16),
            pltpu.VMEM((part, WIDTH), BF16),
            *[pltpu.VMEM((SHORT,), F32)] * 8,
            pltpu.VMEM((LONG,), F32),
            pltpu.VMEM((KINDS, part, WIDTH), F32),
            pltpu.VMEM((8, 128), F32),
            pltpu.SemaphoreType.DMA((SEND_COUNT,)),
            pltpu.SemaphoreType.DMA((DOOR_COUNT,)),
            pltpu.SemaphoreType.DMA((25,)),
        ],
        compiler_params=pltpu.CompilerParams(collective_id=0, has_side_effects=True, vmem_limit_bytes=LIMIT),
        name="whole_layer",
    )(tokens, *rest)


def finish_kernel(count, *refs):
    sums_in, outs_in, backs_in, totals_in = refs[:4]
    results, rest = refs[4:4 + count], refs[4 + count:]
    sums, outs, backs, totals, input_grad, g_query, g_key, g_value, g_output = rest[:9]
    vectors, (sems, sent) = rest[9:-2], rest[-2:]
    quarters = range(backs.shape[0])
    pairs = [(backs_in.at[i], backs.at[i]) for i in quarters] + [(sums_in.at[k], sums.at[k]) for k in range(KINDS)]
    pairs += [(totals_in, totals), (outs_in, outs)]
    reads = [pltpu.make_async_copy(*pair, sems.at[i]) for i, pair in enumerate(pairs)]
    start_all(reads)
    writes = []

    def write(source, target):
        writes.append(pltpu.make_async_copy(source, target, sent.at[len(writes)]))
        writes[-1].start()

    for i in quarters:
        reads[i].wait()
        input_grad[i] = backs[i].astype(F32)
        write(input_grad.at[i], results[1].at[i])
    joint_read, inner_read, outer_read, totals_read, outs_read = reads[len(quarters):]
    joint_read.wait()
    g_query[...], g_key[...], g_value[...], g_turned = unpack_joint(sums[0])
    g_output[...] = g_turned.T
    for ref, target in zip((g_query, g_key, g_value, g_output), results[2:6]):
        write(ref, target)
    inner_read.wait()
    write(sums.at[1], results[6])
    outer_read.wait()
    write(sums.at[2], results[7])
    totals_read.wait()
    short = [0, 1, 2, None, 3, 4, 5, 6, 7]
    for row, ref, target in zip(short, vectors, results[8:]):
        ref[...] = (totals[0:1, 32:128] if row is None else totals[row:row + 1, 0:SHORT]).reshape(ref.shape)
        write(ref, target)
    outs_read.wait()
    write(outs, results[0])
    wait_local(writes)


def finish_layer(sums, outs, backs, totals):
    part = sums.shape[1]
    share = WIDTH // 4
    shapes = [outs.shape, backs.shape] + [(part, share)] * 3 + [(share, part), (part, WIDTH), (part, WIDTH)]
    shapes += [(SHORT,)] * 3 + [(LONG,)] + [(SHORT,)] * 5
    given = (sums, outs, backs, totals)
    reads, writes = backs.shape[0] + KINDS + 2, backs.shape[0] + len(shapes) - 1
    return pl.pallas_call(
        partial(finish_kernel, len(shapes)),
        out_shape=[jax.ShapeDtypeStruct(shape, F32 if i else BF16) for i, shape in enumerate(shapes)],
        in_specs=[ANY_SPEC] * len(given),
        out_specs=[ANY_SPEC] * len(shapes),
        scratch_shapes=[pltpu.VMEM(ref.shape, ref.dtype) for ref in given]
        + [pltpu.VMEM(shape, F32) for shape in shapes[1:6] + shapes[8:]]
        + [pltpu.SemaphoreType.DMA((reads,)), pltpu.SemaphoreType.DMA((writes,))],
        compiler_params=pltpu.CompilerParams(vmem_limit_bytes=LIMIT),
        name="finish_layer",
    )(*given)


def pack_joint(q, k, v, o):
    return jnp.concatenate(
        [q[:, :128], k[:, :128], v[:, :128], v[:, 128:], q[:, 128:], o[:, :128], o[:, 128:], k[:, 128:]], axis=1
    )


def unpack_joint(joint):
    q = jnp.concatenate([joint[:, 0:128], joint[:, 448:512]], axis=1)
    k = jnp.concatenate([joint[:, 128:256], joint[:, 704:768]], axis=1)
    return q, k, joint[:, 256:448], joint[:, 512:704]


def local_fast(*given):
    given = given[:8] + (given[8].T,) + given[9:]
    results = finish_layer(*whole_layer(*given))
    return (*results[:7], results[7].T, *results[8:])


def solution(mesh):
    placed = (
        P(FSDP, TENSOR, None),
        P(FSDP),
        P(FSDP, TENSOR, None),
        P(FSDP, TENSOR),
        P(FSDP, TENSOR),
        P(FSDP, TENSOR),
        P(TENSOR, FSDP),
        P(FSDP, TENSOR),
        P(TENSOR, FSDP),
        P((FSDP, TENSOR)),
        P((FSDP, TENSOR)),
        P((FSDP, TENSOR)),
        P((FSDP, TENSOR)),
        P((FSDP, TENSOR)),
        P((FSDP, TENSOR)),
        P((FSDP, TENSOR)),
        P((FSDP, TENSOR)),
        P((FSDP, TENSOR)),
    )
    return jax.shard_map(
        local_fast if fits(mesh.shape) else local_generic,
        mesh=mesh,
        in_specs=placed,
        out_specs=(
            P(FSDP, TENSOR, None),
            P(FSDP, TENSOR, None),
            P(FSDP, TENSOR),
            P(FSDP, TENSOR),
            P(FSDP, TENSOR),
            P(TENSOR, FSDP),
            P(FSDP, TENSOR),
            P(TENSOR, FSDP),
            P((FSDP, TENSOR)),
            P((FSDP, TENSOR)),
            P((FSDP, TENSOR)),
            P((FSDP, TENSOR)),
            P((FSDP, TENSOR)),
            P((FSDP, TENSOR)),
            P((FSDP, TENSOR)),
            P((FSDP, TENSOR)),
            P((FSDP, TENSOR)),
        ),
        check_vma=False,
    )
```
